32 devices in a mesh: replica: 8 (over z, core), shard: 4 (over y, x).
Axes of the slice: x: 2, y: 2, z: 4, core: 2. Of those that a mesh axis runs over, the one named last changes fastest.
Arguments:
- block_input: bfloat16 [4096, 1536], P(('replica', 'shard')), may hold values from -6 to 6
- attn_gain: bfloat16 [1536], P('shard'), may hold values from 0.099609375 to 1.8984375
- qkv_weight: bfloat16 [1536, 2048], P('shard'), may hold values from -0.15625 to 0.15625
- qkv_bias: bfloat16 [2048], P('shard'), may hold values from -3 to 3
- out_weight: bfloat16 [1536, 1536], P('shard'), may hold values from -0.875 to 0.875
- mlp_gain: bfloat16 [1536], P('shard'), may hold values from 0.099609375 to 1.8984375
- gate_weight: bfloat16 [1536, 8960], P('shard'), may hold values from -0.15625 to 0.15625
- up_weight: bfloat16 [1536, 8960], P('shard'), may hold values from -0.15625 to 0.15625
- down_weight: bfloat16 [8960, 1536], P('shard'), may hold values from -0.09375 to 0.09375
- cotangent: bfloat16 [4096, 1536], P(('replica', 'shard')), may hold values from -6 to 6
Outputs:
- block_output: bfloat16 [4096, 1536], P(('replica', 'shard'))
- input_grad: float32 [4096, 1536], P(('replica', 'shard'))
- attn_gain_grad: float32 [1536], P('shard')
- qkv_weight_grad: float32 [1536, 2048], P('shard')
- qkv_bias_grad: float32 [2048], P('shard')
- out_weight_grad: float32 [1536, 1536], P('shard')
- mlp_gain_grad: float32 [1536], P('shard')
- gate_weight_grad: float32 [1536, 8960], P('shard')
- up_weight_grad: float32 [1536, 8960], P('shard')
- down_weight_grad: float32 [8960, 1536], P('shard')
The draws below stay inside these ranges and needn't reach their ends.
All inputs are finite; a program needn't handle non-finite values.
Results may differ from the reference program's by a relative error of at most 0.013.
Values may be sent and summed in bfloat16 or wider, within the bound.
A program may use at most 320 MiB of HBM per device.

```python
import math
import jax
import jax.numpy as jnp
from jax import lax

D = 1536
HEADS = 12
KV = 2
HD = 128
FF = 8960
SEQ = 128
QKV = 2048
TOKENS = 4096


def block_scale(key, dims, pieces, low, largest):
    def one(axis_at, blocks):
        steps = jax.random.uniform(jax.random.fold_in(jax.random.fold_in(key, 6), axis_at), (blocks,), jnp.float32, low / len(pieces), largest / len(pieces))
        return jnp.repeat(jnp.exp(steps), dims[axis_at] // blocks).reshape((-1,) + (1,) * (len(dims) - axis_at - 1))

    factor_of = one(*pieces[0])
    for cut in pieces[1:]:
        factor_of = factor_of * one(*cut)
    return factor_of


def noise(own_key, extent, width, limit, shards=(), held_as=jnp.bfloat16):
    gain = block_scale(own_key, extent, shards, -0.22, 0.18) if shards else 1.0
    result = jax.random.normal(own_key, extent, jnp.float32) * width * gain
    return jnp.minimum(jnp.maximum(result, -limit), limit).astype(held_as)


def setup_inputs(seed: int = 0) -> dict:
    seeds = jax.random.split(jax.random.key(seed), 11)
    block_input = noise(seeds[0], (TOKENS, D), 1.0, 6.0, ((0, 32),))
    attn_gain = jnp.clip(1.0 + 0.18 * jax.random.normal(seeds[1], (D,), jnp.float32), 0.099609375, 1.8984375).astype(jnp.bfloat16)
    qkv_weight = noise(seeds[2], (D, QKV), D ** -0.5, 0.15625, ((0, 4),))
    qkv_bias = noise(seeds[3], (QKV,), 0.5, 3.0, ((0, 4),))
    out_weight = noise(seeds[4], (D, D), (D // 32) ** -0.5, 0.875, ((0, 4),))
    mlp_gain = jnp.clip(1.0 + 0.18 * jax.random.normal(seeds[5], (D,), jnp.float32), 0.099609375, 1.8984375).astype(jnp.bfloat16)
    gate_weight = noise(seeds[6], (D, FF), D ** -0.5, 0.15625, ((0, 4),))
    up_weight = noise(seeds[7], (D, FF), D ** -0.5, 0.15625, ((0, 4),))
    down_weight = noise(seeds[8], (FF, D), (FF // 2) ** -0.5, 0.09375, ((0, 4),))
    cotangent = noise(seeds[9], (TOKENS, D), 1.0, 6.0, ((0, 32),))
    return {"block_input": block_input, "attn_gain": attn_gain, "qkv_weight": qkv_weight, "qkv_bias": qkv_bias, "out_weight": out_weight, "mlp_gain": mlp_gain, "gate_weight": gate_weight, "up_weight": up_weight, "down_weight": down_weight, "cotangent": cotangent}


NORM_EPS = 1e-06
ROPE_BASE = 1000000.0

def rope_tables():
    half_dim = HD // 2
    position = jnp.arange(SEQ, dtype=jnp.float32)
    inverse = ROPE_BASE ** (-(jnp.arange(half_dim, dtype=jnp.float32) * 2.0 / HD))
    angles = position[:, None] * inverse[None, :]
    return (jnp.cos(angles)[:, None, :], jnp.sin(angles)[:, None, :])

def rotate(vectors, cosine, sine_table):
    half_dim = HD // 2
    lower_half = vectors[..., :half_dim]
    upper_half = vectors[..., half_dim:]
    return jnp.concatenate([lower_half * cosine - upper_half * sine_table, upper_half * cosine + lower_half * sine_table], axis=-1)

def unrotate(grads, cosine, sine_table):
    half_dim = HD // 2
    lower_half = grads[..., :half_dim]
    upper_half = grads[..., half_dim:]
    return jnp.concatenate([lower_half * cosine + upper_half * sine_table, upper_half * cosine - lower_half * sine_table], axis=-1)

def masked_scores(queries, key_rot):
    scores = jnp.einsum('bqkgd,bskd->bkgqs', queries.astype(jnp.float32), key_rot.astype(jnp.float32)) * (1.0 / math.sqrt(HD))
    causal = jnp.arange(SEQ)[:, None] >= jnp.arange(SEQ)[None, :]
    return jnp.where(causal, scores, -1e+30)

def reference(block_input, attn_gain, qkv_weight, qkv_bias, out_weight, mlp_gain, gate_weight, up_weight, down_weight, cotangent):
    f32 = jnp.float32
    bf16 = jnp.bfloat16
    seq_count = TOKENS // SEQ
    batch_seqs = math.gcd(seq_count, max(1, 4096 // SEQ))
    block_count = seq_count // batch_seqs
    group_size = HEADS // KV
    q_width = HEADS * HD
    k_end = q_width + KV * HD
    cosine, sine_table = rope_tables()
    gain_one = attn_gain.astype(f32)
    gain_two = mlp_gain.astype(f32)
    score_scale = 1.0 / math.sqrt(HD)

    def layer_block(running, inputs):
        x_block, cot_block = inputs
        row_total = batch_seqs * SEQ
        xfloat = x_block.astype(f32).reshape(row_total, D)
        cot_rows = cot_block.reshape(row_total, D)
        inv_one = lax.rsqrt(lax.optimization_barrier(jnp.mean(xfloat * xfloat, axis=-1, keepdims=True)) + NORM_EPS)
        normed_one = (xfloat * inv_one * gain_one).astype(bf16)
        projected = jnp.dot(normed_one, qkv_weight, preferred_element_type=f32) + qkv_bias.astype(f32)
        queries = rotate(projected[:, :q_width].reshape(batch_seqs, SEQ, HEADS, HD), cosine, sine_table).astype(bf16)
        queries = queries.reshape(batch_seqs, SEQ, KV, group_size, HD)
        key_rot = rotate(projected[:, q_width:k_end].reshape(batch_seqs, SEQ, KV, HD), cosine, sine_table).astype(bf16)
        values = projected[:, k_end:].reshape(batch_seqs, SEQ, KV, HD).astype(bf16)
        scores = masked_scores(queries, key_rot)
        row_max = lax.optimization_barrier(jnp.max(scores, axis=-1, keepdims=True))
        logsum = row_max + jnp.log(lax.optimization_barrier(jnp.sum(jnp.exp(scores - row_max), axis=-1, keepdims=True)))
        attn_probs = jnp.exp(scores - logsum).astype(bf16)
        context = jnp.einsum('bkgqs,bskd->bqkgd', attn_probs.astype(f32), values.astype(f32)).astype(bf16).reshape(row_total, D)
        hidden_res = xfloat + jnp.dot(context, out_weight, preferred_element_type=f32)
        inv_two = lax.rsqrt(lax.optimization_barrier(jnp.mean(hidden_res * hidden_res, axis=-1, keepdims=True)) + NORM_EPS)
        normed_two = (hidden_res * inv_two * gain_two).astype(bf16)
        gate_pre = jnp.dot(normed_two, gate_weight, preferred_element_type=f32)
        up_pre = jnp.dot(normed_two, up_weight, preferred_element_type=f32)
        sigmoid_gate = jax.nn.sigmoid(gate_pre)
        silu_gate = gate_pre * sigmoid_gate
        activation = (silu_gate * up_pre).astype(bf16)
        block_output = (hidden_res + jnp.dot(activation, down_weight, preferred_element_type=f32)).astype(bf16)
        down_grad = jnp.dot(activation.T, cot_rows, preferred_element_type=f32)
        act_grad = jnp.dot(cot_rows, down_weight.T, preferred_element_type=f32)
        gate_delta = (act_grad * up_pre * sigmoid_gate * (1.0 + gate_pre * (1.0 - sigmoid_gate))).astype(bf16)
        up_delta = (act_grad * silu_gate).astype(bf16)
        gate_grad = jnp.dot(normed_two.T, gate_delta, preferred_element_type=f32)
        up_grad = jnp.dot(normed_two.T, up_delta, preferred_element_type=f32)
        normed_two_grad = jnp.dot(gate_delta, gate_weight.T, preferred_element_type=f32) + jnp.dot(up_delta, up_weight.T, preferred_element_type=f32)
        gain_two_grad = lax.optimization_barrier(jnp.sum(normed_two_grad * hidden_res * inv_two, axis=0))
        hidden_grad = cot_rows.astype(f32) + inv_two * (gain_two * normed_two_grad - hidden_res * inv_two * inv_two * lax.optimization_barrier(jnp.mean(gain_two * normed_two_grad * hidden_res, axis=-1, keepdims=True)))
        hidden_low = hidden_grad.astype(bf16)
        out_grad = jnp.dot(context.T, hidden_low, preferred_element_type=f32)
        context_grad = jnp.dot(hidden_low, out_weight.T, preferred_element_type=f32).astype(bf16)
        grad_heads = context_grad.reshape(batch_seqs, SEQ, KV, group_size, HD).astype(f32)
        wide_probs = attn_probs.astype(f32)
        prob_grad = jnp.einsum('bqkgd,bskd->bkgqs', grad_heads, values.astype(f32))
        row_delta = lax.optimization_barrier(jnp.sum(wide_probs * prob_grad, axis=-1, keepdims=True))
        score_low = lax.optimization_barrier((wide_probs * (prob_grad - row_delta) * score_scale).astype(bf16))
        score_grad = score_low.astype(f32)
        query_grad = jnp.einsum('bkgqs,bskd->bqkgd', score_grad, key_rot.astype(f32)).reshape(batch_seqs, SEQ, HEADS, HD)
        key_grad = jnp.einsum('bkgqs,bqkgd->bskd', score_grad, queries.astype(f32))
        value_grad = jnp.einsum('bkgqs,bqkgd->bskd', wide_probs, grad_heads)
        query_grad = unrotate(query_grad, cosine, sine_table).reshape(row_total, q_width)
        key_grad = unrotate(key_grad, cosine, sine_table).reshape(row_total, KV * HD)
        projected_grad = jnp.concatenate([query_grad, key_grad, value_grad.reshape(row_total, KV * HD)], axis=-1).astype(bf16)
        qkv_grad = jnp.dot(normed_one.T, projected_grad, preferred_element_type=f32)
        bias_grad = lax.optimization_barrier(jnp.sum(projected_grad.astype(f32), axis=0))
        normed_one_grad = jnp.dot(projected_grad, qkv_weight.T, preferred_element_type=f32)
        gain_one_grad = lax.optimization_barrier(jnp.sum(normed_one_grad * xfloat * inv_one, axis=0))
        input_grad = hidden_grad + inv_one * (gain_one * normed_one_grad - xfloat * inv_one * inv_one * lax.optimization_barrier(jnp.mean(gain_one * normed_one_grad * xfloat, axis=-1, keepdims=True)))
        terms = (gain_one_grad, qkv_grad, bias_grad, out_grad, gain_two_grad, gate_grad, up_grad, down_grad)
        running = tuple((total + term for total, term in zip(running, terms)))
        return (running, (block_output.reshape(batch_seqs, SEQ, D), input_grad.reshape(batch_seqs, SEQ, D)))
    start_sums = (jnp.zeros((D,), f32), jnp.zeros((D, QKV), f32), jnp.zeros((QKV,), f32), jnp.zeros((D, D), f32), jnp.zeros((D,), f32), jnp.zeros((D, FF), f32), jnp.zeros((D, FF), f32), jnp.zeros((FF, D), f32))
    x_blocks = block_input.reshape(block_count, batch_seqs, SEQ, D)
    cot_blocks = cotangent.reshape(block_count, batch_seqs, SEQ, D)
    sums, (outputs, in_grads) = lax.scan(layer_block, start_sums, (x_blocks, cot_blocks))
    grad_scale = 1.0 / math.sqrt(TOKENS)
    sums = tuple((total * grad_scale for total in sums))
    return (outputs.reshape(TOKENS, D), in_grads.reshape(TOKENS, D), sums[0], sums[1], sums[2], sums[3], sums[4], sums[5], sums[6], sums[7])
```

```python
import functools
import math

import jax
import jax.numpy as jnp
from jax import lax
from jax.experimental import pallas as pl
from jax.experimental.pallas import tpu as pltpu
from jax.sharding import PartitionSpec as P

HEADS = 12
KV = 2
HD = 128


NORM_EPS = 1e-06
ROPE_BASE = 1000000.0


def rope_tables(tok_count):
    half_dim = HD // 2
    position = jnp.arange(tok_count, dtype=jnp.float32)
    inverse = ROPE_BASE ** (-(jnp.arange(half_dim, dtype=jnp.float32) * 2.0 / HD))
    angles = position[:, None] * inverse[None, :]
    return (jnp.cos(angles)[:, None, :], jnp.sin(angles)[:, None, :])


def rotate(vectors, cosine, sine_table):
    half_dim = HD // 2
    lower_half = vectors[..., :half_dim]
    upper_half = vectors[..., half_dim:]
    return jnp.concatenate(
        [
            lower_half * cosine - upper_half * sine_table,
            upper_half * cosine + lower_half * sine_table,
        ],
        axis=-1,
    )


def unrotate(grads, cosine, sine_table):
    half_dim = HD // 2
    lower_half = grads[..., :half_dim]
    upper_half = grads[..., half_dim:]
    return jnp.concatenate(
        [
            lower_half * cosine + upper_half * sine_table,
            upper_half * cosine - lower_half * sine_table,
        ],
        axis=-1,
    )


def block_scores(query_block, key_rot, first_row):
    row_count = query_block.shape[0]
    scores = jnp.einsum(
        "qkgd,skd->kgqs", query_block, key_rot, preferred_element_type=jnp.float32
    ) * (1.0 / math.sqrt(HD))
    causal = (first_row + jnp.arange(row_count))[:, None] >= jnp.arange(key_rot.shape[0])[None, :]
    return jnp.where(causal, scores, -1e30)


def block_layout(tok_count):
    block_rows = min(tok_count, 512)
    block_count = tok_count // block_rows
    firsts = jnp.arange(block_count, dtype=jnp.int32) * block_rows
    return (block_rows, block_count, firsts)


def attend_forward(queries, key_rot, values):
    tok_count = queries.shape[0]
    block_rows, block_count, firsts = block_layout(tok_count)
    query_blocks = queries.reshape(block_count, block_rows, KV, HEADS // KV, HD)

    def one_block(inputs):
        query_block, first_row = inputs
        scores = block_scores(query_block, key_rot, first_row)
        row_max = jnp.max(scores, axis=-1, keepdims=True)
        logsum = row_max + jnp.log(jnp.sum(jnp.exp(scores - row_max), axis=-1, keepdims=True))
        attn_probs = jnp.exp(scores - logsum).astype(jnp.bfloat16)
        context = jnp.einsum(
            "kgqs,skd->qkgd", attn_probs, values, preferred_element_type=jnp.float32
        ).astype(jnp.bfloat16)
        return (context, logsum)

    context, logsum = lax.map(one_block, (query_blocks, firsts))
    return (context.reshape(tok_count, HEADS * HD), logsum)


def attend_backward(queries, key_rot, values, logsum, context_grad):
    tok_count = queries.shape[0]
    block_rows, block_count, firsts = block_layout(tok_count)
    query_blocks = queries.reshape(block_count, block_rows, KV, HEADS // KV, HD)
    grad_blocks = context_grad.reshape(block_count, block_rows, KV, HEADS // KV, HD)
    score_scale = 1.0 / math.sqrt(HD)

    def one_block(running, inputs):
        key_total, value_total = running
        query_block, grad_block, log_block, first_row = inputs
        scores = block_scores(query_block, key_rot, first_row)
        attn_probs = jnp.exp(scores - log_block).astype(jnp.bfloat16)
        prob_grad = jnp.einsum(
            "qkgd,skd->kgqs", grad_block, values, preferred_element_type=jnp.float32
        )
        wide_probs = attn_probs.astype(jnp.float32)
        row_delta = jnp.sum(wide_probs * prob_grad, axis=-1, keepdims=True)
        score_grad = (wide_probs * (prob_grad - row_delta) * score_scale).astype(jnp.bfloat16)
        query_grad = jnp.einsum(
            "kgqs,skd->qkgd", score_grad, key_rot, preferred_element_type=jnp.float32
        )
        key_total = key_total + jnp.einsum(
            "kgqs,qkgd->skd", score_grad, query_block, preferred_element_type=jnp.float32
        )
        value_total = value_total + jnp.einsum(
            "kgqs,qkgd->skd", attn_probs, grad_block, preferred_element_type=jnp.float32
        )
        return ((key_total, value_total), query_grad)

    zero_keys = jnp.zeros((tok_count, KV, HD), jnp.float32)
    (key_grad, value_grad), query_grad = lax.scan(
        one_block, (zero_keys, zero_keys), (query_blocks, grad_blocks, logsum, firsts)
    )
    return (query_grad.reshape(tok_count, HEADS, HD), key_grad, value_grad)


def general_device(
    block_input,
    attn_gain,
    qkv_weight,
    qkv_bias,
    out_weight,
    mlp_gain,
    gate_weight,
    up_weight,
    down_weight,
    cotangent,
):
    f32 = jnp.float32
    bf16 = jnp.bfloat16
    tok_count = block_input.shape[0]
    grad_scale = 1.0 / math.sqrt(tok_count * lax.axis_size("replica") * lax.axis_size("shard"))
    q_width = HEADS * HD
    k_end = q_width + KV * HD
    cosine, sine_table = rope_tables(tok_count)
    attn_full = (
        lax.all_gather(attn_gain, "shard", axis=0, tiled=True),
        lax.all_gather(qkv_weight, "shard", axis=0, tiled=True),
        lax.all_gather(qkv_bias, "shard", axis=0, tiled=True),
        lax.all_gather(out_weight, "shard", axis=0, tiled=True),
    )
    gain_full, qkv_full, bias_full, out_full = attn_full
    gain_one = gain_full.astype(f32)
    xfloat = block_input.astype(f32)
    inv_one = lax.rsqrt(jnp.mean(xfloat * xfloat, axis=-1, keepdims=True) + NORM_EPS)
    normed_one = (xfloat * inv_one * gain_one).astype(bf16)
    projected = jnp.dot(normed_one, qkv_full, preferred_element_type=f32) + bias_full.astype(f32)
    queries = rotate(
        projected[:, :q_width].reshape(tok_count, HEADS, HD), cosine, sine_table
    ).astype(bf16)
    queries = queries.reshape(tok_count, KV, HEADS // KV, HD)
    key_rot = rotate(
        projected[:, q_width:k_end].reshape(tok_count, KV, HD), cosine, sine_table
    ).astype(bf16)
    values = projected[:, k_end:].reshape(tok_count, KV, HD).astype(bf16)
    context, logsum = attend_forward(queries, key_rot, values)
    hidden_res = xfloat + jnp.dot(context, out_full, preferred_element_type=f32)
    mlp_full = (
        lax.all_gather(mlp_gain, "shard", axis=0, tiled=True),
        lax.all_gather(gate_weight, "shard", axis=0, tiled=True),
        lax.all_gather(up_weight, "shard", axis=0, tiled=True),
        lax.all_gather(down_weight, "shard", axis=0, tiled=True),
    )
    gain_full_two, gate_full, up_full, down_full = mlp_full
    gain_two = gain_full_two.astype(f32)
    inv_two = lax.rsqrt(jnp.mean(hidden_res * hidden_res, axis=-1, keepdims=True) + NORM_EPS)
    normed_two = (hidden_res * inv_two * gain_two).astype(bf16)
    gate_pre = jnp.dot(normed_two, gate_full, preferred_element_type=f32)
    up_pre = jnp.dot(normed_two, up_full, preferred_element_type=f32)
    sigmoid_gate = jax.nn.sigmoid(gate_pre)
    silu_gate = gate_pre * sigmoid_gate
    activation = (silu_gate * up_pre).astype(bf16)
    block_output = (hidden_res + jnp.dot(activation, down_full, preferred_element_type=f32)).astype(
        bf16
    )
    act_grad = jnp.einsum("td,fd->tf", cotangent, down_full, preferred_element_type=f32)
    gate_delta = (
        act_grad * up_pre * sigmoid_gate * (1.0 + gate_pre * (1.0 - sigmoid_gate))
    ).astype(bf16)
    up_delta = (act_grad * silu_gate).astype(bf16)
    normed_two_grad = jnp.einsum(
        "tf,df->td", gate_delta, gate_full, preferred_element_type=f32
    ) + jnp.einsum("tf,df->td", up_delta, up_full, preferred_element_type=f32)
    gain_two_grad = jnp.sum(normed_two_grad * hidden_res * inv_two, axis=0) * grad_scale
    own_rows = (
        lax.all_to_all(activation, "shard", split_axis=1, concat_axis=0, tiled=True),
        lax.all_to_all(normed_two, "shard", split_axis=1, concat_axis=0, tiled=True),
    )
    group_act, group_normed = own_rows
    group_rows = (
        lax.all_gather(cotangent, "shard", axis=0, tiled=True),
        lax.all_gather(gate_delta, "shard", axis=0, tiled=True),
        lax.all_gather(up_delta, "shard", axis=0, tiled=True),
    )
    group_cot, group_gate, group_up = group_rows
    down_part = (
        jnp.einsum("tf,td->fd", group_act, group_cot, preferred_element_type=f32) * grad_scale
    )
    gate_own = (
        jnp.einsum("td,tf->df", group_normed, group_gate, preferred_element_type=f32) * grad_scale
    )
    up_own = (
        jnp.einsum("td,tf->df", group_normed, group_up, preferred_element_type=f32) * grad_scale
    )
    gain_two_own = lax.psum_scatter(gain_two_grad, "shard", scatter_dimension=0, tiled=True)
    mlp_parts = (gain_two_own, gate_own, up_own)
    hidden_grad = cotangent.astype(f32) + inv_two * (
        gain_two * normed_two_grad
        - hidden_res
        * inv_two
        * inv_two
        * jnp.mean(gain_two * normed_two_grad * hidden_res, axis=-1, keepdims=True)
    )
    hidden_low = hidden_grad.astype(bf16)
    context_grad = jnp.einsum("td,ed->te", hidden_low, out_full, preferred_element_type=f32).astype(
        bf16
    )
    query_grad, key_grad, value_grad = attend_backward(
        queries, key_rot, values, logsum, context_grad
    )
    query_grad = unrotate(query_grad, cosine, sine_table).reshape(tok_count, q_width)
    key_grad = unrotate(key_grad, cosine, sine_table).reshape(tok_count, KV * HD)
    projected_grad = jnp.concatenate(
        [query_grad, key_grad, value_grad.reshape(tok_count, KV * HD)], axis=-1
    ).astype(bf16)
    normed_one_grad = jnp.einsum("tc,dc->td", projected_grad, qkv_full, preferred_element_type=f32)
    gain_one_grad = jnp.sum(normed_one_grad * xfloat * inv_one, axis=0) * grad_scale
    bias_grad = jnp.sum(projected_grad.astype(f32), axis=0) * grad_scale
    own_attn = (
        lax.all_to_all(context, "shard", split_axis=1, concat_axis=0, tiled=True),
        lax.all_to_all(normed_one, "shard", split_axis=1, concat_axis=0, tiled=True),
    )
    group_context, group_normed_one = own_attn
    group_rows = (
        lax.all_gather(hidden_low, "shard", axis=0, tiled=True),
        lax.all_gather(projected_grad, "shard", axis=0, tiled=True),
    )
    group_hidden, group_projected = group_rows
    out_own = (
        jnp.einsum("te,td->ed", group_context, group_hidden, preferred_element_type=f32)
        * grad_scale
    )
    qkv_part = (
        jnp.einsum("td,tc->dc", group_normed_one, group_projected, preferred_element_type=f32)
        * grad_scale
    )
    small_parts = (
        lax.psum_scatter(gain_one_grad, "shard", scatter_dimension=0, tiled=True),
        lax.psum_scatter(bias_grad, "shard", scatter_dimension=0, tiled=True),
    )
    attn_parts = (small_parts[0], qkv_part, small_parts[1], out_own)
    input_grad = hidden_grad + inv_one * (
        gain_one * normed_one_grad
        - xfloat
        * inv_one
        * inv_one
        * jnp.mean(gain_one * normed_one_grad * xfloat, axis=-1, keepdims=True)
    )
    summed = lax.psum(
        (
            attn_parts[0],
            attn_parts[1],
            attn_parts[2],
            attn_parts[3],
            mlp_parts[0],
            mlp_parts[1],
            mlp_parts[2],
            down_part,
        ),
        "replica",
    )
    attn_parts = (summed[0], summed[1], summed[2], summed[3])
    mlp_parts = (summed[4], summed[5], summed[6])
    down_part = summed[7]
    return (
        block_output,
        input_grad,
        attn_parts[0],
        attn_parts[1],
        attn_parts[2],
        attn_parts[3],
        mlp_parts[0],
        mlp_parts[1],
        mlp_parts[2],
        down_part,
    )


MESH = pl.DeviceIdType.MESH
VMEM_BYTES = 62 * 2**20
WINDOW = 1152


def place():
    replica = lax.axis_index("replica")
    shard = lax.axis_index("shard")
    core = lax.rem(replica, 2)
    return replica, shard, core


def peer_of(shard, d):
    across = lax.rem(lax.rem(shard, 2) + d % 2, 2)
    up = lax.rem(shard // 2 + d // 2, 2)
    return up * 2 + across


def window_start(shard, core):
    return ((shard * 35) // 2 + core * 9) * 128


def remote(src, dst, send, recv, device):
    return pltpu.make_async_remote_copy(
        src_ref=src,
        dst_ref=dst,
        send_sem=send,
        recv_sem=recv,
        device_id=device,
        device_id_type=MESH,
    )


def front_kernel(
    wq, wo, wg, wu, cot, small, q_full, o_full, g_own, u_own, cot_all, small_all,
    bq, bo, bg, bu, bc, bs, send, recv, fsend, frecv, local,
):
    replica, shard, core = place()
    mate = (replica + 1 - 2 * core, shard)
    half = 192

    def rows(owner):
        return pl.ds(pl.multiple_of(owner * 384, 384), 384)

    def half_rows(owner, c):
        return pl.ds(pl.multiple_of(owner * 384 + c * half, half), half)

    def cols(target):
        return pl.ds(pl.multiple_of(window_start(target, core), 128), WINDOW)

    def block(owner, c):
        return pl.ds(pl.multiple_of((c * 4 + owner) * 128, 128), 128)

    mine = pl.ds(pl.multiple_of(core * half, half), half)
    loads = [
        (wq, bq, q_full.at[rows(shard)]),
        (wo, bo, o_full.at[rows(shard)]),
        (wg.at[:, cols(shard)], bg, g_own.at[rows(shard)]),
        (wu.at[:, cols(shard)], bu, u_own.at[rows(shard)]),
        (cot, bc, cot_all.at[block(shard, core)]),
        (small, bs, small_all.at[shard]),
    ]
    items = [
        (lambda t: small, lambda o: small_all.at[o], False),
        (lambda t: wq.at[mine], lambda o: q_full.at[half_rows(o, core)], True),
        (lambda t: wo.at[mine], lambda o: o_full.at[half_rows(o, core)], True),
        (lambda t: cot, lambda o: cot_all.at[block(o, core)], True),
        (lambda t: wg.at[:, cols(t)], lambda o: g_own.at[rows(o)], False),
        (lambda t: wu.at[:, cols(t)], lambda o: u_own.at[rows(o)], False),
    ]

    def hop(i, d, t, o):
        source, target, _ = items[i]
        n = i * 3 + d - 1
        return remote(source(t), target(o), send.at[n], recv.at[n], (replica, t))

    def onward(i, d, ref):
        n = i * 3 + d - 1
        return remote(ref, ref, fsend.at[n], frecv.at[n], mate)

    for i in range(len(items)):
        for d in (3, 1, 2):
            hop(i, d, peer_of(shard, d), shard).start()
    own_block = remote(cot, cot_all.at[block(shard, core)], fsend.at[18], frecv.at[18], mate)
    own_block.start()
    for n, (src, buf, _) in enumerate(loads):
        pltpu.make_async_copy(src, buf, local.at[n]).start()
    for n, (src, buf, dst) in enumerate(loads):
        pltpu.make_async_copy(src, buf, local.at[n]).wait()
        pltpu.make_async_copy(buf, dst, local.at[n]).start()
    for i, (_, target, passed) in enumerate(items):
        for d in (3, 1, 2):
            p = peer_of(shard, d)
            hop(i, d, p, p).wait_recv()
            if passed:
                onward(i, d, target(p)).start()
    for i, (_, target, passed) in enumerate(items):
        for d in (3, 1, 2):
            p = peer_of(shard, d)
            hop(i, d, p, shard).wait_send()
            if passed:
                onward(i, d, target(p)).wait_send()
    other = 1 - core
    arrivals = {1: lambda o: q_full.at[half_rows(o, other)], 2: lambda o: o_full.at[half_rows(o, other)],
                3: lambda o: cot_all.at[block(o, other)]}
    for i, target in arrivals.items():
        for d in (3, 1, 2):
            onward(i, d, target(peer_of(shard, d))).wait_recv()
    own_block.wait_send()
    remote(cot, cot_all.at[block(shard, other)], fsend.at[18], frecv.at[18], mate).wait_recv()
    for n, (src, buf, dst) in enumerate(loads):
        pltpu.make_async_copy(buf, dst, local.at[n]).wait()


def any_spec():
    return pl.BlockSpec(memory_space=pl.ANY)


def vmem_spec():
    return pl.BlockSpec(memory_space=pltpu.VMEM)


def params(**more):
    return pltpu.CompilerParams(has_side_effects=True, vmem_limit_bytes=VMEM_BYTES, **more)


def front(wq, wo, wg, wu, cot, small):
    bf16 = jnp.bfloat16
    shapes = [(1536, 2048), (1536, 1536), (1536, WINDOW), (1536, WINDOW), (1024, 1536), (4, 16, 512)]
    bounce = [wq.shape, wo.shape, (384, WINDOW), (384, WINDOW), cot.shape, small.shape]
    return pl.pallas_call(
        front_kernel,
        out_shape=[jax.ShapeDtypeStruct(s, bf16) for s in shapes],
        in_specs=[any_spec()] * 6,
        out_specs=[any_spec()] * 6,
        scratch_shapes=[pltpu.VMEM(s, bf16) for s in bounce]
        + [
            pltpu.SemaphoreType.DMA((18,)),
            pltpu.SemaphoreType.DMA((18,)),
            pltpu.SemaphoreType.DMA((19,)),
            pltpu.SemaphoreType.DMA((19,)),
            pltpu.SemaphoreType.DMA((6,)),
        ],
        compiler_params=params(),
    )(wq, wo, wg, wu, cot, small)


def gather_kernel(x, out, send, recv, fsend, frecv, local):
    replica, shard, core = place()
    mate = (replica + 1 - 2 * core, shard)

    def block(owner, c):
        return out.at[pl.ds(pl.multiple_of((c * 4 + owner) * 128, 128), 128)]

    for d in (3, 1, 2):
        remote(x, block(shard, core), send.at[d], recv.at[d], (replica, peer_of(shard, d))).start()
    remote(x, block(shard, core), fsend.at[0], frecv.at[0], mate).start()
    own = pltpu.make_async_copy(x, block(shard, core), local)
    own.start()
    for d in (1, 2, 3):
        p = peer_of(shard, d)
        remote(x, block(p, core), send.at[d], recv.at[d], (replica, p)).wait_recv()
        remote(block(p, core), block(p, core), fsend.at[d], frecv.at[d], mate).start()
    own.wait()
    for d in (1, 2, 3):
        p = peer_of(shard, d)
        remote(x, block(shard, core), send.at[d], recv.at[d], (replica, p)).wait_send()
        remote(block(p, core), block(p, core), fsend.at[d], frecv.at[d], mate).wait_send()
        remote(x, block(p, 1 - core), fsend.at[d], frecv.at[d], mate).wait_recv()
    remote(x, block(shard, core), fsend.at[0], frecv.at[0], mate).wait_send()
    remote(x, block(shard, 1 - core), fsend.at[0], frecv.at[0], mate).wait_recv()


def plane_gather(x):
    return pl.pallas_call(
        gather_kernel,
        out_shape=jax.ShapeDtypeStruct((x.shape[0] * 8, x.shape[1]), x.dtype),
        in_specs=[vmem_spec()],
        out_specs=vmem_spec(),
        scratch_shapes=[pltpu.SemaphoreType.DMA((4,))] * 4 + [pltpu.SemaphoreType.DMA],
        compiler_params=params(),
    )(x)


def scatter_kernel(pa, pb, oa, ob, held, sums, parts, csend, crecv, send, recv):
    replica, shard, core = place()
    mate = (replica + 1 - 2 * core, shard)
    f32 = jnp.float32
    inputs = (pa, pb)
    outputs = (oa, ob)

    def block(c, target):
        return pl.ds(pl.multiple_of((c * 4 + target) * 128, 128), 128)

    order = (3, 1, 2, 0)
    for a in range(2):
        for d in order:
            t = peer_of(shard, d)
            remote(inputs[a].at[block(1 - core, t)], held.at[a, d], csend.at[a * 4 + d], crecv.at[a * 4 + d], mate).start()

    def summed(a, d):
        t = peer_of(shard, d)
        n = a * 4 + d
        remote(inputs[a].at[block(core, t)], held.at[a, d], csend.at[n], crecv.at[n], mate).wait_recv()
        return inputs[a][block(core, t), :].astype(f32) + held[a, d].astype(f32)

    for a in range(2):
        for d in (3, 1, 2):
            sums[a, d - 1] = summed(a, d).astype(sums.dtype)
            n = a * 3 + d - 1
            remote(sums.at[a, d - 1], parts.at[a, d - 1], send.at[n], recv.at[n], (replica, peer_of(shard, d))).start()
    for a in range(2):
        outputs[a][...] = summed(a, 0)
    for a in range(2):
        for d in (1, 2, 3):
            n = a * 3 + d - 1
            remote(sums.at[a, d - 1], parts.at[a, d - 1], send.at[n], recv.at[n], (replica, peer_of(shard, d))).wait()
            outputs[a][...] += parts[a, d - 1].astype(f32)
    for a in range(2):
        for d in order:
            t = peer_of(shard, d)
            n = a * 4 + d
            remote(inputs[a].at[block(1 - core, t)], held.at[a, d], csend.at[n], crecv.at[n], mate).wait_send()


def plane_scatter(pa, pb):
    width = pa.shape[1]
    bf16 = jnp.bfloat16
    out = jax.ShapeDtypeStruct((128, width), jnp.float32)
    return pl.pallas_call(
        scatter_kernel,
        out_shape=[out, out],
        in_specs=[vmem_spec()] * 2,
        out_specs=[vmem_spec()] * 2,
        scratch_shapes=[
            pltpu.VMEM((2, 4, 128, width), bf16),
            pltpu.VMEM((2, 3, 128, width), bf16),
            pltpu.VMEM((2, 3, 128, width), bf16),
            pltpu.SemaphoreType.DMA((8,)),
            pltpu.SemaphoreType.DMA((8,)),
            pltpu.SemaphoreType.DMA((6,)),
            pltpu.SemaphoreType.DMA((6,)),
        ],
        compiler_params=params(),
    )(pa, pb)


def attn_gather_kernel(ctx, nrm, hid, prj, ctx_all, nrm_all, hid_all, prj_all, send, recv, fsend, frecv, local):
    replica, shard, core = place()
    other = 1 - core
    mate = (replica + 1 - 2 * core, shard)

    def block(out, owner, c):
        return out.at[pl.ds(pl.multiple_of((c * 4 + owner) * 128, 128), 128)]

    def part(ref, index, width):
        return ref.at[:, pl.ds(pl.multiple_of(index * width, width), width)]

    def device(c, t):
        return (replica - core + c, t)

    wide = ((hid, hid_all, 768), (prj, prj_all, 1024))
    narrow = ((ctx, ctx_all, 384), (nrm, nrm_all, 384))
    def wide_copy(a, d, same, source_core, owner, t):
        ref, out, width = wide[a]
        c = core if same else other
        n = (a * 4 + d) * 2 + (0 if same else 1)
        return remote(part(ref, c, width), block(out, owner, source_core), send.at[n], recv.at[n], device(c, t))

    def narrow_copy(a, d, owner, t):
        ref, out, width = narrow[a]
        n = 16 + a * 4 + d
        return remote(part(ref, t, width), block(out, owner, core), send.at[n], recv.at[n], (replica, t))

    def onward(a, d, source, owner, c):
        _, out, _ = narrow[a]
        n = a * 4 + d
        return remote(source, block(out, owner, c), fsend.at[n], frecv.at[n], mate)

    for d in (3, 1, 2, 0):
        t = peer_of(shard, d)
        for a in range(2):
            if d:
                wide_copy(a, d, True, core, shard, t).start()
            wide_copy(a, d, False, core, shard, t).start()
            if d:
                narrow_copy(a, d, shard, t).start()
            else:
                ref, out, width = narrow[a]
                onward(a, 0, part(ref, shard, width), shard, core).start()
    locals_ = []
    for a in range(2):
        ref, out, width = narrow[a]
        locals_.append(pltpu.make_async_copy(part(ref, shard, width), block(out, shard, core), local.at[a]))
        ref, out, width = wide[a]
        locals_.append(pltpu.make_async_copy(part(ref, core, width), block(out, shard, core), local.at[2 + a]))
    for copy in locals_:
        copy.start()
    for d in (1, 2, 3):
        p = peer_of(shard, d)
        for a in range(2):
            narrow_copy(a, d, p, p).wait_recv()
            onward(a, d, block(narrow[a][1], p, core), p, core).start()
    for copy in locals_:
        copy.wait()
    for d in (0, 1, 2, 3):
        p = peer_of(shard, d)
        for a in range(2):
            if d:
                wide_copy(a, d, True, core, p, p).wait_recv()
                wide_copy(a, d, True, core, shard, p).wait_send()
                narrow_copy(a, d, shard, p).wait_send()
            wide_copy(a, d, False, other, p, p).wait_recv()
            wide_copy(a, d, False, core, shard, p).wait_send()
            onward(a, d, block(narrow[a][1], p, core), p, core).wait_send()
            onward(a, d, block(narrow[a][1], p, other), p, other).wait_recv()


def attn_gather(ctx, nrm, hid, prj):
    bf16 = jnp.bfloat16
    shapes = [(1024, 384), (1024, 384), (1024, 768), (1024, 1024)]
    return pl.pallas_call(
        attn_gather_kernel,
        out_shape=[jax.ShapeDtypeStruct(s, bf16) for s in shapes],
        in_specs=[vmem_spec()] * 4,
        out_specs=[vmem_spec()] * 4,
        scratch_shapes=[
            pltpu.SemaphoreType.DMA((24,)),
            pltpu.SemaphoreType.DMA((24,)),
            pltpu.SemaphoreType.DMA((8,)),
            pltpu.SemaphoreType.DMA((8,)),
            pltpu.SemaphoreType.DMA((4,)),
        ],
        compiler_params=params(),
    )(ctx, nrm, hid, prj)


CHUNK = 128


def reduce_kernel(
    levels, pa, pd, pg, pu, fa, fd, fg, fu,
    own_a, own_d, own_g, low_a, low_d, low_g, high_a, high_d, high_g,
    xsend, xrecv, up_sem, down_sem, low_sem, high_sem, mate_send, mate_recv, out_sem, in_sem,
):
    replica, shard, core = place()
    level = replica // 2
    mate = (replica + 1 - 2 * core, shard)
    above, below = (replica + 2, shard), (replica - 2, shard)
    f32 = jnp.float32
    sources = (pg, pu)

    def exchange(a, d, p):
        rows = pl.ds(pl.multiple_of(p * 384, 384), 384)
        n = a * 4 + d
        return remote(sources[a].at[rows], own_g.at[pl.ds(a * 1536 + d * 384, 384)], xsend.at[n], xrecv.at[n], (replica, p))

    fills = [
        pltpu.make_async_copy(pa, own_a, in_sem.at[0]),
        pltpu.make_async_copy(pd, own_d, in_sem.at[1]),
    ]
    for a in range(2):
        rows = pl.ds(pl.multiple_of(shard * 384, 384), 384)
        fills.append(pltpu.make_async_copy(sources[a].at[rows], own_g.at[pl.ds(a * 1536, 384)], in_sem.at[2 + a]))
    for copy in fills:
        copy.start()
    for a in range(2):
        for d in (1, 2, 3):
            exchange(a, d, peer_of(shard, d)).start()

    chunks = []
    for k in range(3):
        at = pl.ds(k * CHUNK, CHUNK)
        chunks.append((own_a, low_a, high_a, at, ("fill", 0), lambda c, at=at: fa.at[c, at]))
    for k in range(9):
        at = pl.ds(k * CHUNK, CHUNK)
        chunks.append((own_d, low_d, high_d, at, ("fill", 1), lambda c, at=at: fd.at[c, at]))
    for d in range(4):
        for a in range(2):
            for k in range(3):
                at = pl.ds(a * 1536 + d * 384 + k * CHUNK, CHUNK)
                dst = (fg, fu)[a]
                source = peer_of(shard, d)
                chunks.append((
                    own_g, low_g, high_g, at, ("fill", 2 + a) if d == 0 else ("x", a, d),
                    lambda c, k=k, dst=dst, source=source: dst.at[c, source, pl.ds(k * CHUNK, CHUNK)],
                ))
    total = len(chunks)
    awaited = set()

    def arrive(what):
        if what in awaited:
            return
        awaited.add(what)
        if what[0] == "fill":
            fills[what[1]].wait()
        else:
            exchange(what[1], what[2], peer_of(shard, what[2])).wait_recv()

    def up(k, ref):
        own, low, high, at, _, _ = chunks[k]
        return remote(ref.at[at], low.at[at], up_sem.at[k], low_sem.at[k], above)

    def down(k, ref):
        own, low, high, at, _, _ = chunks[k]
        return remote(ref.at[at], high.at[at], down_sem.at[k], high_sem.at[k], below)

    def add(k, *refs):
        own, _, _, at, _, _ = chunks[k]
        step = 32

        def body(j, carry):
            rows = pl.ds(pl.multiple_of(at.start + j * step, step), step)
            value = own[rows, :].astype(f32)
            for ref in refs:
                value = value + ref[rows, :].astype(f32)
            own[rows, :] = value.astype(own.dtype)
            return carry

        lax.fori_loop(0, CHUNK // step, body, 0)

    def finish(k, ref):
        _, _, _, at, _, dst = chunks[k]
        pltpu.make_async_copy(ref.at[at], dst(core), out_sem.at[k]).start()
        remote(ref.at[at], dst(core), mate_send.at[k], mate_recv.at[k], mate).start()

    def root_of(k):
        return levels // 2 - 1 + k % 2

    def gather_step(k):
        own, low, high, at, what, _ = chunks[k]
        arrive(what)
        root = root_of(k)

        @pl.when(level < root)
        def _():
            if root > 1:

                @pl.when(level > 0)
                def _():
                    up(k, own).wait_recv()
                    add(k, low)

            up(k, own).start()

        @pl.when(level > root)
        def _():
            if root < levels - 2:

                @pl.when(level < levels - 1)
                def _():
                    down(k, own).wait_recv()
                    add(k, high)

            down(k, own).start()

    def root_step(k):
        own, low, high, at, _, _ = chunks[k]

        @pl.when(level == root_of(k))
        def _():
            up(k, own).wait_recv()
            down(k, own).wait_recv()
            add(k, low, high)
            up(k, own).start()
            down(k, own).start()
            finish(k, own)

    def spread_step(k):
        own, low, high, at, _, _ = chunks[k]
        root = root_of(k)

        @pl.when(level < root)
        def _():
            down(k, own).wait_recv()
            if root > 1:

                @pl.when(level > 0)
                def _():
                    down(k, high).start()

            finish(k, high)

        @pl.when(level > root)
        def _():
            up(k, own).wait_recv()
            if root < levels - 2:

                @pl.when(level < levels - 1)
                def _():
                    up(k, low).start()

            finish(k, low)

    for t in range(total + 6):
        if t < total:
            gather_step(t)
        if 0 <= t - 3 < total:
            root_step(t - 3)
        if 0 <= t - 6 < total:
            spread_step(t - 6)
    for a in range(2):
        for d in (1, 2, 3):
            exchange(a, d, peer_of(shard, d)).wait_send()
    for k in range(total):
        own, low, high, at, _, dst = chunks[k]

        @pl.when(level < levels - 1)
        def _():
            up(k, own).wait_send()

        @pl.when(level > 0)
        def _():
            down(k, own).wait_send()

        pltpu.make_async_copy(own.at[at], dst(core), out_sem.at[k]).wait()
        remote(own.at[at], dst(core), mate_send.at[k], mate_recv.at[k], mate).wait_send()
        remote(own.at[at], dst(1 - core), mate_send.at[k], mate_recv.at[k], mate).wait_recv()


def reduce_gradients(levels, pa, pd, pg, pu):
    bf16 = jnp.bfloat16
    shapes = [(2, 384, 1792), (2, WINDOW, 1536), (2, 4, 384, WINDOW), (2, 4, 384, WINDOW)]
    buffers = [(384, 1792), (WINDOW, 1536), (3072, WINDOW)]
    total = 36
    dma = pltpu.SemaphoreType.DMA
    return pl.pallas_call(
        functools.partial(reduce_kernel, levels),
        out_shape=[jax.ShapeDtypeStruct(s, bf16) for s in shapes],
        in_specs=[any_spec()] * 4,
        out_specs=[any_spec()] * 4,
        scratch_shapes=[pltpu.VMEM(s, bf16) for s in buffers * 3]
        + [dma((8,)), dma((8,))]
        + [dma((total,))] * 7
        + [dma((4,))],
        compiler_params=params(),
    )(pa, pd, pg, pu)


def widen_kernel(x, out):
    f32 = jnp.float32
    for s in range(4):
        for c in range(2):
            first = (s * 35) // 2 + c * 9
            joined = s % 2 == 1 and c == 0
            rest = 1 if joined else 0
            out[:, (first + rest) * 128 : (first + 9) * 128] = x[c, s][:, rest * 128 :].astype(f32)
    for s in (1, 3):
        first = (s * 35) // 2
        out[:, first * 128 : (first + 1) * 128] = x[1, s - 1][:, 1024:].astype(f32) + x[0, s][:, :128].astype(f32)


def widen(x):
    rows = 32
    return pl.pallas_call(
        widen_kernel,
        grid=(384 // rows,),
        out_shape=jax.ShapeDtypeStruct((384, 8960), jnp.float32),
        in_specs=[pl.BlockSpec((2, 4, rows, WINDOW), lambda i: (0, 0, i, 0))],
        out_specs=pl.BlockSpec((rows, 8960), lambda i: (i, 0)),
    )(x)


def fast_device(
    block_input,
    attn_gain,
    qkv_weight,
    qkv_bias,
    out_weight,
    mlp_gain,
    gate_weight,
    up_weight,
    down_weight,
    cotangent,
):
    f32 = jnp.float32
    bf16 = jnp.bfloat16
    tok_count = block_input.shape[0]
    levels = lax.axis_size("replica") // 2
    grad_scale = 1.0 / math.sqrt(tok_count * lax.axis_size("replica") * lax.axis_size("shard"))
    q_width = HEADS * HD
    k_end = q_width + KV * HD
    replica, shard, core = place()
    cosine, sine_table = rope_tables(tok_count)
    small = jnp.zeros((16, 512), bf16)
    small = small.at[0, :384].set(attn_gain).at[1, :].set(qkv_bias).at[2, :384].set(mlp_gain)
    qkv_full, out_full, gate_own, up_own, cot_all, small_all = front(
        qkv_weight, out_weight, gate_weight, up_weight, cotangent, small
    )
    gain_one = small_all[:, 0, :384].reshape(-1).astype(f32)
    bias = small_all[:, 1, :].reshape(-1).astype(f32)
    gain_two = small_all[:, 2, :384].reshape(-1).astype(f32)

    xfloat = block_input.astype(f32)
    inv_one = lax.rsqrt(jnp.mean(xfloat * xfloat, axis=-1, keepdims=True) + NORM_EPS)
    normed_one = (xfloat * inv_one * gain_one).astype(bf16)
    projected = jnp.dot(normed_one, qkv_full, preferred_element_type=f32) + bias
    queries = rotate(projected[:, :q_width].reshape(tok_count, HEADS, HD), cosine, sine_table).astype(bf16)
    queries = queries.reshape(tok_count, KV, HEADS // KV, HD)
    key_rot = rotate(projected[:, q_width:k_end].reshape(tok_count, KV, HD), cosine, sine_table).astype(bf16)
    values = projected[:, k_end:].reshape(tok_count, KV, HD).astype(bf16)
    context, logsum = attend_forward(queries, key_rot, values)
    hidden_res = xfloat + jnp.dot(context, out_full, preferred_element_type=f32)
    inv_two = lax.rsqrt(jnp.mean(hidden_res * hidden_res, axis=-1, keepdims=True) + NORM_EPS)
    normed_two = (hidden_res * inv_two * gain_two).astype(bf16)

    normed_all = plane_gather(normed_two)
    first = window_start(shard, core)
    column = first + jnp.arange(WINDOW)
    owned = (column >= shard * 2240) & (column < (shard + 1) * 2240)
    padded = jnp.pad(down_weight, ((64, 64), (0, 0)))
    down_own = lax.dynamic_slice_in_dim(padded, first - shard * 2240 + 64, WINDOW, 0)
    gate_pre = jnp.dot(normed_all, gate_own, preferred_element_type=f32)
    up_pre = jnp.dot(normed_all, up_own, preferred_element_type=f32)
    sigmoid_gate = jax.nn.sigmoid(gate_pre)
    silu_gate = gate_pre * sigmoid_gate
    act_grad = jnp.einsum("td,fd->tf", cot_all, down_own, preferred_element_type=f32)
    activation = jnp.where(owned, silu_gate * up_pre, 0.0).astype(bf16)
    gate_delta = jnp.where(
        owned, act_grad * up_pre * sigmoid_gate * (1.0 + gate_pre * (1.0 - sigmoid_gate)), 0.0
    ).astype(bf16)
    up_delta = jnp.where(owned, act_grad * silu_gate, 0.0).astype(bf16)
    down_out = jnp.dot(activation, down_own, preferred_element_type=f32).astype(bf16)
    back = (
        jnp.einsum("tf,df->td", gate_delta, gate_own, preferred_element_type=f32)
        + jnp.einsum("tf,df->td", up_delta, up_own, preferred_element_type=f32)
    ).astype(bf16)
    gate_part = (jnp.einsum("td,tf->df", normed_all, gate_delta, preferred_element_type=f32) * grad_scale).astype(bf16)
    up_part = (jnp.einsum("td,tf->df", normed_all, up_delta, preferred_element_type=f32) * grad_scale).astype(bf16)
    down_part = (jnp.einsum("tf,td->fd", activation, cot_all, preferred_element_type=f32) * grad_scale).astype(bf16)

    down_sum, normed_two_grad = plane_scatter(down_out, back)
    block_output = (hidden_res + down_sum).astype(bf16)
    gain_two_grad = jnp.sum(normed_two_grad * hidden_res * inv_two, axis=0) * grad_scale
    hidden_grad = cotangent.astype(f32) + inv_two * (
        gain_two * normed_two_grad
        - hidden_res
        * inv_two
        * inv_two
        * jnp.mean(gain_two * normed_two_grad * hidden_res, axis=-1, keepdims=True)
    )
    hidden_low = hidden_grad.astype(bf16)
    context_grad = jnp.einsum("td,ed->te", hidden_low, out_full, preferred_element_type=f32).astype(bf16)
    query_grad, key_grad, value_grad = attend_backward(queries, key_rot, values, logsum, context_grad)
    query_grad = unrotate(query_grad, cosine, sine_table).reshape(tok_count, q_width)
    key_grad = unrotate(key_grad, cosine, sine_table).reshape(tok_count, KV * HD)
    projected_grad = jnp.concatenate(
        [query_grad, key_grad, value_grad.reshape(tok_count, KV * HD)], axis=-1
    ).astype(bf16)
    normed_one_grad = jnp.einsum("tc,dc->td", projected_grad, qkv_full, preferred_element_type=f32)
    gain_one_grad = jnp.sum(normed_one_grad * xfloat * inv_one, axis=0) * grad_scale
    bias_grad = jnp.sum(projected_grad.astype(f32), axis=0) * grad_scale
    input_grad = hidden_grad + inv_one * (
        gain_one * normed_one_grad
        - xfloat
        * inv_one
        * inv_one
        * jnp.mean(gain_one * normed_one_grad * xfloat, axis=-1, keepdims=True)
    )
    vectors = lax.psum(jnp.concatenate([gain_one_grad, bias_grad, gain_two_grad]), ("replica", "shard"))
    gain_one_own = lax.dynamic_slice_in_dim(vectors, shard * 384, 384)
    bias_own = lax.dynamic_slice_in_dim(vectors, 1536 + shard * 512, 512)
    gain_two_own = lax.dynamic_slice_in_dim(vectors, 3584 + shard * 384, 384)

    ctx_rows, normed_rows, hidden_rows, projected_rows = attn_gather(context, normed_one, hidden_low, projected_grad)
    qkv_part = jnp.einsum("td,tc->dc", normed_rows, projected_rows, preferred_element_type=f32)
    out_part = jnp.einsum("te,td->ed", ctx_rows, hidden_rows, preferred_element_type=f32)
    attn_part = (jnp.concatenate([qkv_part, out_part], axis=1) * grad_scale).astype(bf16)

    sum_attn, sum_down, sum_gate, sum_up = reduce_gradients(levels, attn_part, down_part, gate_part, up_part)
    qkv_grad = jnp.concatenate([sum_attn[0, :, :1024], sum_attn[1, :, :1024]], axis=1).astype(f32)
    out_grad = jnp.concatenate([sum_attn[0, :, 1024:], sum_attn[1, :, 1024:]], axis=1).astype(f32)
    down_grad = lax.dynamic_slice_in_dim(
        sum_down.reshape(2 * WINDOW, 1536), lax.rem(shard, 2) * 64, 2240, 0
    ).astype(f32)
    return (
        block_output,
        input_grad,
        gain_one_own,
        qkv_grad,
        bias_own,
        out_grad,
        gain_two_own,
        widen(sum_gate),
        widen(sum_up),
        down_grad,
    )


def solution(mesh):
    placed = (
        P(("replica", "shard"), None),
        P("shard"),
        P("shard", None),
        P("shard"),
        P("shard", None),
        P("shard"),
        P("shard", None),
        P("shard", None),
        P("shard", None),
        P(("replica", "shard"), None),
    )
    fits = mesh.shape["shard"] == 4 and mesh.shape["replica"] % 2 == 0 and mesh.shape["replica"] >= 8
    per_device = fast_device if fits else general_device
    return jax.shard_map(
        per_device,
        mesh=mesh,
        in_specs=placed,
        out_specs=(
            P(("replica", "shard"), None),
            P(("replica", "shard"), None),
            P("shard"),
            P("shard", None),
            P("shard"),
            P("shard", None),
            P("shard"),
            P("shard", None),
            P("shard", None),
            P("shard", None),
        ),
        check_vma=False,
    )
```

```python
import functools
import math

import jax
import jax.numpy as jnp
from jax import lax
from jax.experimental import pallas as pl
from jax.experimental.pallas import tpu as pltpu
from jax.sharding import PartitionSpec as P

HEADS = 12
KV = 2
HD = 128


NORM_EPS = 1e-06
ROPE_BASE = 1000000.0


def rope_tables(tok_count):
    half_dim = HD // 2
    position = jnp.arange(tok_count, dtype=jnp.float32)
    inverse = ROPE_BASE ** (-(jnp.arange(half_dim, dtype=jnp.float32) * 2.0 / HD))
    angles = position[:, None] * inverse[None, :]
    return (jnp.cos(angles)[:, None, :], jnp.sin(angles)[:, None, :])


def rotate(vectors, cosine, sine_table):
    half_dim = HD // 2
    lower_half = vectors[..., :half_dim]
    upper_half = vectors[..., half_dim:]
    return jnp.concatenate(
        [
            lower_half * cosine - upper_half * sine_table,
            upper_half * cosine + lower_half * sine_table,
        ],
        axis=-1,
    )


def unrotate(grads, cosine, sine_table):
    half_dim = HD // 2
    lower_half = grads[..., :half_dim]
    upper_half = grads[..., half_dim:]
    return jnp.concatenate(
        [
            lower_half * cosine + upper_half * sine_table,
            upper_half * cosine - lower_half * sine_table,
        ],
        axis=-1,
    )


def block_scores(query_block, key_rot, first_row):
    row_count = query_block.shape[0]
    scores = jnp.einsum(
        "qkgd,skd->kgqs", query_block, key_rot, preferred_element_type=jnp.float32
    ) * (1.0 / math.sqrt(HD))
    causal = (first_row + jnp.arange(row_count))[:, None] >= jnp.arange(key_rot.shape[0])[None, :]
    return jnp.where(causal, scores, -1e30)


def block_layout(tok_count):
    block_rows = min(tok_count, 512)
    block_count = tok_count // block_rows
    firsts = jnp.arange(block_count, dtype=jnp.int32) * block_rows
    return (block_rows, block_count, firsts)


def attend_forward(queries, key_rot, values):
    tok_count = queries.shape[0]
    block_rows, block_count, firsts = block_layout(tok_count)
    query_blocks = queries.reshape(block_count, block_rows, KV, HEADS // KV, HD)

    def one_block(inputs):
        query_block, first_row = inputs
        scores = block_scores(query_block, key_rot, first_row)
        row_max = jnp.max(scores, axis=-1, keepdims=True)
        logsum = row_max + jnp.log(jnp.sum(jnp.exp(scores - row_max), axis=-1, keepdims=True))
        attn_probs = jnp.exp(scores - logsum).astype(jnp.bfloat16)
        context = jnp.einsum(
            "kgqs,skd->qkgd", attn_probs, values, preferred_element_type=jnp.float32
        ).astype(jnp.bfloat16)
        return (context, logsum)

    context, logsum = lax.map(one_block, (query_blocks, firsts))
    return (context.reshape(tok_count, HEADS * HD), logsum)


def attend_backward(queries, key_rot, values, logsum, context_grad):
    tok_count = queries.shape[0]
    block_rows, block_count, firsts = block_layout(tok_count)
    query_blocks = queries.reshape(block_count, block_rows, KV, HEADS // KV, HD)
    grad_blocks = context_grad.reshape(block_count, block_rows, KV, HEADS // KV, HD)
    score_scale = 1.0 / math.sqrt(HD)

    def one_block(running, inputs):
        key_total, value_total = running
        query_block, grad_block, log_block, first_row = inputs
        scores = block_scores(query_block, key_rot, first_row)
        attn_probs = jnp.exp(scores - log_block).astype(jnp.bfloat16)
        prob_grad = jnp.einsum(
            "qkgd,skd->kgqs", grad_block, values, preferred_element_type=jnp.float32
        )
        wide_probs = attn_probs.astype(jnp.float32)
        row_delta = jnp.sum(wide_probs * prob_grad, axis=-1, keepdims=True)
        score_grad = (wide_probs * (prob_grad - row_delta) * score_scale).astype(jnp.bfloat16)
        query_grad = jnp.einsum(
            "kgqs,skd->qkgd", score_grad, key_rot, preferred_element_type=jnp.float32
        )
        key_total = key_total + jnp.einsum(
            "kgqs,qkgd->skd", score_grad, query_block, preferred_element_type=jnp.float32
        )
        value_total = value_total + jnp.einsum(
            "kgqs,qkgd->skd", attn_probs, grad_block, preferred_element_type=jnp.float32
        )
        return ((key_total, value_total), query_grad)

    zero_keys = jnp.zeros((tok_count, KV, HD), jnp.float32)
    (key_grad, value_grad), query_grad = lax.scan(
        one_block, (zero_keys, zero_keys), (query_blocks, grad_blocks, logsum, firsts)
    )
    return (query_grad.reshape(tok_count, HEADS, HD), key_grad, value_grad)


def general_device(
    block_input,
    attn_gain,
    qkv_weight,
    qkv_bias,
    out_weight,
    mlp_gain,
    gate_weight,
    up_weight,
    down_weight,
    cotangent,
):
    f32 = jnp.float32
    bf16 = jnp.bfloat16
    tok_count = block_input.shape[0]
    grad_scale = 1.0 / math.sqrt(tok_count * lax.axis_size("replica") * lax.axis_size("shard"))
    q_width = HEADS * HD
    k_end = q_width + KV * HD
    cosine, sine_table = rope_tables(tok_count)
    attn_full = (
        lax.all_gather(attn_gain, "shard", axis=0, tiled=True),
        lax.all_gather(qkv_weight, "shard", axis=0, tiled=True),
        lax.all_gather(qkv_bias, "shard", axis=0, tiled=True),
        lax.all_gather(out_weight, "shard", axis=0, tiled=True),
    )
    gain_full, qkv_full, bias_full, out_full = attn_full
    gain_one = gain_full.astype(f32)
    xfloat = block_input.astype(f32)
    inv_one = lax.rsqrt(jnp.mean(xfloat * xfloat, axis=-1, keepdims=True) + NORM_EPS)
    normed_one = (xfloat * inv_one * gain_one).astype(bf16)
    projected = jnp.dot(normed_one, qkv_full, preferred_element_type=f32) + bias_full.astype(f32)
    queries = rotate(
        projected[:, :q_width].reshape(tok_count, HEADS, HD), cosine, sine_table
    ).astype(bf16)
    queries = queries.reshape(tok_count, KV, HEADS // KV, HD)
    key_rot = rotate(
        projected[:, q_width:k_end].reshape(tok_count, KV, HD), cosine, sine_table
    ).astype(bf16)
    values = projected[:, k_end:].reshape(tok_count, KV, HD).astype(bf16)
    context, logsum = attend_forward(queries, key_rot, values)
    hidden_res = xfloat + jnp.dot(context, out_full, preferred_element_type=f32)
    mlp_full = (
        lax.all_gather(mlp_gain, "shard", axis=0, tiled=True),
        lax.all_gather(gate_weight, "shard", axis=0, tiled=True),
        lax.all_gather(up_weight, "shard", axis=0, tiled=True),
        lax.all_gather(down_weight, "shard", axis=0, tiled=True),
    )
    gain_full_two, gate_full, up_full, down_full = mlp_full
    gain_two = gain_full_two.astype(f32)
    inv_two = lax.rsqrt(jnp.mean(hidden_res * hidden_res, axis=-1, keepdims=True) + NORM_EPS)
    normed_two = (hidden_res * inv_two * gain_two).astype(bf16)
    gate_pre = jnp.dot(normed_two, gate_full, preferred_element_type=f32)
    up_pre = jnp.dot(normed_two, up_full, preferred_element_type=f32)
    sigmoid_gate = jax.nn.sigmoid(gate_pre)
    silu_gate = gate_pre * sigmoid_gate
    activation = (silu_gate * up_pre).astype(bf16)
    block_output = (hidden_res + jnp.dot(activation, down_full, preferred_element_type=f32)).astype(
        bf16
    )
    act_grad = jnp.einsum("td,fd->tf", cotangent, down_full, preferred_element_type=f32)
    gate_delta = (
        act_grad * up_pre * sigmoid_gate * (1.0 + gate_pre * (1.0 - sigmoid_gate))
    ).astype(bf16)
    up_delta = (act_grad * silu_gate).astype(bf16)
    normed_two_grad = jnp.einsum(
        "tf,df->td", gate_delta, gate_full, preferred_element_type=f32
    ) + jnp.einsum("tf,df->td", up_delta, up_full, preferred_element_type=f32)
    gain_two_grad = jnp.sum(normed_two_grad * hidden_res * inv_two, axis=0) * grad_scale
    own_rows = (
        lax.all_to_all(activation, "shard", split_axis=1, concat_axis=0, tiled=True),
        lax.all_to_all(normed_two, "shard", split_axis=1, concat_axis=0, tiled=True),
    )
    group_act, group_normed = own_rows
    group_rows = (
        lax.all_gather(cotangent, "shard", axis=0, tiled=True),
        lax.all_gather(gate_delta, "shard", axis=0, tiled=True),
        lax.all_gather(up_delta, "shard", axis=0, tiled=True),
    )
    group_cot, group_gate, group_up = group_rows
    down_part = (
        jnp.einsum("tf,td->fd", group_act, group_cot, preferred_element_type=f32) * grad_scale
    )
    gate_own = (
        jnp.einsum("td,tf->df", group_normed, group_gate, preferred_element_type=f32) * grad_scale
    )
    up_own = (
        jnp.einsum("td,tf->df", group_normed, group_up, preferred_element_type=f32) * grad_scale
    )
    gain_two_own = lax.psum_scatter(gain_two_grad, "shard", scatter_dimension=0, tiled=True)
    mlp_parts = (gain_two_own, gate_own, up_own)
    hidden_grad = cotangent.astype(f32) + inv_two * (
        gain_two * normed_two_grad
        - hidden_res
        * inv_two
        * inv_two
        * jnp.mean(gain_two * normed_two_grad * hidden_res, axis=-1, keepdims=True)
    )
    hidden_low = hidden_grad.astype(bf16)
    context_grad = jnp.einsum("td,ed->te", hidden_low, out_full, preferred_element_type=f32).astype(
        bf16
    )
    query_grad, key_grad, value_grad = attend_backward(
        queries, key_rot, values, logsum, context_grad
    )
    query_grad = unrotate(query_grad, cosine, sine_table).reshape(tok_count, q_width)
    key_grad = unrotate(key_grad, cosine, sine_table).reshape(tok_count, KV * HD)
    projected_grad = jnp.concatenate(
        [query_grad, key_grad, value_grad.reshape(tok_count, KV * HD)], axis=-1
    ).astype(bf16)
    normed_one_grad = jnp.einsum("tc,dc->td", projected_grad, qkv_full, preferred_element_type=f32)
    gain_one_grad = jnp.sum(normed_one_grad * xfloat * inv_one, axis=0) * grad_scale
    bias_grad = jnp.sum(projected_grad.astype(f32), axis=0) * grad_scale
    own_attn = (
        lax.all_to_all(context, "shard", split_axis=1, concat_axis=0, tiled=True),
        lax.all_to_all(normed_one, "shard", split_axis=1, concat_axis=0, tiled=True),
    )
    group_context, group_normed_one = own_attn
    group_rows = (
        lax.all_gather(hidden_low, "shard", axis=0, tiled=True),
        lax.all_gather(projected_grad, "shard", axis=0, tiled=True),
    )
    group_hidden, group_projected = group_rows
    out_own = (
        jnp.einsum("te,td->ed", group_context, group_hidden, preferred_element_type=f32)
        * grad_scale
    )
    qkv_part = (
        jnp.einsum("td,tc->dc", group_normed_one, group_projected, preferred_element_type=f32)
        * grad_scale
    )
    small_parts = (
        lax.psum_scatter(gain_one_grad, "shard", scatter_dimension=0, tiled=True),
        lax.psum_scatter(bias_grad, "shard", scatter_dimension=0, tiled=True),
    )
    attn_parts = (small_parts[0], qkv_part, small_parts[1], out_own)
    input_grad = hidden_grad + inv_one * (
        gain_one * normed_one_grad
        - xfloat
        * inv_one
        * inv_one
        * jnp.mean(gain_one * normed_one_grad * xfloat, axis=-1, keepdims=True)
    )
    summed = lax.psum(
        (
            attn_parts[0],
            attn_parts[1],
            attn_parts[2],
            attn_parts[3],
            mlp_parts[0],
            mlp_parts[1],
            mlp_parts[2],
            down_part,
        ),
        "replica",
    )
    attn_parts = (summed[0], summed[1], summed[2], summed[3])
    mlp_parts = (summed[4], summed[5], summed[6])
    down_part = summed[7]
    return (
        block_output,
        input_grad,
        attn_parts[0],
        attn_parts[1],
        attn_parts[2],
        attn_parts[3],
        mlp_parts[0],
        mlp_parts[1],
        mlp_parts[2],
        down_part,
    )


MESH = pl.DeviceIdType.MESH
VMEM_BYTES = 62 * 2**20
WINDOW = 1152


def place():
    replica = lax.axis_index("replica")
    shard = lax.axis_index("shard")
    core = lax.rem(replica, 2)
    return replica, shard, core


def peer_of(shard, d):
    across = lax.rem(lax.rem(shard, 2) + d % 2, 2)
    up = lax.rem(shard // 2 + d // 2, 2)
    return up * 2 + across


def window_start(shard, core):
    return ((shard * 35) // 2 + core * 9) * 128


def remote(src, dst, send, recv, device):
    return pltpu.make_async_remote_copy(
        src_ref=src,
        dst_ref=dst,
        send_sem=send,
        recv_sem=recv,
        device_id=device,
        device_id_type=MESH,
    )


def front_kernel(
    wq, wo, wg, wu, cot, small, q_full, o_full, g_own, u_own, cot_all, small_all,
    bq, bo, bg, bu, bc, bs, send, recv, fsend, frecv, zsend, zrecv, local,
):
    replica, shard, core = place()
    other = 1 - core
    mate = (replica + 1 - 2 * core, shard)
    odd = lax.rem(replica // 2, 2)
    pair = (replica + 2 - 4 * odd, shard)

    def span(start, size):
        return pl.ds(pl.multiple_of(start, 16), size)

    def cols(target):
        return pl.ds(pl.multiple_of(window_start(target, core), 128), WINDOW)

    def block(owner, c):
        return pl.ds(pl.multiple_of((c * 4 + owner) * 128, 128), 128)

    def rows(owner):
        return pl.ds(pl.multiple_of(owner * 384, 384), 384)

    loads = [
        (wq, bq, q_full.at[rows(shard)]),
        (wo, bo, o_full.at[rows(shard)]),
        (wg.at[:, cols(shard)], bg, g_own.at[rows(shard)]),
        (wu.at[:, cols(shard)], bu, u_own.at[rows(shard)]),
        (cot, bc, cot_all.at[block(shard, core)]),
        (small, bs, small_all.at[shard]),
    ]
    weights = [
        (lambda t: wq, q_full, 192, 80, True),
        (lambda t: wo, o_full, 192, 80, True),
        (lambda t: wg.at[:, cols(t)], g_own, 384, 176, False),
        (lambda t: wu.at[:, cols(t)], u_own, 384, 176, False),
    ]

    def base(i, c):
        return c * 192 if weights[i][4] else 0

    def hop(i, d, t, o):
        source, out, size, shared, _ = weights[i]
        first = base(i, core) + odd * shared
        n = i * 3 + d - 1
        return remote(
            source(t).at[span(first, size - shared)], out.at[span(o * 384 + first, size - shared)],
            send.at[n], recv.at[n], (replica, t),
        )

    def across(i, d, o, whose):
        _, out, size, shared, _ = weights[i]
        ref = out.at[span(o * 384 + base(i, core) + whose * (size - shared), shared)]
        n = i * 3 + d - 1
        return remote(ref, ref, zsend.at[n], zrecv.at[n], pair)

    def onward(i, d, o, c, shared_part):
        _, out, size, shared, _ = weights[i]
        first = o * 384 + base(i, c) + ((1 - odd) * (size - shared) if shared_part else odd * shared)
        ref = out.at[span(first, shared if shared_part else size - shared)]
        n = i * 3 + d - 1 + (6 if shared_part else 0)
        return remote(ref, ref, fsend.at[n], frecv.at[n], mate)

    def cot_hop(d, t, o):
        return remote(cot, cot_all.at[block(o, core)], send.at[11 + d], recv.at[11 + d], (replica, t))

    def cot_onward(d, o, c):
        ref = cot_all.at[block(o, c)] if d else cot
        return remote(ref, cot_all.at[block(o, c)], fsend.at[12 + d], frecv.at[12 + d], mate)

    def small_hop(d, t, o):
        return remote(small, small_all.at[o], send.at[14 + d], recv.at[14 + d], (replica, t))

    order = (3, 1, 2)
    for d in order:
        small_hop(d, peer_of(shard, d), shard).start()
    for i in range(4):
        if i == 2:
            for d in order:
                cot_hop(d, peer_of(shard, d), shard).start()
        for d in order:
            hop(i, d, peer_of(shard, d), shard).start()
    cot_onward(0, shard, core).start()
    for n, (src, buf, _) in enumerate(loads):
        pltpu.make_async_copy(src, buf, local.at[n]).start()
    for n, (src, buf, dst) in enumerate(loads):
        pltpu.make_async_copy(src, buf, local.at[n]).wait()
        pltpu.make_async_copy(buf, dst, local.at[n]).start()

    def take(i):
        for d in order:
            p = peer_of(shard, d)
            hop(i, d, p, p).wait_recv()
            across(i, d, p, odd).start()
            if weights[i][4]:
                onward(i, d, p, core, False).start()

    def take_shared(i):
        for d in order:
            p = peer_of(shard, d)
            across(i, d, p, 1 - odd).wait_recv()
            if weights[i][4]:
                onward(i, d, p, core, True).start()

    take(0)
    take(1)
    for d in order:
        p = peer_of(shard, d)
        cot_hop(d, p, p).wait_recv()
        cot_onward(d, p, core).start()
    take_shared(0)
    take_shared(1)
    take(2)
    take(3)
    take_shared(2)
    take_shared(3)
    for d in order:
        p = peer_of(shard, d)
        small_hop(d, p, p).wait_recv()
        small_hop(d, p, shard).wait_send()
        cot_hop(d, p, shard).wait_send()
        cot_onward(d, p, core).wait_send()
        cot_onward(d, p, other).wait_recv()
        for i in range(4):
            hop(i, d, p, shard).wait_send()
            across(i, d, p, odd).wait_send()
            if weights[i][4]:
                for part in (False, True):
                    onward(i, d, p, core, part).wait_send()
                    onward(i, d, p, other, part).wait_recv()
    cot_onward(0, shard, core).wait_send()
    cot_onward(0, shard, other).wait_recv()
    for n, (src, buf, dst) in enumerate(loads):
        pltpu.make_async_copy(buf, dst, local.at[n]).wait()


def any_spec():
    return pl.BlockSpec(memory_space=pl.ANY)


def vmem_spec():
    return pl.BlockSpec(memory_space=pltpu.VMEM)


def params(**more):
    return pltpu.CompilerParams(has_side_effects=True, vmem_limit_bytes=VMEM_BYTES, **more)


def front(wq, wo, wg, wu, cot, small):
    bf16 = jnp.bfloat16
    shapes = [(1536, 2048), (1536, 1536), (1536, WINDOW), (1536, WINDOW), (1024, 1536), (4, 16, 512)]
    bounce = [wq.shape, wo.shape, (384, WINDOW), (384, WINDOW), cot.shape, small.shape]
    return pl.pallas_call(
        front_kernel,
        out_shape=[jax.ShapeDtypeStruct(s, bf16) for s in shapes],
        in_specs=[any_spec()] * 6,
        out_specs=[any_spec()] * 6,
        scratch_shapes=[pltpu.VMEM(s, bf16) for s in bounce]
        + [
            pltpu.SemaphoreType.DMA((18,)),
            pltpu.SemaphoreType.DMA((18,)),
            pltpu.SemaphoreType.DMA((16,)),
            pltpu.SemaphoreType.DMA((16,)),
            pltpu.SemaphoreType.DMA((12,)),
            pltpu.SemaphoreType.DMA((12,)),
            pltpu.SemaphoreType.DMA((6,)),
        ],
        compiler_params=params(),
    )(wq, wo, wg, wu, cot, small)


def gather_kernel(x, out, send, recv, fsend, frecv, local):
    replica, shard, core = place()
    mate = (replica + 1 - 2 * core, shard)

    def block(owner, c):
        return out.at[pl.ds(pl.multiple_of((c * 4 + owner) * 128, 128), 128)]

    for d in (3, 1, 2):
        remote(x, block(shard, core), send.at[d], recv.at[d], (replica, peer_of(shard, d))).start()
    remote(x, block(shard, core), fsend.at[0], frecv.at[0], mate).start()
    own = pltpu.make_async_copy(x, block(shard, core), local)
    own.start()
    for d in (1, 2, 3):
        p = peer_of(shard, d)
        remote(x, block(p, core), send.at[d], recv.at[d], (replica, p)).wait_recv()
        remote(block(p, core), block(p, core), fsend.at[d], frecv.at[d], mate).start()
    own.wait()
    for d in (1, 2, 3):
        p = peer_of(shard, d)
        remote(x, block(shard, core), send.at[d], recv.at[d], (replica, p)).wait_send()
        remote(block(p, core), block(p, core), fsend.at[d], frecv.at[d], mate).wait_send()
        remote(x, block(p, 1 - core), fsend.at[d], frecv.at[d], mate).wait_recv()
    remote(x, block(shard, core), fsend.at[0], frecv.at[0], mate).wait_send()
    remote(x, block(shard, 1 - core), fsend.at[0], frecv.at[0], mate).wait_recv()


def plane_gather(x):
    return pl.pallas_call(
        gather_kernel,
        out_shape=jax.ShapeDtypeStruct((x.shape[0] * 8, x.shape[1]), x.dtype),
        in_specs=[vmem_spec()],
        out_specs=vmem_spec(),
        scratch_shapes=[pltpu.SemaphoreType.DMA((4,))] * 4 + [pltpu.SemaphoreType.DMA],
        compiler_params=params(),
    )(x)


def scatter_kernel(pa, pb, oa, ob, held, sums, parts, csend, crecv, send, recv):
    replica, shard, core = place()
    mate = (replica + 1 - 2 * core, shard)
    f32 = jnp.float32
    inputs = (pa, pb)
    outputs = (oa, ob)

    def block(c, target):
        return pl.ds(pl.multiple_of((c * 4 + target) * 128, 128), 128)

    order = (3, 1, 2, 0)
    for a in range(2):
        for d in order:
            t = peer_of(shard, d)
            remote(inputs[a].at[block(1 - core, t)], held.at[a, d], csend.at[a * 4 + d], crecv.at[a * 4 + d], mate).start()

    def summed(a, d):
        t = peer_of(shard, d)
        n = a * 4 + d
        remote(inputs[a].at[block(core, t)], held.at[a, d], csend.at[n], crecv.at[n], mate).wait_recv()
        return inputs[a][block(core, t), :].astype(f32) + held[a, d].astype(f32)

    for a in range(2):
        for d in (3, 1, 2):
            sums[a, d - 1] = summed(a, d).astype(sums.dtype)
            n = a * 3 + d - 1
            remote(sums.at[a, d - 1], parts.at[a, d - 1], send.at[n], recv.at[n], (replica, peer_of(shard, d))).start()
    for a in range(2):
        outputs[a][...] = summed(a, 0)
    for a in range(2):
        for d in (1, 2, 3):
            n = a * 3 + d - 1
            remote(sums.at[a, d - 1], parts.at[a, d - 1], send.at[n], recv.at[n], (replica, peer_of(shard, d))).wait()
            outputs[a][...] += parts[a, d - 1].astype(f32)
    for a in range(2):
        for d in order:
            t = peer_of(shard, d)
            n = a * 4 + d
            remote(inputs[a].at[block(1 - core, t)], held.at[a, d], csend.at[n], crecv.at[n], mate).wait_send()


def plane_scatter(pa, pb):
    width = pa.shape[1]
    bf16 = jnp.bfloat16
    out = jax.ShapeDtypeStruct((128, width), jnp.float32)
    return pl.pallas_call(
        scatter_kernel,
        out_shape=[out, out],
        in_specs=[vmem_spec()] * 2,
        out_specs=[vmem_spec()] * 2,
        scratch_shapes=[
            pltpu.VMEM((2, 4, 128, width), bf16),
            pltpu.VMEM((2, 3, 128, width), bf16),
            pltpu.VMEM((2, 3, 128, width), bf16),
            pltpu.SemaphoreType.DMA((8,)),
            pltpu.SemaphoreType.DMA((8,)),
            pltpu.SemaphoreType.DMA((6,)),
            pltpu.SemaphoreType.DMA((6,)),
        ],
        compiler_params=params(),
    )(pa, pb)


def attn_gather_kernel(ctx, nrm, hid, prj, ctx_all, nrm_all, hid_all, prj_all, send, recv, fsend, frecv, local):
    replica, shard, core = place()
    other = 1 - core
    mate = (replica + 1 - 2 * core, shard)

    def block(out, owner, c):
        return out.at[pl.ds(pl.multiple_of((c * 4 + owner) * 128, 128), 128)]

    def part(ref, index, width):
        return ref.at[:, pl.ds(pl.multiple_of(index * width, width), width)]

    def device(c, t):
        return (replica - core + c, t)

    wide = ((hid, hid_all, 768), (prj, prj_all, 1024))
    narrow = ((ctx, ctx_all, 384), (nrm, nrm_all, 384))
    def wide_copy(a, d, same, source_core, owner, t):
        ref, out, width = wide[a]
        c = core if same else other
        n = (a * 4 + d) * 2 + (0 if same else 1)
        return remote(part(ref, c, width), block(out, owner, source_core), send.at[n], recv.at[n], device(c, t))

    def narrow_copy(a, d, owner, t):
        ref, out, width = narrow[a]
        n = 16 + a * 4 + d
        return remote(part(ref, t, width), block(out, owner, core), send.at[n], recv.at[n], (replica, t))

    def onward(a, d, source, owner, c):
        _, out, _ = narrow[a]
        n = a * 4 + d
        return remote(source, block(out, owner, c), fsend.at[n], frecv.at[n], mate)

    for d in (3, 1, 2, 0):
        t = peer_of(shard, d)
        for a in range(2):
            if d:
                wide_copy(a, d, True, core, shard, t).start()
            wide_copy(a, d, False, core, shard, t).start()
            if d:
                narrow_copy(a, d, shard, t).start()
            else:
                ref, out, width = narrow[a]
                onward(a, 0, part(ref, shard, width), shard, core).start()
    locals_ = []
    for a in range(2):
        ref, out, width = narrow[a]
        locals_.append(pltpu.make_async_copy(part(ref, shard, width), block(out, shard, core), local.at[a]))
        ref, out, width = wide[a]
        locals_.append(pltpu.make_async_copy(part(ref, core, width), block(out, shard, core), local.at[2 + a]))
    for copy in locals_:
        copy.start()
    for d in (1, 2, 3):
        p = peer_of(shard, d)
        for a in range(2):
            narrow_copy(a, d, p, p).wait_recv()
            onward(a, d, block(narrow[a][1], p, core), p, core).start()
    for copy in locals_:
        copy.wait()
    for d in (0, 1, 2, 3):
        p = peer_of(shard, d)
        for a in range(2):
            if d:
                wide_copy(a, d, True, core, p, p).wait_recv()
                wide_copy(a, d, True, core, shard, p).wait_send()
                narrow_copy(a, d, shard, p).wait_send()
            wide_copy(a, d, False, other, p, p).wait_recv()
            wide_copy(a, d, False, core, shard, p).wait_send()
            onward(a, d, block(narrow[a][1], p, core), p, core).wait_send()
            onward(a, d, block(narrow[a][1], p, other), p, other).wait_recv()


def attn_gather(ctx, nrm, hid, prj):
    bf16 = jnp.bfloat16
    shapes = [(1024, 384), (1024, 384), (1024, 768), (1024, 1024)]
    return pl.pallas_call(
        attn_gather_kernel,
        out_shape=[jax.ShapeDtypeStruct(s, bf16) for s in shapes],
        in_specs=[vmem_spec()] * 4,
        out_specs=[vmem_spec()] * 4,
        scratch_shapes=[
            pltpu.SemaphoreType.DMA((24,)),
            pltpu.SemaphoreType.DMA((24,)),
            pltpu.SemaphoreType.DMA((8,)),
            pltpu.SemaphoreType.DMA((8,)),
            pltpu.SemaphoreType.DMA((4,)),
        ],
        compiler_params=params(),
    )(ctx, nrm, hid, prj)


CHUNK = 128


def reduce_kernel(
    levels, pa, pd, pg, pu, fa, fd, fg, fu,
    own_a, own_d, own_g, low_a, low_d, low_g, high_a, high_d, high_g,
    xsend, xrecv, up_sem, down_sem, low_sem, high_sem, mate_send, mate_recv, out_sem, in_sem,
):
    replica, shard, core = place()
    level = replica // 2
    mate = (replica + 1 - 2 * core, shard)
    above, below = (replica + 2, shard), (replica - 2, shard)
    f32 = jnp.float32
    sources = (pg, pu)

    def exchange(a, d, p):
        rows = pl.ds(pl.multiple_of(p * 384, 384), 384)
        n = a * 4 + d
        return remote(sources[a].at[rows], own_g.at[pl.ds(a * 1536 + d * 384, 384)], xsend.at[n], xrecv.at[n], (replica, p))

    fills = [
        pltpu.make_async_copy(pa, own_a, in_sem.at[0]),
        pltpu.make_async_copy(pd, own_d, in_sem.at[1]),
    ]
    for a in range(2):
        rows = pl.ds(pl.multiple_of(shard * 384, 384), 384)
        fills.append(pltpu.make_async_copy(sources[a].at[rows], own_g.at[pl.ds(a * 1536, 384)], in_sem.at[2 + a]))
    for copy in fills:
        copy.start()
    for a in range(2):
        for d in (1, 2, 3):
            exchange(a, d, peer_of(shard, d)).start()

    chunks = []
    for k in range(3):
        at = pl.ds(k * CHUNK, CHUNK)
        chunks.append((own_a, low_a, high_a, at, ("fill", 0), lambda c, at=at: fa.at[c, at]))
    for k in range(9):
        at = pl.ds(k * CHUNK, CHUNK)
        chunks.append((own_d, low_d, high_d, at, ("fill", 1), lambda c, at=at: fd.at[c, at]))
    for d in range(4):
        for a in range(2):
            for k in range(3):
                at = pl.ds(a * 1536 + d * 384 + k * CHUNK, CHUNK)
                dst = (fg, fu)[a]
                source = peer_of(shard, d)
                chunks.append((
                    own_g, low_g, high_g, at, ("fill", 2 + a) if d == 0 else ("x", a, d),
                    lambda c, k=k, dst=dst, source=source: dst.at[c, source, pl.ds(k * CHUNK, CHUNK)],
                ))
    total = len(chunks)
    awaited = (set(), set())
    end = (level == 0) | (level == levels - 1)

    def arrive(what, seen):
        if what in seen:
            return
        seen.add(what)
        if what[0] == "fill":
            fills[what[1]].wait()
        else:
            exchange(what[1], what[2], peer_of(shard, what[2])).wait_recv()

    def up(k, ref):
        own, low, high, at, _, _ = chunks[k]
        return remote(ref.at[at], low.at[at], up_sem.at[k], low_sem.at[k], above)

    def down(k, ref):
        own, low, high, at, _, _ = chunks[k]
        return remote(ref.at[at], high.at[at], down_sem.at[k], high_sem.at[k], below)

    def add(k, *refs):
        own, _, _, at, _, _ = chunks[k]
        step = 32

        def body(j, carry):
            rows = pl.ds(pl.multiple_of(at.start + j * step, step), step)
            value = own[rows, :].astype(f32)
            for ref in refs:
                value = value + ref[rows, :].astype(f32)
            own[rows, :] = value.astype(own.dtype)
            return carry

        lax.fori_loop(0, CHUNK // step, body, 0)

    def finish(k, ref):
        _, _, _, at, _, dst = chunks[k]
        pltpu.make_async_copy(ref.at[at], dst(core), out_sem.at[k]).start()
        remote(ref.at[at], dst(core), mate_send.at[k], mate_recv.at[k], mate).start()

    def root_of(k):
        return levels // 2 - 1 + k % 2

    def end_gather(k):
        own = chunks[k][0]

        @pl.when(end)
        def _():
            arrive(chunks[k][4], awaited[0])

        @pl.when(level == 0)
        def _():
            up(k, own).start()

        @pl.when(level == levels - 1)
        def _():
            down(k, own).start()

    def gather_step(k):
        own, low, high, at, what, _ = chunks[k]
        root = root_of(k)

        @pl.when(~end)
        def _():
            arrive(what, awaited[1])

        if root > 1:

            @pl.when((level > 0) & (level < root))
            def _():
                up(k, own).wait_recv()
                add(k, low)
                up(k, own).start()

        if root < levels - 2:

            @pl.when((level < levels - 1) & (level > root))
            def _():
                down(k, own).wait_recv()
                add(k, high)
                down(k, own).start()

    def root_step(k):
        own, low, high, at, _, _ = chunks[k]

        @pl.when(level == root_of(k))
        def _():
            up(k, own).wait_recv()
            down(k, own).wait_recv()
            add(k, low, high)
            up(k, own).start()
            down(k, own).start()
            finish(k, own)

    def spread_step(k):
        own, low, high, at, _, _ = chunks[k]
        root = root_of(k)

        if root > 1:

            @pl.when((level > 0) & (level < root))
            def _():
                down(k, own).wait_recv()
                down(k, high).start()
                finish(k, high)

        if root < levels - 2:

            @pl.when((level < levels - 1) & (level > root))
            def _():
                up(k, own).wait_recv()
                up(k, low).start()
                finish(k, low)

    def end_spread(k):
        own, low, high, at, _, _ = chunks[k]

        @pl.when(level == 0)
        def _():
            down(k, own).wait_recv()
            finish(k, high)

        @pl.when(level == levels - 1)
        def _():
            up(k, own).wait_recv()
            finish(k, low)

    stages = ((end_gather, 0), (gather_step, 4), (root_step, 7), (spread_step, 10), (end_spread, 14))
    for t in range(total + stages[-1][1]):
        for stage, lag in stages:
            if 0 <= t - lag < total:
                stage(t - lag)
    for a in range(2):
        for d in (1, 2, 3):
            exchange(a, d, peer_of(shard, d)).wait_send()
    for k in range(total):
        own, low, high, at, _, dst = chunks[k]

        @pl.when(level < levels - 1)
        def _():
            up(k, own).wait_send()

        @pl.when(level > 0)
        def _():
            down(k, own).wait_send()

        pltpu.make_async_copy(own.at[at], dst(core), out_sem.at[k]).wait()
        remote(own.at[at], dst(core), mate_send.at[k], mate_recv.at[k], mate).wait_send()
        remote(own.at[at], dst(1 - core), mate_send.at[k], mate_recv.at[k], mate).wait_recv()


def reduce_gradients(levels, pa, pd, pg, pu):
    bf16 = jnp.bfloat16
    shapes = [(2, 384, 1792), (2, WINDOW, 1536), (2, 4, 384, WINDOW), (2, 4, 384, WINDOW)]
    buffers = [(384, 1792), (WINDOW, 1536), (3072, WINDOW)]
    total = 36
    dma = pltpu.SemaphoreType.DMA
    return pl.pallas_call(
        functools.partial(reduce_kernel, levels),
        out_shape=[jax.ShapeDtypeStruct(s, bf16) for s in shapes],
        in_specs=[any_spec()] * 4,
        out_specs=[any_spec()] * 4,
        scratch_shapes=[pltpu.VMEM(s, bf16) for s in buffers * 3]
        + [dma((8,)), dma((8,))]
        + [dma((total,))] * 7
        + [dma((4,))],
        compiler_params=params(),
    )(pa, pd, pg, pu)


def widen_kernel(x, out):
    f32 = jnp.float32
    for s in range(4):
        for c in range(2):
            first = (s * 35) // 2 + c * 9
            joined = s % 2 == 1 and c == 0
            rest = 1 if joined else 0
            out[:, (first + rest) * 128 : (first + 9) * 128] = x[c, s][:, rest * 128 :].astype(f32)
    for s in (1, 3):
        first = (s * 35) // 2
        out[:, first * 128 : (first + 1) * 128] = x[1, s - 1][:, 1024:].astype(f32) + x[0, s][:, :128].astype(f32)


def widen(x):
    rows = 32
    return pl.pallas_call(
        widen_kernel,
        grid=(384 // rows,),
        out_shape=jax.ShapeDtypeStruct((384, 8960), jnp.float32),
        in_specs=[pl.BlockSpec((2, 4, rows, WINDOW), lambda i: (0, 0, i, 0))],
        out_specs=pl.BlockSpec((rows, 8960), lambda i: (i, 0)),
    )(x)


def fast_device(
    block_input,
    attn_gain,
    qkv_weight,
    qkv_bias,
    out_weight,
    mlp_gain,
    gate_weight,
    up_weight,
    down_weight,
    cotangent,
):
    f32 = jnp.float32
    bf16 = jnp.bfloat16
    tok_count = block_input.shape[0]
    levels = lax.axis_size("replica") // 2
    grad_scale = 1.0 / math.sqrt(tok_count * lax.axis_size("replica") * lax.axis_size("shard"))
    q_width = HEADS * HD
    k_end = q_width + KV * HD
    replica, shard, core = place()
    cosine, sine_table = rope_tables(tok_count)
    small = jnp.zeros((16, 512), bf16)
    small = small.at[0, :384].set(attn_gain).at[1, :].set(qkv_bias).at[2, :384].set(mlp_gain)
    qkv_full, out_full, gate_own, up_own, cot_all, small_all = front(
        qkv_weight, out_weight, gate_weight, up_weight, cotangent, small
    )
    gain_one = small_all[:, 0, :384].reshape(-1).astype(f32)
    bias = small_all[:, 1, :].reshape(-1).astype(f32)
    gain_two = small_all[:, 2, :384].reshape(-1).astype(f32)

    xfloat = block_input.astype(f32)
    inv_one = lax.rsqrt(jnp.mean(xfloat * xfloat, axis=-1, keepdims=True) + NORM_EPS)
    normed_one = (xfloat * inv_one * gain_one).astype(bf16)
    projected = jnp.dot(normed_one, qkv_full, preferred_element_type=f32) + bias
    queries = rotate(projected[:, :q_width].reshape(tok_count, HEADS, HD), cosine, sine_table).astype(bf16)
    queries = queries.reshape(tok_count, KV, HEADS // KV, HD)
    key_rot = rotate(projected[:, q_width:k_end].reshape(tok_count, KV, HD), cosine, sine_table).astype(bf16)
    values = projected[:, k_end:].reshape(tok_count, KV, HD).astype(bf16)
    context, logsum = attend_forward(queries, key_rot, values)
    hidden_res = xfloat + jnp.dot(context, out_full, preferred_element_type=f32)
    inv_two = lax.rsqrt(jnp.mean(hidden_res * hidden_res, axis=-1, keepdims=True) + NORM_EPS)
    normed_two = (hidden_res * inv_two * gain_two).astype(bf16)

    normed_all = plane_gather(normed_two)
    first = window_start(shard, core)
    column = first + jnp.arange(WINDOW)
    owned = (column >= shard * 2240) & (column < (shard + 1) * 2240)
    padded = jnp.pad(down_weight, ((64, 64), (0, 0)))
    down_own = lax.dynamic_slice_in_dim(padded, first - shard * 2240 + 64, WINDOW, 0)
    gate_pre = jnp.dot(normed_all, gate_own, preferred_element_type=f32)
    up_pre = jnp.dot(normed_all, up_own, preferred_element_type=f32)
    sigmoid_gate = jax.nn.sigmoid(gate_pre)
    silu_gate = gate_pre * sigmoid_gate
    act_grad = jnp.einsum("td,fd->tf", cot_all, down_own, preferred_element_type=f32)
    activation = jnp.where(owned, silu_gate * up_pre, 0.0).astype(bf16)
    gate_delta = jnp.where(
        owned, act_grad * up_pre * sigmoid_gate * (1.0 + gate_pre * (1.0 - sigmoid_gate)), 0.0
    ).astype(bf16)
    up_delta = jnp.where(owned, act_grad * silu_gate, 0.0).astype(bf16)
    down_out = jnp.dot(activation, down_own, preferred_element_type=f32).astype(bf16)
    back = (
        jnp.einsum("tf,df->td", gate_delta, gate_own, preferred_element_type=f32)
        + jnp.einsum("tf,df->td", up_delta, up_own, preferred_element_type=f32)
    ).astype(bf16)
    gate_part = (jnp.einsum("td,tf->df", normed_all, gate_delta, preferred_element_type=f32) * grad_scale).astype(bf16)
    up_part = (jnp.einsum("td,tf->df", normed_all, up_delta, preferred_element_type=f32) * grad_scale).astype(bf16)
    down_part = (jnp.einsum("tf,td->fd", activation, cot_all, preferred_element_type=f32) * grad_scale).astype(bf16)

    down_sum, normed_two_grad = plane_scatter(down_out, back)
    block_output = (hidden_res + down_sum).astype(bf16)
    gain_two_grad = jnp.sum(normed_two_grad * hidden_res * inv_two, axis=0) * grad_scale
    hidden_grad = cotangent.astype(f32) + inv_two * (
        gain_two * normed_two_grad
        - hidden_res
        * inv_two
        * inv_two
        * jnp.mean(gain_two * normed_two_grad * hidden_res, axis=-1, keepdims=True)
    )
    hidden_low = hidden_grad.astype(bf16)
    context_grad = jnp.einsum("td,ed->te", hidden_low, out_full, preferred_element_type=f32).astype(bf16)
    query_grad, key_grad, value_grad = attend_backward(queries, key_rot, values, logsum, context_grad)
    query_grad = unrotate(query_grad, cosine, sine_table).reshape(tok_count, q_width)
    key_grad = unrotate(key_grad, cosine, sine_table).reshape(tok_count, KV * HD)
    projected_grad = jnp.concatenate(
        [query_grad, key_grad, value_grad.reshape(tok_count, KV * HD)], axis=-1
    ).astype(bf16)
    normed_one_grad = jnp.einsum("tc,dc->td", projected_grad, qkv_full, preferred_element_type=f32)
    gain_one_grad = jnp.sum(normed_one_grad * xfloat * inv_one, axis=0) * grad_scale
    bias_grad = jnp.sum(projected_grad.astype(f32), axis=0) * grad_scale
    input_grad = hidden_grad + inv_one * (
        gain_one * normed_one_grad
        - xfloat
        * inv_one
        * inv_one
        * jnp.mean(gain_one * normed_one_grad * xfloat, axis=-1, keepdims=True)
    )
    vectors = lax.psum(jnp.concatenate([gain_one_grad, bias_grad, gain_two_grad]), ("replica", "shard"))
    gain_one_own = lax.dynamic_slice_in_dim(vectors, shard * 384, 384)
    bias_own = lax.dynamic_slice_in_dim(vectors, 1536 + shard * 512, 512)
    gain_two_own = lax.dynamic_slice_in_dim(vectors, 3584 + shard * 384, 384)

    ctx_rows, normed_rows, hidden_rows, projected_rows = attn_gather(context, normed_one, hidden_low, projected_grad)
    qkv_part = jnp.einsum("td,tc->dc", normed_rows, projected_rows, preferred_element_type=f32)
    out_part = jnp.einsum("te,td->ed", ctx_rows, hidden_rows, preferred_element_type=f32)
    attn_part = (jnp.concatenate([qkv_part, out_part], axis=1) * grad_scale).astype(bf16)

    sum_attn, sum_down, sum_gate, sum_up = reduce_gradients(levels, attn_part, down_part, gate_part, up_part)
    qkv_grad = jnp.concatenate([sum_attn[0, :, :1024], sum_attn[1, :, :1024]], axis=1).astype(f32)
    out_grad = jnp.concatenate([sum_attn[0, :, 1024:], sum_attn[1, :, 1024:]], axis=1).astype(f32)
    down_grad = lax.dynamic_slice_in_dim(
        sum_down.reshape(2 * WINDOW, 1536), lax.rem(shard, 2) * 64, 2240, 0
    ).astype(f32)
    return (
        block_output,
        input_grad,
        gain_one_own,
        qkv_grad,
        bias_own,
        out_grad,
        gain_two_own,
        widen(sum_gate),
        widen(sum_up),
        down_grad,
    )


def solution(mesh):
    placed = (
        P(("replica", "shard"), None),
        P("shard"),
        P("shard", None),
        P("shard"),
        P("shard", None),
        P("shard"),
        P("shard", None),
        P("shard", None),
        P("shard", None),
        P(("replica", "shard"), None),
    )
    fits = mesh.shape["shard"] == 4 and mesh.shape["replica"] % 4 == 0
    per_device = fast_device if fits else general_device
    return jax.shard_map(
        per_device,
        mesh=mesh,
        in_specs=placed,
        out_specs=(
            P(("replica", "shard"), None),
            P(("replica", "shard"), None),
            P("shard"),
            P("shard", None),
            P("shard"),
            P("shard", None),
            P("shard"),
            P("shard", None),
            P("shard", None),
            P("shard", None),
        ),
        check_vma=False,
    )
```

```python
import functools
import math

import jax
import jax.numpy as jnp
from jax import lax
from jax.experimental import pallas as pl
from jax.experimental.pallas import tpu as pltpu
from jax.sharding import PartitionSpec as P

HEADS = 12
KV = 2
HD = 128


NORM_EPS = 1e-06
ROPE_BASE = 1000000.0


def rope_tables(tok_count):
    half_dim = HD // 2
    position = jnp.arange(tok_count, dtype=jnp.float32)
    inverse = ROPE_BASE ** (-(jnp.arange(half_dim, dtype=jnp.float32) * 2.0 / HD))
    angles = position[:, None] * inverse[None, :]
    return (jnp.cos(angles)[:, None, :], jnp.sin(angles)[:, None, :])


def rotate(vectors, cosine, sine_table):
    half_dim = HD // 2
    lower_half = vectors[..., :half_dim]
    upper_half = vectors[..., half_dim:]
    return jnp.concatenate(
        [
            lower_half * cosine - upper_half * sine_table,
            upper_half * cosine + lower_half * sine_table,
        ],
        axis=-1,
    )


def unrotate(grads, cosine, sine_table):
    half_dim = HD // 2
    lower_half = grads[..., :half_dim]
    upper_half = grads[..., half_dim:]
    return jnp.concatenate(
        [
            lower_half * cosine + upper_half * sine_table,
            upper_half * cosine - lower_half * sine_table,
        ],
        axis=-1,
    )


def block_scores(query_block, key_rot, first_row):
    row_count = query_block.shape[0]
    scores = jnp.einsum(
        "qkgd,skd->kgqs", query_block, key_rot, preferred_element_type=jnp.float32
    ) * (1.0 / math.sqrt(HD))
    causal = (first_row + jnp.arange(row_count))[:, None] >= jnp.arange(key_rot.shape[0])[None, :]
    return jnp.where(causal, scores, -1e30)


def block_layout(tok_count):
    block_rows = min(tok_count, 512)
    block_count = tok_count // block_rows
    firsts = jnp.arange(block_count, dtype=jnp.int32) * block_rows
    return (block_rows, block_count, firsts)


def attend_forward(queries, key_rot, values):
    tok_count = queries.shape[0]
    block_rows, block_count, firsts = block_layout(tok_count)
    query_blocks = queries.reshape(block_count, block_rows, KV, HEADS // KV, HD)

    def one_block(inputs):
        query_block, first_row = inputs
        scores = block_scores(query_block, key_rot, first_row)
        row_max = jnp.max(scores, axis=-1, keepdims=True)
        logsum = row_max + jnp.log(jnp.sum(jnp.exp(scores - row_max), axis=-1, keepdims=True))
        attn_probs = jnp.exp(scores - logsum).astype(jnp.bfloat16)
        context = jnp.einsum(
            "kgqs,skd->qkgd", attn_probs, values, preferred_element_type=jnp.float32
        ).astype(jnp.bfloat16)
        return (context, logsum)

    context, logsum = lax.map(one_block, (query_blocks, firsts))
    return (context.reshape(tok_count, HEADS * HD), logsum)


def attend_backward(queries, key_rot, values, logsum, context_grad):
    tok_count = queries.shape[0]
    block_rows, block_count, firsts = block_layout(tok_count)
    query_blocks = queries.reshape(block_count, block_rows, KV, HEADS // KV, HD)
    grad_blocks = context_grad.reshape(block_count, block_rows, KV, HEADS // KV, HD)
    score_scale = 1.0 / math.sqrt(HD)

    def one_block(running, inputs):
        key_total, value_total = running
        query_block, grad_block, log_block, first_row = inputs
        scores = block_scores(query_block, key_rot, first_row)
        attn_probs = jnp.exp(scores - log_block).astype(jnp.bfloat16)
        prob_grad = jnp.einsum(
            "qkgd,skd->kgqs", grad_block, values, preferred_element_type=jnp.float32
        )
        wide_probs = attn_probs.astype(jnp.float32)
        row_delta = jnp.sum(wide_probs * prob_grad, axis=-1, keepdims=True)
        score_grad = (wide_probs * (prob_grad - row_delta) * score_scale).astype(jnp.bfloat16)
        query_grad = jnp.einsum(
            "kgqs,skd->qkgd", score_grad, key_rot, preferred_element_type=jnp.float32
        )
        key_total = key_total + jnp.einsum(
            "kgqs,qkgd->skd", score_grad, query_block, preferred_element_type=jnp.float32
        )
        value_total = value_total + jnp.einsum(
            "kgqs,qkgd->skd", attn_probs, grad_block, preferred_element_type=jnp.float32
        )
        return ((key_total, value_total), query_grad)

    zero_keys = jnp.zeros((tok_count, KV, HD), jnp.float32)
    (key_grad, value_grad), query_grad = lax.scan(
        one_block, (zero_keys, zero_keys), (query_blocks, grad_blocks, logsum, firsts)
    )
    return (query_grad.reshape(tok_count, HEADS, HD), key_grad, value_grad)


def general_device(
    block_input,
    attn_gain,
    qkv_weight,
    qkv_bias,
    out_weight,
    mlp_gain,
    gate_weight,
    up_weight,
    down_weight,
    cotangent,
):
    f32 = jnp.float32
    bf16 = jnp.bfloat16
    tok_count = block_input.shape[0]
    grad_scale = 1.0 / math.sqrt(tok_count * lax.axis_size("replica") * lax.axis_size("shard"))
    q_width = HEADS * HD
    k_end = q_width + KV * HD
    cosine, sine_table = rope_tables(tok_count)
    attn_full = (
        lax.all_gather(attn_gain, "shard", axis=0, tiled=True),
        lax.all_gather(qkv_weight, "shard", axis=0, tiled=True),
        lax.all_gather(qkv_bias, "shard", axis=0, tiled=True),
        lax.all_gather(out_weight, "shard", axis=0, tiled=True),
    )
    gain_full, qkv_full, bias_full, out_full = attn_full
    gain_one = gain_full.astype(f32)
    xfloat = block_input.astype(f32)
    inv_one = lax.rsqrt(jnp.mean(xfloat * xfloat, axis=-1, keepdims=True) + NORM_EPS)
    normed_one = (xfloat * inv_one * gain_one).astype(bf16)
    projected = jnp.dot(normed_one, qkv_full, preferred_element_type=f32) + bias_full.astype(f32)
    queries = rotate(
        projected[:, :q_width].reshape(tok_count, HEADS, HD), cosine, sine_table
    ).astype(bf16)
    queries = queries.reshape(tok_count, KV, HEADS // KV, HD)
    key_rot = rotate(
        projected[:, q_width:k_end].reshape(tok_count, KV, HD), cosine, sine_table
    ).astype(bf16)
    values = projected[:, k_end:].reshape(tok_count, KV, HD).astype(bf16)
    context, logsum = attend_forward(queries, key_rot, values)
    hidden_res = xfloat + jnp.dot(context, out_full, preferred_element_type=f32)
    mlp_full = (
        lax.all_gather(mlp_gain, "shard", axis=0, tiled=True),
        lax.all_gather(gate_weight, "shard", axis=0, tiled=True),
        lax.all_gather(up_weight, "shard", axis=0, tiled=True),
        lax.all_gather(down_weight, "shard", axis=0, tiled=True),
    )
    gain_full_two, gate_full, up_full, down_full = mlp_full
    gain_two = gain_full_two.astype(f32)
    inv_two = lax.rsqrt(jnp.mean(hidden_res * hidden_res, axis=-1, keepdims=True) + NORM_EPS)
    normed_two = (hidden_res * inv_two * gain_two).astype(bf16)
    gate_pre = jnp.dot(normed_two, gate_full, preferred_element_type=f32)
    up_pre = jnp.dot(normed_two, up_full, preferred_element_type=f32)
    sigmoid_gate = jax.nn.sigmoid(gate_pre)
    silu_gate = gate_pre * sigmoid_gate
    activation = (silu_gate * up_pre).astype(bf16)
    block_output = (hidden_res + jnp.dot(activation, down_full, preferred_element_type=f32)).astype(
        bf16
    )
    act_grad = jnp.einsum("td,fd->tf", cotangent, down_full, preferred_element_type=f32)
    gate_delta = (
        act_grad * up_pre * sigmoid_gate * (1.0 + gate_pre * (1.0 - sigmoid_gate))
    ).astype(bf16)
    up_delta = (act_grad * silu_gate).astype(bf16)
    normed_two_grad = jnp.einsum(
        "tf,df->td", gate_delta, gate_full, preferred_element_type=f32
    ) + jnp.einsum("tf,df->td", up_delta, up_full, preferred_element_type=f32)
    gain_two_grad = jnp.sum(normed_two_grad * hidden_res * inv_two, axis=0) * grad_scale
    own_rows = (
        lax.all_to_all(activation, "shard", split_axis=1, concat_axis=0, tiled=True),
        lax.all_to_all(normed_two, "shard", split_axis=1, concat_axis=0, tiled=True),
    )
    group_act, group_normed = own_rows
    group_rows = (
        lax.all_gather(cotangent, "shard", axis=0, tiled=True),
        lax.all_gather(gate_delta, "shard", axis=0, tiled=True),
        lax.all_gather(up_delta, "shard", axis=0, tiled=True),
    )
    group_cot, group_gate, group_up = group_rows
    down_part = (
        jnp.einsum("tf,td->fd", group_act, group_cot, preferred_element_type=f32) * grad_scale
    )
    gate_own = (
        jnp.einsum("td,tf->df", group_normed, group_gate, preferred_element_type=f32) * grad_scale
    )
    up_own = (
        jnp.einsum("td,tf->df", group_normed, group_up, preferred_element_type=f32) * grad_scale
    )
    gain_two_own = lax.psum_scatter(gain_two_grad, "shard", scatter_dimension=0, tiled=True)
    mlp_parts = (gain_two_own, gate_own, up_own)
    hidden_grad = cotangent.astype(f32) + inv_two * (
        gain_two * normed_two_grad
        - hidden_res
        * inv_two
        * inv_two
        * jnp.mean(gain_two * normed_two_grad * hidden_res, axis=-1, keepdims=True)
    )
    hidden_low = hidden_grad.astype(bf16)
    context_grad = jnp.einsum("td,ed->te", hidden_low, out_full, preferred_element_type=f32).astype(
        bf16
    )
    query_grad, key_grad, value_grad = attend_backward(
        queries, key_rot, values, logsum, context_grad
    )
    query_grad = unrotate(query_grad, cosine, sine_table).reshape(tok_count, q_width)
    key_grad = unrotate(key_grad, cosine, sine_table).reshape(tok_count, KV * HD)
    projected_grad = jnp.concatenate(
        [query_grad, key_grad, value_grad.reshape(tok_count, KV * HD)], axis=-1
    ).astype(bf16)
    normed_one_grad = jnp.einsum("tc,dc->td", projected_grad, qkv_full, preferred_element_type=f32)
    gain_one_grad = jnp.sum(normed_one_grad * xfloat * inv_one, axis=0) * grad_scale
    bias_grad = jnp.sum(projected_grad.astype(f32), axis=0) * grad_scale
    own_attn = (
        lax.all_to_all(context, "shard", split_axis=1, concat_axis=0, tiled=True),
        lax.all_to_all(normed_one, "shard", split_axis=1, concat_axis=0, tiled=True),
    )
    group_context, group_normed_one = own_attn
    group_rows = (
        lax.all_gather(hidden_low, "shard", axis=0, tiled=True),
        lax.all_gather(projected_grad, "shard", axis=0, tiled=True),
    )
    group_hidden, group_projected = group_rows
    out_own = (
        jnp.einsum("te,td->ed", group_context, group_hidden, preferred_element_type=f32)
        * grad_scale
    )
    qkv_part = (
        jnp.einsum("td,tc->dc", group_normed_one, group_projected, preferred_element_type=f32)
        * grad_scale
    )
    small_parts = (
        lax.psum_scatter(gain_one_grad, "shard", scatter_dimension=0, tiled=True),
        lax.psum_scatter(bias_grad, "shard", scatter_dimension=0, tiled=True),
    )
    attn_parts = (small_parts[0], qkv_part, small_parts[1], out_own)
    input_grad = hidden_grad + inv_one * (
        gain_one * normed_one_grad
        - xfloat
        * inv_one
        * inv_one
        * jnp.mean(gain_one * normed_one_grad * xfloat, axis=-1, keepdims=True)
    )
    summed = lax.psum(
        (
            attn_parts[0],
            attn_parts[1],
            attn_parts[2],
            attn_parts[3],
            mlp_parts[0],
            mlp_parts[1],
            mlp_parts[2],
            down_part,
        ),
        "replica",
    )
    attn_parts = (summed[0], summed[1], summed[2], summed[3])
    mlp_parts = (summed[4], summed[5], summed[6])
    down_part = summed[7]
    return (
        block_output,
        input_grad,
        attn_parts[0],
        attn_parts[1],
        attn_parts[2],
        attn_parts[3],
        mlp_parts[0],
        mlp_parts[1],
        mlp_parts[2],
        down_part,
    )


MESH = pl.DeviceIdType.MESH
VMEM_BYTES = 62 * 2**20
WINDOW = 1152


def place():
    replica = lax.axis_index("replica")
    shard = lax.axis_index("shard")
    core = lax.rem(replica, 2)
    return replica, shard, core


def peer_of(shard, d):
    across = lax.rem(lax.rem(shard, 2) + d % 2, 2)
    up = lax.rem(shard // 2 + d // 2, 2)
    return up * 2 + across


def window_start(shard, core):
    return ((shard * 35) // 2 + core * 9) * 128


def remote(src, dst, send, recv, device):
    return pltpu.make_async_remote_copy(
        src_ref=src,
        dst_ref=dst,
        send_sem=send,
        recv_sem=recv,
        device_id=device,
        device_id_type=MESH,
    )


def front_kernel(
    wq, wo, wg, wu, cot, small, q_full, o_full, g_own, u_own, cot_all, small_all,
    bq, bo, bg, bu, bc, bs, send, recv, fsend, frecv, zsend, zrecv, local,
):
    replica, shard, core = place()
    other = 1 - core
    mate = (replica + 1 - 2 * core, shard)
    odd = lax.rem(replica // 2, 2)
    pair = (replica + 2 - 4 * odd, shard)

    def span(start, size):
        return pl.ds(pl.multiple_of(start, 16), size)

    def cols(target):
        return pl.ds(pl.multiple_of(window_start(target, core), 128), WINDOW)

    def block(owner, c):
        return pl.ds(pl.multiple_of((c * 4 + owner) * 128, 128), 128)

    def rows(owner):
        return pl.ds(pl.multiple_of(owner * 384, 384), 384)

    loads = [
        (wq, bq, q_full.at[rows(shard)]),
        (wo, bo, o_full.at[rows(shard)]),
        (wg.at[:, cols(shard)], bg, g_own.at[rows(shard)]),
        (wu.at[:, cols(shard)], bu, u_own.at[rows(shard)]),
        (cot, bc, cot_all.at[block(shard, core)]),
        (small, bs, small_all.at[shard]),
    ]
    weights = [
        (lambda t: wq, q_full, 192, 80, True),
        (lambda t: wo, o_full, 192, 80, True),
        (lambda t: wg.at[:, cols(t)], g_own, 384, 176, False),
        (lambda t: wu.at[:, cols(t)], u_own, 384, 176, False),
    ]

    def base(i, c):
        return c * 192 if weights[i][4] else 0

    def hop(i, d, t, o):
        source, out, size, shared, _ = weights[i]
        first = base(i, core) + odd * shared
        n = i * 3 + d - 1
        return remote(
            source(t).at[span(first, size - shared)], out.at[span(o * 384 + first, size - shared)],
            send.at[n], recv.at[n], (replica, t),
        )

    def across(i, d, o, whose):
        _, out, size, shared, _ = weights[i]
        ref = out.at[span(o * 384 + base(i, core) + whose * (size - shared), shared)]
        n = i * 3 + d - 1
        return remote(ref, ref, zsend.at[n], zrecv.at[n], pair)

    def onward(i, d, o, c, shared_part):
        _, out, size, shared, _ = weights[i]
        first = o * 384 + base(i, c) + ((1 - odd) * (size - shared) if shared_part else odd * shared)
        ref = out.at[span(first, shared if shared_part else size - shared)]
        n = i * 3 + d - 1 + (6 if shared_part else 0)
        return remote(ref, ref, fsend.at[n], frecv.at[n], mate)

    def cot_hop(d, t, o):
        return remote(cot, cot_all.at[block(o, core)], send.at[11 + d], recv.at[11 + d], (replica, t))

    def cot_onward(d, o, c):
        ref = cot_all.at[block(o, c)] if d else cot
        return remote(ref, cot_all.at[block(o, c)], fsend.at[12 + d], frecv.at[12 + d], mate)

    def small_hop(d, t, o):
        return remote(small, small_all.at[o], send.at[14 + d], recv.at[14 + d], (replica, t))

    order = (3, 1, 2)
    for d in order:
        small_hop(d, peer_of(shard, d), shard).start()
    for i in range(4):
        if i == 2:
            for d in order:
                cot_hop(d, peer_of(shard, d), shard).start()
        for d in order:
            hop(i, d, peer_of(shard, d), shard).start()
    cot_onward(0, shard, core).start()
    for n, (src, buf, _) in enumerate(loads):
        pltpu.make_async_copy(src, buf, local.at[n]).start()
    for n, (src, buf, dst) in enumerate(loads):
        pltpu.make_async_copy(src, buf, local.at[n]).wait()
        pltpu.make_async_copy(buf, dst, local.at[n]).start()

    def take(i):
        for d in order:
            p = peer_of(shard, d)
            hop(i, d, p, p).wait_recv()
            across(i, d, p, odd).start()
            if weights[i][4]:
                onward(i, d, p, core, False).start()

    def take_shared(i):
        for d in order:
            p = peer_of(shard, d)
            across(i, d, p, 1 - odd).wait_recv()
            if weights[i][4]:
                onward(i, d, p, core, True).start()

    take(0)
    take(1)
    for d in order:
        p = peer_of(shard, d)
        cot_hop(d, p, p).wait_recv()
        cot_onward(d, p, core).start()
    take_shared(0)
    take_shared(1)
    take(2)
    take(3)
    take_shared(2)
    take_shared(3)
    for d in order:
        p = peer_of(shard, d)
        small_hop(d, p, p).wait_recv()
        small_hop(d, p, shard).wait_send()
        cot_hop(d, p, shard).wait_send()
        cot_onward(d, p, core).wait_send()
        cot_onward(d, p, other).wait_recv()
        for i in range(4):
            hop(i, d, p, shard).wait_send()
            across(i, d, p, odd).wait_send()
            if weights[i][4]:
                for part in (False, True):
                    onward(i, d, p, core, part).wait_send()
                    onward(i, d, p, other, part).wait_recv()
    cot_onward(0, shard, core).wait_send()
    cot_onward(0, shard, other).wait_recv()
    for n, (src, buf, dst) in enumerate(loads):
        pltpu.make_async_copy(buf, dst, local.at[n]).wait()


def any_spec():
    return pl.BlockSpec(memory_space=pl.ANY)


def vmem_spec():
    return pl.BlockSpec(memory_space=pltpu.VMEM)


def params(**more):
    return pltpu.CompilerParams(has_side_effects=True, vmem_limit_bytes=VMEM_BYTES, **more)


def front(wq, wo, wg, wu, cot, small):
    bf16 = jnp.bfloat16
    shapes = [(1536, 2048), (1536, 1536), (1536, WINDOW), (1536, WINDOW), (1024, 1536), (4, 16, 512)]
    bounce = [wq.shape, wo.shape, (384, WINDOW), (384, WINDOW), cot.shape, small.shape]
    return pl.pallas_call(
        front_kernel,
        out_shape=[jax.ShapeDtypeStruct(s, bf16) for s in shapes],
        in_specs=[any_spec()] * 6,
        out_specs=[any_spec()] * 6,
        scratch_shapes=[pltpu.VMEM(s, bf16) for s in bounce]
        + [
            pltpu.SemaphoreType.DMA((18,)),
            pltpu.SemaphoreType.DMA((18,)),
            pltpu.SemaphoreType.DMA((16,)),
            pltpu.SemaphoreType.DMA((16,)),
            pltpu.SemaphoreType.DMA((12,)),
            pltpu.SemaphoreType.DMA((12,)),
            pltpu.SemaphoreType.DMA((6,)),
        ],
        compiler_params=params(),
    )(wq, wo, wg, wu, cot, small)


def gather_kernel(x, out, send, recv, fsend, frecv, local):
    replica, shard, core = place()
    mate = (replica + 1 - 2 * core, shard)

    def block(owner, c):
        return out.at[pl.ds(pl.multiple_of((c * 4 + owner) * 128, 128), 128)]

    for d in (3, 1, 2):
        remote(x, block(shard, core), send.at[d], recv.at[d], (replica, peer_of(shard, d))).start()
    remote(x, block(shard, core), fsend.at[0], frecv.at[0], mate).start()
    own = pltpu.make_async_copy(x, block(shard, core), local)
    own.start()
    for d in (1, 2, 3):
        p = peer_of(shard, d)
        remote(x, block(p, core), send.at[d], recv.at[d], (replica, p)).wait_recv()
        remote(block(p, core), block(p, core), fsend.at[d], frecv.at[d], mate).start()
    own.wait()
    for d in (1, 2, 3):
        p = peer_of(shard, d)
        remote(x, block(shard, core), send.at[d], recv.at[d], (replica, p)).wait_send()
        remote(block(p, core), block(p, core), fsend.at[d], frecv.at[d], mate).wait_send()
        remote(x, block(p, 1 - core), fsend.at[d], frecv.at[d], mate).wait_recv()
    remote(x, block(shard, core), fsend.at[0], frecv.at[0], mate).wait_send()
    remote(x, block(shard, 1 - core), fsend.at[0], frecv.at[0], mate).wait_recv()


def plane_gather(x):
    return pl.pallas_call(
        gather_kernel,
        out_shape=jax.ShapeDtypeStruct((x.shape[0] * 8, x.shape[1]), x.dtype),
        in_specs=[vmem_spec()],
        out_specs=vmem_spec(),
        scratch_shapes=[pltpu.SemaphoreType.DMA((4,))] * 4 + [pltpu.SemaphoreType.DMA],
        compiler_params=params(),
    )(x)


CHUNK = 128
SCORE_SCALE = 1.0 / math.sqrt(HD)


def dot_nt(a, b):
    return lax.dot_general(a, b, (((1,), (1,)), ((), ())), preferred_element_type=jnp.float32)


def dot_tn(a, b):
    return lax.dot_general(a, b, (((0,), (0,)), ((), ())), preferred_element_type=jnp.float32)


def row_loop(rows, step, body, init):
    return lax.fori_loop(0, rows // step, lambda j, c: body(pl.ds(pl.multiple_of(j * step, step), step), c), init)


def backward_kernel(levels, grad_scale, names, *refs):
    v = dict(zip(names, refs))
    replica, shard, core = place()
    other = 1 - core
    level = replica // 2
    mate = (replica + 1 - 2 * core, shard)
    above, below = (replica + 2, shard), (replica - 2, shard)
    f32 = jnp.float32
    bf16 = jnp.bfloat16
    order = (3, 1, 2)
    own_a, own_d, own_g = v["own_a"], v["own_d"], v["own_g"]
    sources = (v["pg"], v["pu"])

    def tokens(owner, c):
        return pl.ds(pl.multiple_of((c * 4 + owner) * 128, 128), 128)

    def exchange(a, d, p):
        rows = pl.ds(pl.multiple_of(p * 384, 384), 384)
        n = a * 4 + d
        return remote(
            sources[a].at[rows], own_g.at[pl.ds(a * 1536 + d * 384, 384)],
            v["xsend"].at[n], v["xrecv"].at[n], (replica, p),
        )

    fills = [
        None,
        pltpu.make_async_copy(v["pd"], own_d, v["in_sem"].at[1]),
    ]
    for a in range(2):
        rows = pl.ds(pl.multiple_of(shard * 384, 384), 384)
        fills.append(
            pltpu.make_async_copy(sources[a].at[rows], own_g.at[pl.ds(a * 1536, 384)], v["in_sem"].at[2 + a])
        )

    partial = (v["p_back"], v["p_out"])
    held, kept, parts = v["held"], v["kept"], v["parts"]

    def to_mate(a, d):
        t = peer_of(shard, d)
        n = a * 4 + d
        return remote(partial[a].at[tokens(t, other)], held.at[a, d],
                      v["csend"].at[n], v["crecv"].at[n], mate)

    def keep(a, d):
        return pltpu.make_async_copy(partial[a].at[tokens(peer_of(shard, d), core)], kept.at[a, d], v["keep_sem"].at[a * 4 + d])

    def to_owner(a, d):
        n = a * 3 + d - 1
        return remote(kept.at[a, d], parts.at[a, d - 1], v["psend"].at[n], v["precv"].at[n], (replica, peer_of(shard, d)))

    def pair_sums(a):
        for d in order:
            to_mate(a, d).wait_recv()
            keep(a, d).wait()

            def body(rows, carry):
                kept[a, d, rows, :] = (kept[a, d, rows, :].astype(f32) + held[a, d, rows, :].astype(f32)).astype(bf16)
                return carry

            row_loop(128, 32, body, 0)
            to_owner(a, d).start()

    def collect(a):
        to_mate(a, 0).wait_recv()
        keep(a, 0).wait()
        for d in order:
            to_owner(a, d).wait_recv()

    def full_sum(a, rows):
        total = kept[a, 0, rows, :].astype(f32) + held[a, 0, rows, :].astype(f32)
        for d in (1, 2, 3):
            total = total + parts[a, d - 1, rows, :].astype(f32)
        return total

    wide = ((v["hid"], v["hid_all"], 768), (v["prj"], v["prj_all"], 1024))
    narrow = ((v["ctx"], v["ctx_all"], 384), (v["nrm"], v["nrm_all"], 384))

    def block(out, owner, c):
        return out.at[tokens(owner, c)]

    def columns(ref, index, width):
        return ref.at[:, pl.ds(pl.multiple_of(index * width, width), width)]

    def wide_copy(a, d, same, source_core, owner, t):
        ref, out, width = wide[a]
        c = core if same else other
        n = (a * 4 + d) * 2 + (0 if same else 1)
        return remote(
            columns(ref, c, width), block(out, owner, source_core), v["gsend"].at[n], v["grecv"].at[n],
            (replica - core + c, t),
        )

    def narrow_copy(a, d, owner, t):
        ref, out, width = narrow[a]
        n = 16 + a * 4 + d
        return remote(columns(ref, t, width), block(out, owner, core), v["gsend"].at[n], v["grecv"].at[n], (replica, t))

    def onward(a, d, source, owner, c):
        out = narrow[a][1]
        n = a * 4 + d
        return remote(source, block(out, owner, c), v["fsend"].at[n], v["frecv"].at[n], mate)

    def own_narrow(a):
        ref, out, width = narrow[a]
        return pltpu.make_async_copy(columns(ref, shard, width), block(out, shard, core), v["local"].at[a])

    def own_wide(a):
        ref, out, width = wide[a]
        return pltpu.make_async_copy(columns(ref, core, width), block(out, shard, core), v["local"].at[2 + a])

    wbuf = v["wbuf"]
    load_out = pltpu.make_async_copy(v["wo"], wbuf.at[:, pl.ds(0, 1536)], v["local"].at[4])
    load_qkv = pltpu.make_async_copy(v["wq"], wbuf, v["local"].at[5])

    def stage_sums():
        pair_sums(0)
        for d in order:
            for a in range(2):
                narrow_copy(a, d, shard, peer_of(shard, d)).start()
        for d in (1, 2, 3):
            for a in range(2):
                exchange(a, d, peer_of(shard, d)).start()

    def stage_hidden():
        collect(0)
        gain = v["gain_two"][...]

        def body(rows, total):
            grad = full_sum(0, rows)
            hidden = v["hidden"][rows, :]
            inv = lax.rsqrt(jnp.mean(hidden * hidden, axis=-1, keepdims=True) + NORM_EPS)
            scaled = gain * grad
            out = v["cot"][rows, :].astype(f32) + inv * (
                scaled - hidden * inv * inv * jnp.mean(scaled * hidden, axis=-1, keepdims=True)
            )
            v["hgrad"][rows, :] = out
            v["hid"][rows, :] = out.astype(bf16)
            return total + jnp.sum(grad * hidden * inv, axis=0, keepdims=True)

        v["row_two"][...] = row_loop(128, 16, body, jnp.zeros((1, 1536), f32)) * grad_scale
        for d in (0,) + order:
            if d:
                wide_copy(0, d, True, core, shard, peer_of(shard, d)).start()
            wide_copy(0, d, False, core, shard, peer_of(shard, d)).start()
        own_wide(0).start()

    def stage_context():
        load_out.wait()
        for e in range(4):
            cols = pl.ds(e * 384, 384)
            v["cgrad"][:, cols] = dot_nt(v["hid"][...], wbuf[cols, 0:1536]).astype(bf16)
        load_qkv.start()

    def unrotated(x):
        return x * v["cos"][...] + pltpu.roll(x, HD // 2, 1) * v["sin"][...]

    def stage_heads(g):
        keys = v["key"][:, g * HD : (g + 1) * HD]
        values = v["val"][:, g * HD : (g + 1) * HD]
        causal = lax.broadcasted_iota(jnp.int32, (128, 128), 0) >= lax.broadcasted_iota(jnp.int32, (128, 128), 1)
        key_grad = jnp.zeros((128, HD), f32)
        value_grad = jnp.zeros((128, HD), f32)
        for h in range(g * (HEADS // KV), (g + 1) * (HEADS // KV)):
            at = slice(h * HD, (h + 1) * HD)
            query = v["qry"][:, at]
            grad = v["cgrad"][:, at]
            scores = jnp.where(causal, dot_nt(query, keys) * SCORE_SCALE, -1e30)
            probs = jnp.exp(scores - v["lse"][:, h : h + 1]).astype(bf16)
            wide_probs = probs.astype(f32)
            prob_grad = dot_nt(grad, values)
            delta = jnp.sum(wide_probs * prob_grad, axis=-1, keepdims=True)
            score_grad = (wide_probs * (prob_grad - delta) * SCORE_SCALE).astype(bf16)
            v["prj"][:, at] = unrotated(jnp.dot(score_grad, keys, preferred_element_type=f32)).astype(bf16)
            key_grad = key_grad + dot_tn(score_grad, query)
            value_grad = value_grad + dot_tn(probs, grad)
        first = HEADS * HD + g * HD
        v["prj"][:, first : first + HD] = unrotated(key_grad).astype(bf16)
        first = first + KV * HD
        v["prj"][:, first : first + HD] = value_grad.astype(bf16)

    def stage_send_projected():
        for d in (0,) + order:
            if d:
                wide_copy(1, d, True, core, shard, peer_of(shard, d)).start()
            wide_copy(1, d, False, core, shard, peer_of(shard, d)).start()
        own_wide(1).start()

    def stage_normed():
        load_qkv.wait()
        for e in range(4):
            cols = pl.ds(e * 384, 384)
            v["ngrad"][:, cols] = dot_nt(v["prj"][...], wbuf[cols, :])

    vec, vin, vall = v["vec"], v["vin"], v["vall"]
    replicas = 2 * levels

    def vec_hop(d):
        return remote(vec.at[peer_of(shard, d)], vin.at[d - 1], v["vsend"].at[d - 1], v["vrecv"].at[d - 1],
                      (replica, peer_of(shard, d)))

    def vec_spread(j, slot):
        target = lax.rem(replica + j, replicas)
        return remote(v["vsum"], vall.at[slot], v["vsend"].at[2 + j], v["vrecv"].at[2 + j], (target, shard))

    def stage_input():
        gain = v["gain_one"][...]

        def body(rows, totals):
            total, bias = totals
            x = v["x"][rows, :].astype(f32)
            grad = v["ngrad"][rows, :]
            inv = lax.rsqrt(jnp.mean(x * x, axis=-1, keepdims=True) + NORM_EPS)
            scaled = gain * grad
            v["input_grad"][rows, :] = v["hgrad"][rows, :] + inv * (
                scaled - x * inv * inv * jnp.mean(scaled * x, axis=-1, keepdims=True)
            )
            return (
                total + jnp.sum(grad * x * inv, axis=0, keepdims=True),
                bias + jnp.sum(v["prj"][rows, :].astype(f32), axis=0, keepdims=True),
            )

        row_one, row_bias = row_loop(128, 16, body, (jnp.zeros((1, 1536), f32), jnp.zeros((1, 2048), f32)))
        row_one = row_one * grad_scale
        row_bias = row_bias * grad_scale
        row_two = v["row_two"][...]
        for s in range(4):
            vec[s, :, 0:384] = jnp.broadcast_to(row_one[:, s * 384 : (s + 1) * 384], (8, 384))
            vec[s, :, 384:896] = jnp.broadcast_to(row_bias[:, s * 512 : (s + 1) * 512], (8, 512))
            vec[s, :, 896:1280] = jnp.broadcast_to(row_two[:, s * 384 : (s + 1) * 384], (8, 384))
        for d in order:
            vec_hop(d).start()

    def stage_vec():
        total = vec[shard]
        for d in (1, 2, 3):
            vec_hop(d).wait_recv()
            total = total + vin[d - 1]
        v["vsum"][...] = total
        for j in range(1, replicas):
            vec_spread(j, replica).start()
        pair_sums(1)

    def stage_vec_out():
        vall[replica] = v["vsum"][...]
        for j in range(1, replicas):
            vec_spread(j, lax.rem(replica + replicas - j, replicas)).wait_recv()
        total = vall[0]
        for j in range(1, replicas):
            total = total + vall[j]
        v["vec_out"][...] = total

    def stage_output():
        collect(1)

        def body(rows, carry):
            v["block_out"][rows, :] = (v["hidden"][rows, :] + full_sum(1, rows)).astype(bf16)
            return carry

        row_loop(128, 32, body, 0)

    def stage_relay():
        for d in order:
            p = peer_of(shard, d)
            for a in range(2):
                narrow_copy(a, d, p, p).wait_recv()
                onward(a, d, block(narrow[a][1], p, core), p, core).start()

    def stage_attention_parts():
        for a in range(2):
            own_narrow(a).wait()
            own_wide(a).wait()
            for d in (0, 1, 2, 3):
                p = peer_of(shard, d)
                if d:
                    wide_copy(a, d, True, core, p, p).wait_recv()
                wide_copy(a, d, False, other, p, p).wait_recv()
                onward(a, d, block(narrow[a][1], p, other), p, other).wait_recv()
        for j in range(3):
            at = pl.ds(j * 128, 128)
            own_a[at, 0:1024] = (dot_tn(v["nrm_all"][:, at], v["prj_all"][...]) * grad_scale).astype(bf16)
            own_a[at, 1024:1792] = (dot_tn(v["ctx_all"][:, at], v["hid_all"][...]) * grad_scale).astype(bf16)

    chunks = []
    for k in range(9):
        at = pl.ds(k * CHUNK, CHUNK)
        chunks.append((own_d, v["low_d"], v["high_d"], at, ("fill", 1), lambda c, at=at: v["fd"].at[c, at]))
    for d in range(4):
        for a in range(2):
            for k in range(3):
                at = pl.ds(a * 1536 + d * 384 + k * CHUNK, CHUNK)
                dst = (v["fg"], v["fu"])[a]
                source = peer_of(shard, d)
                chunks.append((
                    own_g, v["low_g"], v["high_g"], at, ("fill", 2 + a) if d == 0 else ("x", a, d),
                    lambda c, k=k, dst=dst, source=source: dst.at[c, source, pl.ds(k * CHUNK, CHUNK)],
                ))
    for k in range(3):
        at = pl.ds(k * CHUNK, CHUNK)
        chunks.append((own_a, v["low_a"], v["high_a"], at, ("none",), lambda c, at=at: v["fa"].at[c, at]))
    total = len(chunks)
    awaited = (set(), set())
    end = (level == 0) | (level == levels - 1)

    def arrive(what, seen):
        if what in seen or what[0] == "none":
            return
        seen.add(what)
        if what[0] == "fill":
            fills[what[1]].wait()
        else:
            exchange(what[1], what[2], peer_of(shard, what[2])).wait_recv()

    def up(k, ref):
        own, low, high, at, _, _ = chunks[k]
        return remote(ref.at[at], low.at[at], v["up_sem"].at[k], v["low_sem"].at[k], above)

    def down(k, ref):
        own, low, high, at, _, _ = chunks[k]
        return remote(ref.at[at], high.at[at], v["down_sem"].at[k], v["high_sem"].at[k], below)

    def add(k, *refs):
        own, _, _, at, _, _ = chunks[k]
        step = 32

        def body(j, carry):
            rows = pl.ds(pl.multiple_of(at.start + j * step, step), step)
            value = own[rows, :].astype(f32)
            for ref in refs:
                value = value + ref[rows, :].astype(f32)
            own[rows, :] = value.astype(own.dtype)
            return carry

        lax.fori_loop(0, CHUNK // step, body, 0)

    def finish(k, ref):
        _, _, _, at, _, dst = chunks[k]
        pltpu.make_async_copy(ref.at[at], dst(core), v["out_sem"].at[k]).start()
        remote(ref.at[at], dst(core), v["mate_send"].at[k], v["mate_recv"].at[k], mate).start()

    def root_of(k):
        return levels // 2 - 1 + k % 2

    def end_gather(k):
        own = chunks[k][0]

        @pl.when(end)
        def _():
            arrive(chunks[k][4], awaited[0])

        @pl.when(level == 0)
        def _():
            up(k, own).start()

        @pl.when(level == levels - 1)
        def _():
            down(k, own).start()

    def gather_step(k):
        own, low, high, at, what, _ = chunks[k]
        root = root_of(k)

        @pl.when(~end)
        def _():
            arrive(what, awaited[1])

        if root > 1:

            @pl.when((level > 0) & (level < root))
            def _():
                up(k, own).wait_recv()
                add(k, low)
                up(k, own).start()

        if root < levels - 2:

            @pl.when((level < levels - 1) & (level > root))
            def _():
                down(k, own).wait_recv()
                add(k, high)
                down(k, own).start()

    def root_step(k):
        own, low, high, at, _, _ = chunks[k]

        @pl.when(level == root_of(k))
        def _():
            up(k, own).wait_recv()
            down(k, own).wait_recv()
            add(k, low, high)
            up(k, own).start()
            down(k, own).start()
            finish(k, own)

    def spread_step(k):
        own, low, high, at, _, _ = chunks[k]
        root = root_of(k)

        if root > 1:

            @pl.when((level > 0) & (level < root))
            def _():
                down(k, own).wait_recv()
                down(k, high).start()
                finish(k, high)

        if root < levels - 2:

            @pl.when((level < levels - 1) & (level > root))
            def _():
                up(k, own).wait_recv()
                up(k, low).start()
                finish(k, low)

    def end_spread(k):
        own, low, high, at, _, _ = chunks[k]

        @pl.when(level == 0)
        def _():
            down(k, own).wait_recv()
            finish(k, high)

        @pl.when(level == levels - 1)
        def _():
            up(k, own).wait_recv()
            finish(k, low)

    for a in range(2):
        for d in order + (0,):
            to_mate(a, d).start()
            keep(a, d).start()
    for copy in fills[1:]:
        copy.start()
    load_out.start()
    for a in range(2):
        own_narrow(a).start()
        onward(a, 0, columns(narrow[a][0], shard, 384), shard, core).start()
    beside = {
        0: [stage_sums],
        3: [stage_hidden],
        4: [stage_context],
        5: [functools.partial(stage_heads, 0)],
        6: [functools.partial(stage_heads, 1), stage_send_projected],
        7: [stage_normed],
        8: [stage_input],
        10: [stage_vec],
        12: [stage_relay],
        14: [stage_vec_out],
        24: [stage_output],
        27: [stage_attention_parts],
    }
    stages = ((end_gather, 0), (gather_step, 4), (root_step, 7), (spread_step, 10), (end_spread, 14))
    for t in range(total + stages[-1][1]):
        for stage, lag in stages:
            if 0 <= t - lag < total:
                stage(t - lag)
        for stage in beside.get(t, ()):
            stage()
    for a in range(2):
        for d in (1, 2, 3):
            exchange(a, d, peer_of(shard, d)).wait_send()
    for k in range(total):
        own, low, high, at, _, dst = chunks[k]

        @pl.when(level < levels - 1)
        def _():
            up(k, own).wait_send()

        @pl.when(level > 0)
        def _():
            down(k, own).wait_send()

        pltpu.make_async_copy(own.at[at], dst(core), v["out_sem"].at[k]).wait()
        remote(own.at[at], dst(core), v["mate_send"].at[k], v["mate_recv"].at[k], mate).wait_send()
        remote(own.at[at], dst(1 - core), v["mate_send"].at[k], v["mate_recv"].at[k], mate).wait_recv()
    for a in range(2):
        for d in (0, 1, 2, 3):
            p = peer_of(shard, d)
            to_mate(a, d).wait_send()
            wide_copy(a, d, False, core, shard, p).wait_send()
            onward(a, d, block(narrow[a][1], p, core), p, core).wait_send()
            if d:
                to_owner(a, d).wait_send()
                wide_copy(a, d, True, core, shard, p).wait_send()
                narrow_copy(a, d, shard, p).wait_send()
    for d in order:
        vec_hop(d).wait_send()
    for j in range(1, replicas):
        vec_spread(j, replica).wait_send()


def backward(levels, grad_scale, **given):
    bf16 = jnp.bfloat16
    f32 = jnp.float32
    dma = pltpu.SemaphoreType.DMA
    in_hbm = ("pd", "pg", "pu", "p_back", "p_out", "wo", "wq")
    outs = {
        "fa": ((2, 384, 1792), bf16, any_spec()),
        "fd": ((2, WINDOW, 1536), bf16, any_spec()),
        "fg": ((2, 4, 384, WINDOW), bf16, any_spec()),
        "fu": ((2, 4, 384, WINDOW), bf16, any_spec()),
        "block_out": ((128, 1536), bf16, vmem_spec()),
        "input_grad": ((128, 1536), f32, vmem_spec()),
        "vec_out": ((8, 1280), f32, vmem_spec()),
    }
    scratch = {}
    for where in ("own", "low", "high"):
        scratch[where + "_a"] = pltpu.VMEM((384, 1792), bf16)
        scratch[where + "_d"] = pltpu.VMEM((WINDOW, 1536), bf16)
        scratch[where + "_g"] = pltpu.VMEM((3072, WINDOW), bf16)
    scratch |= {
        "held": pltpu.VMEM((2, 4, 128, 1536), bf16),
        "kept": pltpu.VMEM((2, 4, 128, 1536), bf16),
        "parts": pltpu.VMEM((2, 3, 128, 1536), bf16),
        "wbuf": pltpu.VMEM((1536, 2048), bf16),
        "hgrad": pltpu.VMEM((128, 1536), f32),
        "ngrad": pltpu.VMEM((128, 1536), f32),
        "hid": pltpu.VMEM((128, 1536), bf16),
        "cgrad": pltpu.VMEM((128, 1536), bf16),
        "prj": pltpu.VMEM((128, 2048), bf16),
        "ctx_all": pltpu.VMEM((1024, 384), bf16),
        "nrm_all": pltpu.VMEM((1024, 384), bf16),
        "hid_all": pltpu.VMEM((1024, 768), bf16),
        "prj_all": pltpu.VMEM((1024, 1024), bf16),
        "row_two": pltpu.VMEM((1, 1536), f32),
        "vec": pltpu.VMEM((4, 8, 1280), f32),
        "vin": pltpu.VMEM((3, 8, 1280), f32),
        "vsum": pltpu.VMEM((8, 1280), f32),
        "vall": pltpu.VMEM((2 * levels, 8, 1280), f32),
    }
    counts = {
        "xsend": 8, "xrecv": 8, "csend": 8, "crecv": 8, "keep_sem": 8, "psend": 6, "precv": 6, "gsend": 24, "grecv": 24,
        "fsend": 8, "frecv": 8, "local": 6, "in_sem": 4, "vsend": 2 + 2 * levels, "vrecv": 2 + 2 * levels,
    }
    for name in ("up_sem", "down_sem", "low_sem", "high_sem", "mate_send", "mate_recv", "out_sem"):
        counts[name] = 36
    scratch |= {name: dma((n,)) for name, n in counts.items()}
    return pl.pallas_call(
        functools.partial(backward_kernel, levels, grad_scale, (*given, *outs, *scratch)),
        out_shape=[jax.ShapeDtypeStruct(s, dt) for s, dt, _ in outs.values()],
        in_specs=[any_spec() if name in in_hbm else vmem_spec() for name in given],
        out_specs=[spec for _, _, spec in outs.values()],
        scratch_shapes=list(scratch.values()),
        compiler_params=pltpu.CompilerParams(has_side_effects=True, vmem_limit_bytes=67043328),
    )(*given.values())


def widen_kernel(x, out):
    f32 = jnp.float32
    for s in range(4):
        for c in range(2):
            first = (s * 35) // 2 + c * 9
            joined = s % 2 == 1 and c == 0
            rest = 1 if joined else 0
            out[:, (first + rest) * 128 : (first + 9) * 128] = x[c, s][:, rest * 128 :].astype(f32)
    for s in (1, 3):
        first = (s * 35) // 2
        out[:, first * 128 : (first + 1) * 128] = x[1, s - 1][:, 1024:].astype(f32) + x[0, s][:, :128].astype(f32)


def widen(x):
    rows = 32
    return pl.pallas_call(
        widen_kernel,
        grid=(384 // rows,),
        out_shape=jax.ShapeDtypeStruct((384, 8960), jnp.float32),
        in_specs=[pl.BlockSpec((2, 4, rows, WINDOW), lambda i: (0, 0, i, 0))],
        out_specs=pl.BlockSpec((rows, 8960), lambda i: (i, 0)),
    )(x)


def fast_device(
    block_input,
    attn_gain,
    qkv_weight,
    qkv_bias,
    out_weight,
    mlp_gain,
    gate_weight,
    up_weight,
    down_weight,
    cotangent,
):
    f32 = jnp.float32
    bf16 = jnp.bfloat16
    tok_count = block_input.shape[0]
    levels = lax.axis_size("replica") // 2
    grad_scale = 1.0 / math.sqrt(tok_count * lax.axis_size("replica") * lax.axis_size("shard"))
    q_width = HEADS * HD
    k_end = q_width + KV * HD
    replica, shard, core = place()
    cosine, sine_table = rope_tables(tok_count)
    small = jnp.zeros((16, 512), bf16)
    small = small.at[0, :384].set(attn_gain).at[1, :].set(qkv_bias).at[2, :384].set(mlp_gain)
    qkv_full, out_full, gate_own, up_own, cot_all, small_all = front(
        qkv_weight, out_weight, gate_weight, up_weight, cotangent, small
    )
    gain_one = small_all[:, 0, :384].reshape(-1).astype(f32)
    bias = small_all[:, 1, :].reshape(-1).astype(f32)
    gain_two = small_all[:, 2, :384].reshape(-1).astype(f32)

    xfloat = block_input.astype(f32)
    inv_one = lax.rsqrt(jnp.mean(xfloat * xfloat, axis=-1, keepdims=True) + NORM_EPS)
    normed_one = (xfloat * inv_one * gain_one).astype(bf16)
    projected = jnp.dot(normed_one, qkv_full, preferred_element_type=f32) + bias
    queries = rotate(projected[:, :q_width].reshape(tok_count, HEADS, HD), cosine, sine_table).astype(bf16)
    queries = queries.reshape(tok_count, KV, HEADS // KV, HD)
    key_rot = rotate(projected[:, q_width:k_end].reshape(tok_count, KV, HD), cosine, sine_table).astype(bf16)
    values = projected[:, k_end:].reshape(tok_count, KV, HD).astype(bf16)
    context, logsum = attend_forward(queries, key_rot, values)
    hidden_res = xfloat + jnp.dot(context, out_full, preferred_element_type=f32)
    inv_two = lax.rsqrt(jnp.mean(hidden_res * hidden_res, axis=-1, keepdims=True) + NORM_EPS)
    normed_two = (hidden_res * inv_two * gain_two).astype(bf16)

    normed_all = plane_gather(normed_two)
    first = window_start(shard, core)
    column = first + jnp.arange(WINDOW)
    owned = (column >= shard * 2240) & (column < (shard + 1) * 2240)
    padded = jnp.pad(down_weight, ((64, 64), (0, 0)))
    down_own = lax.dynamic_slice_in_dim(padded, first - shard * 2240 + 64, WINDOW, 0)
    gate_pre = jnp.dot(normed_all, gate_own, preferred_element_type=f32)
    up_pre = jnp.dot(normed_all, up_own, preferred_element_type=f32)
    sigmoid_gate = jax.nn.sigmoid(gate_pre)
    silu_gate = gate_pre * sigmoid_gate
    act_grad = jnp.einsum("td,fd->tf", cot_all, down_own, preferred_element_type=f32)
    activation = jnp.where(owned, silu_gate * up_pre, 0.0).astype(bf16)
    gate_delta = jnp.where(
        owned, act_grad * up_pre * sigmoid_gate * (1.0 + gate_pre * (1.0 - sigmoid_gate)), 0.0
    ).astype(bf16)
    up_delta = jnp.where(owned, act_grad * silu_gate, 0.0).astype(bf16)
    down_out = jnp.dot(activation, down_own, preferred_element_type=f32).astype(bf16)
    back = (
        jnp.einsum("tf,df->td", gate_delta, gate_own, preferred_element_type=f32)
        + jnp.einsum("tf,df->td", up_delta, up_own, preferred_element_type=f32)
    ).astype(bf16)
    gate_part = (jnp.einsum("td,tf->df", normed_all, gate_delta, preferred_element_type=f32) * grad_scale).astype(bf16)
    up_part = (jnp.einsum("td,tf->df", normed_all, up_delta, preferred_element_type=f32) * grad_scale).astype(bf16)
    down_part = (jnp.einsum("tf,td->fd", activation, cot_all, preferred_element_type=f32) * grad_scale).astype(bf16)

    sums = logsum.reshape(HEADS, tok_count).T
    sum_attn, sum_down, sum_gate, sum_up, block_output, input_grad, vectors = backward(
        levels,
        grad_scale,
        pd=down_part,
        pg=gate_part,
        pu=up_part,
        p_back=back,
        p_out=down_out,
        wo=out_full,
        wq=qkv_full,
        hidden=hidden_res,
        x=block_input,
        cot=cotangent,
        gain_one=gain_one[None, :],
        gain_two=gain_two[None, :],
        ctx=context,
        nrm=normed_one,
        qry=queries.reshape(tok_count, q_width),
        key=key_rot.reshape(tok_count, KV * HD),
        val=values.reshape(tok_count, KV * HD),
        lse=jnp.pad(sums, ((0, 0), (0, HD - HEADS))),
        cos=jnp.concatenate([cosine[:, 0], cosine[:, 0]], axis=1),
        sin=jnp.concatenate([sine_table[:, 0], -sine_table[:, 0]], axis=1),
    )
    gain_one_own, bias_own, gain_two_own = vectors[0, :384], vectors[0, 384:896], vectors[0, 896:]
    qkv_grad = jnp.concatenate([sum_attn[0, :, :1024], sum_attn[1, :, :1024]], axis=1).astype(f32)
    out_grad = jnp.concatenate([sum_attn[0, :, 1024:], sum_attn[1, :, 1024:]], axis=1).astype(f32)
    down_grad = lax.dynamic_slice_in_dim(
        sum_down.reshape(2 * WINDOW, 1536), lax.rem(shard, 2) * 64, 2240, 0
    ).astype(f32)
    return (
        block_output,
        input_grad,
        gain_one_own,
        qkv_grad,
        bias_own,
        out_grad,
        gain_two_own,
        widen(sum_gate),
        widen(sum_up),
        down_grad,
    )


def solution(mesh):
    placed = (
        P(("replica", "shard"), None),
        P("shard"),
        P("shard", None),
        P("shard"),
        P("shard", None),
        P("shard"),
        P("shard", None),
        P("shard", None),
        P("shard", None),
        P(("replica", "shard"), None),
    )
    fits = mesh.shape["shard"] == 4 and mesh.shape["replica"] % 4 == 0
    per_device = fast_device if fits else general_device
    return jax.shard_map(
        per_device,
        mesh=mesh,
        in_specs=placed,
        out_specs=(
            P(("replica", "shard"), None),
            P(("replica", "shard"), None),
            P("shard"),
            P("shard", None),
            P("shard"),
            P("shard", None),
            P("shard"),
            P("shard", None),
            P("shard", None),
            P("shard", None),
        ),
        check_vma=False,
    )
```

```python
import functools
import math

import jax
import jax.numpy as jnp
from jax import lax
from jax.experimental import pallas as pl
from jax.experimental.pallas import tpu as pltpu
from jax.sharding import PartitionSpec as P

HEADS = 12
KV = 2
HD = 128


NORM_EPS = 1e-06
ROPE_BASE = 1000000.0


def rope_tables(tok_count):
    half_dim = HD // 2
    position = jnp.arange(tok_count, dtype=jnp.float32)
    inverse = ROPE_BASE ** (-(jnp.arange(half_dim, dtype=jnp.float32) * 2.0 / HD))
    angles = position[:, None] * inverse[None, :]
    return (jnp.cos(angles)[:, None, :], jnp.sin(angles)[:, None, :])


def rotate(vectors, cosine, sine_table):
    half_dim = HD // 2
    lower_half = vectors[..., :half_dim]
    upper_half = vectors[..., half_dim:]
    return jnp.concatenate(
        [
            lower_half * cosine - upper_half * sine_table,
            upper_half * cosine + lower_half * sine_table,
        ],
        axis=-1,
    )


def unrotate(grads, cosine, sine_table):
    half_dim = HD // 2
    lower_half = grads[..., :half_dim]
    upper_half = grads[..., half_dim:]
    return jnp.concatenate(
        [
            lower_half * cosine + upper_half * sine_table,
            upper_half * cosine - lower_half * sine_table,
        ],
        axis=-1,
    )


def block_scores(query_block, key_rot, first_row):
    row_count = query_block.shape[0]
    scores = jnp.einsum(
        "qkgd,skd->kgqs", query_block, key_rot, preferred_element_type=jnp.float32
    ) * (1.0 / math.sqrt(HD))
    causal = (first_row + jnp.arange(row_count))[:, None] >= jnp.arange(key_rot.shape[0])[None, :]
    return jnp.where(causal, scores, -1e30)


def block_layout(tok_count):
    block_rows = min(tok_count, 512)
    block_count = tok_count // block_rows
    firsts = jnp.arange(block_count, dtype=jnp.int32) * block_rows
    return (block_rows, block_count, firsts)


def attend_forward(queries, key_rot, values):
    tok_count = queries.shape[0]
    block_rows, block_count, firsts = block_layout(tok_count)
    query_blocks = queries.reshape(block_count, block_rows, KV, HEADS // KV, HD)

    def one_block(inputs):
        query_block, first_row = inputs
        scores = block_scores(query_block, key_rot, first_row)
        row_max = jnp.max(scores, axis=-1, keepdims=True)
        logsum = row_max + jnp.log(jnp.sum(jnp.exp(scores - row_max), axis=-1, keepdims=True))
        attn_probs = jnp.exp(scores - logsum).astype(jnp.bfloat16)
        context = jnp.einsum(
            "kgqs,skd->qkgd", attn_probs, values, preferred_element_type=jnp.float32
        ).astype(jnp.bfloat16)
        return (context, logsum)

    context, logsum = lax.map(one_block, (query_blocks, firsts))
    return (context.reshape(tok_count, HEADS * HD), logsum)


def attend_backward(queries, key_rot, values, logsum, context_grad):
    tok_count = queries.shape[0]
    block_rows, block_count, firsts = block_layout(tok_count)
    query_blocks = queries.reshape(block_count, block_rows, KV, HEADS // KV, HD)
    grad_blocks = context_grad.reshape(block_count, block_rows, KV, HEADS // KV, HD)
    score_scale = 1.0 / math.sqrt(HD)

    def one_block(running, inputs):
        key_total, value_total = running
        query_block, grad_block, log_block, first_row = inputs
        scores = block_scores(query_block, key_rot, first_row)
        attn_probs = jnp.exp(scores - log_block).astype(jnp.bfloat16)
        prob_grad = jnp.einsum(
            "qkgd,skd->kgqs", grad_block, values, preferred_element_type=jnp.float32
        )
        wide_probs = attn_probs.astype(jnp.float32)
        row_delta = jnp.sum(wide_probs * prob_grad, axis=-1, keepdims=True)
        score_grad = (wide_probs * (prob_grad - row_delta) * score_scale).astype(jnp.bfloat16)
        query_grad = jnp.einsum(
            "kgqs,skd->qkgd", score_grad, key_rot, preferred_element_type=jnp.float32
        )
        key_total = key_total + jnp.einsum(
            "kgqs,qkgd->skd", score_grad, query_block, preferred_element_type=jnp.float32
        )
        value_total = value_total + jnp.einsum(
            "kgqs,qkgd->skd", attn_probs, grad_block, preferred_element_type=jnp.float32
        )
        return ((key_total, value_total), query_grad)

    zero_keys = jnp.zeros((tok_count, KV, HD), jnp.float32)
    (key_grad, value_grad), query_grad = lax.scan(
        one_block, (zero_keys, zero_keys), (query_blocks, grad_blocks, logsum, firsts)
    )
    return (query_grad.reshape(tok_count, HEADS, HD), key_grad, value_grad)


def general_device(
    block_input,
    attn_gain,
    qkv_weight,
    qkv_bias,
    out_weight,
    mlp_gain,
    gate_weight,
    up_weight,
    down_weight,
    cotangent,
):
    f32 = jnp.float32
    bf16 = jnp.bfloat16
    tok_count = block_input.shape[0]
    grad_scale = 1.0 / math.sqrt(tok_count * lax.axis_size("replica") * lax.axis_size("shard"))
    q_width = HEADS * HD
    k_end = q_width + KV * HD
    cosine, sine_table = rope_tables(tok_count)
    attn_full = (
        lax.all_gather(attn_gain, "shard", axis=0, tiled=True),
        lax.all_gather(qkv_weight, "shard", axis=0, tiled=True),
        lax.all_gather(qkv_bias, "shard", axis=0, tiled=True),
        lax.all_gather(out_weight, "shard", axis=0, tiled=True),
    )
    gain_full, qkv_full, bias_full, out_full = attn_full
    gain_one = gain_full.astype(f32)
    xfloat = block_input.astype(f32)
    inv_one = lax.rsqrt(jnp.mean(xfloat * xfloat, axis=-1, keepdims=True) + NORM_EPS)
    normed_one = (xfloat * inv_one * gain_one).astype(bf16)
    projected = jnp.dot(normed_one, qkv_full, preferred_element_type=f32) + bias_full.astype(f32)
    queries = rotate(
        projected[:, :q_width].reshape(tok_count, HEADS, HD), cosine, sine_table
    ).astype(bf16)
    queries = queries.reshape(tok_count, KV, HEADS // KV, HD)
    key_rot = rotate(
        projected[:, q_width:k_end].reshape(tok_count, KV, HD), cosine, sine_table
    ).astype(bf16)
    values = projected[:, k_end:].reshape(tok_count, KV, HD).astype(bf16)
    context, logsum = attend_forward(queries, key_rot, values)
    hidden_res = xfloat + jnp.dot(context, out_full, preferred_element_type=f32)
    mlp_full = (
        lax.all_gather(mlp_gain, "shard", axis=0, tiled=True),
        lax.all_gather(gate_weight, "shard", axis=0, tiled=True),
        lax.all_gather(up_weight, "shard", axis=0, tiled=True),
        lax.all_gather(down_weight, "shard", axis=0, tiled=True),
    )
    gain_full_two, gate_full, up_full, down_full = mlp_full
    gain_two = gain_full_two.astype(f32)
    inv_two = lax.rsqrt(jnp.mean(hidden_res * hidden_res, axis=-1, keepdims=True) + NORM_EPS)
    normed_two = (hidden_res * inv_two * gain_two).astype(bf16)
    gate_pre = jnp.dot(normed_two, gate_full, preferred_element_type=f32)
    up_pre = jnp.dot(normed_two, up_full, preferred_element_type=f32)
    sigmoid_gate = jax.nn.sigmoid(gate_pre)
    silu_gate = gate_pre * sigmoid_gate
    activation = (silu_gate * up_pre).astype(bf16)
    block_output = (hidden_res + jnp.dot(activation, down_full, preferred_element_type=f32)).astype(
        bf16
    )
    act_grad = jnp.einsum("td,fd->tf", cotangent, down_full, preferred_element_type=f32)
    gate_delta = (
        act_grad * up_pre * sigmoid_gate * (1.0 + gate_pre * (1.0 - sigmoid_gate))
    ).astype(bf16)
    up_delta = (act_grad * silu_gate).astype(bf16)
    normed_two_grad = jnp.einsum(
        "tf,df->td", gate_delta, gate_full, preferred_element_type=f32
    ) + jnp.einsum("tf,df->td", up_delta, up_full, preferred_element_type=f32)
    gain_two_grad = jnp.sum(normed_two_grad * hidden_res * inv_two, axis=0) * grad_scale
    own_rows = (
        lax.all_to_all(activation, "shard", split_axis=1, concat_axis=0, tiled=True),
        lax.all_to_all(normed_two, "shard", split_axis=1, concat_axis=0, tiled=True),
    )
    group_act, group_normed = own_rows
    group_rows = (
        lax.all_gather(cotangent, "shard", axis=0, tiled=True),
        lax.all_gather(gate_delta, "shard", axis=0, tiled=True),
        lax.all_gather(up_delta, "shard", axis=0, tiled=True),
    )
    group_cot, group_gate, group_up = group_rows
    down_part = (
        jnp.einsum("tf,td->fd", group_act, group_cot, preferred_element_type=f32) * grad_scale
    )
    gate_own = (
        jnp.einsum("td,tf->df", group_normed, group_gate, preferred_element_type=f32) * grad_scale
    )
    up_own = (
        jnp.einsum("td,tf->df", group_normed, group_up, preferred_element_type=f32) * grad_scale
    )
    gain_two_own = lax.psum_scatter(gain_two_grad, "shard", scatter_dimension=0, tiled=True)
    mlp_parts = (gain_two_own, gate_own, up_own)
    hidden_grad = cotangent.astype(f32) + inv_two * (
        gain_two * normed_two_grad
        - hidden_res
        * inv_two
        * inv_two
        * jnp.mean(gain_two * normed_two_grad * hidden_res, axis=-1, keepdims=True)
    )
    hidden_low = hidden_grad.astype(bf16)
    context_grad = jnp.einsum("td,ed->te", hidden_low, out_full, preferred_element_type=f32).astype(
        bf16
    )
    query_grad, key_grad, value_grad = attend_backward(
        queries, key_rot, values, logsum, context_grad
    )
    query_grad = unrotate(query_grad, cosine, sine_table).reshape(tok_count, q_width)
    key_grad = unrotate(key_grad, cosine, sine_table).reshape(tok_count, KV * HD)
    projected_grad = jnp.concatenate(
        [query_grad, key_grad, value_grad.reshape(tok_count, KV * HD)], axis=-1
    ).astype(bf16)
    normed_one_grad = jnp.einsum("tc,dc->td", projected_grad, qkv_full, preferred_element_type=f32)
    gain_one_grad = jnp.sum(normed_one_grad * xfloat * inv_one, axis=0) * grad_scale
    bias_grad = jnp.sum(projected_grad.astype(f32), axis=0) * grad_scale
    own_attn = (
        lax.all_to_all(context, "shard", split_axis=1, concat_axis=0, tiled=True),
        lax.all_to_all(normed_one, "shard", split_axis=1, concat_axis=0, tiled=True),
    )
    group_context, group_normed_one = own_attn
    group_rows = (
        lax.all_gather(hidden_low, "shard", axis=0, tiled=True),
        lax.all_gather(projected_grad, "shard", axis=0, tiled=True),
    )
    group_hidden, group_projected = group_rows
    out_own = (
        jnp.einsum("te,td->ed", group_context, group_hidden, preferred_element_type=f32)
        * grad_scale
    )
    qkv_part = (
        jnp.einsum("td,tc->dc", group_normed_one, group_projected, preferred_element_type=f32)
        * grad_scale
    )
    small_parts = (
        lax.psum_scatter(gain_one_grad, "shard", scatter_dimension=0, tiled=True),
        lax.psum_scatter(bias_grad, "shard", scatter_dimension=0, tiled=True),
    )
    attn_parts = (small_parts[0], qkv_part, small_parts[1], out_own)
    input_grad = hidden_grad + inv_one * (
        gain_one * normed_one_grad
        - xfloat
        * inv_one
        * inv_one
        * jnp.mean(gain_one * normed_one_grad * xfloat, axis=-1, keepdims=True)
    )
    summed = lax.psum(
        (
            attn_parts[0],
            attn_parts[1],
            attn_parts[2],
            attn_parts[3],
            mlp_parts[0],
            mlp_parts[1],
            mlp_parts[2],
            down_part,
        ),
        "replica",
    )
    attn_parts = (summed[0], summed[1], summed[2], summed[3])
    mlp_parts = (summed[4], summed[5], summed[6])
    down_part = summed[7]
    return (
        block_output,
        input_grad,
        attn_parts[0],
        attn_parts[1],
        attn_parts[2],
        attn_parts[3],
        mlp_parts[0],
        mlp_parts[1],
        mlp_parts[2],
        down_part,
    )


MESH = pl.DeviceIdType.MESH
VMEM_BYTES = 62 * 2**20
WINDOW = 1152


def place():
    replica = lax.axis_index("replica")
    shard = lax.axis_index("shard")
    core = lax.rem(replica, 2)
    return replica, shard, core


def peer_of(shard, d):
    across = lax.rem(lax.rem(shard, 2) + d % 2, 2)
    up = lax.rem(shard // 2 + d // 2, 2)
    return up * 2 + across


def window_start(shard, core):
    return ((shard * 35) // 2 + core * 9) * 128


def remote(src, dst, send, recv, device):
    return pltpu.make_async_remote_copy(
        src_ref=src,
        dst_ref=dst,
        send_sem=send,
        recv_sem=recv,
        device_id=device,
        device_id_type=MESH,
    )


def front_kernel(
    wq, wo, wg, wu, cot, small, q_full, o_full, g_own, u_own, cot_all, small_all,
    bq, bo, bg, bu, bc, bs, send, recv, fsend, frecv, zsend, zrecv, local,
):
    replica, shard, core = place()
    other = 1 - core
    mate = (replica + 1 - 2 * core, shard)
    odd = lax.rem(replica // 2, 2)
    pair = (replica + 2 - 4 * odd, shard)

    def span(start, size):
        return pl.ds(pl.multiple_of(start, 16), size)

    def cols(target):
        return pl.ds(pl.multiple_of(window_start(target, core), 128), WINDOW)

    def block(owner, c):
        return pl.ds(pl.multiple_of((c * 4 + owner) * 128, 128), 128)

    def rows(owner):
        return pl.ds(pl.multiple_of(owner * 384, 384), 384)

    loads = [
        (wq, bq, q_full.at[rows(shard)]),
        (wo, bo, o_full.at[rows(shard)]),
        (wg.at[:, cols(shard)], bg, g_own.at[rows(shard)]),
        (wu.at[:, cols(shard)], bu, u_own.at[rows(shard)]),
        (cot, bc, cot_all.at[block(shard, core)]),
        (small, bs, small_all.at[shard]),
    ]
    weights = [
        (lambda t: wq, q_full, 192, 80, True),
        (lambda t: wo, o_full, 192, 80, True),
        (lambda t: wg.at[:, cols(t)], g_own, 384, 176, False),
        (lambda t: wu.at[:, cols(t)], u_own, 384, 176, False),
    ]

    def base(i, c):
        return c * 192 if weights[i][4] else 0

    def hop(i, d, t, o):
        source, out, size, shared, _ = weights[i]
        first = base(i, core) + odd * shared
        n = i * 3 + d - 1
        return remote(
            source(t).at[span(first, size - shared)], out.at[span(o * 384 + first, size - shared)],
            send.at[n], recv.at[n], (replica, t),
        )

    def across(i, d, o, whose):
        _, out, size, shared, _ = weights[i]
        ref = out.at[span(o * 384 + base(i, core) + whose * (size - shared), shared)]
        n = i * 3 + d - 1
        return remote(ref, ref, zsend.at[n], zrecv.at[n], pair)

    def onward(i, d, o, c, shared_part):
        _, out, size, shared, _ = weights[i]
        first = o * 384 + base(i, c) + ((1 - odd) * (size - shared) if shared_part else odd * shared)
        ref = out.at[span(first, shared if shared_part else size - shared)]
        n = i * 3 + d - 1 + (6 if shared_part else 0)
        return remote(ref, ref, fsend.at[n], frecv.at[n], mate)

    def cot_hop(d, t, o):
        return remote(cot, cot_all.at[block(o, core)], send.at[11 + d], recv.at[11 + d], (replica, t))

    def cot_onward(d, o, c):
        ref = cot_all.at[block(o, c)] if d else cot
        return remote(ref, cot_all.at[block(o, c)], fsend.at[12 + d], frecv.at[12 + d], mate)

    def small_hop(d, t, o):
        return remote(small, small_all.at[o], send.at[14 + d], recv.at[14 + d], (replica, t))

    order = (3, 1, 2)
    for d in order:
        small_hop(d, peer_of(shard, d), shard).start()
    for i in range(4):
        if i == 2:
            for d in order:
                cot_hop(d, peer_of(shard, d), shard).start()
        for d in order:
            hop(i, d, peer_of(shard, d), shard).start()
    cot_onward(0, shard, core).start()
    for n, (src, buf, _) in enumerate(loads):
        pltpu.make_async_copy(src, buf, local.at[n]).start()
    for n, (src, buf, dst) in enumerate(loads):
        pltpu.make_async_copy(src, buf, local.at[n]).wait()
        pltpu.make_async_copy(buf, dst, local.at[n]).start()

    def take(i):
        for d in order:
            p = peer_of(shard, d)
            hop(i, d, p, p).wait_recv()
            across(i, d, p, odd).start()
            if weights[i][4]:
                onward(i, d, p, core, False).start()

    def take_shared(i):
        for d in order:
            p = peer_of(shard, d)
            across(i, d, p, 1 - odd).wait_recv()
            if weights[i][4]:
                onward(i, d, p, core, True).start()

    take(0)
    take(1)
    for d in order:
        p = peer_of(shard, d)
        cot_hop(d, p, p).wait_recv()
        cot_onward(d, p, core).start()
    take_shared(0)
    take_shared(1)
    take(2)
    take(3)
    take_shared(2)
    take_shared(3)
    for d in order:
        p = peer_of(shard, d)
        small_hop(d, p, p).wait_recv()
        small_hop(d, p, shard).wait_send()
        cot_hop(d, p, shard).wait_send()
        cot_onward(d, p, core).wait_send()
        cot_onward(d, p, other).wait_recv()
        for i in range(4):
            hop(i, d, p, shard).wait_send()
            across(i, d, p, odd).wait_send()
            if weights[i][4]:
                for part in (False, True):
                    onward(i, d, p, core, part).wait_send()
                    onward(i, d, p, other, part).wait_recv()
    cot_onward(0, shard, core).wait_send()
    cot_onward(0, shard, other).wait_recv()
    for n, (src, buf, dst) in enumerate(loads):
        pltpu.make_async_copy(buf, dst, local.at[n]).wait()


def any_spec():
    return pl.BlockSpec(memory_space=pl.ANY)


def vmem_spec():
    return pl.BlockSpec(memory_space=pltpu.VMEM)


def params(**more):
    return pltpu.CompilerParams(has_side_effects=True, vmem_limit_bytes=VMEM_BYTES, **more)


def front(wq, wo, wg, wu, cot, small):
    bf16 = jnp.bfloat16
    shapes = [(1536, 2048), (1536, 1536), (1536, WINDOW), (1536, WINDOW), (1024, 1536), (4, 16, 512)]
    bounce = [wq.shape, wo.shape, (384, WINDOW), (384, WINDOW), cot.shape, small.shape]
    return pl.pallas_call(
        front_kernel,
        out_shape=[jax.ShapeDtypeStruct(s, bf16) for s in shapes],
        in_specs=[any_spec()] * 6,
        out_specs=[any_spec()] * 6,
        scratch_shapes=[pltpu.VMEM(s, bf16) for s in bounce]
        + [
            pltpu.SemaphoreType.DMA((18,)),
            pltpu.SemaphoreType.DMA((18,)),
            pltpu.SemaphoreType.DMA((16,)),
            pltpu.SemaphoreType.DMA((16,)),
            pltpu.SemaphoreType.DMA((12,)),
            pltpu.SemaphoreType.DMA((12,)),
            pltpu.SemaphoreType.DMA((6,)),
        ],
        compiler_params=params(),
    )(wq, wo, wg, wu, cot, small)


def gather_kernel(x, out, send, recv, fsend, frecv, local):
    replica, shard, core = place()
    mate = (replica + 1 - 2 * core, shard)

    def block(owner, c):
        return out.at[pl.ds(pl.multiple_of((c * 4 + owner) * 128, 128), 128)]

    for d in (3, 1, 2):
        remote(x, block(shard, core), send.at[d], recv.at[d], (replica, peer_of(shard, d))).start()
    remote(x, block(shard, core), fsend.at[0], frecv.at[0], mate).start()
    own = pltpu.make_async_copy(x, block(shard, core), local)
    own.start()
    for d in (1, 2, 3):
        p = peer_of(shard, d)
        remote(x, block(p, core), send.at[d], recv.at[d], (replica, p)).wait_recv()
        remote(block(p, core), block(p, core), fsend.at[d], frecv.at[d], mate).start()
    own.wait()
    for d in (1, 2, 3):
        p = peer_of(shard, d)
        remote(x, block(shard, core), send.at[d], recv.at[d], (replica, p)).wait_send()
        remote(block(p, core), block(p, core), fsend.at[d], frecv.at[d], mate).wait_send()
        remote(x, block(p, 1 - core), fsend.at[d], frecv.at[d], mate).wait_recv()
    remote(x, block(shard, core), fsend.at[0], frecv.at[0], mate).wait_send()
    remote(x, block(shard, 1 - core), fsend.at[0], frecv.at[0], mate).wait_recv()


def plane_gather(x):
    return pl.pallas_call(
        gather_kernel,
        out_shape=jax.ShapeDtypeStruct((x.shape[0] * 8, x.shape[1]), x.dtype),
        in_specs=[vmem_spec()],
        out_specs=vmem_spec(),
        scratch_shapes=[pltpu.SemaphoreType.DMA((4,))] * 4 + [pltpu.SemaphoreType.DMA],
        compiler_params=params(),
    )(x)


CHUNK = 128
DOWN_CHUNKS = (64, 64) + (128,) * 8
ATTENTION_CHUNKS = (64, 64, 64, 64, 32, 32, 32, 32)
CHUNKS = len(DOWN_CHUNKS) + 24 + len(ATTENTION_CHUNKS)
SCORE_SCALE = 1.0 / math.sqrt(HD)


def row_spans(sizes):
    return [pl.ds(sum(sizes[:k]), size) for k, size in enumerate(sizes)]


def dot_nt(a, b):
    return lax.dot_general(a, b, (((1,), (1,)), ((), ())), preferred_element_type=jnp.float32)


def dot_tn(a, b):
    return lax.dot_general(a, b, (((0,), (0,)), ((), ())), preferred_element_type=jnp.float32)


def row_loop(rows, step, body, init):
    return lax.fori_loop(0, rows // step, lambda j, c: body(pl.ds(pl.multiple_of(j * step, step), step), c), init)


def backward_kernel(levels, grad_scale, names, *refs):
    v = dict(zip(names, refs))
    replica, shard, core = place()
    other = 1 - core
    level = replica // 2
    mate = (replica + 1 - 2 * core, shard)
    above, below = (replica + 2, shard), (replica - 2, shard)
    f32 = jnp.float32
    bf16 = jnp.bfloat16
    order = (3, 1, 2)
    own_a, own_d, own_g = v["own_a"], v["own_d"], v["own_g"]
    sources = (v["pg"], v["pu"])

    def tokens(owner, c):
        return pl.ds(pl.multiple_of((c * 4 + owner) * 128, 128), 128)

    def exchange(a, d, p):
        rows = pl.ds(pl.multiple_of(p * 384, 384), 384)
        n = a * 4 + d
        return remote(
            sources[a].at[rows], own_g.at[pl.ds(a * 1536 + d * 384, 384)],
            v["xsend"].at[n], v["xrecv"].at[n], (replica, p),
        )

    fills = [
        None,
        pltpu.make_async_copy(v["pd"], own_d, v["in_sem"].at[1]),
    ]
    for a in range(2):
        rows = pl.ds(pl.multiple_of(shard * 384, 384), 384)
        fills.append(
            pltpu.make_async_copy(sources[a].at[rows], own_g.at[pl.ds(a * 1536, 384)], v["in_sem"].at[2 + a])
        )

    partial = (v["p_back"], v["p_out"])
    held, kept, parts = v["held"], v["kept"], v["parts"]

    def to_mate(a, d):
        t = peer_of(shard, d)
        n = a * 4 + d
        return remote(partial[a].at[tokens(t, other)], held.at[a, d],
                      v["csend"].at[n], v["crecv"].at[n], mate)

    def keep(a, d):
        return pltpu.make_async_copy(partial[a].at[tokens(peer_of(shard, d), core)], kept.at[a, d], v["keep_sem"].at[a * 4 + d])

    def to_owner(a, d):
        n = a * 3 + d - 1
        return remote(kept.at[a, d], parts.at[a, d - 1], v["psend"].at[n], v["precv"].at[n], (replica, peer_of(shard, d)))

    def pair_sums(a):
        for d in order:
            to_mate(a, d).wait_recv()
            keep(a, d).wait()

            def body(rows, carry):
                kept[a, d, rows, :] = (kept[a, d, rows, :].astype(f32) + held[a, d, rows, :].astype(f32)).astype(bf16)
                return carry

            row_loop(128, 32, body, 0)
            to_owner(a, d).start()

    def collect(a):
        to_mate(a, 0).wait_recv()
        keep(a, 0).wait()
        for d in order:
            to_owner(a, d).wait_recv()

    def full_sum(a, rows):
        total = kept[a, 0, rows, :].astype(f32) + held[a, 0, rows, :].astype(f32)
        for d in (1, 2, 3):
            total = total + parts[a, d - 1, rows, :].astype(f32)
        return total

    wide = ((v["hid"], v["hid_all"], 768), (v["prj"], v["prj_all"], 1024))
    narrow = ((v["ctx"], v["ctx_all"], 384), (v["nrm"], v["nrm_all"], 384))

    def block(out, owner, c):
        return out.at[tokens(owner, c)]

    def columns(ref, index, width):
        return ref.at[:, pl.ds(pl.multiple_of(index * width, width), width)]

    def wide_copy(a, d, same, source_core, owner, t):
        ref, out, width = wide[a]
        c = core if same else other
        n = (a * 4 + d) * 2 + (0 if same else 1)
        return remote(
            columns(ref, c, width), block(out, owner, source_core), v["gsend"].at[n], v["grecv"].at[n],
            (replica - core + c, t),
        )

    def narrow_copy(a, d, owner, t):
        ref, out, width = narrow[a]
        n = 16 + a * 4 + d
        return remote(columns(ref, t, width), block(out, owner, core), v["gsend"].at[n], v["grecv"].at[n], (replica, t))

    def onward(a, d, source, owner, c):
        out = narrow[a][1]
        n = a * 4 + d
        return remote(source, block(out, owner, c), v["fsend"].at[n], v["frecv"].at[n], mate)

    def own_narrow(a):
        ref, out, width = narrow[a]
        return pltpu.make_async_copy(columns(ref, shard, width), block(out, shard, core), v["local"].at[a])

    def own_wide(a):
        ref, out, width = wide[a]
        return pltpu.make_async_copy(columns(ref, core, width), block(out, shard, core), v["local"].at[2 + a])

    wbuf = v["wbuf"]
    load_out = pltpu.make_async_copy(v["wo"], wbuf.at[:, pl.ds(0, 1536)], v["local"].at[4])
    load_qkv = pltpu.make_async_copy(v["wq"], wbuf, v["local"].at[5])

    def stage_sums():
        pair_sums(0)
        for d in order:
            for a in range(2):
                narrow_copy(a, d, shard, peer_of(shard, d)).start()
        for d in (1, 2, 3):
            for a in range(2):
                exchange(a, d, peer_of(shard, d)).start()

    def stage_hidden():
        collect(0)
        gain = v["gain_two"][...]

        def body(rows, total):
            grad = full_sum(0, rows)
            hidden = v["hidden"][rows, :]
            inv = lax.rsqrt(jnp.mean(hidden * hidden, axis=-1, keepdims=True) + NORM_EPS)
            scaled = gain * grad
            out = v["cot"][rows, :].astype(f32) + inv * (
                scaled - hidden * inv * inv * jnp.mean(scaled * hidden, axis=-1, keepdims=True)
            )
            v["hgrad"][rows, :] = out
            v["hid"][rows, :] = out.astype(bf16)
            return total + jnp.sum(grad * hidden * inv, axis=0, keepdims=True)

        v["row_two"][...] = row_loop(128, 16, body, jnp.zeros((1, 1536), f32)) * grad_scale
        for d in (0,) + order:
            if d:
                wide_copy(0, d, True, core, shard, peer_of(shard, d)).start()
            wide_copy(0, d, False, core, shard, peer_of(shard, d)).start()
        own_wide(0).start()

    def stage_context():
        load_out.wait()
        for e in range(4):
            cols = pl.ds(e * 384, 384)
            v["cgrad"][:, cols] = dot_nt(v["hid"][...], wbuf[cols, 0:1536]).astype(bf16)
        load_qkv.start()

    def unrotated(x):
        return x * v["cos"][...] + pltpu.roll(x, HD // 2, 1) * v["sin"][...]

    def stage_heads(g, part):
        keys = v["key"][:, g * HD : (g + 1) * HD]
        values = v["val"][:, g * HD : (g + 1) * HD]
        causal = lax.broadcasted_iota(jnp.int32, (128, 128), 0) >= lax.broadcasted_iota(jnp.int32, (128, 128), 1)
        key_grad = jnp.zeros((128, HD), f32) if part == 0 else v["kv_sum"][0]
        value_grad = jnp.zeros((128, HD), f32) if part == 0 else v["kv_sum"][1]
        first_head = g * (HEADS // KV) + part * 2
        for h in range(first_head, first_head + 2):
            at = slice(h * HD, (h + 1) * HD)
            query = v["qry"][:, at]
            grad = v["cgrad"][:, at]
            scores = jnp.where(causal, dot_nt(query, keys) * SCORE_SCALE, -1e30)
            probs = jnp.exp(scores - v["lse"][:, h : h + 1]).astype(bf16)
            wide_probs = probs.astype(f32)
            prob_grad = dot_nt(grad, values)
            delta = jnp.sum(wide_probs * prob_grad, axis=-1, keepdims=True)
            score_grad = (wide_probs * (prob_grad - delta) * SCORE_SCALE).astype(bf16)
            v["prj"][:, at] = unrotated(jnp.dot(score_grad, keys, preferred_element_type=f32)).astype(bf16)
            key_grad = key_grad + dot_tn(score_grad, query)
            value_grad = value_grad + dot_tn(probs, grad)
        if part < 2:
            v["kv_sum"][0] = key_grad
            v["kv_sum"][1] = value_grad
            return
        first = HEADS * HD + g * HD
        v["prj"][:, first : first + HD] = unrotated(key_grad).astype(bf16)
        first = first + KV * HD
        v["prj"][:, first : first + HD] = value_grad.astype(bf16)

    def stage_send_projected():
        for d in (0,) + order:
            if d:
                wide_copy(1, d, True, core, shard, peer_of(shard, d)).start()
            wide_copy(1, d, False, core, shard, peer_of(shard, d)).start()
        own_wide(1).start()

    def stage_normed(part):
        if part == 0:
            load_qkv.wait()
        for e in (2 * part, 2 * part + 1):
            cols = pl.ds(e * 384, 384)
            v["ngrad"][:, cols] = dot_nt(v["prj"][...], wbuf[cols, :])

    vec, vin, vall = v["vec"], v["vin"], v["vall"]
    replicas = 2 * levels

    def vec_hop(d):
        return remote(vec.at[peer_of(shard, d)], vin.at[d - 1], v["vsend"].at[d - 1], v["vrecv"].at[d - 1],
                      (replica, peer_of(shard, d)))

    def vec_spread(j, slot):
        target = lax.rem(replica + j, replicas)
        return remote(v["vsum"], vall.at[slot], v["vsend"].at[2 + j], v["vrecv"].at[2 + j], (target, shard))

    def stage_input():
        gain = v["gain_one"][...]

        def body(rows, totals):
            total, bias = totals
            x = v["x"][rows, :].astype(f32)
            grad = v["ngrad"][rows, :]
            inv = lax.rsqrt(jnp.mean(x * x, axis=-1, keepdims=True) + NORM_EPS)
            scaled = gain * grad
            v["input_grad"][rows, :] = v["hgrad"][rows, :] + inv * (
                scaled - x * inv * inv * jnp.mean(scaled * x, axis=-1, keepdims=True)
            )
            return (
                total + jnp.sum(grad * x * inv, axis=0, keepdims=True),
                bias + jnp.sum(v["prj"][rows, :].astype(f32), axis=0, keepdims=True),
            )

        row_one, row_bias = row_loop(128, 16, body, (jnp.zeros((1, 1536), f32), jnp.zeros((1, 2048), f32)))
        row_one = row_one * grad_scale
        row_bias = row_bias * grad_scale
        row_two = v["row_two"][...]
        for s in range(4):
            vec[s, :, 0:384] = jnp.broadcast_to(row_one[:, s * 384 : (s + 1) * 384], (8, 384))
            vec[s, :, 384:896] = jnp.broadcast_to(row_bias[:, s * 512 : (s + 1) * 512], (8, 512))
            vec[s, :, 896:1280] = jnp.broadcast_to(row_two[:, s * 384 : (s + 1) * 384], (8, 384))
        for d in order:
            vec_hop(d).start()

    def stage_vec():
        total = vec[shard]
        for d in (1, 2, 3):
            vec_hop(d).wait_recv()
            total = total + vin[d - 1]
        v["vsum"][...] = total
        for j in range(1, replicas):
            vec_spread(j, replica).start()
        pair_sums(1)

    def stage_vec_out():
        vall[replica] = v["vsum"][...]
        for j in range(1, replicas):
            vec_spread(j, lax.rem(replica + replicas - j, replicas)).wait_recv()
        total = vall[0]
        for j in range(1, replicas):
            total = total + vall[j]
        v["vec_out"][...] = total

    def stage_output():
        collect(1)

        def body(rows, carry):
            v["block_out"][rows, :] = (v["hidden"][rows, :] + full_sum(1, rows)).astype(bf16)
            return carry

        row_loop(128, 32, body, 0)

    def stage_relay():
        for d in order:
            p = peer_of(shard, d)
            for a in range(2):
                narrow_copy(a, d, p, p).wait_recv()
                onward(a, d, block(narrow[a][1], p, core), p, core).start()

    def stage_gathered():
        for a in range(2):
            own_narrow(a).wait()
            own_wide(a).wait()
            for d in (0, 1, 2, 3):
                p = peer_of(shard, d)
                if d:
                    wide_copy(a, d, True, core, p, p).wait_recv()
                wide_copy(a, d, False, other, p, p).wait_recv()
                onward(a, d, block(narrow[a][1], p, other), p, other).wait_recv()

    def stage_attention_parts(j):
        at = pl.ds(j * 128, 128)
        own_a[at, 0:1024] = (dot_tn(v["nrm_all"][:, at], v["prj_all"][...]) * grad_scale).astype(bf16)
        own_a[at, 1024:1792] = (dot_tn(v["ctx_all"][:, at], v["hid_all"][...]) * grad_scale).astype(bf16)

    chunks = []
    for at in row_spans(DOWN_CHUNKS):
        chunks.append((own_d, v["low_d"], v["high_d"], at, ("fill", 1), lambda c, at=at: v["fd"].at[c, at]))
    for d in range(4):
        for a in range(2):
            for k in range(3):
                at = pl.ds(a * 1536 + d * 384 + k * CHUNK, CHUNK)
                dst = (v["fg"], v["fu"])[a]
                source = peer_of(shard, d)
                chunks.append((
                    own_g, v["low_g"], v["high_g"], at, ("fill", 2 + a) if d == 0 else ("x", a, d),
                    lambda c, k=k, dst=dst, source=source: dst.at[c, source, pl.ds(k * CHUNK, CHUNK)],
                ))
    for at in row_spans(ATTENTION_CHUNKS):
        chunks.append((own_a, v["low_a"], v["high_a"], at, ("none",), lambda c, at=at: v["fa"].at[c, at]))
    total = len(chunks)
    awaited = (set(), set())
    end = (level == 0) | (level == levels - 1)

    def arrive(what, seen):
        if what in seen or what[0] == "none":
            return
        seen.add(what)
        if what[0] == "fill":
            fills[what[1]].wait()
        else:
            exchange(what[1], what[2], peer_of(shard, what[2])).wait_recv()

    def up(k, ref):
        own, low, high, at, _, _ = chunks[k]
        return remote(ref.at[at], low.at[at], v["up_sem"].at[k], v["low_sem"].at[k], above)

    def down(k, ref):
        own, low, high, at, _, _ = chunks[k]
        return remote(ref.at[at], high.at[at], v["down_sem"].at[k], v["high_sem"].at[k], below)

    def add(k, *refs):
        own, _, _, at, _, _ = chunks[k]
        step = 32

        def body(j, carry):
            rows = pl.ds(pl.multiple_of(at.start + j * step, step), step)
            value = own[rows, :].astype(f32)
            for ref in refs:
                value = value + ref[rows, :].astype(f32)
            own[rows, :] = value.astype(own.dtype)
            return carry

        lax.fori_loop(0, at.size // step, body, 0)

    def finish(k, ref):
        _, _, _, at, _, dst = chunks[k]
        pltpu.make_async_copy(ref.at[at], dst(core), v["out_sem"].at[k]).start()
        remote(ref.at[at], dst(core), v["mate_send"].at[k], v["mate_recv"].at[k], mate).start()

    def root_of(k):
        return levels // 2 - 1 + k % 2

    def end_gather(k):
        own = chunks[k][0]

        @pl.when(end)
        def _():
            arrive(chunks[k][4], awaited[0])

        @pl.when(level == 0)
        def _():
            up(k, own).start()

        @pl.when(level == levels - 1)
        def _():
            down(k, own).start()

    def gather_step(k):
        own, low, high, at, what, _ = chunks[k]
        root = root_of(k)

        @pl.when(~end)
        def _():
            arrive(what, awaited[1])

        if root > 1:

            @pl.when((level > 0) & (level < root))
            def _():
                up(k, own).wait_recv()
                add(k, low)
                up(k, own).start()

        if root < levels - 2:

            @pl.when((level < levels - 1) & (level > root))
            def _():
                down(k, own).wait_recv()
                add(k, high)
                down(k, own).start()

    def root_step(k):
        own, low, high, at, _, _ = chunks[k]

        @pl.when(level == root_of(k))
        def _():
            up(k, own).wait_recv()
            down(k, own).wait_recv()
            add(k, low, high)
            up(k, own).start()
            down(k, own).start()
            finish(k, own)

    def spread_step(k):
        own, low, high, at, _, _ = chunks[k]
        root = root_of(k)

        if root > 1:

            @pl.when((level > 0) & (level < root))
            def _():
                down(k, own).wait_recv()
                down(k, high).start()
                finish(k, high)

        if root < levels - 2:

            @pl.when((level < levels - 1) & (level > root))
            def _():
                up(k, own).wait_recv()
                up(k, low).start()
                finish(k, low)

    def end_spread(k):
        own, low, high, at, _, _ = chunks[k]

        @pl.when(level == 0)
        def _():
            down(k, own).wait_recv()
            finish(k, high)

        @pl.when(level == levels - 1)
        def _():
            up(k, own).wait_recv()
            finish(k, low)

    for a in range(2):
        for d in order + (0,):
            to_mate(a, d).start()
            keep(a, d).start()
    for copy in fills[1:]:
        copy.start()
    load_out.start()
    for a in range(2):
        own_narrow(a).start()
        onward(a, 0, columns(narrow[a][0], shard, 384), shard, core).start()
    beside = {
        0: [stage_sums],
        11: [stage_hidden],
        12: [stage_context],
        13: [functools.partial(stage_heads, 0, 0)],
        14: [functools.partial(stage_heads, 0, 1), stage_relay],
        15: [functools.partial(stage_heads, 0, 2)],
        16: [functools.partial(stage_heads, 1, 0)],
        17: [functools.partial(stage_heads, 1, 1)],
        18: [functools.partial(stage_heads, 1, 2), stage_send_projected],
        19: [functools.partial(stage_normed, 0)],
        20: [functools.partial(stage_normed, 1)],
        21: [stage_input],
        22: [stage_vec],
        25: [stage_vec_out],
        29: [stage_output],
        30: [stage_gathered, functools.partial(stage_attention_parts, 0)],
        31: [functools.partial(stage_attention_parts, 1)],
        32: [functools.partial(stage_attention_parts, 2)],
    }
    stages = ((end_gather, 0), (gather_step, 6), (root_step, 10), (spread_step, 14), (end_spread, 20))
    for t in range(total + stages[-1][1]):
        for stage, lag in stages:
            if 0 <= t - lag < total:
                stage(t - lag)
        for stage in beside.get(t, ()):
            stage()
    for a in range(2):
        for d in (1, 2, 3):
            exchange(a, d, peer_of(shard, d)).wait_send()
    for k in range(total):
        own, low, high, at, _, dst = chunks[k]

        @pl.when(level < levels - 1)
        def _():
            up(k, own).wait_send()

        @pl.when(level > 0)
        def _():
            down(k, own).wait_send()

        pltpu.make_async_copy(own.at[at], dst(core), v["out_sem"].at[k]).wait()
        remote(own.at[at], dst(core), v["mate_send"].at[k], v["mate_recv"].at[k], mate).wait_send()
        remote(own.at[at], dst(1 - core), v["mate_send"].at[k], v["mate_recv"].at[k], mate).wait_recv()
    for a in range(2):
        for d in (0, 1, 2, 3):
            p = peer_of(shard, d)
            to_mate(a, d).wait_send()
            wide_copy(a, d, False, core, shard, p).wait_send()
            onward(a, d, block(narrow[a][1], p, core), p, core).wait_send()
            if d:
                to_owner(a, d).wait_send()
                wide_copy(a, d, True, core, shard, p).wait_send()
                narrow_copy(a, d, shard, p).wait_send()
    for d in order:
        vec_hop(d).wait_send()
    for j in range(1, replicas):
        vec_spread(j, replica).wait_send()


def backward(levels, grad_scale, **given):
    bf16 = jnp.bfloat16
    f32 = jnp.float32
    dma = pltpu.SemaphoreType.DMA
    in_hbm = ("pd", "pg", "pu", "p_back", "p_out", "wo", "wq")
    outs = {
        "fa": ((2, 384, 1792), bf16, any_spec()),
        "fd": ((2, WINDOW, 1536), bf16, any_spec()),
        "fg": ((2, 4, 384, WINDOW), bf16, any_spec()),
        "fu": ((2, 4, 384, WINDOW), bf16, any_spec()),
        "block_out": ((128, 1536), bf16, vmem_spec()),
        "input_grad": ((128, 1536), f32, vmem_spec()),
        "vec_out": ((8, 1280), f32, vmem_spec()),
    }
    scratch = {}
    for where in ("own", "low", "high"):
        scratch[where + "_a"] = pltpu.VMEM((384, 1792), bf16)
        scratch[where + "_d"] = pltpu.VMEM((WINDOW, 1536), bf16)
        scratch[where + "_g"] = pltpu.VMEM((3072, WINDOW), bf16)
    scratch |= {
        "held": pltpu.VMEM((2, 4, 128, 1536), bf16),
        "kept": pltpu.VMEM((2, 4, 128, 1536), bf16),
        "parts": pltpu.VMEM((2, 3, 128, 1536), bf16),
        "wbuf": pltpu.VMEM((1536, 2048), bf16),
        "hgrad": pltpu.VMEM((128, 1536), f32),
        "ngrad": pltpu.VMEM((128, 1536), f32),
        "hid": pltpu.VMEM((128, 1536), bf16),
        "cgrad": pltpu.VMEM((128, 1536), bf16),
        "prj": pltpu.VMEM((128, 2048), bf16),
        "ctx_all": pltpu.VMEM((1024, 384), bf16),
        "nrm_all": pltpu.VMEM((1024, 384), bf16),
        "hid_all": pltpu.VMEM((1024, 768), bf16),
        "prj_all": pltpu.VMEM((1024, 1024), bf16),
        "row_two": pltpu.VMEM((1, 1536), f32),
        "kv_sum": pltpu.VMEM((2, 128, HD), f32),
        "vec": pltpu.VMEM((4, 8, 1280), f32),
        "vin": pltpu.VMEM((3, 8, 1280), f32),
        "vsum": pltpu.VMEM((8, 1280), f32),
        "vall": pltpu.VMEM((2 * levels, 8, 1280), f32),
    }
    counts = {
        "xsend": 8, "xrecv": 8, "csend": 8, "crecv": 8, "keep_sem": 8, "psend": 6, "precv": 6, "gsend": 24, "grecv": 24,
        "fsend": 8, "frecv": 8, "local": 6, "in_sem": 4, "vsend": 2 + 2 * levels, "vrecv": 2 + 2 * levels,
    }
    for name in ("up_sem", "down_sem", "low_sem", "high_sem", "mate_send", "mate_recv", "out_sem"):
        counts[name] = CHUNKS
    scratch |= {name: dma((n,)) for name, n in counts.items()}
    return pl.pallas_call(
        functools.partial(backward_kernel, levels, grad_scale, (*given, *outs, *scratch)),
        out_shape=[jax.ShapeDtypeStruct(s, dt) for s, dt, _ in outs.values()],
        in_specs=[any_spec() if name in in_hbm else vmem_spec() for name in given],
        out_specs=[spec for _, _, spec in outs.values()],
        scratch_shapes=list(scratch.values()),
        compiler_params=pltpu.CompilerParams(has_side_effects=True, vmem_limit_bytes=67043328),
    )(*given.values())


def widen_kernel(x_gate, x_up, out_gate, out_up):
    f32 = jnp.float32
    for x, out in ((x_gate, out_gate), (x_up, out_up)):
        for s in range(4):
            for c in range(2):
                first = (s * 35) // 2 + c * 9
                rest = 1 if s % 2 == 1 and c == 0 else 0
                out[:, (first + rest) * 128 : (first + 9) * 128] = x[c, s][:, rest * 128 :].astype(f32)
        for s in (1, 3):
            first = (s * 35) // 2
            out[:, first * 128 : (first + 1) * 128] = x[1, s - 1][:, 1024:].astype(f32) + x[0, s][:, :128].astype(f32)


def widen(*sums):
    rows = 32
    return pl.pallas_call(
        widen_kernel,
        grid=(384 // rows,),
        out_shape=[jax.ShapeDtypeStruct((384, 8960), jnp.float32)] * 2,
        in_specs=[pl.BlockSpec((2, 4, rows, WINDOW), lambda i: (0, 0, i, 0))] * 2,
        out_specs=[pl.BlockSpec((rows, 8960), lambda i: (i, 0))] * 2,
    )(*sums)


def fast_device(
    block_input,
    attn_gain,
    qkv_weight,
    qkv_bias,
    out_weight,
    mlp_gain,
    gate_weight,
    up_weight,
    down_weight,
    cotangent,
):
    f32 = jnp.float32
    bf16 = jnp.bfloat16
    tok_count = block_input.shape[0]
    levels = lax.axis_size("replica") // 2
    grad_scale = 1.0 / math.sqrt(tok_count * lax.axis_size("replica") * lax.axis_size("shard"))
    q_width = HEADS * HD
    k_end = q_width + KV * HD
    replica, shard, core = place()
    cosine, sine_table = rope_tables(tok_count)
    small = jnp.zeros((16, 512), bf16)
    small = small.at[0, :384].set(attn_gain).at[1, :].set(qkv_bias).at[2, :384].set(mlp_gain)
    qkv_full, out_full, gate_own, up_own, cot_all, small_all = front(
        qkv_weight, out_weight, gate_weight, up_weight, cotangent, small
    )
    gain_one = small_all[:, 0, :384].reshape(-1).astype(f32)
    bias = small_all[:, 1, :].reshape(-1).astype(f32)
    gain_two = small_all[:, 2, :384].reshape(-1).astype(f32)

    xfloat = block_input.astype(f32)
    inv_one = lax.rsqrt(jnp.mean(xfloat * xfloat, axis=-1, keepdims=True) + NORM_EPS)
    normed_one = (xfloat * inv_one * gain_one).astype(bf16)
    projected = jnp.dot(normed_one, qkv_full, preferred_element_type=f32) + bias
    queries = rotate(projected[:, :q_width].reshape(tok_count, HEADS, HD), cosine, sine_table).astype(bf16)
    queries = queries.reshape(tok_count, KV, HEADS // KV, HD)
    key_rot = rotate(projected[:, q_width:k_end].reshape(tok_count, KV, HD), cosine, sine_table).astype(bf16)
    values = projected[:, k_end:].reshape(tok_count, KV, HD).astype(bf16)
    context, logsum = attend_forward(queries, key_rot, values)
    hidden_res = xfloat + jnp.dot(context, out_full, preferred_element_type=f32)
    inv_two = lax.rsqrt(jnp.mean(hidden_res * hidden_res, axis=-1, keepdims=True) + NORM_EPS)
    normed_two = (hidden_res * inv_two * gain_two).astype(bf16)

    normed_all = plane_gather(normed_two)
    first = window_start(shard, core)
    column = first + jnp.arange(WINDOW)
    owned = (column >= shard * 2240) & (column < (shard + 1) * 2240)
    padded = jnp.pad(down_weight, ((64, 64), (0, 0)))
    down_own = lax.dynamic_slice_in_dim(padded, first - shard * 2240 + 64, WINDOW, 0)
    gate_pre = jnp.dot(normed_all, gate_own, preferred_element_type=f32)
    up_pre = jnp.dot(normed_all, up_own, preferred_element_type=f32)
    sigmoid_gate = jax.nn.sigmoid(gate_pre)
    silu_gate = gate_pre * sigmoid_gate
    act_grad = jnp.einsum("td,fd->tf", cot_all, down_own, preferred_element_type=f32)
    activation = jnp.where(owned, silu_gate * up_pre, 0.0).astype(bf16)
    gate_delta = jnp.where(
        owned, act_grad * up_pre * sigmoid_gate * (1.0 + gate_pre * (1.0 - sigmoid_gate)), 0.0
    ).astype(bf16)
    up_delta = jnp.where(owned, act_grad * silu_gate, 0.0).astype(bf16)
    down_out = jnp.dot(activation, down_own, preferred_element_type=f32).astype(bf16)
    back = (
        jnp.einsum("tf,df->td", gate_delta, gate_own, preferred_element_type=f32)
        + jnp.einsum("tf,df->td", up_delta, up_own, preferred_element_type=f32)
    ).astype(bf16)
    gate_part = (jnp.einsum("td,tf->df", normed_all, gate_delta, preferred_element_type=f32) * grad_scale).astype(bf16)
    up_part = (jnp.einsum("td,tf->df", normed_all, up_delta, preferred_element_type=f32) * grad_scale).astype(bf16)
    down_part = (jnp.einsum("tf,td->fd", activation, cot_all, preferred_element_type=f32) * grad_scale).astype(bf16)

    sums = logsum.reshape(HEADS, tok_count).T
    sum_attn, sum_down, sum_gate, sum_up, block_output, input_grad, vectors = backward(
        levels,
        grad_scale,
        pd=down_part,
        pg=gate_part,
        pu=up_part,
        p_back=back,
        p_out=down_out,
        wo=out_full,
        wq=qkv_full,
        hidden=hidden_res,
        x=block_input,
        cot=cotangent,
        gain_one=gain_one[None, :],
        gain_two=gain_two[None, :],
        ctx=context,
        nrm=normed_one,
        qry=queries.reshape(tok_count, q_width),
        key=key_rot.reshape(tok_count, KV * HD),
        val=values.reshape(tok_count, KV * HD),
        lse=jnp.pad(sums, ((0, 0), (0, HD - HEADS))),
        cos=jnp.concatenate([cosine[:, 0], cosine[:, 0]], axis=1),
        sin=jnp.concatenate([sine_table[:, 0], -sine_table[:, 0]], axis=1),
    )
    gain_one_own, bias_own, gain_two_own = vectors[0, :384], vectors[0, 384:896], vectors[0, 896:]
    qkv_grad = jnp.concatenate([sum_attn[0, :, :1024], sum_attn[1, :, :1024]], axis=1).astype(f32)
    out_grad = jnp.concatenate([sum_attn[0, :, 1024:], sum_attn[1, :, 1024:]], axis=1).astype(f32)
    down_grad = lax.dynamic_slice_in_dim(
        sum_down.reshape(2 * WINDOW, 1536), lax.rem(shard, 2) * 64, 2240, 0
    ).astype(f32)
    gate_grad, up_grad = widen(sum_gate, sum_up)
    return (
        block_output,
        input_grad,
        gain_one_own,
        qkv_grad,
        bias_own,
        out_grad,
        gain_two_own,
        gate_grad,
        up_grad,
        down_grad,
    )


def solution(mesh):
    placed = (
        P(("replica", "shard"), None),
        P("shard"),
        P("shard", None),
        P("shard"),
        P("shard", None),
        P("shard"),
        P("shard", None),
        P("shard", None),
        P("shard", None),
        P(("replica", "shard"), None),
    )
    fits = mesh.shape["shard"] == 4 and mesh.shape["replica"] % 4 == 0
    per_device = fast_device if fits else general_device
    return jax.shard_map(
        per_device,
        mesh=mesh,
        in_specs=placed,
        out_specs=(
            P(("replica", "shard"), None),
            P(("replica", "shard"), None),
            P("shard"),
            P("shard", None),
            P("shard"),
            P("shard", None),
            P("shard"),
            P("shard", None),
            P("shard", None),
            P("shard", None),
        ),
        check_vma=False,
    )
```

```python
import functools
import math

import jax
import jax.numpy as jnp
from jax import lax
from jax.experimental import pallas as pl
from jax.experimental.pallas import tpu as pltpu
from jax.sharding import PartitionSpec as P

HEADS = 12
KV = 2
HD = 128


NORM_EPS = 1e-06
ROPE_BASE = 1000000.0


def rope_tables(tok_count):
    half_dim = HD // 2
    position = jnp.arange(tok_count, dtype=jnp.float32)
    inverse = ROPE_BASE ** (-(jnp.arange(half_dim, dtype=jnp.float32) * 2.0 / HD))
    angles = position[:, None] * inverse[None, :]
    return (jnp.cos(angles)[:, None, :], jnp.sin(angles)[:, None, :])


def rotate(vectors, cosine, sine_table):
    half_dim = HD // 2
    lower_half = vectors[..., :half_dim]
    upper_half = vectors[..., half_dim:]
    return jnp.concatenate(
        [
            lower_half * cosine - upper_half * sine_table,
            upper_half * cosine + lower_half * sine_table,
        ],
        axis=-1,
    )


def unrotate(grads, cosine, sine_table):
    half_dim = HD // 2
    lower_half = grads[..., :half_dim]
    upper_half = grads[..., half_dim:]
    return jnp.concatenate(
        [
            lower_half * cosine + upper_half * sine_table,
            upper_half * cosine - lower_half * sine_table,
        ],
        axis=-1,
    )


def block_scores(query_block, key_rot, first_row):
    row_count = query_block.shape[0]
    scores = jnp.einsum(
        "qkgd,skd->kgqs", query_block, key_rot, preferred_element_type=jnp.float32
    ) * (1.0 / math.sqrt(HD))
    causal = (first_row + jnp.arange(row_count))[:, None] >= jnp.arange(key_rot.shape[0])[None, :]
    return jnp.where(causal, scores, -1e30)


def block_layout(tok_count):
    block_rows = min(tok_count, 512)
    block_count = tok_count // block_rows
    firsts = jnp.arange(block_count, dtype=jnp.int32) * block_rows
    return (block_rows, block_count, firsts)


def attend_forward(queries, key_rot, values):
    tok_count = queries.shape[0]
    block_rows, block_count, firsts = block_layout(tok_count)
    query_blocks = queries.reshape(block_count, block_rows, KV, HEADS // KV, HD)

    def one_block(inputs):
        query_block, first_row = inputs
        scores = block_scores(query_block, key_rot, first_row)
        row_max = jnp.max(scores, axis=-1, keepdims=True)
        logsum = row_max + jnp.log(jnp.sum(jnp.exp(scores - row_max), axis=-1, keepdims=True))
        attn_probs = jnp.exp(scores - logsum).astype(jnp.bfloat16)
        context = jnp.einsum(
            "kgqs,skd->qkgd", attn_probs, values, preferred_element_type=jnp.float32
        ).astype(jnp.bfloat16)
        return (context, logsum)

    context, logsum = lax.map(one_block, (query_blocks, firsts))
    return (context.reshape(tok_count, HEADS * HD), logsum)


def attend_backward(queries, key_rot, values, logsum, context_grad):
    tok_count = queries.shape[0]
    block_rows, block_count, firsts = block_layout(tok_count)
    query_blocks = queries.reshape(block_count, block_rows, KV, HEADS // KV, HD)
    grad_blocks = context_grad.reshape(block_count, block_rows, KV, HEADS // KV, HD)
    score_scale = 1.0 / math.sqrt(HD)

    def one_block(running, inputs):
        key_total, value_total = running
        query_block, grad_block, log_block, first_row = inputs
        scores = block_scores(query_block, key_rot, first_row)
        attn_probs = jnp.exp(scores - log_block).astype(jnp.bfloat16)
        prob_grad = jnp.einsum(
            "qkgd,skd->kgqs", grad_block, values, preferred_element_type=jnp.float32
        )
        wide_probs = attn_probs.astype(jnp.float32)
        row_delta = jnp.sum(wide_probs * prob_grad, axis=-1, keepdims=True)
        score_grad = (wide_probs * (prob_grad - row_delta) * score_scale).astype(jnp.bfloat16)
        query_grad = jnp.einsum(
            "kgqs,skd->qkgd", score_grad, key_rot, preferred_element_type=jnp.float32
        )
        key_total = key_total + jnp.einsum(
            "kgqs,qkgd->skd", score_grad, query_block, preferred_element_type=jnp.float32
        )
        value_total = value_total + jnp.einsum(
            "kgqs,qkgd->skd", attn_probs, grad_block, preferred_element_type=jnp.float32
        )
        return ((key_total, value_total), query_grad)

    zero_keys = jnp.zeros((tok_count, KV, HD), jnp.float32)
    (key_grad, value_grad), query_grad = lax.scan(
        one_block, (zero_keys, zero_keys), (query_blocks, grad_blocks, logsum, firsts)
    )
    return (query_grad.reshape(tok_count, HEADS, HD), key_grad, value_grad)


def general_device(
    block_input,
    attn_gain,
    qkv_weight,
    qkv_bias,
    out_weight,
    mlp_gain,
    gate_weight,
    up_weight,
    down_weight,
    cotangent,
):
    f32 = jnp.float32
    bf16 = jnp.bfloat16
    tok_count = block_input.shape[0]
    grad_scale = 1.0 / math.sqrt(tok_count * lax.axis_size("replica") * lax.axis_size("shard"))
    q_width = HEADS * HD
    k_end = q_width + KV * HD
    cosine, sine_table = rope_tables(tok_count)
    attn_full = (
        lax.all_gather(attn_gain, "shard", axis=0, tiled=True),
        lax.all_gather(qkv_weight, "shard", axis=0, tiled=True),
        lax.all_gather(qkv_bias, "shard", axis=0, tiled=True),
        lax.all_gather(out_weight, "shard", axis=0, tiled=True),
    )
    gain_full, qkv_full, bias_full, out_full = attn_full
    gain_one = gain_full.astype(f32)
    xfloat = block_input.astype(f32)
    inv_one = lax.rsqrt(jnp.mean(xfloat * xfloat, axis=-1, keepdims=True) + NORM_EPS)
    normed_one = (xfloat * inv_one * gain_one).astype(bf16)
    projected = jnp.dot(normed_one, qkv_full, preferred_element_type=f32) + bias_full.astype(f32)
    queries = rotate(
        projected[:, :q_width].reshape(tok_count, HEADS, HD), cosine, sine_table
    ).astype(bf16)
    queries = queries.reshape(tok_count, KV, HEADS // KV, HD)
    key_rot = rotate(
        projected[:, q_width:k_end].reshape(tok_count, KV, HD), cosine, sine_table
    ).astype(bf16)
    values = projected[:, k_end:].reshape(tok_count, KV, HD).astype(bf16)
    context, logsum = attend_forward(queries, key_rot, values)
    hidden_res = xfloat + jnp.dot(context, out_full, preferred_element_type=f32)
    mlp_full = (
        lax.all_gather(mlp_gain, "shard", axis=0, tiled=True),
        lax.all_gather(gate_weight, "shard", axis=0, tiled=True),
        lax.all_gather(up_weight, "shard", axis=0, tiled=True),
        lax.all_gather(down_weight, "shard", axis=0, tiled=True),
    )
    gain_full_two, gate_full, up_full, down_full = mlp_full
    gain_two = gain_full_two.astype(f32)
    inv_two = lax.rsqrt(jnp.mean(hidden_res * hidden_res, axis=-1, keepdims=True) + NORM_EPS)
    normed_two = (hidden_res * inv_two * gain_two).astype(bf16)
    gate_pre = jnp.dot(normed_two, gate_full, preferred_element_type=f32)
    up_pre = jnp.dot(normed_two, up_full, preferred_element_type=f32)
    sigmoid_gate = jax.nn.sigmoid(gate_pre)
    silu_gate = gate_pre * sigmoid_gate
    activation = (silu_gate * up_pre).astype(bf16)
    block_output = (hidden_res + jnp.dot(activation, down_full, preferred_element_type=f32)).astype(
        bf16
    )
    act_grad = jnp.einsum("td,fd->tf", cotangent, down_full, preferred_element_type=f32)
    gate_delta = (
        act_grad * up_pre * sigmoid_gate * (1.0 + gate_pre * (1.0 - sigmoid_gate))
    ).astype(bf16)
    up_delta = (act_grad * silu_gate).astype(bf16)
    normed_two_grad = jnp.einsum(
        "tf,df->td", gate_delta, gate_full, preferred_element_type=f32
    ) + jnp.einsum("tf,df->td", up_delta, up_full, preferred_element_type=f32)
    gain_two_grad = jnp.sum(normed_two_grad * hidden_res * inv_two, axis=0) * grad_scale
    own_rows = (
        lax.all_to_all(activation, "shard", split_axis=1, concat_axis=0, tiled=True),
        lax.all_to_all(normed_two, "shard", split_axis=1, concat_axis=0, tiled=True),
    )
    group_act, group_normed = own_rows
    group_rows = (
        lax.all_gather(cotangent, "shard", axis=0, tiled=True),
        lax.all_gather(gate_delta, "shard", axis=0, tiled=True),
        lax.all_gather(up_delta, "shard", axis=0, tiled=True),
    )
    group_cot, group_gate, group_up = group_rows
    down_part = (
        jnp.einsum("tf,td->fd", group_act, group_cot, preferred_element_type=f32) * grad_scale
    )
    gate_own = (
        jnp.einsum("td,tf->df", group_normed, group_gate, preferred_element_type=f32) * grad_scale
    )
    up_own = (
        jnp.einsum("td,tf->df", group_normed, group_up, preferred_element_type=f32) * grad_scale
    )
    gain_two_own = lax.psum_scatter(gain_two_grad, "shard", scatter_dimension=0, tiled=True)
    mlp_parts = (gain_two_own, gate_own, up_own)
    hidden_grad = cotangent.astype(f32) + inv_two * (
        gain_two * normed_two_grad
        - hidden_res
        * inv_two
        * inv_two
        * jnp.mean(gain_two * normed_two_grad * hidden_res, axis=-1, keepdims=True)
    )
    hidden_low = hidden_grad.astype(bf16)
    context_grad = jnp.einsum("td,ed->te", hidden_low, out_full, preferred_element_type=f32).astype(
        bf16
    )
    query_grad, key_grad, value_grad = attend_backward(
        queries, key_rot, values, logsum, context_grad
    )
    query_grad = unrotate(query_grad, cosine, sine_table).reshape(tok_count, q_width)
    key_grad = unrotate(key_grad, cosine, sine_table).reshape(tok_count, KV * HD)
    projected_grad = jnp.concatenate(
        [query_grad, key_grad, value_grad.reshape(tok_count, KV * HD)], axis=-1
    ).astype(bf16)
    normed_one_grad = jnp.einsum("tc,dc->td", projected_grad, qkv_full, preferred_element_type=f32)
    gain_one_grad = jnp.sum(normed_one_grad * xfloat * inv_one, axis=0) * grad_scale
    bias_grad = jnp.sum(projected_grad.astype(f32), axis=0) * grad_scale
    own_attn = (
        lax.all_to_all(context, "shard", split_axis=1, concat_axis=0, tiled=True),
        lax.all_to_all(normed_one, "shard", split_axis=1, concat_axis=0, tiled=True),
    )
    group_context, group_normed_one = own_attn
    group_rows = (
        lax.all_gather(hidden_low, "shard", axis=0, tiled=True),
        lax.all_gather(projected_grad, "shard", axis=0, tiled=True),
    )
    group_hidden, group_projected = group_rows
    out_own = (
        jnp.einsum("te,td->ed", group_context, group_hidden, preferred_element_type=f32)
        * grad_scale
    )
    qkv_part = (
        jnp.einsum("td,tc->dc", group_normed_one, group_projected, preferred_element_type=f32)
        * grad_scale
    )
    small_parts = (
        lax.psum_scatter(gain_one_grad, "shard", scatter_dimension=0, tiled=True),
        lax.psum_scatter(bias_grad, "shard", scatter_dimension=0, tiled=True),
    )
    attn_parts = (small_parts[0], qkv_part, small_parts[1], out_own)
    input_grad = hidden_grad + inv_one * (
        gain_one * normed_one_grad
        - xfloat
        * inv_one
        * inv_one
        * jnp.mean(gain_one * normed_one_grad * xfloat, axis=-1, keepdims=True)
    )
    summed = lax.psum(
        (
            attn_parts[0],
            attn_parts[1],
            attn_parts[2],
            attn_parts[3],
            mlp_parts[0],
            mlp_parts[1],
            mlp_parts[2],
            down_part,
        ),
        "replica",
    )
    attn_parts = (summed[0], summed[1], summed[2], summed[3])
    mlp_parts = (summed[4], summed[5], summed[6])
    down_part = summed[7]
    return (
        block_output,
        input_grad,
        attn_parts[0],
        attn_parts[1],
        attn_parts[2],
        attn_parts[3],
        mlp_parts[0],
        mlp_parts[1],
        mlp_parts[2],
        down_part,
    )


MESH = pl.DeviceIdType.MESH
VMEM_BYTES = 62 * 2**20
WINDOW = 1152


def place():
    replica = lax.axis_index("replica")
    shard = lax.axis_index("shard")
    core = lax.rem(replica, 2)
    return replica, shard, core


def peer_of(shard, d):
    across = lax.rem(lax.rem(shard, 2) + d % 2, 2)
    up = lax.rem(shard // 2 + d // 2, 2)
    return up * 2 + across


def window_start(shard, core):
    return ((shard * 35) // 2 + core * 9) * 128


def remote(src, dst, send, recv, device):
    return pltpu.make_async_remote_copy(
        src_ref=src,
        dst_ref=dst,
        send_sem=send,
        recv_sem=recv,
        device_id=device,
        device_id_type=MESH,
    )


def any_spec():
    return pl.BlockSpec(memory_space=pl.ANY)


def vmem_spec():
    return pl.BlockSpec(memory_space=pltpu.VMEM)


def params(**more):
    return pltpu.CompilerParams(has_side_effects=True, vmem_limit_bytes=VMEM_BYTES, **more)


CHUNK = 128
DOWN_CHUNKS = (64, 64) + (128,) * 8
ATTENTION_CHUNKS = (64, 64, 64, 64, 32, 32, 32, 32)
CHUNKS = len(DOWN_CHUNKS) + 24 + len(ATTENTION_CHUNKS)
SCORE_SCALE = 1.0 / math.sqrt(HD)


def row_spans(sizes):
    return [pl.ds(sum(sizes[:k]), size) for k, size in enumerate(sizes)]


def dot_nt(a, b):
    return lax.dot_general(a, b, (((1,), (1,)), ((), ())), preferred_element_type=jnp.float32)


def dot_tn(a, b):
    return lax.dot_general(a, b, (((0,), (0,)), ((), ())), preferred_element_type=jnp.float32)


def row_loop(rows, step, body, init):
    return lax.fori_loop(0, rows // step, lambda j, c: body(pl.ds(pl.multiple_of(j * step, step), step), c), init)


TILES = ((0, 640, 192), (640, 512, 160))


def forward_kernel(grad_scale, names, *refs):
    v = dict(zip(names, refs))
    f32 = jnp.float32
    bf16 = jnp.bfloat16
    replica, shard, core = place()
    other = 1 - core
    mate = (replica + 1 - 2 * core, shard)
    odd = lax.rem(replica // 2, 2)
    pair = (replica + 2 - 4 * odd, shard)
    order = (3, 1, 2)
    first_unit = window_start(shard, core)
    q_buf, o_buf, g_buf, u_buf, d_buf = v["q_buf"], v["o_buf"], v["g_buf"], v["u_buf"], v["d_buf"]
    n_all, cot_all, small_all = v["n_all"], v["cot_all"], v["small_all"]

    def span(start, size):
        return pl.ds(pl.multiple_of(start, 16), size)

    def units(target, offset, width):
        return pl.ds(pl.multiple_of(window_start(target, core) + offset, 128), width)

    def tokens(owner, c):
        return pl.ds(pl.multiple_of((c * 4 + owner) * 128, 128), 128)

    weights = [
        (lambda t: v["wq"], q_buf, 192, 80, True),
        (lambda t: v["wo"], o_buf, 192, 80, True),
    ]
    for offset, width, shared in TILES:
        for name, buf in (("wg", g_buf), ("wu", u_buf)):
            weights.append((
                lambda t, name=name, offset=offset, width=width: v[name].at[:, units(t, offset, width)],
                buf.at[:, pl.ds(offset, width)], 384, shared, False,
            ))

    def base(i, c):
        return c * 192 if weights[i][4] else 0

    def hop(i, d, t, o):
        source, out, size, shared, _ = weights[i]
        first = base(i, core) + odd * shared
        n = i * 3 + d - 1
        return remote(
            source(t).at[span(first, size - shared)], out.at[span(o * 384 + first, size - shared)],
            v["send"].at[n], v["recv"].at[n], (replica, t),
        )

    def across(i, d, o, whose):
        _, out, size, shared, _ = weights[i]
        ref = out.at[span(o * 384 + base(i, core) + whose * (size - shared), shared)]
        n = i * 3 + d - 1
        return remote(ref, ref, v["zsend"].at[n], v["zrecv"].at[n], pair)

    def onward(i, d, o, c, shared_part):
        _, out, size, shared, _ = weights[i]
        first = o * 384 + base(i, c) + ((1 - odd) * (size - shared) if shared_part else odd * shared)
        ref = out.at[span(first, shared if shared_part else size - shared)]
        n = i * 3 + d - 1 + (6 if shared_part else 0)
        return remote(ref, ref, v["fsend"].at[n], v["frecv"].at[n], mate)

    row_sets = (cot_all, n_all)

    def row_hop(a, d, t, o):
        n = 18 + a * 3 + d - 1
        return remote(row_sets[a].at[tokens(shard, core)], row_sets[a].at[tokens(o, core)], v["send"].at[n], v["recv"].at[n],
                      (replica, t))

    def row_onward(a, d, o, c):
        n = 12 + a * 4 + d
        ref = row_sets[a].at[tokens(o, c)]
        return remote(ref, ref, v["fsend"].at[n], v["frecv"].at[n], mate)

    def small_hop(d, t, o):
        n = 24 + d - 1
        return remote(v["small"], small_all.at[o], v["send"].at[n], v["recv"].at[n], (replica, t))

    def send_rows(a):
        for d in order:
            row_hop(a, d, peer_of(shard, d), shard).start()
        row_onward(a, 0, shard, core).start()

    def take_rows(a):
        for d in order:
            p = peer_of(shard, d)
            row_hop(a, d, p, p).wait_recv()
            row_onward(a, d, p, core).start()

    def have_rows(a):
        for d in (0,) + order:
            row_onward(a, d, peer_of(shard, d), other).wait_recv()

    def send_weight(i):
        for d in order:
            hop(i, d, peer_of(shard, d), shard).start()

    def take(i, d):
        p = peer_of(shard, d)
        hop(i, d, p, p).wait_recv()
        across(i, d, p, odd).start()
        if weights[i][4]:
            onward(i, d, p, core, False).start()

    def take_shared(i):
        for d in order:
            p = peer_of(shard, d)
            across(i, d, p, 1 - odd).wait_recv()
            if weights[i][4]:
                onward(i, d, p, core, True).start()

    def have_other_half(i):
        for d in order:
            for part in (False, True):
                onward(i, d, peer_of(shard, d), other, part).wait_recv()

    rows = span(shard * 384, 384)
    loads = [
        pltpu.make_async_copy(v["cot"], cot_all.at[tokens(shard, core)], v["local"].at[0]),
        pltpu.make_async_copy(v["wq"], q_buf.at[rows], v["local"].at[1]),
        pltpu.make_async_copy(v["wo"], o_buf.at[rows], v["local"].at[2]),
        pltpu.make_async_copy(v["wg"].at[:, units(shard, 0, WINDOW)], g_buf.at[rows], v["local"].at[3]),
        pltpu.make_async_copy(v["wu"].at[:, units(shard, 0, WINDOW)], u_buf.at[rows], v["local"].at[4]),
    ]
    odd_chip = lax.rem(shard, 2)
    inside = odd_chip == core
    loads.append(pltpu.make_async_copy(
        v["wd"].at[span((1152 - 64 * odd_chip) * core, 1088)],
        d_buf.at[span(odd_chip * (1 - core) * 64, 1088)], v["local"].at[5],
    ))

    for d in order:
        small_hop(d, peer_of(shard, d), shard).start()
    send_weight(0)
    send_weight(1)
    for copy in loads:
        copy.start()
    rest = pltpu.make_async_copy(
        v["wd"].at[span((2176 - 1088) * core + 1088, 64)], d_buf.at[pl.ds(1088, 64)], v["local"].at[6]
    )

    @pl.when(inside)
    def _():
        rest.start()

    @pl.when(~inside)
    def _():
        d_buf[span(1088 - 1088 * odd_chip, 64), :] = jnp.zeros((64, 1536), bf16)

    loads[0].wait()
    send_rows(0)
    send_weight(2)
    send_weight(3)

    small_all[shard] = v["small"][...]
    for d in order:
        p = peer_of(shard, d)
        small_hop(d, p, p).wait_recv()

    def gathered(row, width):
        return jnp.concatenate([small_all[s, row : row + 1, 0:width].astype(f32) for s in range(4)], axis=1)

    gain_one = gathered(0, 384)

    def norm_body(at, carry):
        x = v["x"][at, :].astype(f32)
        inv = lax.rsqrt(jnp.mean(x * x, axis=-1, keepdims=True) + NORM_EPS)
        v["nrm"][at, :] = (x * inv * gain_one).astype(bf16)
        return carry

    row_loop(128, 16, norm_body, 0)
    for copy in loads[1:]:
        copy.wait()

    @pl.when(inside)
    def _():
        rest.wait()

    for i in (0, 1):
        for d in order:
            take(i, d)
    take_shared(0)
    have_other_half(0)
    keep_q = pltpu.make_async_copy(q_buf, v["q_full"], v["local"].at[7])
    keep_q.start()
    bias = gathered(1, 512)

    def rotated(x):
        return x * v["cos"][...] + pltpu.roll(x, HD // 2, 1) * v["sin"][...]

    def project(head, out, at, turn):
        cols = slice(head * HD, (head + 1) * HD)
        x = v["prj"][:, cols] + bias[:, cols]
        out[:, at * HD : (at + 1) * HD] = (rotated(x) if turn else x).astype(bf16)

    for n in range(4):
        v["prj"][:, n * 512 : (n + 1) * 512] = jnp.dot(
            v["nrm"][...], q_buf[:, n * 512 : (n + 1) * 512], preferred_element_type=f32
        )
    take_shared(1)
    for h in range(HEADS):
        project(h, v["qry"], h, True)
    for g in range(KV):
        project(HEADS + g, v["key"], g, True)
        project(HEADS + KV + g, v["val"], g, False)
    causal = lax.broadcasted_iota(jnp.int32, (128, 128), 0) >= lax.broadcasted_iota(jnp.int32, (128, 128), 1)
    v["lse"][...] = jnp.zeros((128, HD), f32)
    for h in range(HEADS):
        g = h // (HEADS // KV)
        at = slice(h * HD, (h + 1) * HD)
        scores = dot_nt(v["qry"][:, at], v["key"][:, g * HD : (g + 1) * HD]) * SCORE_SCALE
        scores = jnp.where(causal, scores, -1e30)
        row_max = jnp.max(scores, axis=-1, keepdims=True)
        logsum = row_max + jnp.log(jnp.sum(jnp.exp(scores - row_max), axis=-1, keepdims=True))
        v["lse"][:, h : h + 1] = logsum
        probs = jnp.exp(scores - logsum).astype(bf16)
        v["ctx"][:, at] = jnp.dot(probs, v["val"][:, g * HD : (g + 1) * HD], preferred_element_type=f32).astype(bf16)
    have_other_half(1)
    keep_o = pltpu.make_async_copy(o_buf, v["o_full"], v["local"].at[8])
    keep_o.start()
    for n in range(3):
        cols = slice(n * 512, (n + 1) * 512)
        v["hidden"][:, cols] = v["x"][:, cols].astype(f32) + jnp.dot(
            v["ctx"][...], o_buf[:, cols], preferred_element_type=f32
        )
    gain_two = gathered(2, 384)
    v["gains"][0:1, :] = gain_one
    v["gains"][1:2, :] = gain_two

    def norm_two(j, carry):
        at = pl.ds(pl.multiple_of(j * 16, 16), 16)
        hidden = v["hidden"][at, :]
        inv = lax.rsqrt(jnp.mean(hidden * hidden, axis=-1, keepdims=True) + NORM_EPS)
        n_all[span((core * 4 + shard) * 128 + j * 16, 16), :] = (hidden * inv * gain_two).astype(bf16)
        return carry

    lax.fori_loop(0, 8, norm_two, 0)
    send_rows(1)
    send_weight(4)
    send_weight(5)
    take_rows(0)
    for i in (2, 3):
        for d in order:
            take(i, d)
    take_rows(1)
    take_shared(2)
    take_shared(3)
    have_rows(0)
    have_rows(1)

    act, gate_delta, up_delta = v["act"], v["gd"], v["ud"]
    gs, us, gr = v["gs"], v["us"], v["gr"]
    pending = [(i, d) for i in (4, 5) for d in order]

    def service():
        if pending:
            take(*pending.pop(0))

    def products(offset, width, m):
        at = pl.ds(m * 512, 512)
        for n in range(0, width, 256):
            size = min(256, width - n)
            cols = pl.ds(offset + n, size)
            gs[:, n : n + size] = jnp.dot(n_all[at, :], g_buf[:, cols], preferred_element_type=f32)
            us[:, n : n + size] = jnp.dot(n_all[at, :], u_buf[:, cols], preferred_element_type=f32)
            gr[:, n : n + size] = dot_nt(cot_all[at, :], d_buf[cols, :])
        column = first_unit + offset + lax.broadcasted_iota(jnp.int32, (1, width), 1)
        owned = (column >= shard * 2240) & (column < (shard + 1) * 2240)

        def body(j, carry):
            part = pl.ds(pl.multiple_of(j * 16, 16), 16)
            to = pl.ds(pl.multiple_of(m * 512 + j * 16, 16), 16)
            cols = pl.ds(offset, width)
            gate, up, grad = gs[part, 0:width], us[part, 0:width], gr[part, 0:width]
            sig = jax.nn.sigmoid(gate)
            silu = gate * sig
            act[to, cols] = jnp.where(owned, silu * up, 0.0).astype(bf16)
            gate_delta[to, cols] = jnp.where(owned, grad * up * sig * (1.0 + gate * (1.0 - sig)), 0.0).astype(bf16)
            up_delta[to, cols] = jnp.where(owned, grad * silu, 0.0).astype(bf16)
            return carry

        lax.fori_loop(0, 32, body, 0)

    def transpose(src, cols, dst):
        def body(j, carry):
            at = pl.ds(pl.multiple_of(j * 128, 128), 128)
            dst[:, at] = src[at, cols].T
            return carry

        lax.fori_loop(0, 8, body, 0)

    outs = {}

    def write(name, buf, at, cols=None):
        n = 9 + len(outs)
        src = buf.at[at] if cols is None else buf.at[at, cols]
        dst = v[name].at[at] if cols is None else v[name].at[at, cols]
        copy = pltpu.make_async_copy(src, dst, v["local"].at[n])
        copy.start()
        outs[n] = copy

    for tile, (offset, width, _) in enumerate(TILES):
        cols = pl.ds(offset, width)
        for m in range(2):
            products(offset, width, m)
            service()
        transpose(act, cols, v["act_t"].at[pl.ds(0, width)])
        if tile == 0:
            transpose(n_all, pl.ds(0, 1536), v["n_t"])
        service()
        for n in range(3):
            out = pl.ds(n * 512, 512)
            v["d_grad"][cols, out] = (
                jnp.dot(v["act_t"][0:width, :], cot_all[:, out], preferred_element_type=f32) * grad_scale
            ).astype(bf16)
        write("pd", v["d_grad"], cols)
        service()
        for delta, buf, name in ((gate_delta, v["g_grad"], "pg"), (up_delta, v["u_grad"], "pu")):
            for m in range(3):
                at = pl.ds(m * 512, 512)
                buf[at, cols] = (
                    jnp.dot(v["n_t"][at, :], delta[:, cols], preferred_element_type=f32) * grad_scale
                ).astype(bf16)
            write(name, buf, pl.ds(0, 1536), cols)
            service()
        while pending:
            service()
        if tile == 0:
            take_shared(4)
            take_shared(5)
    keep_q.wait()
    keep_o.wait()
    for i in (0, 1):
        for d in order:
            p = peer_of(shard, d)
            hop(i, d, p, shard).wait_send()
            across(i, d, p, odd).wait_send()
            for part in (False, True):
                onward(i, d, p, core, part).wait_send()
    for m in range(2):
        at = pl.ds(m * 512, 512)
        for n in range(3):
            cols = pl.ds(n * 512, 512)
            q_buf[at, cols] = (dot_nt(gate_delta[at, :], g_buf[cols, :]) + dot_nt(up_delta[at, :], u_buf[cols, :])).astype(bf16)
        write("p_back", q_buf, at, pl.ds(0, 1536))
    for m in range(2):
        at = pl.ds(m * 512, 512)
        for n in range(3):
            cols = pl.ds(n * 512, 512)
            o_buf[at, cols] = jnp.dot(act[at, :], d_buf[:, cols], preferred_element_type=f32).astype(bf16)
        write("p_out", o_buf, at)
    for copy in outs.values():
        copy.wait()
    for d in order:
        p = peer_of(shard, d)
        small_hop(d, p, shard).wait_send()
        for i in (2, 3, 4, 5):
            hop(i, d, p, shard).wait_send()
            across(i, d, p, odd).wait_send()
        for a in range(2):
            row_hop(a, d, p, shard).wait_send()
    for a in range(2):
        for d in (0,) + order:
            row_onward(a, d, peer_of(shard, d), core).wait_send()


def forward(grad_scale, **given):
    bf16 = jnp.bfloat16
    f32 = jnp.float32
    dma = pltpu.SemaphoreType.DMA
    in_vmem = ("x", "small", "cos", "sin")
    outs = {
        "q_full": ((1536, 2048), bf16, any_spec()),
        "o_full": ((1536, 1536), bf16, any_spec()),
        "pd": ((WINDOW, 1536), bf16, any_spec()),
        "pg": ((1536, WINDOW), bf16, any_spec()),
        "pu": ((1536, WINDOW), bf16, any_spec()),
        "p_back": ((1024, 1536), bf16, any_spec()),
        "p_out": ((1024, 1536), bf16, any_spec()),
        "hidden": ((128, 1536), f32, vmem_spec()),
        "nrm": ((128, 1536), bf16, vmem_spec()),
        "ctx": ((128, 1536), bf16, vmem_spec()),
        "qry": ((128, 1536), bf16, vmem_spec()),
        "key": ((128, KV * HD), bf16, vmem_spec()),
        "val": ((128, KV * HD), bf16, vmem_spec()),
        "lse": ((128, HD), f32, vmem_spec()),
        "gains": ((8, 1536), f32, vmem_spec()),
    }
    scratch = {
        "q_buf": pltpu.VMEM((1536, 2048), bf16),
        "o_buf": pltpu.VMEM((1536, 1536), bf16),
        "g_buf": pltpu.VMEM((1536, WINDOW), bf16),
        "u_buf": pltpu.VMEM((1536, WINDOW), bf16),
        "d_buf": pltpu.VMEM((WINDOW, 1536), bf16),
        "n_all": pltpu.VMEM((1024, 1536), bf16),
        "n_t": pltpu.VMEM((1536, 1024), bf16),
        "cot_all": pltpu.VMEM((1024, 1536), bf16),
        "small_all": pltpu.VMEM((4, 16, 512), bf16),
        "prj": pltpu.VMEM((128, 2048), f32),
        "act": pltpu.VMEM((1024, WINDOW), bf16),
        "gd": pltpu.VMEM((1024, WINDOW), bf16),
        "ud": pltpu.VMEM((1024, WINDOW), bf16),
        "act_t": pltpu.VMEM((640, 1024), bf16),
        "gs": pltpu.VMEM((512, 640), f32),
        "us": pltpu.VMEM((512, 640), f32),
        "gr": pltpu.VMEM((512, 640), f32),
        "d_grad": pltpu.VMEM((WINDOW, 1536), bf16),
        "g_grad": pltpu.VMEM((1536, WINDOW), bf16),
        "u_grad": pltpu.VMEM((1536, WINDOW), bf16),
        "send": dma((27,)),
        "recv": dma((27,)),
        "zsend": dma((18,)),
        "zrecv": dma((18,)),
        "fsend": dma((20,)),
        "frecv": dma((20,)),
        "local": dma((20,)),
    }
    return dict(zip(outs, pl.pallas_call(
        functools.partial(forward_kernel, grad_scale, (*given, *outs, *scratch)),
        out_shape=[jax.ShapeDtypeStruct(s, dt) for s, dt, _ in outs.values()],
        in_specs=[vmem_spec() if name in in_vmem else any_spec() for name in given],
        out_specs=[spec for _, _, spec in outs.values()],
        scratch_shapes=list(scratch.values()),
        compiler_params=pltpu.CompilerParams(has_side_effects=True, vmem_limit_bytes=67043328),
    )(*given.values())))


def backward_kernel(levels, grad_scale, names, *refs):
    v = dict(zip(names, refs))
    replica, shard, core = place()
    other = 1 - core
    level = replica // 2
    mate = (replica + 1 - 2 * core, shard)
    above, below = (replica + 2, shard), (replica - 2, shard)
    f32 = jnp.float32
    bf16 = jnp.bfloat16
    order = (3, 1, 2)
    own_a, own_d, own_g = v["own_a"], v["own_d"], v["own_g"]
    sources = (v["pg"], v["pu"])

    def tokens(owner, c):
        return pl.ds(pl.multiple_of((c * 4 + owner) * 128, 128), 128)

    def exchange(a, d, p):
        rows = pl.ds(pl.multiple_of(p * 384, 384), 384)
        n = a * 4 + d
        return remote(
            sources[a].at[rows], own_g.at[pl.ds(a * 1536 + d * 384, 384)],
            v["xsend"].at[n], v["xrecv"].at[n], (replica, p),
        )

    fills = [
        None,
        pltpu.make_async_copy(v["pd"], own_d, v["in_sem"].at[1]),
    ]
    for a in range(2):
        rows = pl.ds(pl.multiple_of(shard * 384, 384), 384)
        fills.append(
            pltpu.make_async_copy(sources[a].at[rows], own_g.at[pl.ds(a * 1536, 384)], v["in_sem"].at[2 + a])
        )

    partial = (v["p_back"], v["p_out"])
    held, kept, parts = v["held"], v["kept"], v["parts"]

    def to_mate(a, d):
        t = peer_of(shard, d)
        n = a * 4 + d
        return remote(partial[a].at[tokens(t, other)], held.at[a, d],
                      v["csend"].at[n], v["crecv"].at[n], mate)

    def keep(a, d):
        return pltpu.make_async_copy(partial[a].at[tokens(peer_of(shard, d), core)], kept.at[a, d], v["keep_sem"].at[a * 4 + d])

    def to_owner(a, d):
        n = a * 3 + d - 1
        return remote(kept.at[a, d], parts.at[a, d - 1], v["psend"].at[n], v["precv"].at[n], (replica, peer_of(shard, d)))

    def pair_sums(a):
        for d in order:
            to_mate(a, d).wait_recv()
            keep(a, d).wait()

            def body(rows, carry):
                kept[a, d, rows, :] = (kept[a, d, rows, :].astype(f32) + held[a, d, rows, :].astype(f32)).astype(bf16)
                return carry

            row_loop(128, 32, body, 0)
            to_owner(a, d).start()

    def collect(a):
        to_mate(a, 0).wait_recv()
        keep(a, 0).wait()
        for d in order:
            to_owner(a, d).wait_recv()

    def full_sum(a, rows):
        total = kept[a, 0, rows, :].astype(f32) + held[a, 0, rows, :].astype(f32)
        for d in (1, 2, 3):
            total = total + parts[a, d - 1, rows, :].astype(f32)
        return total

    wide = ((v["hid"], v["hid_all"], 768), (v["prj"], v["prj_all"], 1024))
    narrow = ((v["ctx"], v["ctx_all"], 384), (v["nrm"], v["nrm_all"], 384))

    def block(out, owner, c):
        return out.at[tokens(owner, c)]

    def columns(ref, index, width):
        return ref.at[:, pl.ds(pl.multiple_of(index * width, width), width)]

    def wide_copy(a, d, same, source_core, owner, t):
        ref, out, width = wide[a]
        c = core if same else other
        n = (a * 4 + d) * 2 + (0 if same else 1)
        return remote(
            columns(ref, c, width), block(out, owner, source_core), v["gsend"].at[n], v["grecv"].at[n],
            (replica - core + c, t),
        )

    def narrow_copy(a, d, owner, t):
        ref, out, width = narrow[a]
        n = 16 + a * 4 + d
        return remote(columns(ref, t, width), block(out, owner, core), v["gsend"].at[n], v["grecv"].at[n], (replica, t))

    def onward(a, d, source, owner, c):
        out = narrow[a][1]
        n = a * 4 + d
        return remote(source, block(out, owner, c), v["fsend"].at[n], v["frecv"].at[n], mate)

    def own_narrow(a):
        ref, out, width = narrow[a]
        return pltpu.make_async_copy(columns(ref, shard, width), block(out, shard, core), v["local"].at[a])

    def own_wide(a):
        ref, out, width = wide[a]
        return pltpu.make_async_copy(columns(ref, core, width), block(out, shard, core), v["local"].at[2 + a])

    wbuf = v["wbuf"]
    load_out = pltpu.make_async_copy(v["wo"], wbuf.at[:, pl.ds(0, 1536)], v["local"].at[4])
    load_qkv = pltpu.make_async_copy(v["wq"], wbuf, v["local"].at[5])

    def stage_sums():
        pair_sums(0)
        for d in order:
            for a in range(2):
                narrow_copy(a, d, shard, peer_of(shard, d)).start()
        for d in (1, 2, 3):
            for a in range(2):
                exchange(a, d, peer_of(shard, d)).start()

    def stage_hidden():
        collect(0)
        gain = v["gain_two"][...]

        def body(rows, total):
            grad = full_sum(0, rows)
            hidden = v["hidden"][rows, :]
            inv = lax.rsqrt(jnp.mean(hidden * hidden, axis=-1, keepdims=True) + NORM_EPS)
            scaled = gain * grad
            out = v["cot"][rows, :].astype(f32) + inv * (
                scaled - hidden * inv * inv * jnp.mean(scaled * hidden, axis=-1, keepdims=True)
            )
            v["hgrad"][rows, :] = out
            v["hid"][rows, :] = out.astype(bf16)
            return total + jnp.sum(grad * hidden * inv, axis=0, keepdims=True)

        v["row_two"][...] = row_loop(128, 16, body, jnp.zeros((1, 1536), f32)) * grad_scale
        for d in (0,) + order:
            if d:
                wide_copy(0, d, True, core, shard, peer_of(shard, d)).start()
            wide_copy(0, d, False, core, shard, peer_of(shard, d)).start()
        own_wide(0).start()

    def stage_context():
        load_out.wait()
        for e in range(4):
            cols = pl.ds(e * 384, 384)
            v["cgrad"][:, cols] = dot_nt(v["hid"][...], wbuf[cols, 0:1536]).astype(bf16)
        load_qkv.start()

    def unrotated(x):
        return x * v["cos"][...] + pltpu.roll(x, HD // 2, 1) * v["sin"][...]

    def stage_heads(g, part):
        keys = v["key"][:, g * HD : (g + 1) * HD]
        values = v["val"][:, g * HD : (g + 1) * HD]
        causal = lax.broadcasted_iota(jnp.int32, (128, 128), 0) >= lax.broadcasted_iota(jnp.int32, (128, 128), 1)
        key_grad = jnp.zeros((128, HD), f32) if part == 0 else v["kv_sum"][0]
        value_grad = jnp.zeros((128, HD), f32) if part == 0 else v["kv_sum"][1]
        first_head = g * (HEADS // KV) + part * 2
        for h in range(first_head, first_head + 2):
            at = slice(h * HD, (h + 1) * HD)
            query = v["qry"][:, at]
            grad = v["cgrad"][:, at]
            scores = jnp.where(causal, dot_nt(query, keys) * SCORE_SCALE, -1e30)
            probs = jnp.exp(scores - v["lse"][:, h : h + 1]).astype(bf16)
            wide_probs = probs.astype(f32)
            prob_grad = dot_nt(grad, values)
            delta = jnp.sum(wide_probs * prob_grad, axis=-1, keepdims=True)
            score_grad = (wide_probs * (prob_grad - delta) * SCORE_SCALE).astype(bf16)
            v["prj"][:, at] = unrotated(jnp.dot(score_grad, keys, preferred_element_type=f32)).astype(bf16)
            key_grad = key_grad + dot_tn(score_grad, query)
            value_grad = value_grad + dot_tn(probs, grad)
        if part < 2:
            v["kv_sum"][0] = key_grad
            v["kv_sum"][1] = value_grad
            return
        first = HEADS * HD + g * HD
        v["prj"][:, first : first + HD] = unrotated(key_grad).astype(bf16)
        first = first + KV * HD
        v["prj"][:, first : first + HD] = value_grad.astype(bf16)

    def stage_send_projected():
        for d in (0,) + order:
            if d:
                wide_copy(1, d, True, core, shard, peer_of(shard, d)).start()
            wide_copy(1, d, False, core, shard, peer_of(shard, d)).start()
        own_wide(1).start()

    def stage_normed(part):
        if part == 0:
            load_qkv.wait()
        for e in (2 * part, 2 * part + 1):
            cols = pl.ds(e * 384, 384)
            v["ngrad"][:, cols] = dot_nt(v["prj"][...], wbuf[cols, :])

    vec, vin, vall = v["vec"], v["vin"], v["vall"]
    replicas = 2 * levels

    def vec_hop(d):
        return remote(vec.at[peer_of(shard, d)], vin.at[d - 1], v["vsend"].at[d - 1], v["vrecv"].at[d - 1],
                      (replica, peer_of(shard, d)))

    def vec_spread(j, slot):
        target = lax.rem(replica + j, replicas)
        return remote(v["vsum"], vall.at[slot], v["vsend"].at[2 + j], v["vrecv"].at[2 + j], (target, shard))

    def stage_input():
        gain = v["gain_one"][...]

        def body(rows, totals):
            total, bias = totals
            x = v["x"][rows, :].astype(f32)
            grad = v["ngrad"][rows, :]
            inv = lax.rsqrt(jnp.mean(x * x, axis=-1, keepdims=True) + NORM_EPS)
            scaled = gain * grad
            v["input_grad"][rows, :] = v["hgrad"][rows, :] + inv * (
                scaled - x * inv * inv * jnp.mean(scaled * x, axis=-1, keepdims=True)
            )
            return (
                total + jnp.sum(grad * x * inv, axis=0, keepdims=True),
                bias + jnp.sum(v["prj"][rows, :].astype(f32), axis=0, keepdims=True),
            )

        row_one, row_bias = row_loop(128, 16, body, (jnp.zeros((1, 1536), f32), jnp.zeros((1, 2048), f32)))
        row_one = row_one * grad_scale
        row_bias = row_bias * grad_scale
        row_two = v["row_two"][...]
        for s in range(4):
            vec[s, :, 0:384] = jnp.broadcast_to(row_one[:, s * 384 : (s + 1) * 384], (8, 384))
            vec[s, :, 384:896] = jnp.broadcast_to(row_bias[:, s * 512 : (s + 1) * 512], (8, 512))
            vec[s, :, 896:1280] = jnp.broadcast_to(row_two[:, s * 384 : (s + 1) * 384], (8, 384))
        for d in order:
            vec_hop(d).start()

    def stage_vec():
        total = vec[shard]
        for d in (1, 2, 3):
            vec_hop(d).wait_recv()
            total = total + vin[d - 1]
        v["vsum"][...] = total
        for j in range(1, replicas):
            vec_spread(j, replica).start()
        pair_sums(1)

    def stage_vec_out():
        vall[replica] = v["vsum"][...]
        for j in range(1, replicas):
            vec_spread(j, lax.rem(replica + replicas - j, replicas)).wait_recv()
        total = vall[0]
        for j in range(1, replicas):
            total = total + vall[j]
        v["vec_out"][...] = total

    def stage_output():
        collect(1)

        def body(rows, carry):
            v["block_out"][rows, :] = (v["hidden"][rows, :] + full_sum(1, rows)).astype(bf16)
            return carry

        row_loop(128, 32, body, 0)

    def stage_relay():
        for d in order:
            p = peer_of(shard, d)
            for a in range(2):
                narrow_copy(a, d, p, p).wait_recv()
                onward(a, d, block(narrow[a][1], p, core), p, core).start()

    def stage_gathered():
        for a in range(2):
            own_narrow(a).wait()
            own_wide(a).wait()
            for d in (0, 1, 2, 3):
                p = peer_of(shard, d)
                if d:
                    wide_copy(a, d, True, core, p, p).wait_recv()
                wide_copy(a, d, False, other, p, p).wait_recv()
                onward(a, d, block(narrow[a][1], p, other), p, other).wait_recv()

    def stage_attention_parts(j):
        at = pl.ds(j * 128, 128)
        own_a[at, 0:1024] = (dot_tn(v["nrm_all"][:, at], v["prj_all"][...]) * grad_scale).astype(bf16)
        own_a[at, 1024:1792] = (dot_tn(v["ctx_all"][:, at], v["hid_all"][...]) * grad_scale).astype(bf16)

    chunks = []
    for at in row_spans(DOWN_CHUNKS):
        chunks.append((own_d, v["low_d"], v["high_d"], at, ("fill", 1), lambda c, at=at: v["fd"].at[c, at]))
    for d in range(4):
        for a in range(2):
            for k in range(3):
                at = pl.ds(a * 1536 + d * 384 + k * CHUNK, CHUNK)
                dst = (v["fg"], v["fu"])[a]
                source = peer_of(shard, d)
                chunks.append((
                    own_g, v["low_g"], v["high_g"], at, ("fill", 2 + a) if d == 0 else ("x", a, d),
                    lambda c, k=k, dst=dst, source=source: dst.at[c, source, pl.ds(k * CHUNK, CHUNK)],
                ))
    for at in row_spans(ATTENTION_CHUNKS):
        chunks.append((own_a, v["low_a"], v["high_a"], at, ("none",), lambda c, at=at: v["fa"].at[c, at]))
    total = len(chunks)
    awaited = (set(), set())
    end = (level == 0) | (level == levels - 1)

    def arrive(what, seen):
        if what in seen or what[0] == "none":
            return
        seen.add(what)
        if what[0] == "fill":
            fills[what[1]].wait()
        else:
            exchange(what[1], what[2], peer_of(shard, what[2])).wait_recv()

    def up(k, ref):
        own, low, high, at, _, _ = chunks[k]
        return remote(ref.at[at], low.at[at], v["up_sem"].at[k], v["low_sem"].at[k], above)

    def down(k, ref):
        own, low, high, at, _, _ = chunks[k]
        return remote(ref.at[at], high.at[at], v["down_sem"].at[k], v["high_sem"].at[k], below)

    def add(k, *refs):
        own, _, _, at, _, _ = chunks[k]
        step = 32

        def body(j, carry):
            rows = pl.ds(pl.multiple_of(at.start + j * step, step), step)
            value = own[rows, :].astype(f32)
            for ref in refs:
                value = value + ref[rows, :].astype(f32)
            own[rows, :] = value.astype(own.dtype)
            return carry

        lax.fori_loop(0, at.size // step, body, 0)

    def finish(k, ref):
        _, _, _, at, _, dst = chunks[k]
        pltpu.make_async_copy(ref.at[at], dst(core), v["out_sem"].at[k]).start()
        remote(ref.at[at], dst(core), v["mate_send"].at[k], v["mate_recv"].at[k], mate).start()

    def root_of(k):
        return levels // 2 - 1 + k % 2

    def end_gather(k):
        own = chunks[k][0]

        @pl.when(end)
        def _():
            arrive(chunks[k][4], awaited[0])

        @pl.when(level == 0)
        def _():
            up(k, own).start()

        @pl.when(level == levels - 1)
        def _():
            down(k, own).start()

    def gather_step(k):
        own, low, high, at, what, _ = chunks[k]
        root = root_of(k)

        @pl.when(~end)
        def _():
            arrive(what, awaited[1])

        if root > 1:

            @pl.when((level > 0) & (level < root))
            def _():
                up(k, own).wait_recv()
                add(k, low)
                up(k, own).start()

        if root < levels - 2:

            @pl.when((level < levels - 1) & (level > root))
            def _():
                down(k, own).wait_recv()
                add(k, high)
                down(k, own).start()

    def root_step(k):
        own, low, high, at, _, _ = chunks[k]

        @pl.when(level == root_of(k))
        def _():
            up(k, own).wait_recv()
            down(k, own).wait_recv()
            add(k, low, high)
            up(k, own).start()
            down(k, own).start()
            finish(k, own)

    def spread_step(k):
        own, low, high, at, _, _ = chunks[k]
        root = root_of(k)

        if root > 1:

            @pl.when((level > 0) & (level < root))
            def _():
                down(k, own).wait_recv()
                down(k, high).start()
                finish(k, high)

        if root < levels - 2:

            @pl.when((level < levels - 1) & (level > root))
            def _():
                up(k, own).wait_recv()
                up(k, low).start()
                finish(k, low)

    def end_spread(k):
        own, low, high, at, _, _ = chunks[k]

        @pl.when(level == 0)
        def _():
            down(k, own).wait_recv()
            finish(k, high)

        @pl.when(level == levels - 1)
        def _():
            up(k, own).wait_recv()
            finish(k, low)

    for a in range(2):
        for d in order + (0,):
            to_mate(a, d).start()
            keep(a, d).start()
    for copy in fills[1:]:
        copy.start()
    load_out.start()
    for a in range(2):
        own_narrow(a).start()
        onward(a, 0, columns(narrow[a][0], shard, 384), shard, core).start()
    beside = {
        0: [stage_sums],
        11: [stage_hidden],
        12: [stage_context],
        13: [functools.partial(stage_heads, 0, 0)],
        14: [functools.partial(stage_heads, 0, 1), stage_relay],
        15: [functools.partial(stage_heads, 0, 2)],
        16: [functools.partial(stage_heads, 1, 0)],
        17: [functools.partial(stage_heads, 1, 1)],
        18: [functools.partial(stage_heads, 1, 2), stage_send_projected],
        19: [functools.partial(stage_normed, 0)],
        20: [functools.partial(stage_normed, 1)],
        21: [stage_input],
        22: [stage_vec],
        25: [stage_vec_out],
        29: [stage_output],
        30: [stage_gathered, functools.partial(stage_attention_parts, 0)],
        31: [functools.partial(stage_attention_parts, 1)],
        32: [functools.partial(stage_attention_parts, 2)],
    }
    stages = ((end_gather, 0), (gather_step, 6), (root_step, 10), (spread_step, 14), (end_spread, 20))
    for t in range(total + stages[-1][1]):
        for stage, lag in stages:
            if 0 <= t - lag < total:
                stage(t - lag)
        for stage in beside.get(t, ()):
            stage()
    for a in range(2):
        for d in (1, 2, 3):
            exchange(a, d, peer_of(shard, d)).wait_send()
    for k in range(total):
        own, low, high, at, _, dst = chunks[k]

        @pl.when(level < levels - 1)
        def _():
            up(k, own).wait_send()

        @pl.when(level > 0)
        def _():
            down(k, own).wait_send()

        pltpu.make_async_copy(own.at[at], dst(core), v["out_sem"].at[k]).wait()
        remote(own.at[at], dst(core), v["mate_send"].at[k], v["mate_recv"].at[k], mate).wait_send()
        remote(own.at[at], dst(1 - core), v["mate_send"].at[k], v["mate_recv"].at[k], mate).wait_recv()
    for a in range(2):
        for d in (0, 1, 2, 3):
            p = peer_of(shard, d)
            to_mate(a, d).wait_send()
            wide_copy(a, d, False, core, shard, p).wait_send()
            onward(a, d, block(narrow[a][1], p, core), p, core).wait_send()
            if d:
                to_owner(a, d).wait_send()
                wide_copy(a, d, True, core, shard, p).wait_send()
                narrow_copy(a, d, shard, p).wait_send()
    for d in order:
        vec_hop(d).wait_send()
    for j in range(1, replicas):
        vec_spread(j, replica).wait_send()


def backward(levels, grad_scale, **given):
    bf16 = jnp.bfloat16
    f32 = jnp.float32
    dma = pltpu.SemaphoreType.DMA
    in_hbm = ("pd", "pg", "pu", "p_back", "p_out", "wo", "wq")
    outs = {
        "fa": ((2, 384, 1792), bf16, any_spec()),
        "fd": ((2, WINDOW, 1536), bf16, any_spec()),
        "fg": ((2, 4, 384, WINDOW), bf16, any_spec()),
        "fu": ((2, 4, 384, WINDOW), bf16, any_spec()),
        "block_out": ((128, 1536), bf16, vmem_spec()),
        "input_grad": ((128, 1536), f32, vmem_spec()),
        "vec_out": ((8, 1280), f32, vmem_spec()),
    }
    scratch = {}
    for where in ("own", "low", "high"):
        scratch[where + "_a"] = pltpu.VMEM((384, 1792), bf16)
        scratch[where + "_d"] = pltpu.VMEM((WINDOW, 1536), bf16)
        scratch[where + "_g"] = pltpu.VMEM((3072, WINDOW), bf16)
    scratch |= {
        "held": pltpu.VMEM((2, 4, 128, 1536), bf16),
        "kept": pltpu.VMEM((2, 4, 128, 1536), bf16),
        "parts": pltpu.VMEM((2, 3, 128, 1536), bf16),
        "wbuf": pltpu.VMEM((1536, 2048), bf16),
        "hgrad": pltpu.VMEM((128, 1536), f32),
        "ngrad": pltpu.VMEM((128, 1536), f32),
        "hid": pltpu.VMEM((128, 1536), bf16),
        "cgrad": pltpu.VMEM((128, 1536), bf16),
        "prj": pltpu.VMEM((128, 2048), bf16),
        "ctx_all": pltpu.VMEM((1024, 384), bf16),
        "nrm_all": pltpu.VMEM((1024, 384), bf16),
        "hid_all": pltpu.VMEM((1024, 768), bf16),
        "prj_all": pltpu.VMEM((1024, 1024), bf16),
        "row_two": pltpu.VMEM((1, 1536), f32),
        "kv_sum": pltpu.VMEM((2, 128, HD), f32),
        "vec": pltpu.VMEM((4, 8, 1280), f32),
        "vin": pltpu.VMEM((3, 8, 1280), f32),
        "vsum": pltpu.VMEM((8, 1280), f32),
        "vall": pltpu.VMEM((2 * levels, 8, 1280), f32),
    }
    counts = {
        "xsend": 8, "xrecv": 8, "csend": 8, "crecv": 8, "keep_sem": 8, "psend": 6, "precv": 6, "gsend": 24, "grecv": 24,
        "fsend": 8, "frecv": 8, "local": 6, "in_sem": 4, "vsend": 2 + 2 * levels, "vrecv": 2 + 2 * levels,
    }
    for name in ("up_sem", "down_sem", "low_sem", "high_sem", "mate_send", "mate_recv", "out_sem"):
        counts[name] = CHUNKS
    scratch |= {name: dma((n,)) for name, n in counts.items()}
    return pl.pallas_call(
        functools.partial(backward_kernel, levels, grad_scale, (*given, *outs, *scratch)),
        out_shape=[jax.ShapeDtypeStruct(s, dt) for s, dt, _ in outs.values()],
        in_specs=[any_spec() if name in in_hbm else vmem_spec() for name in given],
        out_specs=[spec for _, _, spec in outs.values()],
        scratch_shapes=list(scratch.values()),
        compiler_params=pltpu.CompilerParams(has_side_effects=True, vmem_limit_bytes=67043328),
    )(*given.values())


def widen_kernel(x_gate, x_up, out_gate, out_up):
    f32 = jnp.float32
    for x, out in ((x_gate, out_gate), (x_up, out_up)):
        for s in range(4):
            for c in range(2):
                first = (s * 35) // 2 + c * 9
                rest = 1 if s % 2 == 1 and c == 0 else 0
                out[:, (first + rest) * 128 : (first + 9) * 128] = x[c, s][:, rest * 128 :].astype(f32)
        for s in (1, 3):
            first = (s * 35) // 2
            out[:, first * 128 : (first + 1) * 128] = x[1, s - 1][:, 1024:].astype(f32) + x[0, s][:, :128].astype(f32)


def widen(*sums):
    rows = 32
    return pl.pallas_call(
        widen_kernel,
        grid=(384 // rows,),
        out_shape=[jax.ShapeDtypeStruct((384, 8960), jnp.float32)] * 2,
        in_specs=[pl.BlockSpec((2, 4, rows, WINDOW), lambda i: (0, 0, i, 0))] * 2,
        out_specs=[pl.BlockSpec((rows, 8960), lambda i: (i, 0))] * 2,
    )(*sums)


def fast_device(
    block_input,
    attn_gain,
    qkv_weight,
    qkv_bias,
    out_weight,
    mlp_gain,
    gate_weight,
    up_weight,
    down_weight,
    cotangent,
):
    f32 = jnp.float32
    tok_count = block_input.shape[0]
    levels = lax.axis_size("replica") // 2
    grad_scale = 1.0 / math.sqrt(tok_count * lax.axis_size("replica") * lax.axis_size("shard"))
    shard = lax.axis_index("shard")
    cosine, sine_table = rope_tables(tok_count)
    small = jnp.zeros((16, 512), jnp.bfloat16)
    small = small.at[0, :384].set(attn_gain).at[1, :].set(qkv_bias).at[2, :384].set(mlp_gain)
    twice = jnp.concatenate([cosine[:, 0], cosine[:, 0]], axis=1)
    turn = jnp.concatenate([-sine_table[:, 0], sine_table[:, 0]], axis=1)
    got = forward(
        grad_scale,
        x=block_input,
        small=small,
        cos=twice,
        sin=turn,
        wq=qkv_weight,
        wo=out_weight,
        wg=gate_weight,
        wu=up_weight,
        wd=down_weight,
        cot=cotangent,
    )
    sum_attn, sum_down, sum_gate, sum_up, block_output, input_grad, vectors = backward(
        levels,
        grad_scale,
        pd=got["pd"],
        pg=got["pg"],
        pu=got["pu"],
        p_back=got["p_back"],
        p_out=got["p_out"],
        wo=got["o_full"],
        wq=got["q_full"],
        hidden=got["hidden"],
        x=block_input,
        cot=cotangent,
        gain_one=got["gains"][0:1],
        gain_two=got["gains"][1:2],
        ctx=got["ctx"],
        nrm=got["nrm"],
        qry=got["qry"],
        key=got["key"],
        val=got["val"],
        lse=got["lse"],
        cos=twice,
        sin=-turn,
    )
    gain_one_own, bias_own, gain_two_own = vectors[0, :384], vectors[0, 384:896], vectors[0, 896:]
    qkv_grad = jnp.concatenate([sum_attn[0, :, :1024], sum_attn[1, :, :1024]], axis=1).astype(f32)
    out_grad = jnp.concatenate([sum_attn[0, :, 1024:], sum_attn[1, :, 1024:]], axis=1).astype(f32)
    down_grad = lax.dynamic_slice_in_dim(
        sum_down.reshape(2 * WINDOW, 1536), lax.rem(shard, 2) * 64, 2240, 0
    ).astype(f32)
    gate_grad, up_grad = widen(sum_gate, sum_up)
    return (
        block_output,
        input_grad,
        gain_one_own,
        qkv_grad,
        bias_own,
        out_grad,
        gain_two_own,
        gate_grad,
        up_grad,
        down_grad,
    )


def solution(mesh):
    placed = (
        P(("replica", "shard"), None),
        P("shard"),
        P("shard", None),
        P("shard"),
        P("shard", None),
        P("shard"),
        P("shard", None),
        P("shard", None),
        P("shard", None),
        P(("replica", "shard"), None),
    )
    fits = mesh.shape["shard"] == 4 and mesh.shape["replica"] % 4 == 0
    per_device = fast_device if fits else general_device
    return jax.shard_map(
        per_device,
        mesh=mesh,
        in_specs=placed,
        out_specs=(
            P(("replica", "shard"), None),
            P(("replica", "shard"), None),
            P("shard"),
            P("shard", None),
            P("shard"),
            P("shard", None),
            P("shard"),
            P("shard", None),
            P("shard", None),
            P("shard", None),
        ),
        check_vma=False,
    )
```

```python
import functools
import math

import jax
import jax.numpy as jnp
from jax import lax
from jax.experimental import pallas as pl
from jax.experimental.pallas import tpu as pltpu
from jax.sharding import PartitionSpec as P

HEADS = 12
KV = 2
HD = 128


NORM_EPS = 1e-06
ROPE_BASE = 1000000.0


def rope_tables(tok_count):
    half_dim = HD // 2
    position = jnp.arange(tok_count, dtype=jnp.float32)
    inverse = ROPE_BASE ** (-(jnp.arange(half_dim, dtype=jnp.float32) * 2.0 / HD))
    angles = position[:, None] * inverse[None, :]
    return (jnp.cos(angles)[:, None, :], jnp.sin(angles)[:, None, :])


def rotate(vectors, cosine, sine_table):
    half_dim = HD // 2
    lower_half = vectors[..., :half_dim]
    upper_half = vectors[..., half_dim:]
    return jnp.concatenate(
        [
            lower_half * cosine - upper_half * sine_table,
            upper_half * cosine + lower_half * sine_table,
        ],
        axis=-1,
    )


def unrotate(grads, cosine, sine_table):
    half_dim = HD // 2
    lower_half = grads[..., :half_dim]
    upper_half = grads[..., half_dim:]
    return jnp.concatenate(
        [
            lower_half * cosine + upper_half * sine_table,
            upper_half * cosine - lower_half * sine_table,
        ],
        axis=-1,
    )


def block_scores(query_block, key_rot, first_row):
    row_count = query_block.shape[0]
    scores = jnp.einsum(
        "qkgd,skd->kgqs", query_block, key_rot, preferred_element_type=jnp.float32
    ) * (1.0 / math.sqrt(HD))
    causal = (first_row + jnp.arange(row_count))[:, None] >= jnp.arange(key_rot.shape[0])[None, :]
    return jnp.where(causal, scores, -1e30)


def block_layout(tok_count):
    block_rows = min(tok_count, 512)
    block_count = tok_count // block_rows
    firsts = jnp.arange(block_count, dtype=jnp.int32) * block_rows
    return (block_rows, block_count, firsts)


def attend_forward(queries, key_rot, values):
    tok_count = queries.shape[0]
    block_rows, block_count, firsts = block_layout(tok_count)
    query_blocks = queries.reshape(block_count, block_rows, KV, HEADS // KV, HD)

    def one_block(inputs):
        query_block, first_row = inputs
        scores = block_scores(query_block, key_rot, first_row)
        row_max = jnp.max(scores, axis=-1, keepdims=True)
        logsum = row_max + jnp.log(jnp.sum(jnp.exp(scores - row_max), axis=-1, keepdims=True))
        attn_probs = jnp.exp(scores - logsum).astype(jnp.bfloat16)
        context = jnp.einsum(
            "kgqs,skd->qkgd", attn_probs, values, preferred_element_type=jnp.float32
        ).astype(jnp.bfloat16)
        return (context, logsum)

    context, logsum = lax.map(one_block, (query_blocks, firsts))
    return (context.reshape(tok_count, HEADS * HD), logsum)


def attend_backward(queries, key_rot, values, logsum, context_grad):
    tok_count = queries.shape[0]
    block_rows, block_count, firsts = block_layout(tok_count)
    query_blocks = queries.reshape(block_count, block_rows, KV, HEADS // KV, HD)
    grad_blocks = context_grad.reshape(block_count, block_rows, KV, HEADS // KV, HD)
    score_scale = 1.0 / math.sqrt(HD)

    def one_block(running, inputs):
        key_total, value_total = running
        query_block, grad_block, log_block, first_row = inputs
        scores = block_scores(query_block, key_rot, first_row)
        attn_probs = jnp.exp(scores - log_block).astype(jnp.bfloat16)
        prob_grad = jnp.einsum(
            "qkgd,skd->kgqs", grad_block, values, preferred_element_type=jnp.float32
        )
        wide_probs = attn_probs.astype(jnp.float32)
        row_delta = jnp.sum(wide_probs * prob_grad, axis=-1, keepdims=True)
        score_grad = (wide_probs * (prob_grad - row_delta) * score_scale).astype(jnp.bfloat16)
        query_grad = jnp.einsum(
            "kgqs,skd->qkgd", score_grad, key_rot, preferred_element_type=jnp.float32
        )
        key_total = key_total + jnp.einsum(
            "kgqs,qkgd->skd", score_grad, query_block, preferred_element_type=jnp.float32
        )
        value_total = value_total + jnp.einsum(
            "kgqs,qkgd->skd", attn_probs, grad_block, preferred_element_type=jnp.float32
        )
        return ((key_total, value_total), query_grad)

    zero_keys = jnp.zeros((tok_count, KV, HD), jnp.float32)
    (key_grad, value_grad), query_grad = lax.scan(
        one_block, (zero_keys, zero_keys), (query_blocks, grad_blocks, logsum, firsts)
    )
    return (query_grad.reshape(tok_count, HEADS, HD), key_grad, value_grad)


def general_device(
    block_input,
    attn_gain,
    qkv_weight,
    qkv_bias,
    out_weight,
    mlp_gain,
    gate_weight,
    up_weight,
    down_weight,
    cotangent,
):
    f32 = jnp.float32
    bf16 = jnp.bfloat16
    tok_count = block_input.shape[0]
    grad_scale = 1.0 / math.sqrt(tok_count * lax.axis_size("replica") * lax.axis_size("shard"))
    q_width = HEADS * HD
    k_end = q_width + KV * HD
    cosine, sine_table = rope_tables(tok_count)
    attn_full = (
        lax.all_gather(attn_gain, "shard", axis=0, tiled=True),
        lax.all_gather(qkv_weight, "shard", axis=0, tiled=True),
        lax.all_gather(qkv_bias, "shard", axis=0, tiled=True),
        lax.all_gather(out_weight, "shard", axis=0, tiled=True),
    )
    gain_full, qkv_full, bias_full, out_full = attn_full
    gain_one = gain_full.astype(f32)
    xfloat = block_input.astype(f32)
    inv_one = lax.rsqrt(jnp.mean(xfloat * xfloat, axis=-1, keepdims=True) + NORM_EPS)
    normed_one = (xfloat * inv_one * gain_one).astype(bf16)
    projected = jnp.dot(normed_one, qkv_full, preferred_element_type=f32) + bias_full.astype(f32)
    queries = rotate(
        projected[:, :q_width].reshape(tok_count, HEADS, HD), cosine, sine_table
    ).astype(bf16)
    queries = queries.reshape(tok_count, KV, HEADS // KV, HD)
    key_rot = rotate(
        projected[:, q_width:k_end].reshape(tok_count, KV, HD), cosine, sine_table
    ).astype(bf16)
    values = projected[:, k_end:].reshape(tok_count, KV, HD).astype(bf16)
    context, logsum = attend_forward(queries, key_rot, values)
    hidden_res = xfloat + jnp.dot(context, out_full, preferred_element_type=f32)
    mlp_full = (
        lax.all_gather(mlp_gain, "shard", axis=0, tiled=True),
        lax.all_gather(gate_weight, "shard", axis=0, tiled=True),
        lax.all_gather(up_weight, "shard", axis=0, tiled=True),
        lax.all_gather(down_weight, "shard", axis=0, tiled=True),
    )
    gain_full_two, gate_full, up_full, down_full = mlp_full
    gain_two = gain_full_two.astype(f32)
    inv_two = lax.rsqrt(jnp.mean(hidden_res * hidden_res, axis=-1, keepdims=True) + NORM_EPS)
    normed_two = (hidden_res * inv_two * gain_two).astype(bf16)
    gate_pre = jnp.dot(normed_two, gate_full, preferred_element_type=f32)
    up_pre = jnp.dot(normed_two, up_full, preferred_element_type=f32)
    sigmoid_gate = jax.nn.sigmoid(gate_pre)
    silu_gate = gate_pre * sigmoid_gate
    activation = (silu_gate * up_pre).astype(bf16)
    block_output = (hidden_res + jnp.dot(activation, down_full, preferred_element_type=f32)).astype(
        bf16
    )
    act_grad = jnp.einsum("td,fd->tf", cotangent, down_full, preferred_element_type=f32)
    gate_delta = (
        act_grad * up_pre * sigmoid_gate * (1.0 + gate_pre * (1.0 - sigmoid_gate))
    ).astype(bf16)
    up_delta = (act_grad * silu_gate).astype(bf16)
    normed_two_grad = jnp.einsum(
        "tf,df->td", gate_delta, gate_full, preferred_element_type=f32
    ) + jnp.einsum("tf,df->td", up_delta, up_full, preferred_element_type=f32)
    gain_two_grad = jnp.sum(normed_two_grad * hidden_res * inv_two, axis=0) * grad_scale
    own_rows = (
        lax.all_to_all(activation, "shard", split_axis=1, concat_axis=0, tiled=True),
        lax.all_to_all(normed_two, "shard", split_axis=1, concat_axis=0, tiled=True),
    )
    group_act, group_normed = own_rows
    group_rows = (
        lax.all_gather(cotangent, "shard", axis=0, tiled=True),
        lax.all_gather(gate_delta, "shard", axis=0, tiled=True),
        lax.all_gather(up_delta, "shard", axis=0, tiled=True),
    )
    group_cot, group_gate, group_up = group_rows
    down_part = (
        jnp.einsum("tf,td->fd", group_act, group_cot, preferred_element_type=f32) * grad_scale
    )
    gate_own = (
        jnp.einsum("td,tf->df", group_normed, group_gate, preferred_element_type=f32) * grad_scale
    )
    up_own = (
        jnp.einsum("td,tf->df", group_normed, group_up, preferred_element_type=f32) * grad_scale
    )
    gain_two_own = lax.psum_scatter(gain_two_grad, "shard", scatter_dimension=0, tiled=True)
    mlp_parts = (gain_two_own, gate_own, up_own)
    hidden_grad = cotangent.astype(f32) + inv_two * (
        gain_two * normed_two_grad
        - hidden_res
        * inv_two
        * inv_two
        * jnp.mean(gain_two * normed_two_grad * hidden_res, axis=-1, keepdims=True)
    )
    hidden_low = hidden_grad.astype(bf16)
    context_grad = jnp.einsum("td,ed->te", hidden_low, out_full, preferred_element_type=f32).astype(
        bf16
    )
    query_grad, key_grad, value_grad = attend_backward(
        queries, key_rot, values, logsum, context_grad
    )
    query_grad = unrotate(query_grad, cosine, sine_table).reshape(tok_count, q_width)
    key_grad = unrotate(key_grad, cosine, sine_table).reshape(tok_count, KV * HD)
    projected_grad = jnp.concatenate(
        [query_grad, key_grad, value_grad.reshape(tok_count, KV * HD)], axis=-1
    ).astype(bf16)
    normed_one_grad = jnp.einsum("tc,dc->td", projected_grad, qkv_full, preferred_element_type=f32)
    gain_one_grad = jnp.sum(normed_one_grad * xfloat * inv_one, axis=0) * grad_scale
    bias_grad = jnp.sum(projected_grad.astype(f32), axis=0) * grad_scale
    own_attn = (
        lax.all_to_all(context, "shard", split_axis=1, concat_axis=0, tiled=True),
        lax.all_to_all(normed_one, "shard", split_axis=1, concat_axis=0, tiled=True),
    )
    group_context, group_normed_one = own_attn
    group_rows = (
        lax.all_gather(hidden_low, "shard", axis=0, tiled=True),
        lax.all_gather(projected_grad, "shard", axis=0, tiled=True),
    )
    group_hidden, group_projected = group_rows
    out_own = (
        jnp.einsum("te,td->ed", group_context, group_hidden, preferred_element_type=f32)
        * grad_scale
    )
    qkv_part = (
        jnp.einsum("td,tc->dc", group_normed_one, group_projected, preferred_element_type=f32)
        * grad_scale
    )
    small_parts = (
        lax.psum_scatter(gain_one_grad, "shard", scatter_dimension=0, tiled=True),
        lax.psum_scatter(bias_grad, "shard", scatter_dimension=0, tiled=True),
    )
    attn_parts = (small_parts[0], qkv_part, small_parts[1], out_own)
    input_grad = hidden_grad + inv_one * (
        gain_one * normed_one_grad
        - xfloat
        * inv_one
        * inv_one
        * jnp.mean(gain_one * normed_one_grad * xfloat, axis=-1, keepdims=True)
    )
    summed = lax.psum(
        (
            attn_parts[0],
            attn_parts[1],
            attn_parts[2],
            attn_parts[3],
            mlp_parts[0],
            mlp_parts[1],
            mlp_parts[2],
            down_part,
        ),
        "replica",
    )
    attn_parts = (summed[0], summed[1], summed[2], summed[3])
    mlp_parts = (summed[4], summed[5], summed[6])
    down_part = summed[7]
    return (
        block_output,
        input_grad,
        attn_parts[0],
        attn_parts[1],
        attn_parts[2],
        attn_parts[3],
        mlp_parts[0],
        mlp_parts[1],
        mlp_parts[2],
        down_part,
    )


MESH = pl.DeviceIdType.MESH
VMEM_BYTES = 62 * 2**20
WINDOW = 1152


def place():
    replica = lax.axis_index("replica")
    shard = lax.axis_index("shard")
    core = lax.rem(replica, 2)
    return replica, shard, core


def peer_of(shard, d):
    across = lax.rem(lax.rem(shard, 2) + d % 2, 2)
    up = lax.rem(shard // 2 + d // 2, 2)
    return up * 2 + across


def window_start(shard, core):
    return ((shard * 35) // 2 + core * 9) * 128


def remote(src, dst, send, recv, device):
    return pltpu.make_async_remote_copy(
        src_ref=src,
        dst_ref=dst,
        send_sem=send,
        recv_sem=recv,
        device_id=device,
        device_id_type=MESH,
    )


def any_spec():
    return pl.BlockSpec(memory_space=pl.ANY)


def vmem_spec():
    return pl.BlockSpec(memory_space=pltpu.VMEM)


def params(**more):
    return pltpu.CompilerParams(has_side_effects=True, vmem_limit_bytes=VMEM_BYTES, **more)


CHUNK = 128
DOWN_CHUNKS = (64, 64) + (128,) * 7 + (64, 64)
ATTENTION_CHUNKS = (64, 64, 64, 64, 32, 32, 32, 32)
CHUNKS = len(DOWN_CHUNKS) + 24 + len(ATTENTION_CHUNKS)
SCORE_SCALE = 1.0 / math.sqrt(HD)


def row_spans(sizes):
    return [pl.ds(sum(sizes[:k]), size) for k, size in enumerate(sizes)]


def dot_nt(a, b):
    return lax.dot_general(a, b, (((1,), (1,)), ((), ())), preferred_element_type=jnp.float32)


def dot_tn(a, b):
    return lax.dot_general(a, b, (((0,), (0,)), ((), ())), preferred_element_type=jnp.float32)


def row_loop(rows, step, body, init):
    return lax.fori_loop(0, rows // step, lambda j, c: body(pl.ds(pl.multiple_of(j * step, step), step), c), init)


TILES = ((0, 640, 192), (640, 512, 160))


def forward_kernel(grad_scale, names, *refs):
    v = dict(zip(names, refs))
    f32 = jnp.float32
    bf16 = jnp.bfloat16
    replica, shard, core = place()
    other = 1 - core
    mate = (replica + 1 - 2 * core, shard)
    odd = lax.rem(replica // 2, 2)
    pair = (replica + 2 - 4 * odd, shard)
    order = (3, 1, 2)
    first_unit = window_start(shard, core)
    q_buf, o_buf, g_buf, u_buf, d_buf = v["q_buf"], v["o_buf"], v["g_buf"], v["u_buf"], v["d_buf"]
    n_all, cot_all, small_all = v["n_all"], v["cot_all"], v["small_all"]

    def span(start, size):
        return pl.ds(pl.multiple_of(start, 16), size)

    def units(target, offset, width):
        return pl.ds(pl.multiple_of(window_start(target, core) + offset, 128), width)

    def tokens(owner, c):
        return pl.ds(pl.multiple_of((c * 4 + owner) * 128, 128), 128)

    weights = [
        (lambda t: v["wq"], q_buf, 192, 80, True),
        (lambda t: v["wo"], o_buf, 192, 80, True),
    ]
    for offset, width, shared in TILES:
        for name, buf in (("wg", g_buf), ("wu", u_buf)):
            weights.append((
                lambda t, name=name, offset=offset, width=width: v[name].at[:, units(t, offset, width)],
                buf.at[:, pl.ds(offset, width)], 384, shared, False,
            ))

    def base(i, c):
        return c * 192 if weights[i][4] else 0

    def hop(i, d, t, o):
        source, out, size, shared, _ = weights[i]
        first = base(i, core) + odd * shared
        n = i * 3 + d - 1
        return remote(
            source(t).at[span(first, size - shared)], out.at[span(o * 384 + first, size - shared)],
            v["send"].at[n], v["recv"].at[n], (replica, t),
        )

    def across(i, d, o, whose):
        _, out, size, shared, _ = weights[i]
        ref = out.at[span(o * 384 + base(i, core) + whose * (size - shared), shared)]
        n = i * 3 + d - 1
        return remote(ref, ref, v["zsend"].at[n], v["zrecv"].at[n], pair)

    def onward(i, d, o, c, shared_part):
        _, out, size, shared, _ = weights[i]
        first = o * 384 + base(i, c) + ((1 - odd) * (size - shared) if shared_part else odd * shared)
        ref = out.at[span(first, shared if shared_part else size - shared)]
        n = i * 3 + d - 1 + (6 if shared_part else 0)
        return remote(ref, ref, v["fsend"].at[n], v["frecv"].at[n], mate)

    row_sets = (cot_all, n_all)

    def row_hop(a, d, t, o):
        n = 18 + a * 3 + d - 1
        return remote(row_sets[a].at[tokens(shard, core)], row_sets[a].at[tokens(o, core)], v["send"].at[n], v["recv"].at[n],
                      (replica, t))

    def row_onward(a, d, o, c):
        n = 12 + a * 4 + d
        ref = row_sets[a].at[tokens(o, c)]
        return remote(ref, ref, v["fsend"].at[n], v["frecv"].at[n], mate)

    def small_hop(d, t, o):
        n = 24 + d - 1
        return remote(v["small"], small_all.at[o], v["send"].at[n], v["recv"].at[n], (replica, t))

    def send_rows(a):
        for d in order:
            row_hop(a, d, peer_of(shard, d), shard).start()
        row_onward(a, 0, shard, core).start()

    def take_rows(a):
        for d in order:
            p = peer_of(shard, d)
            row_hop(a, d, p, p).wait_recv()
            row_onward(a, d, p, core).start()

    def have_rows(a):
        for d in (0,) + order:
            row_onward(a, d, peer_of(shard, d), other).wait_recv()

    def send_weight(i):
        for d in order:
            hop(i, d, peer_of(shard, d), shard).start()

    def take(i, d):
        p = peer_of(shard, d)
        hop(i, d, p, p).wait_recv()
        across(i, d, p, odd).start()
        if weights[i][4]:
            onward(i, d, p, core, False).start()

    def take_shared(i):
        for d in order:
            p = peer_of(shard, d)
            across(i, d, p, 1 - odd).wait_recv()
            if weights[i][4]:
                onward(i, d, p, core, True).start()

    def have_other_half(i):
        for d in order:
            for part in (False, True):
                onward(i, d, peer_of(shard, d), other, part).wait_recv()

    rows = span(shard * 384, 384)
    loads = [
        pltpu.make_async_copy(v["cot"], cot_all.at[tokens(shard, core)], v["local"].at[0]),
        pltpu.make_async_copy(v["wq"], q_buf.at[rows], v["local"].at[1]),
        pltpu.make_async_copy(v["wo"], o_buf.at[rows], v["local"].at[2]),
        pltpu.make_async_copy(v["wg"].at[:, units(shard, 0, WINDOW)], g_buf.at[rows], v["local"].at[3]),
        pltpu.make_async_copy(v["wu"].at[:, units(shard, 0, WINDOW)], u_buf.at[rows], v["local"].at[4]),
    ]
    odd_chip = lax.rem(shard, 2)
    inside = odd_chip == core
    loads.append(pltpu.make_async_copy(
        v["wd"].at[span((1152 - 64 * odd_chip) * core, 1088)],
        d_buf.at[span(odd_chip * (1 - core) * 64, 1088)], v["local"].at[5],
    ))

    for d in order:
        small_hop(d, peer_of(shard, d), shard).start()
    send_weight(0)
    send_weight(1)
    for copy in loads:
        copy.start()
    rest = pltpu.make_async_copy(
        v["wd"].at[span((2176 - 1088) * core + 1088, 64)], d_buf.at[pl.ds(1088, 64)], v["local"].at[6]
    )

    @pl.when(inside)
    def _():
        rest.start()

    @pl.when(~inside)
    def _():
        d_buf[span(1088 - 1088 * odd_chip, 64), :] = jnp.zeros((64, 1536), bf16)

    loads[0].wait()
    send_rows(0)
    send_weight(2)
    send_weight(3)

    small_all[shard] = v["small"][...]
    for d in order:
        p = peer_of(shard, d)
        small_hop(d, p, p).wait_recv()

    def gathered(row, width):
        return jnp.concatenate([small_all[s, row : row + 1, 0:width].astype(f32) for s in range(4)], axis=1)

    gain_one = gathered(0, 384)

    def norm_body(at, carry):
        x = v["x"][at, :].astype(f32)
        inv = lax.rsqrt(jnp.mean(x * x, axis=-1, keepdims=True) + NORM_EPS)
        v["nrm"][at, :] = (x * inv * gain_one).astype(bf16)
        return carry

    row_loop(128, 16, norm_body, 0)
    for copy in loads[1:]:
        copy.wait()

    @pl.when(inside)
    def _():
        rest.wait()

    for i in (0, 1):
        for d in order:
            take(i, d)
    take_shared(0)
    have_other_half(0)
    keep_q = pltpu.make_async_copy(q_buf, v["q_full"], v["local"].at[7])
    keep_q.start()
    bias = gathered(1, 512)

    def rotated(x):
        return x * v["cos"][...] + pltpu.roll(x, HD // 2, 1) * v["sin"][...]

    def project(head, out, at, turn):
        cols = slice(head * HD, (head + 1) * HD)
        x = v["prj"][:, cols] + bias[:, cols]
        out[:, at * HD : (at + 1) * HD] = (rotated(x) if turn else x).astype(bf16)

    for n in range(4):
        v["prj"][:, n * 512 : (n + 1) * 512] = jnp.dot(
            v["nrm"][...], q_buf[:, n * 512 : (n + 1) * 512], preferred_element_type=f32
        )
    take_shared(1)
    for h in range(HEADS):
        project(h, v["qry"], h, True)
    for g in range(KV):
        project(HEADS + g, v["key"], g, True)
        project(HEADS + KV + g, v["val"], g, False)
    causal = lax.broadcasted_iota(jnp.int32, (128, 128), 0) >= lax.broadcasted_iota(jnp.int32, (128, 128), 1)
    v["lse"][...] = jnp.zeros((128, HD), f32)
    for h in range(HEADS):
        g = h // (HEADS // KV)
        at = slice(h * HD, (h + 1) * HD)
        scores = dot_nt(v["qry"][:, at], v["key"][:, g * HD : (g + 1) * HD]) * SCORE_SCALE
        scores = jnp.where(causal, scores, -1e30)
        row_max = jnp.max(scores, axis=-1, keepdims=True)
        logsum = row_max + jnp.log(jnp.sum(jnp.exp(scores - row_max), axis=-1, keepdims=True))
        v["lse"][:, h : h + 1] = logsum
        probs = jnp.exp(scores - logsum).astype(bf16)
        v["ctx"][:, at] = jnp.dot(probs, v["val"][:, g * HD : (g + 1) * HD], preferred_element_type=f32).astype(bf16)
    have_other_half(1)
    keep_o = pltpu.make_async_copy(o_buf, v["o_full"], v["local"].at[8])
    keep_o.start()
    for n in range(3):
        cols = slice(n * 512, (n + 1) * 512)
        v["hidden"][:, cols] = v["x"][:, cols].astype(f32) + jnp.dot(
            v["ctx"][...], o_buf[:, cols], preferred_element_type=f32
        )
    gain_two = gathered(2, 384)
    v["gains"][0:1, :] = gain_one
    v["gains"][1:2, :] = gain_two

    def norm_two(j, carry):
        at = pl.ds(pl.multiple_of(j * 16, 16), 16)
        hidden = v["hidden"][at, :]
        inv = lax.rsqrt(jnp.mean(hidden * hidden, axis=-1, keepdims=True) + NORM_EPS)
        n_all[span((core * 4 + shard) * 128 + j * 16, 16), :] = (hidden * inv * gain_two).astype(bf16)
        return carry

    lax.fori_loop(0, 8, norm_two, 0)
    send_rows(1)
    send_weight(4)
    send_weight(5)
    take_rows(0)
    for i in (2, 3):
        for d in order:
            take(i, d)
    take_rows(1)
    take_shared(2)
    take_shared(3)
    have_rows(0)
    have_rows(1)

    act, gate_delta, up_delta = v["act"], v["gd"], v["ud"]
    gs, us, gr = v["gs"], v["us"], v["gr"]
    pending = [(i, d) for i in (4, 5) for d in order]

    def service():
        if pending:
            take(*pending.pop(0))

    def products(offset, width, m):
        at = pl.ds(m * 512, 512)
        for n in range(0, width, 256):
            size = min(256, width - n)
            cols = pl.ds(offset + n, size)
            gs[:, n : n + size] = jnp.dot(n_all[at, :], g_buf[:, cols], preferred_element_type=f32)
            us[:, n : n + size] = jnp.dot(n_all[at, :], u_buf[:, cols], preferred_element_type=f32)
            gr[:, n : n + size] = dot_nt(cot_all[at, :], d_buf[cols, :])
        column = first_unit + offset + lax.broadcasted_iota(jnp.int32, (1, width), 1)
        owned = (column >= shard * 2240) & (column < (shard + 1) * 2240)

        def body(j, carry):
            part = pl.ds(pl.multiple_of(j * 16, 16), 16)
            to = pl.ds(pl.multiple_of(m * 512 + j * 16, 16), 16)
            cols = pl.ds(offset, width)
            gate, up, grad = gs[part, 0:width], us[part, 0:width], gr[part, 0:width]
            sig = jax.nn.sigmoid(gate)
            silu = gate * sig
            act[to, cols] = jnp.where(owned, silu * up, 0.0).astype(bf16)
            gate_delta[to, cols] = jnp.where(owned, grad * up * sig * (1.0 + gate * (1.0 - sig)), 0.0).astype(bf16)
            up_delta[to, cols] = jnp.where(owned, grad * silu, 0.0).astype(bf16)
            return carry

        lax.fori_loop(0, 32, body, 0)

    def transpose(src, cols, dst):
        def body(j, carry):
            at = pl.ds(pl.multiple_of(j * 128, 128), 128)
            dst[:, at] = src[at, cols].T
            return carry

        lax.fori_loop(0, 8, body, 0)

    outs = {}

    def write(name, buf, at, cols=None):
        n = 9 + len(outs)
        src = buf.at[at] if cols is None else buf.at[at, cols]
        dst = v[name].at[at] if cols is None else v[name].at[at, cols]
        copy = pltpu.make_async_copy(src, dst, v["local"].at[n])
        copy.start()
        outs[n] = copy

    for tile, (offset, width, _) in enumerate(TILES):
        cols = pl.ds(offset, width)
        for m in range(2):
            products(offset, width, m)
            service()
        transpose(act, cols, v["act_t"].at[pl.ds(0, width)])
        if tile == 0:
            transpose(n_all, pl.ds(0, 1536), v["n_t"])
        service()
        for n in range(3):
            out = pl.ds(n * 512, 512)
            v["d_grad"][cols, out] = (
                jnp.dot(v["act_t"][0:width, :], cot_all[:, out], preferred_element_type=f32) * grad_scale
            ).astype(bf16)
        write("pd", v["d_grad"], cols)
        service()
        for delta, buf, name in ((gate_delta, v["g_grad"], "pg"), (up_delta, v["u_grad"], "pu")):
            for m in range(3):
                at = pl.ds(m * 512, 512)
                buf[at, cols] = (
                    jnp.dot(v["n_t"][at, :], delta[:, cols], preferred_element_type=f32) * grad_scale
                ).astype(bf16)
            write(name, buf, pl.ds(0, 1536), cols)
            service()
        while pending:
            service()
        if tile == 0:
            take_shared(4)
            take_shared(5)
    keep_q.wait()
    keep_o.wait()
    for i in (0, 1):
        for d in order:
            p = peer_of(shard, d)
            hop(i, d, p, shard).wait_send()
            across(i, d, p, odd).wait_send()
            for part in (False, True):
                onward(i, d, p, core, part).wait_send()
    for m in range(2):
        at = pl.ds(m * 512, 512)
        for n in range(3):
            cols = pl.ds(n * 512, 512)
            q_buf[at, cols] = (dot_nt(gate_delta[at, :], g_buf[cols, :]) + dot_nt(up_delta[at, :], u_buf[cols, :])).astype(bf16)
        write("p_back", q_buf, at, pl.ds(0, 1536))
    for m in range(2):
        at = pl.ds(m * 512, 512)
        for n in range(3):
            cols = pl.ds(n * 512, 512)
            o_buf[at, cols] = jnp.dot(act[at, :], d_buf[:, cols], preferred_element_type=f32).astype(bf16)
        write("p_out", o_buf, at)
    for copy in outs.values():
        copy.wait()
    for d in order:
        p = peer_of(shard, d)
        small_hop(d, p, shard).wait_send()
        for i in (2, 3, 4, 5):
            hop(i, d, p, shard).wait_send()
            across(i, d, p, odd).wait_send()
        for a in range(2):
            row_hop(a, d, p, shard).wait_send()
    for a in range(2):
        for d in (0,) + order:
            row_onward(a, d, peer_of(shard, d), core).wait_send()


def forward(grad_scale, **given):
    bf16 = jnp.bfloat16
    f32 = jnp.float32
    dma = pltpu.SemaphoreType.DMA
    in_vmem = ("x", "small", "cos", "sin")
    outs = {
        "q_full": ((1536, 2048), bf16, any_spec()),
        "o_full": ((1536, 1536), bf16, any_spec()),
        "pd": ((WINDOW, 1536), bf16, any_spec()),
        "pg": ((1536, WINDOW), bf16, any_spec()),
        "pu": ((1536, WINDOW), bf16, any_spec()),
        "p_back": ((1024, 1536), bf16, any_spec()),
        "p_out": ((1024, 1536), bf16, any_spec()),
        "hidden": ((128, 1536), f32, vmem_spec()),
        "nrm": ((128, 1536), bf16, vmem_spec()),
        "ctx": ((128, 1536), bf16, vmem_spec()),
        "qry": ((128, 1536), bf16, vmem_spec()),
        "key": ((128, KV * HD), bf16, vmem_spec()),
        "val": ((128, KV * HD), bf16, vmem_spec()),
        "lse": ((128, HD), f32, vmem_spec()),
        "gains": ((8, 1536), f32, vmem_spec()),
    }
    scratch = {
        "q_buf": pltpu.VMEM((1536, 2048), bf16),
        "o_buf": pltpu.VMEM((1536, 1536), bf16),
        "g_buf": pltpu.VMEM((1536, WINDOW), bf16),
        "u_buf": pltpu.VMEM((1536, WINDOW), bf16),
        "d_buf": pltpu.VMEM((WINDOW, 1536), bf16),
        "n_all": pltpu.VMEM((1024, 1536), bf16),
        "n_t": pltpu.VMEM((1536, 1024), bf16),
        "cot_all": pltpu.VMEM((1024, 1536), bf16),
        "small_all": pltpu.VMEM((4, 16, 512), bf16),
        "prj": pltpu.VMEM((128, 2048), f32),
        "act": pltpu.VMEM((1024, WINDOW), bf16),
        "gd": pltpu.VMEM((1024, WINDOW), bf16),
        "ud": pltpu.VMEM((1024, WINDOW), bf16),
        "act_t": pltpu.VMEM((640, 1024), bf16),
        "gs": pltpu.VMEM((512, 640), f32),
        "us": pltpu.VMEM((512, 640), f32),
        "gr": pltpu.VMEM((512, 640), f32),
        "d_grad": pltpu.VMEM((WINDOW, 1536), bf16),
        "g_grad": pltpu.VMEM((1536, WINDOW), bf16),
        "u_grad": pltpu.VMEM((1536, WINDOW), bf16),
        "send": dma((27,)),
        "recv": dma((27,)),
        "zsend": dma((18,)),
        "zrecv": dma((18,)),
        "fsend": dma((20,)),
        "frecv": dma((20,)),
        "local": dma((20,)),
    }
    return dict(zip(outs, pl.pallas_call(
        functools.partial(forward_kernel, grad_scale, (*given, *outs, *scratch)),
        out_shape=[jax.ShapeDtypeStruct(s, dt) for s, dt, _ in outs.values()],
        in_specs=[vmem_spec() if name in in_vmem else any_spec() for name in given],
        out_specs=[spec for _, _, spec in outs.values()],
        scratch_shapes=list(scratch.values()),
        compiler_params=pltpu.CompilerParams(has_side_effects=True, vmem_limit_bytes=67043328),
    )(*given.values())))


def backward_kernel(levels, grad_scale, names, *refs):
    v = dict(zip(names, refs))
    replica, shard, core = place()
    other = 1 - core
    level = replica // 2
    mate = (replica + 1 - 2 * core, shard)
    above, below = (replica + 2, shard), (replica - 2, shard)
    f32 = jnp.float32
    bf16 = jnp.bfloat16
    order = (3, 1, 2)
    own_a, own_d, own_g = v["own_a"], v["own_d"], v["own_g"]
    sources = (v["pg"], v["pu"])

    def tokens(owner, c):
        return pl.ds(pl.multiple_of((c * 4 + owner) * 128, 128), 128)

    def exchange(a, d, p):
        rows = pl.ds(pl.multiple_of(p * 384, 384), 384)
        n = a * 4 + d
        return remote(
            sources[a].at[rows], own_g.at[pl.ds(a * 1536 + d * 384, 384)],
            v["xsend"].at[n], v["xrecv"].at[n], (replica, p),
        )

    fills = [
        None,
        pltpu.make_async_copy(v["pd"], own_d, v["in_sem"].at[1]),
    ]
    for a in range(2):
        rows = pl.ds(pl.multiple_of(shard * 384, 384), 384)
        fills.append(
            pltpu.make_async_copy(sources[a].at[rows], own_g.at[pl.ds(a * 1536, 384)], v["in_sem"].at[2 + a])
        )

    partial = (v["p_back"], v["p_out"])
    held, kept, parts = v["held"], v["kept"], v["parts"]

    def to_mate(a, d):
        t = peer_of(shard, d)
        n = a * 4 + d
        return remote(partial[a].at[tokens(t, other)], held.at[a, d],
                      v["csend"].at[n], v["crecv"].at[n], mate)

    def keep(a, d):
        return pltpu.make_async_copy(partial[a].at[tokens(peer_of(shard, d), core)], kept.at[a, d], v["keep_sem"].at[a * 4 + d])

    def to_owner(a, d):
        n = a * 3 + d - 1
        return remote(kept.at[a, d], parts.at[a, d - 1], v["psend"].at[n], v["precv"].at[n], (replica, peer_of(shard, d)))

    def pair_sums(a):
        for d in order:
            to_mate(a, d).wait_recv()
            keep(a, d).wait()

            def body(rows, carry):
                kept[a, d, rows, :] = (kept[a, d, rows, :].astype(f32) + held[a, d, rows, :].astype(f32)).astype(bf16)
                return carry

            row_loop(128, 32, body, 0)
            to_owner(a, d).start()

    def collect(a):
        to_mate(a, 0).wait_recv()
        keep(a, 0).wait()
        for d in order:
            to_owner(a, d).wait_recv()

    def full_sum(a, rows):
        total = kept[a, 0, rows, :].astype(f32) + held[a, 0, rows, :].astype(f32)
        for d in (1, 2, 3):
            total = total + parts[a, d - 1, rows, :].astype(f32)
        return total

    wide = ((v["hid"], v["hid_all"], 768), (v["prj"], v["prj_all"], 1024))
    narrow = ((v["ctx"], v["ctx_all"], 384), (v["nrm"], v["nrm_all"], 384))

    def block(out, owner, c):
        return out.at[tokens(owner, c)]

    def columns(ref, index, width):
        return ref.at[:, pl.ds(pl.multiple_of(index * width, width), width)]

    def wide_copy(a, d, same, source_core, owner, t):
        ref, out, width = wide[a]
        c = core if same else other
        n = (a * 4 + d) * 2 + (0 if same else 1)
        return remote(
            columns(ref, c, width), block(out, owner, source_core), v["gsend"].at[n], v["grecv"].at[n],
            (replica - core + c, t),
        )

    def narrow_copy(a, d, owner, t):
        ref, out, width = narrow[a]
        n = 16 + a * 4 + d
        return remote(columns(ref, t, width), block(out, owner, core), v["gsend"].at[n], v["grecv"].at[n], (replica, t))

    def onward(a, d, source, owner, c):
        out = narrow[a][1]
        n = a * 4 + d
        return remote(source, block(out, owner, c), v["fsend"].at[n], v["frecv"].at[n], mate)

    def own_narrow(a):
        ref, out, width = narrow[a]
        return pltpu.make_async_copy(columns(ref, shard, width), block(out, shard, core), v["local"].at[a])

    def own_wide(a):
        ref, out, width = wide[a]
        return pltpu.make_async_copy(columns(ref, core, width), block(out, shard, core), v["local"].at[2 + a])

    wbuf = v["wbuf"]
    load_out = pltpu.make_async_copy(v["wo"], wbuf.at[:, pl.ds(0, 1536)], v["local"].at[4])
    load_qkv = pltpu.make_async_copy(v["wq"], wbuf, v["local"].at[5])

    def stage_sums():
        pair_sums(0)
        for d in order:
            for a in range(2):
                narrow_copy(a, d, shard, peer_of(shard, d)).start()
        for d in (1, 2, 3):
            for a in range(2):
                exchange(a, d, peer_of(shard, d)).start()

    def stage_hidden():
        collect(0)
        gain = v["gain_two"][...]

        def body(rows, total):
            grad = full_sum(0, rows)
            hidden = v["hidden"][rows, :]
            inv = lax.rsqrt(jnp.mean(hidden * hidden, axis=-1, keepdims=True) + NORM_EPS)
            scaled = gain * grad
            out = v["cot"][rows, :].astype(f32) + inv * (
                scaled - hidden * inv * inv * jnp.mean(scaled * hidden, axis=-1, keepdims=True)
            )
            v["hgrad"][rows, :] = out
            v["hid"][rows, :] = out.astype(bf16)
            return total + jnp.sum(grad * hidden * inv, axis=0, keepdims=True)

        v["row_two"][...] = row_loop(128, 16, body, jnp.zeros((1, 1536), f32)) * grad_scale
        for d in (0,) + order:
            if d:
                wide_copy(0, d, True, core, shard, peer_of(shard, d)).start()
            wide_copy(0, d, False, core, shard, peer_of(shard, d)).start()
        own_wide(0).start()

    def stage_context():
        load_out.wait()
        for e in range(4):
            cols = pl.ds(e * 384, 384)
            v["cgrad"][:, cols] = dot_nt(v["hid"][...], wbuf[cols, 0:1536]).astype(bf16)
        load_qkv.start()

    def unrotated(x):
        return x * v["cos"][...] + pltpu.roll(x, HD // 2, 1) * v["sin"][...]

    def stage_heads(g, part):
        keys = v["key"][:, g * HD : (g + 1) * HD]
        values = v["val"][:, g * HD : (g + 1) * HD]
        causal = lax.broadcasted_iota(jnp.int32, (128, 128), 0) >= lax.broadcasted_iota(jnp.int32, (128, 128), 1)
        key_grad = jnp.zeros((128, HD), f32) if part == 0 else v["kv_sum"][0]
        value_grad = jnp.zeros((128, HD), f32) if part == 0 else v["kv_sum"][1]
        first_head = g * (HEADS // KV) + part * 2
        for h in range(first_head, first_head + 2):
            at = slice(h * HD, (h + 1) * HD)
            query = v["qry"][:, at]
            grad = v["cgrad"][:, at]
            scores = jnp.where(causal, dot_nt(query, keys) * SCORE_SCALE, -1e30)
            probs = jnp.exp(scores - v["lse"][:, h : h + 1]).astype(bf16)
            wide_probs = probs.astype(f32)
            prob_grad = dot_nt(grad, values)
            delta = jnp.sum(wide_probs * prob_grad, axis=-1, keepdims=True)
            score_grad = (wide_probs * (prob_grad - delta) * SCORE_SCALE).astype(bf16)
            v["prj"][:, at] = unrotated(jnp.dot(score_grad, keys, preferred_element_type=f32)).astype(bf16)
            key_grad = key_grad + dot_tn(score_grad, query)
            value_grad = value_grad + dot_tn(probs, grad)
        if part < 2:
            v["kv_sum"][0] = key_grad
            v["kv_sum"][1] = value_grad
            return
        first = HEADS * HD + g * HD
        v["prj"][:, first : first + HD] = unrotated(key_grad).astype(bf16)
        first = first + KV * HD
        v["prj"][:, first : first + HD] = value_grad.astype(bf16)

    def stage_send_projected():
        for d in (0,) + order:
            if d:
                wide_copy(1, d, True, core, shard, peer_of(shard, d)).start()
            wide_copy(1, d, False, core, shard, peer_of(shard, d)).start()
        own_wide(1).start()

    def stage_normed(part):
        if part == 0:
            load_qkv.wait()
        for e in (2 * part, 2 * part + 1):
            cols = pl.ds(e * 384, 384)
            v["ngrad"][:, cols] = dot_nt(v["prj"][...], wbuf[cols, :])

    vec, vin, vall = v["vec"], v["vin"], v["vall"]
    replicas = 2 * levels

    def vec_hop(d):
        return remote(vec.at[peer_of(shard, d)], vin.at[d - 1], v["vsend"].at[d - 1], v["vrecv"].at[d - 1],
                      (replica, peer_of(shard, d)))

    def vec_spread(j, slot):
        target = lax.rem(replica + j, replicas)
        return remote(v["vsum"], vall.at[slot], v["vsend"].at[2 + j], v["vrecv"].at[2 + j], (target, shard))

    def stage_input():
        gain = v["gain_one"][...]

        def body(rows, totals):
            total, bias = totals
            x = v["x"][rows, :].astype(f32)
            grad = v["ngrad"][rows, :]
            inv = lax.rsqrt(jnp.mean(x * x, axis=-1, keepdims=True) + NORM_EPS)
            scaled = gain * grad
            v["input_grad"][rows, :] = v["hgrad"][rows, :] + inv * (
                scaled - x * inv * inv * jnp.mean(scaled * x, axis=-1, keepdims=True)
            )
            return (
                total + jnp.sum(grad * x * inv, axis=0, keepdims=True),
                bias + jnp.sum(v["prj"][rows, :].astype(f32), axis=0, keepdims=True),
            )

        row_one, row_bias = row_loop(128, 16, body, (jnp.zeros((1, 1536), f32), jnp.zeros((1, 2048), f32)))
        row_one = row_one * grad_scale
        row_bias = row_bias * grad_scale
        row_two = v["row_two"][...]
        for s in range(4):
            vec[s, :, 0:384] = jnp.broadcast_to(row_one[:, s * 384 : (s + 1) * 384], (8, 384))
            vec[s, :, 384:896] = jnp.broadcast_to(row_bias[:, s * 512 : (s + 1) * 512], (8, 512))
            vec[s, :, 896:1280] = jnp.broadcast_to(row_two[:, s * 384 : (s + 1) * 384], (8, 384))
        for d in order:
            vec_hop(d).start()

    def stage_vec():
        total = vec[shard]
        for d in (1, 2, 3):
            vec_hop(d).wait_recv()
            total = total + vin[d - 1]
        v["vsum"][...] = total
        for j in range(1, replicas):
            vec_spread(j, replica).start()
        pair_sums(1)

    def stage_vec_out():
        vall[replica] = v["vsum"][...]
        for j in range(1, replicas):
            vec_spread(j, lax.rem(replica + replicas - j, replicas)).wait_recv()
        total = vall[0]
        for j in range(1, replicas):
            total = total + vall[j]
        v["vec_out"][...] = total

    def stage_output():
        collect(1)

        def body(rows, carry):
            v["block_out"][rows, :] = (v["hidden"][rows, :] + full_sum(1, rows)).astype(bf16)
            return carry

        row_loop(128, 32, body, 0)

    def stage_relay():
        for d in order:
            p = peer_of(shard, d)
            for a in range(2):
                narrow_copy(a, d, p, p).wait_recv()
                onward(a, d, block(narrow[a][1], p, core), p, core).start()

    def stage_gathered():
        for a in range(2):
            own_narrow(a).wait()
            own_wide(a).wait()
            for d in (0, 1, 2, 3):
                p = peer_of(shard, d)
                if d:
                    wide_copy(a, d, True, core, p, p).wait_recv()
                wide_copy(a, d, False, other, p, p).wait_recv()
                onward(a, d, block(narrow[a][1], p, other), p, other).wait_recv()

    def stage_attention_parts(j):
        at = pl.ds(j * 128, 128)
        own_a[at, 0:1024] = (dot_tn(v["nrm_all"][:, at], v["prj_all"][...]) * grad_scale).astype(bf16)
        own_a[at, 1024:1792] = (dot_tn(v["ctx_all"][:, at], v["hid_all"][...]) * grad_scale).astype(bf16)

    odd_chip = lax.rem(shard, 2)

    def down_rows(c, at):
        first = odd_chip * (1088 * c - 64 * (1 - c)) + (1 - odd_chip) * 1152 * c
        return pl.ds(pl.multiple_of(first + at.start, 64), at.size)

    chunks = []
    for at in row_spans(DOWN_CHUNKS):
        chunks.append((own_d, v["low_d"], v["high_d"], at, ("none",), lambda c, at=at: v["fd"].at[down_rows(c, at)]))
    for d in range(4):
        for a in range(2):
            for k in range(3):
                at = pl.ds(a * 1536 + d * 384 + k * CHUNK, CHUNK)
                dst = (v["fg"], v["fu"])[a]
                source = peer_of(shard, d)
                chunks.append((
                    own_g, v["low_g"], v["high_g"], at, ("fill", 2 + a) if d == 0 else ("x", a, d),
                    lambda c, k=k, dst=dst, source=source: dst.at[c, source, pl.ds(k * CHUNK, CHUNK)],
                ))
    for at in row_spans(ATTENTION_CHUNKS):
        chunks.append((own_a, v["low_a"], v["high_a"], at, ("none",), lambda c, at=at: v["fa"].at[c, at]))
    total = len(chunks)
    awaited = (set(), set())
    end = (level == 0) | (level == levels - 1)

    def arrive(what, seen):
        if what in seen or what[0] == "none":
            return
        seen.add(what)
        if what[0] == "fill":
            fills[what[1]].wait()
        else:
            exchange(what[1], what[2], peer_of(shard, what[2])).wait_recv()

    def up(k, ref):
        own, low, high, at, _, _ = chunks[k]
        return remote(ref.at[at], low.at[at], v["up_sem"].at[k], v["low_sem"].at[k], above)

    def down(k, ref):
        own, low, high, at, _, _ = chunks[k]
        return remote(ref.at[at], high.at[at], v["down_sem"].at[k], v["high_sem"].at[k], below)

    def add(k, *refs):
        own, _, _, at, _, _ = chunks[k]
        step = 16

        def body(j, carry):
            rows = pl.ds(pl.multiple_of(at.start + j * step, step), step)
            value = own[rows, :].astype(f32)
            for ref in refs:
                value = value + ref[rows, :].astype(f32)
            own[rows, :] = value.astype(own.dtype)
            return carry

        lax.fori_loop(0, at.size // step, body, 0)

    def finish(k, ref):
        _, _, _, at, _, dst = chunks[k]
        pltpu.make_async_copy(ref.at[at], dst(core), v["out_sem"].at[k]).start()
        remote(ref.at[at], dst(core), v["mate_send"].at[k], v["mate_recv"].at[k], mate).start()

    def guarded(stage, k):
        if k == 0:
            pl.when(1 - odd_chip + core > 0)(lambda: stage(k))
        elif k == len(DOWN_CHUNKS) - 1:
            pl.when(odd_chip + 1 - core > 0)(lambda: stage(k))
        else:
            stage(k)

    def guarded_mate(stage, k):
        if k == 0:
            pl.when(1 - odd_chip + other > 0)(lambda: stage(k))
        elif k == len(DOWN_CHUNKS) - 1:
            pl.when(odd_chip + 1 - other > 0)(lambda: stage(k))
        else:
            stage(k)

    def root_of(k):
        return levels // 2 - 1 + k % 2

    def end_gather(k):
        own = chunks[k][0]

        @pl.when(end)
        def _():
            arrive(chunks[k][4], awaited[0])

        @pl.when(level == 0)
        def _():
            up(k, own).start()

        @pl.when(level == levels - 1)
        def _():
            down(k, own).start()

    def gather_step(k):
        own, low, high, at, what, _ = chunks[k]
        root = root_of(k)

        @pl.when(~end)
        def _():
            arrive(what, awaited[1])

        if root > 1:

            @pl.when((level > 0) & (level < root))
            def _():
                up(k, own).wait_recv()
                add(k, low)
                up(k, own).start()

        if root < levels - 2:

            @pl.when((level < levels - 1) & (level > root))
            def _():
                down(k, own).wait_recv()
                add(k, high)
                down(k, own).start()

    def root_step(k):
        own, low, high, at, _, _ = chunks[k]

        @pl.when(level == root_of(k))
        def _():
            up(k, own).wait_recv()
            down(k, own).wait_recv()
            add(k, low, high)
            up(k, own).start()
            down(k, own).start()
            finish(k, own)

    def spread_step(k):
        own, low, high, at, _, _ = chunks[k]
        root = root_of(k)

        if root > 1:

            @pl.when((level > 0) & (level < root))
            def _():
                down(k, own).wait_recv()
                down(k, high).start()
                finish(k, high)

        if root < levels - 2:

            @pl.when((level < levels - 1) & (level > root))
            def _():
                up(k, own).wait_recv()
                up(k, low).start()
                finish(k, low)

    def end_spread(k):
        own, low, high, at, _, _ = chunks[k]

        @pl.when(level == 0)
        def _():
            down(k, own).wait_recv()
            finish(k, high)

        @pl.when(level == levels - 1)
        def _():
            up(k, own).wait_recv()
            finish(k, low)

    for a in range(2):
        for d in order + (0,):
            to_mate(a, d).start()
            keep(a, d).start()
    for copy in fills[1:]:
        copy.start()
    load_out.start()
    fills[1].wait()
    for a in range(2):
        own_narrow(a).start()
        onward(a, 0, columns(narrow[a][0], shard, 384), shard, core).start()
    beside = {
        2: [stage_sums],
        12: [stage_hidden],
        13: [stage_context],
        14: [functools.partial(stage_heads, 0, 0)],
        15: [functools.partial(stage_heads, 0, 1), stage_relay],
        16: [functools.partial(stage_heads, 0, 2)],
        17: [functools.partial(stage_heads, 1, 0)],
        18: [functools.partial(stage_heads, 1, 1)],
        19: [functools.partial(stage_heads, 1, 2), stage_send_projected],
        20: [functools.partial(stage_normed, 0)],
        21: [functools.partial(stage_normed, 1)],
        22: [stage_input],
        32: [stage_gathered, functools.partial(stage_attention_parts, 0)],
        33: [functools.partial(stage_attention_parts, 1)],
        34: [functools.partial(stage_attention_parts, 2)],
        36: [stage_vec],
        total + 8: [stage_vec_out],
        total + 10: [stage_output],
    }
    stages = ((end_gather, 0), (gather_step, 6), (root_step, 10), (spread_step, 14), (end_spread, 20))
    for t in range(total + stages[-1][1]):
        for stage, lag in stages:
            if 0 <= t - lag < total:
                guarded(stage, t - lag)
        for stage in beside.get(t, ()):
            stage()
    for a in range(2):
        for d in (1, 2, 3):
            exchange(a, d, peer_of(shard, d)).wait_send()
    def close(k):
        own, low, high, at, _, dst = chunks[k]

        @pl.when(level < levels - 1)
        def _():
            up(k, own).wait_send()

        @pl.when(level > 0)
        def _():
            down(k, own).wait_send()

        pltpu.make_async_copy(own.at[at], dst(core), v["out_sem"].at[k]).wait()
        remote(own.at[at], dst(core), v["mate_send"].at[k], v["mate_recv"].at[k], mate).wait_send()

    def close_mate(k):
        own, low, high, at, _, dst = chunks[k]
        remote(own.at[at], dst(other), v["mate_send"].at[k], v["mate_recv"].at[k], mate).wait_recv()

    for k in range(total):
        guarded(close, k)
        guarded_mate(close_mate, k)
    for a in range(2):
        for d in (0, 1, 2, 3):
            p = peer_of(shard, d)
            to_mate(a, d).wait_send()
            wide_copy(a, d, False, core, shard, p).wait_send()
            onward(a, d, block(narrow[a][1], p, core), p, core).wait_send()
            if d:
                to_owner(a, d).wait_send()
                wide_copy(a, d, True, core, shard, p).wait_send()
                narrow_copy(a, d, shard, p).wait_send()
    for d in order:
        vec_hop(d).wait_send()
    for j in range(1, replicas):
        vec_spread(j, replica).wait_send()


def backward(levels, grad_scale, **given):
    bf16 = jnp.bfloat16
    f32 = jnp.float32
    dma = pltpu.SemaphoreType.DMA
    in_hbm = ("pd", "pg", "pu", "p_back", "p_out", "wo", "wq")
    outs = {
        "fa": ((2, 384, 1792), bf16, any_spec()),
        "fd": ((2240, 1536), bf16, any_spec()),
        "fg": ((2, 4, 384, WINDOW), bf16, any_spec()),
        "fu": ((2, 4, 384, WINDOW), bf16, any_spec()),
        "block_out": ((128, 1536), bf16, vmem_spec()),
        "input_grad": ((128, 1536), f32, vmem_spec()),
        "vec_out": ((8, 1280), f32, vmem_spec()),
    }
    scratch = {}
    for where in ("own", "low", "high"):
        scratch[where + "_a"] = pltpu.VMEM((384, 1792), bf16)
        scratch[where + "_d"] = pltpu.VMEM((WINDOW, 1536), bf16)
        scratch[where + "_g"] = pltpu.VMEM((3072, WINDOW), bf16)
    scratch |= {
        "held": pltpu.VMEM((2, 4, 128, 1536), bf16),
        "kept": pltpu.VMEM((2, 4, 128, 1536), bf16),
        "parts": pltpu.VMEM((2, 3, 128, 1536), bf16),
        "wbuf": pltpu.VMEM((1536, 2048), bf16),
        "hgrad": pltpu.VMEM((128, 1536), f32),
        "ngrad": pltpu.VMEM((128, 1536), f32),
        "hid": pltpu.VMEM((128, 1536), bf16),
        "cgrad": pltpu.VMEM((128, 1536), bf16),
        "prj": pltpu.VMEM((128, 2048), bf16),
        "ctx_all": pltpu.VMEM((1024, 384), bf16),
        "nrm_all": pltpu.VMEM((1024, 384), bf16),
        "hid_all": pltpu.VMEM((1024, 768), bf16),
        "prj_all": pltpu.VMEM((1024, 1024), bf16),
        "row_two": pltpu.VMEM((1, 1536), f32),
        "kv_sum": pltpu.VMEM((2, 128, HD), f32),
        "vec": pltpu.VMEM((4, 8, 1280), f32),
        "vin": pltpu.VMEM((3, 8, 1280), f32),
        "vsum": pltpu.VMEM((8, 1280), f32),
        "vall": pltpu.VMEM((2 * levels, 8, 1280), f32),
    }
    counts = {
        "xsend": 8, "xrecv": 8, "csend": 8, "crecv": 8, "keep_sem": 8, "psend": 6, "precv": 6, "gsend": 24, "grecv": 24,
        "fsend": 8, "frecv": 8, "local": 6, "in_sem": 4, "vsend": 2 + 2 * levels, "vrecv": 2 + 2 * levels,
    }
    for name in ("up_sem", "down_sem", "low_sem", "high_sem", "mate_send", "mate_recv", "out_sem"):
        counts[name] = CHUNKS
    scratch |= {name: dma((n,)) for name, n in counts.items()}
    return pl.pallas_call(
        functools.partial(backward_kernel, levels, grad_scale, (*given, *outs, *scratch)),
        out_shape=[jax.ShapeDtypeStruct(s, dt) for s, dt, _ in outs.values()],
        in_specs=[any_spec() if name in in_hbm else vmem_spec() for name in given],
        out_specs=[spec for _, _, spec in outs.values()],
        scratch_shapes=list(scratch.values()),
        compiler_params=pltpu.CompilerParams(has_side_effects=True, vmem_limit_bytes=67043328),
    )(*given.values())


def widen_kernel(gate, up, down, attn, out_gate, out_up, out_down, out_qkv, out_out):
    f32 = jnp.float32
    for x, out in ((gate, out_gate), (up, out_up)):
        for s in range(4):
            for c in range(2):
                first = (s * 35) // 2 + c * 9
                rest = 1 if s % 2 == 1 and c == 0 else 0
                out[:, (first + rest) * 128 : (first + 9) * 128] = x[c, s][:, rest * 128 :].astype(f32)
        for s in (1, 3):
            first = (s * 35) // 2
            out[:, first * 128 : (first + 1) * 128] = x[1, s - 1][:, 1024:].astype(f32) + x[0, s][:, :128].astype(f32)
    out_down[...] = down[...].astype(f32)
    for c in range(2):
        out_qkv[:, c * 1024 : (c + 1) * 1024] = attn[c][:, :1024].astype(f32)
        out_out[:, c * 768 : (c + 1) * 768] = attn[c][:, 1024:].astype(f32)


def widen(*sums):
    rows = 32
    f32 = jnp.float32
    blocks = pl.BlockSpec((2, 4, rows, WINDOW), lambda i: (0, 0, i, 0))
    down = pl.BlockSpec((224, 1536), lambda i: (jnp.minimum(i, 9), 0))

    def whole(width):
        return pl.BlockSpec((rows, width), lambda i: (i, 0))

    return pl.pallas_call(
        widen_kernel,
        grid=(384 // rows,),
        out_shape=[
            jax.ShapeDtypeStruct((384, 8960), f32),
            jax.ShapeDtypeStruct((384, 8960), f32),
            jax.ShapeDtypeStruct((2240, 1536), f32),
            jax.ShapeDtypeStruct((384, 2048), f32),
            jax.ShapeDtypeStruct((384, 1536), f32),
        ],
        in_specs=[blocks, blocks, down, pl.BlockSpec((2, rows, 1792), lambda i: (0, i, 0))],
        out_specs=[whole(8960), whole(8960), down, whole(2048), whole(1536)],
    )(*sums)


def fast_device(
    block_input,
    attn_gain,
    qkv_weight,
    qkv_bias,
    out_weight,
    mlp_gain,
    gate_weight,
    up_weight,
    down_weight,
    cotangent,
):
    f32 = jnp.float32
    tok_count = block_input.shape[0]
    levels = lax.axis_size("replica") // 2
    grad_scale = 1.0 / math.sqrt(tok_count * lax.axis_size("replica") * lax.axis_size("shard"))
    cosine, sine_table = rope_tables(tok_count)
    small = jnp.stack([jnp.pad(attn_gain, (0, 128)), qkv_bias, jnp.pad(mlp_gain, (0, 128))])
    small = jnp.pad(small, ((0, 13), (0, 0)))
    twice = jnp.concatenate([cosine[:, 0], cosine[:, 0]], axis=1)
    turn = jnp.concatenate([-sine_table[:, 0], sine_table[:, 0]], axis=1)
    got = forward(
        grad_scale,
        x=block_input,
        small=small,
        cos=twice,
        sin=turn,
        wq=qkv_weight,
        wo=out_weight,
        wg=gate_weight,
        wu=up_weight,
        wd=down_weight,
        cot=cotangent,
    )
    sum_attn, sum_down, sum_gate, sum_up, block_output, input_grad, vectors = backward(
        levels,
        grad_scale,
        pd=got["pd"],
        pg=got["pg"],
        pu=got["pu"],
        p_back=got["p_back"],
        p_out=got["p_out"],
        wo=got["o_full"],
        wq=got["q_full"],
        hidden=got["hidden"],
        x=block_input,
        cot=cotangent,
        gain_one=got["gains"][0:1],
        gain_two=got["gains"][1:2],
        ctx=got["ctx"],
        nrm=got["nrm"],
        qry=got["qry"],
        key=got["key"],
        val=got["val"],
        lse=got["lse"],
        cos=twice,
        sin=-turn,
    )
    gain_one_own, bias_own, gain_two_own = vectors[0, :384], vectors[0, 384:896], vectors[0, 896:]
    gate_grad, up_grad, down_grad, qkv_grad, out_grad = widen(sum_gate, sum_up, sum_down, sum_attn)
    return (
        block_output,
        input_grad,
        gain_one_own,
        qkv_grad,
        bias_own,
        out_grad,
        gain_two_own,
        gate_grad,
        up_grad,
        down_grad,
    )


def solution(mesh):
    placed = (
        P(("replica", "shard"), None),
        P("shard"),
        P("shard", None),
        P("shard"),
        P("shard", None),
        P("shard"),
        P("shard", None),
        P("shard", None),
        P("shard", None),
        P(("replica", "shard"), None),
    )
    fits = mesh.shape["shard"] == 4 and mesh.shape["replica"] % 4 == 0
    per_device = fast_device if fits else general_device
    return jax.shard_map(
        per_device,
        mesh=mesh,
        in_specs=placed,
        out_specs=(
            P(("replica", "shard"), None),
            P(("replica", "shard"), None),
            P("shard"),
            P("shard", None),
            P("shard"),
            P("shard", None),
            P("shard"),
            P("shard", None),
            P("shard", None),
            P("shard", None),
        ),
        check_vma=False,
    )
```

```python
import functools
import math

import jax
import jax.numpy as jnp
from jax import lax
from jax.experimental import pallas as pl
from jax.experimental.pallas import tpu as pltpu
from jax.sharding import PartitionSpec as P

HEADS = 12
KV = 2
HD = 128


NORM_EPS = 1e-06
ROPE_BASE = 1000000.0


def rope_tables(tok_count):
    half_dim = HD // 2
    position = jnp.arange(tok_count, dtype=jnp.float32)
    inverse = ROPE_BASE ** (-(jnp.arange(half_dim, dtype=jnp.float32) * 2.0 / HD))
    angles = position[:, None] * inverse[None, :]
    return (jnp.cos(angles)[:, None, :], jnp.sin(angles)[:, None, :])


def rotate(vectors, cosine, sine_table):
    half_dim = HD // 2
    lower_half = vectors[..., :half_dim]
    upper_half = vectors[..., half_dim:]
    return jnp.concatenate(
        [
            lower_half * cosine - upper_half * sine_table,
            upper_half * cosine + lower_half * sine_table,
        ],
        axis=-1,
    )


def unrotate(grads, cosine, sine_table):
    half_dim = HD // 2
    lower_half = grads[..., :half_dim]
    upper_half = grads[..., half_dim:]
    return jnp.concatenate(
        [
            lower_half * cosine + upper_half * sine_table,
            upper_half * cosine - lower_half * sine_table,
        ],
        axis=-1,
    )


def block_scores(query_block, key_rot, first_row):
    row_count = query_block.shape[0]
    scores = jnp.einsum(
        "qkgd,skd->kgqs", query_block, key_rot, preferred_element_type=jnp.float32
    ) * (1.0 / math.sqrt(HD))
    causal = (first_row + jnp.arange(row_count))[:, None] >= jnp.arange(key_rot.shape[0])[None, :]
    return jnp.where(causal, scores, -1e30)


def block_layout(tok_count):
    block_rows = min(tok_count, 512)
    block_count = tok_count // block_rows
    firsts = jnp.arange(block_count, dtype=jnp.int32) * block_rows
    return (block_rows, block_count, firsts)


def attend_forward(queries, key_rot, values):
    tok_count = queries.shape[0]
    block_rows, block_count, firsts = block_layout(tok_count)
    query_blocks = queries.reshape(block_count, block_rows, KV, HEADS // KV, HD)

    def one_block(inputs):
        query_block, first_row = inputs
        scores = block_scores(query_block, key_rot, first_row)
        row_max = jnp.max(scores, axis=-1, keepdims=True)
        logsum = row_max + jnp.log(jnp.sum(jnp.exp(scores - row_max), axis=-1, keepdims=True))
        attn_probs = jnp.exp(scores - logsum).astype(jnp.bfloat16)
        context = jnp.einsum(
            "kgqs,skd->qkgd", attn_probs, values, preferred_element_type=jnp.float32
        ).astype(jnp.bfloat16)
        return (context, logsum)

    context, logsum = lax.map(one_block, (query_blocks, firsts))
    return (context.reshape(tok_count, HEADS * HD), logsum)


def attend_backward(queries, key_rot, values, logsum, context_grad):
    tok_count = queries.shape[0]
    block_rows, block_count, firsts = block_layout(tok_count)
    query_blocks = queries.reshape(block_count, block_rows, KV, HEADS // KV, HD)
    grad_blocks = context_grad.reshape(block_count, block_rows, KV, HEADS // KV, HD)
    score_scale = 1.0 / math.sqrt(HD)

    def one_block(running, inputs):
        key_total, value_total = running
        query_block, grad_block, log_block, first_row = inputs
        scores = block_scores(query_block, key_rot, first_row)
        attn_probs = jnp.exp(scores - log_block).astype(jnp.bfloat16)
        prob_grad = jnp.einsum(
            "qkgd,skd->kgqs", grad_block, values, preferred_element_type=jnp.float32
        )
        wide_probs = attn_probs.astype(jnp.float32)
        row_delta = jnp.sum(wide_probs * prob_grad, axis=-1, keepdims=True)
        score_grad = (wide_probs * (prob_grad - row_delta) * score_scale).astype(jnp.bfloat16)
        query_grad = jnp.einsum(
            "kgqs,skd->qkgd", score_grad, key_rot, preferred_element_type=jnp.float32
        )
        key_total = key_total + jnp.einsum(
            "kgqs,qkgd->skd", score_grad, query_block, preferred_element_type=jnp.float32
        )
        value_total = value_total + jnp.einsum(
            "kgqs,qkgd->skd", attn_probs, grad_block, preferred_element_type=jnp.float32
        )
        return ((key_total, value_total), query_grad)

    zero_keys = jnp.zeros((tok_count, KV, HD), jnp.float32)
    (key_grad, value_grad), query_grad = lax.scan(
        one_block, (zero_keys, zero_keys), (query_blocks, grad_blocks, logsum, firsts)
    )
    return (query_grad.reshape(tok_count, HEADS, HD), key_grad, value_grad)


def general_device(
    block_input,
    attn_gain,
    qkv_weight,
    qkv_bias,
    out_weight,
    mlp_gain,
    gate_weight,
    up_weight,
    down_weight,
    cotangent,
):
    f32 = jnp.float32
    bf16 = jnp.bfloat16
    tok_count = block_input.shape[0]
    grad_scale = 1.0 / math.sqrt(tok_count * lax.axis_size("replica") * lax.axis_size("shard"))
    q_width = HEADS * HD
    k_end = q_width + KV * HD
    cosine, sine_table = rope_tables(tok_count)
    attn_full = (
        lax.all_gather(attn_gain, "shard", axis=0, tiled=True),
        lax.all_gather(qkv_weight, "shard", axis=0, tiled=True),
        lax.all_gather(qkv_bias, "shard", axis=0, tiled=True),
        lax.all_gather(out_weight, "shard", axis=0, tiled=True),
    )
    gain_full, qkv_full, bias_full, out_full = attn_full
    gain_one = gain_full.astype(f32)
    xfloat = block_input.astype(f32)
    inv_one = lax.rsqrt(jnp.mean(xfloat * xfloat, axis=-1, keepdims=True) + NORM_EPS)
    normed_one = (xfloat * inv_one * gain_one).astype(bf16)
    projected = jnp.dot(normed_one, qkv_full, preferred_element_type=f32) + bias_full.astype(f32)
    queries = rotate(
        projected[:, :q_width].reshape(tok_count, HEADS, HD), cosine, sine_table
    ).astype(bf16)
    queries = queries.reshape(tok_count, KV, HEADS // KV, HD)
    key_rot = rotate(
        projected[:, q_width:k_end].reshape(tok_count, KV, HD), cosine, sine_table
    ).astype(bf16)
    values = projected[:, k_end:].reshape(tok_count, KV, HD).astype(bf16)
    context, logsum = attend_forward(queries, key_rot, values)
    hidden_res = xfloat + jnp.dot(context, out_full, preferred_element_type=f32)
    mlp_full = (
        lax.all_gather(mlp_gain, "shard", axis=0, tiled=True),
        lax.all_gather(gate_weight, "shard", axis=0, tiled=True),
        lax.all_gather(up_weight, "shard", axis=0, tiled=True),
        lax.all_gather(down_weight, "shard", axis=0, tiled=True),
    )
    gain_full_two, gate_full, up_full, down_full = mlp_full
    gain_two = gain_full_two.astype(f32)
    inv_two = lax.rsqrt(jnp.mean(hidden_res * hidden_res, axis=-1, keepdims=True) + NORM_EPS)
    normed_two = (hidden_res * inv_two * gain_two).astype(bf16)
    gate_pre = jnp.dot(normed_two, gate_full, preferred_element_type=f32)
    up_pre = jnp.dot(normed_two, up_full, preferred_element_type=f32)
    sigmoid_gate = jax.nn.sigmoid(gate_pre)
    silu_gate = gate_pre * sigmoid_gate
    activation = (silu_gate * up_pre).astype(bf16)
    block_output = (hidden_res + jnp.dot(activation, down_full, preferred_element_type=f32)).astype(
        bf16
    )
    act_grad = jnp.einsum("td,fd->tf", cotangent, down_full, preferred_element_type=f32)
    gate_delta = (
        act_grad * up_pre * sigmoid_gate * (1.0 + gate_pre * (1.0 - sigmoid_gate))
    ).astype(bf16)
    up_delta = (act_grad * silu_gate).astype(bf16)
    normed_two_grad = jnp.einsum(
        "tf,df->td", gate_delta, gate_full, preferred_element_type=f32
    ) + jnp.einsum("tf,df->td", up_delta, up_full, preferred_element_type=f32)
    gain_two_grad = jnp.sum(normed_two_grad * hidden_res * inv_two, axis=0) * grad_scale
    own_rows = (
        lax.all_to_all(activation, "shard", split_axis=1, concat_axis=0, tiled=True),
        lax.all_to_all(normed_two, "shard", split_axis=1, concat_axis=0, tiled=True),
    )
    group_act, group_normed = own_rows
    group_rows = (
        lax.all_gather(cotangent, "shard", axis=0, tiled=True),
        lax.all_gather(gate_delta, "shard", axis=0, tiled=True),
        lax.all_gather(up_delta, "shard", axis=0, tiled=True),
    )
    group_cot, group_gate, group_up = group_rows
    down_part = (
        jnp.einsum("tf,td->fd", group_act, group_cot, preferred_element_type=f32) * grad_scale
    )
    gate_own = (
        jnp.einsum("td,tf->df", group_normed, group_gate, preferred_element_type=f32) * grad_scale
    )
    up_own = (
        jnp.einsum("td,tf->df", group_normed, group_up, preferred_element_type=f32) * grad_scale
    )
    gain_two_own = lax.psum_scatter(gain_two_grad, "shard", scatter_dimension=0, tiled=True)
    mlp_parts = (gain_two_own, gate_own, up_own)
    hidden_grad = cotangent.astype(f32) + inv_two * (
        gain_two * normed_two_grad
        - hidden_res
        * inv_two
        * inv_two
        * jnp.mean(gain_two * normed_two_grad * hidden_res, axis=-1, keepdims=True)
    )
    hidden_low = hidden_grad.astype(bf16)
    context_grad = jnp.einsum("td,ed->te", hidden_low, out_full, preferred_element_type=f32).astype(
        bf16
    )
    query_grad, key_grad, value_grad = attend_backward(
        queries, key_rot, values, logsum, context_grad
    )
    query_grad = unrotate(query_grad, cosine, sine_table).reshape(tok_count, q_width)
    key_grad = unrotate(key_grad, cosine, sine_table).reshape(tok_count, KV * HD)
    projected_grad = jnp.concatenate(
        [query_grad, key_grad, value_grad.reshape(tok_count, KV * HD)], axis=-1
    ).astype(bf16)
    normed_one_grad = jnp.einsum("tc,dc->td", projected_grad, qkv_full, preferred_element_type=f32)
    gain_one_grad = jnp.sum(normed_one_grad * xfloat * inv_one, axis=0) * grad_scale
    bias_grad = jnp.sum(projected_grad.astype(f32), axis=0) * grad_scale
    own_attn = (
        lax.all_to_all(context, "shard", split_axis=1, concat_axis=0, tiled=True),
        lax.all_to_all(normed_one, "shard", split_axis=1, concat_axis=0, tiled=True),
    )
    group_context, group_normed_one = own_attn
    group_rows = (
        lax.all_gather(hidden_low, "shard", axis=0, tiled=True),
        lax.all_gather(projected_grad, "shard", axis=0, tiled=True),
    )
    group_hidden, group_projected = group_rows
    out_own = (
        jnp.einsum("te,td->ed", group_context, group_hidden, preferred_element_type=f32)
        * grad_scale
    )
    qkv_part = (
        jnp.einsum("td,tc->dc", group_normed_one, group_projected, preferred_element_type=f32)
        * grad_scale
    )
    small_parts = (
        lax.psum_scatter(gain_one_grad, "shard", scatter_dimension=0, tiled=True),
        lax.psum_scatter(bias_grad, "shard", scatter_dimension=0, tiled=True),
    )
    attn_parts = (small_parts[0], qkv_part, small_parts[1], out_own)
    input_grad = hidden_grad + inv_one * (
        gain_one * normed_one_grad
        - xfloat
        * inv_one
        * inv_one
        * jnp.mean(gain_one * normed_one_grad * xfloat, axis=-1, keepdims=True)
    )
    summed = lax.psum(
        (
            attn_parts[0],
            attn_parts[1],
            attn_parts[2],
            attn_parts[3],
            mlp_parts[0],
            mlp_parts[1],
            mlp_parts[2],
            down_part,
        ),
        "replica",
    )
    attn_parts = (summed[0], summed[1], summed[2], summed[3])
    mlp_parts = (summed[4], summed[5], summed[6])
    down_part = summed[7]
    return (
        block_output,
        input_grad,
        attn_parts[0],
        attn_parts[1],
        attn_parts[2],
        attn_parts[3],
        mlp_parts[0],
        mlp_parts[1],
        mlp_parts[2],
        down_part,
    )


MESH = pl.DeviceIdType.MESH
VMEM_BYTES = 62 * 2**20
WINDOW = 1152


def place():
    replica = lax.axis_index("replica")
    shard = lax.axis_index("shard")
    core = lax.rem(replica, 2)
    return replica, shard, core


def peer_of(shard, d):
    across = lax.rem(lax.rem(shard, 2) + d % 2, 2)
    up = lax.rem(shard // 2 + d // 2, 2)
    return up * 2 + across


def window_start(shard, core):
    return ((shard * 35) // 2 + core * 9) * 128


def remote(src, dst, send, recv, device):
    return pltpu.make_async_remote_copy(
        src_ref=src,
        dst_ref=dst,
        send_sem=send,
        recv_sem=recv,
        device_id=device,
        device_id_type=MESH,
    )


def any_spec():
    return pl.BlockSpec(memory_space=pl.ANY)


def vmem_spec():
    return pl.BlockSpec(memory_space=pltpu.VMEM)


def params(**more):
    return pltpu.CompilerParams(has_side_effects=True, vmem_limit_bytes=VMEM_BYTES, **more)


DOWN_STEPS, GATE_STEPS, ATTENTION_STEPS = 18, 48, 12
CHUNKS = DOWN_STEPS + GATE_STEPS + ATTENTION_STEPS
SCORE_SCALE = 1.0 / math.sqrt(HD)


def dot_nt(a, b):
    return lax.dot_general(a, b, (((1,), (1,)), ((), ())), preferred_element_type=jnp.float32)


def dot_tn(a, b):
    return lax.dot_general(a, b, (((0,), (0,)), ((), ())), preferred_element_type=jnp.float32)


def row_loop(rows, step, body, init):
    return lax.fori_loop(0, rows // step, lambda j, c: body(pl.ds(pl.multiple_of(j * step, step), step), c), init)


TILES = ((0, 640, 192), (640, 512, 160))


def forward_kernel(grad_scale, names, *refs):
    v = dict(zip(names, refs))
    f32 = jnp.float32
    bf16 = jnp.bfloat16
    replica, shard, core = place()
    other = 1 - core
    mate = (replica + 1 - 2 * core, shard)
    odd = lax.rem(replica // 2, 2)
    pair = (replica + 2 - 4 * odd, shard)
    order = (3, 1, 2)
    first_unit = window_start(shard, core)
    q_buf, o_buf, g_buf, u_buf, d_buf = v["q_buf"], v["o_buf"], v["g_buf"], v["u_buf"], v["d_buf"]
    n_all, cot_all, small_all = v["n_all"], v["cot_all"], v["small_all"]

    def span(start, size):
        return pl.ds(pl.multiple_of(start, 16), size)

    def units(target, offset, width):
        return pl.ds(pl.multiple_of(window_start(target, core) + offset, 128), width)

    def tokens(owner, c):
        return pl.ds(pl.multiple_of((c * 4 + owner) * 128, 128), 128)

    weights = [
        (lambda t: v["wq"], q_buf, 192, 80, True),
        (lambda t: v["wo"], o_buf, 192, 80, True),
    ]
    for offset, width, shared in TILES:
        for name, buf in (("wg", g_buf), ("wu", u_buf)):
            weights.append((
                lambda t, name=name, offset=offset, width=width: v[name].at[:, units(t, offset, width)],
                buf.at[:, pl.ds(offset, width)], 384, shared, False,
            ))

    def base(i, c):
        return c * 192 if weights[i][4] else 0

    def hop(i, d, t, o):
        source, out, size, shared, _ = weights[i]
        first = base(i, core) + odd * shared
        n = i * 3 + d - 1
        return remote(
            source(t).at[span(first, size - shared)], out.at[span(o * 384 + first, size - shared)],
            v["send"].at[n], v["recv"].at[n], (replica, t),
        )

    def across(i, d, o, whose):
        _, out, size, shared, _ = weights[i]
        ref = out.at[span(o * 384 + base(i, core) + whose * (size - shared), shared)]
        n = i * 3 + d - 1
        return remote(ref, ref, v["zsend"].at[n], v["zrecv"].at[n], pair)

    def onward(i, d, o, c, shared_part):
        _, out, size, shared, _ = weights[i]
        first = o * 384 + base(i, c) + ((1 - odd) * (size - shared) if shared_part else odd * shared)
        ref = out.at[span(first, shared if shared_part else size - shared)]
        n = i * 3 + d - 1 + (6 if shared_part else 0)
        return remote(ref, ref, v["fsend"].at[n], v["frecv"].at[n], mate)

    row_sets = (cot_all, n_all)

    def row_hop(a, d, t, o):
        n = 18 + a * 3 + d - 1
        return remote(row_sets[a].at[tokens(shard, core)], row_sets[a].at[tokens(o, core)], v["send"].at[n], v["recv"].at[n],
                      (replica, t))

    def row_onward(a, d, o, c):
        n = 12 + a * 4 + d
        ref = row_sets[a].at[tokens(o, c)]
        return remote(ref, ref, v["fsend"].at[n], v["frecv"].at[n], mate)

    def small_hop(d, t, o):
        n = 24 + d - 1
        return remote(v["small"], small_all.at[o], v["send"].at[n], v["recv"].at[n], (replica, t))

    def send_rows(a):
        for d in order:
            row_hop(a, d, peer_of(shard, d), shard).start()
        row_onward(a, 0, shard, core).start()

    def take_rows(a):
        for d in order:
            p = peer_of(shard, d)
            row_hop(a, d, p, p).wait_recv()
            row_onward(a, d, p, core).start()

    def have_rows(a):
        for d in (0,) + order:
            row_onward(a, d, peer_of(shard, d), other).wait_recv()

    def send_weight(i):
        for d in order:
            hop(i, d, peer_of(shard, d), shard).start()

    def take(i, d):
        p = peer_of(shard, d)
        hop(i, d, p, p).wait_recv()
        across(i, d, p, odd).start()
        if weights[i][4]:
            onward(i, d, p, core, False).start()

    def take_shared(i):
        for d in order:
            p = peer_of(shard, d)
            across(i, d, p, 1 - odd).wait_recv()
            if weights[i][4]:
                onward(i, d, p, core, True).start()

    def have_other_half(i):
        for d in order:
            for part in (False, True):
                onward(i, d, peer_of(shard, d), other, part).wait_recv()

    rows = span(shard * 384, 384)
    loads = [
        pltpu.make_async_copy(v["cot"], cot_all.at[tokens(shard, core)], v["local"].at[0]),
        pltpu.make_async_copy(v["wq"], q_buf.at[rows], v["local"].at[1]),
        pltpu.make_async_copy(v["wo"], o_buf.at[rows], v["local"].at[2]),
        pltpu.make_async_copy(v["wg"].at[:, units(shard, 0, WINDOW)], g_buf.at[rows], v["local"].at[3]),
        pltpu.make_async_copy(v["wu"].at[:, units(shard, 0, WINDOW)], u_buf.at[rows], v["local"].at[4]),
    ]
    odd_chip = lax.rem(shard, 2)
    inside = odd_chip == core
    loads.append(pltpu.make_async_copy(
        v["wd"].at[span((1152 - 64 * odd_chip) * core, 1088)],
        d_buf.at[span(odd_chip * (1 - core) * 64, 1088)], v["local"].at[5],
    ))

    for d in order:
        small_hop(d, peer_of(shard, d), shard).start()
    send_weight(0)
    send_weight(1)
    for copy in loads:
        copy.start()
    rest = pltpu.make_async_copy(
        v["wd"].at[span((2176 - 1088) * core + 1088, 64)], d_buf.at[pl.ds(1088, 64)], v["local"].at[6]
    )

    @pl.when(inside)
    def _():
        rest.start()

    @pl.when(~inside)
    def _():
        d_buf[span(1088 - 1088 * odd_chip, 64), :] = jnp.zeros((64, 1536), bf16)

    loads[0].wait()
    send_rows(0)
    send_weight(2)
    send_weight(3)

    small_all[shard] = v["small"][...]
    for d in order:
        p = peer_of(shard, d)
        small_hop(d, p, p).wait_recv()

    def gathered(row, width):
        return jnp.concatenate([small_all[s, row : row + 1, 0:width].astype(f32) for s in range(4)], axis=1)

    gain_one = gathered(0, 384)

    def norm_body(at, carry):
        x = v["x"][at, :].astype(f32)
        inv = lax.rsqrt(jnp.mean(x * x, axis=-1, keepdims=True) + NORM_EPS)
        v["nrm"][at, :] = (x * inv * gain_one).astype(bf16)
        return carry

    row_loop(128, 16, norm_body, 0)
    for copy in loads[1:]:
        copy.wait()

    @pl.when(inside)
    def _():
        rest.wait()

    for i in (0, 1):
        for d in order:
            take(i, d)
    take_shared(0)
    have_other_half(0)
    keep_q = pltpu.make_async_copy(q_buf, v["q_full"], v["local"].at[7])
    keep_q.start()
    bias = gathered(1, 512)

    def rotated(x):
        return x * v["cos"][...] + pltpu.roll(x, HD // 2, 1) * v["sin"][...]

    def project(head, out, at, turn):
        cols = slice(head * HD, (head + 1) * HD)
        x = v["prj"][:, cols] + bias[:, cols]
        out[:, at * HD : (at + 1) * HD] = (rotated(x) if turn else x).astype(bf16)

    for n in range(4):
        v["prj"][:, n * 512 : (n + 1) * 512] = jnp.dot(
            v["nrm"][...], q_buf[:, n * 512 : (n + 1) * 512], preferred_element_type=f32
        )
    take_shared(1)
    for h in range(HEADS):
        project(h, v["qry"], h, True)
    for g in range(KV):
        project(HEADS + g, v["key"], g, True)
        project(HEADS + KV + g, v["val"], g, False)
    causal = lax.broadcasted_iota(jnp.int32, (128, 128), 0) >= lax.broadcasted_iota(jnp.int32, (128, 128), 1)
    v["lse"][...] = jnp.zeros((128, HD), f32)
    for h in range(HEADS):
        g = h // (HEADS // KV)
        at = slice(h * HD, (h + 1) * HD)
        scores = dot_nt(v["qry"][:, at], v["key"][:, g * HD : (g + 1) * HD]) * SCORE_SCALE
        scores = jnp.where(causal, scores, -1e30)
        row_max = jnp.max(scores, axis=-1, keepdims=True)
        logsum = row_max + jnp.log(jnp.sum(jnp.exp(scores - row_max), axis=-1, keepdims=True))
        v["lse"][:, h : h + 1] = logsum
        probs = jnp.exp(scores - logsum).astype(bf16)
        v["ctx"][:, at] = jnp.dot(probs, v["val"][:, g * HD : (g + 1) * HD], preferred_element_type=f32).astype(bf16)
    have_other_half(1)
    keep_o = pltpu.make_async_copy(o_buf, v["o_full"], v["local"].at[8])
    keep_o.start()
    for n in range(3):
        cols = slice(n * 512, (n + 1) * 512)
        v["hidden"][:, cols] = v["x"][:, cols].astype(f32) + jnp.dot(
            v["ctx"][...], o_buf[:, cols], preferred_element_type=f32
        )
    gain_two = gathered(2, 384)
    v["gains"][0:1, :] = gain_one
    v["gains"][1:2, :] = gain_two

    def norm_two(j, carry):
        at = pl.ds(pl.multiple_of(j * 16, 16), 16)
        hidden = v["hidden"][at, :]
        inv = lax.rsqrt(jnp.mean(hidden * hidden, axis=-1, keepdims=True) + NORM_EPS)
        n_all[span((core * 4 + shard) * 128 + j * 16, 16), :] = (hidden * inv * gain_two).astype(bf16)
        return carry

    lax.fori_loop(0, 8, norm_two, 0)
    send_rows(1)
    send_weight(4)
    send_weight(5)
    take_rows(0)
    for i in (2, 3):
        for d in order:
            take(i, d)
    take_rows(1)
    take_shared(2)
    take_shared(3)
    have_rows(0)
    have_rows(1)

    act, gate_delta, up_delta = v["act_buf"], v["gd_buf"], v["ud_buf"]
    gs, us, gr = v["gs"], v["us"], v["gr"]
    pending = [(i, d) for i in (4, 5) for d in order]

    def service():
        if pending:
            take(*pending.pop(0))

    def products(offset, width, m):
        at = pl.ds(m * 512, 512)
        for n in range(0, width, 256):
            size = min(256, width - n)
            cols = pl.ds(offset + n, size)
            gs[:, n : n + size] = jnp.dot(n_all[at, :], g_buf[:, cols], preferred_element_type=f32)
            us[:, n : n + size] = jnp.dot(n_all[at, :], u_buf[:, cols], preferred_element_type=f32)
            gr[:, n : n + size] = dot_nt(cot_all[at, :], d_buf[cols, :])
        column = first_unit + offset + lax.broadcasted_iota(jnp.int32, (1, width), 1)
        owned = (column >= shard * 2240) & (column < (shard + 1) * 2240)

        def body(j, carry):
            part = pl.ds(pl.multiple_of(j * 16, 16), 16)
            to = pl.ds(pl.multiple_of(m * 512 + j * 16, 16), 16)
            cols = pl.ds(offset, width)
            gate, up, grad = gs[part, 0:width], us[part, 0:width], gr[part, 0:width]
            sig = jax.nn.sigmoid(gate)
            silu = gate * sig
            act[to, cols] = jnp.where(owned, silu * up, 0.0).astype(bf16)
            gate_delta[to, cols] = jnp.where(owned, grad * up * sig * (1.0 + gate * (1.0 - sig)), 0.0).astype(bf16)
            up_delta[to, cols] = jnp.where(owned, grad * silu, 0.0).astype(bf16)
            return carry

        lax.fori_loop(0, 32, body, 0)

    def transpose(src, cols, dst):
        def body(j, carry):
            at = pl.ds(pl.multiple_of(j * 128, 128), 128)
            dst[:, at] = src[at, cols].T
            return carry

        lax.fori_loop(0, 8, body, 0)

    outs = {}

    def write(name, buf, at, cols=None):
        n = 9 + len(outs)
        src = buf.at[at] if cols is None else buf.at[at, cols]
        dst = v[name].at[at] if cols is None else v[name].at[at, cols]
        copy = pltpu.make_async_copy(src, dst, v["local"].at[n])
        copy.start()
        outs[n] = copy

    for tile, (offset, width, _) in enumerate(TILES):
        cols = pl.ds(offset, width)
        for m in range(2):
            products(offset, width, m)
            service()
        transpose(act, cols, v["act_t"].at[pl.ds(0, width)])
        if tile == 0:
            transpose(n_all, pl.ds(0, 1536), v["n_t_buf"])
        service()
        for n in range(3):
            out = pl.ds(n * 512, 512)
            v["d_grad"][cols, out] = (
                jnp.dot(v["act_t"][0:width, :], cot_all[:, out], preferred_element_type=f32) * grad_scale
            ).astype(bf16)
        write("pd", v["d_grad"], cols)
        service()
        for name, buf in (("act", act), ("gd", gate_delta), ("ud", up_delta)):
            write(name, buf, pl.ds(0, 1024), cols)
        while pending:
            service()
        if tile == 0:
            write("n_t", v["n_t_buf"], pl.ds(0, 1536))
            take_shared(4)
            take_shared(5)
            write("w_g", g_buf, pl.ds(0, 1536))
            write("w_u", u_buf, pl.ds(0, 1536))
            write("w_d", d_buf, pl.ds(0, WINDOW))
    keep_q.wait()
    keep_o.wait()
    for i in (0, 1):
        for d in order:
            p = peer_of(shard, d)
            hop(i, d, p, shard).wait_send()
            across(i, d, p, odd).wait_send()
            for part in (False, True):
                onward(i, d, p, core, part).wait_send()
    for copy in outs.values():
        copy.wait()
    for d in order:
        p = peer_of(shard, d)
        small_hop(d, p, shard).wait_send()
        for i in (2, 3, 4, 5):
            hop(i, d, p, shard).wait_send()
            across(i, d, p, odd).wait_send()
        for a in range(2):
            row_hop(a, d, p, shard).wait_send()
    for a in range(2):
        for d in (0,) + order:
            row_onward(a, d, peer_of(shard, d), core).wait_send()


def forward(grad_scale, **given):
    bf16 = jnp.bfloat16
    f32 = jnp.float32
    dma = pltpu.SemaphoreType.DMA
    in_vmem = ("x", "small", "cos", "sin")
    outs = {
        "q_full": ((1536, 2048), bf16, any_spec()),
        "o_full": ((1536, 1536), bf16, any_spec()),
        "pd": ((WINDOW, 1536), bf16, any_spec()),
        "act": ((1024, WINDOW), bf16, any_spec()),
        "gd": ((1024, WINDOW), bf16, any_spec()),
        "ud": ((1024, WINDOW), bf16, any_spec()),
        "n_t": ((1536, 1024), bf16, any_spec()),
        "w_g": ((1536, WINDOW), bf16, any_spec()),
        "w_u": ((1536, WINDOW), bf16, any_spec()),
        "w_d": ((WINDOW, 1536), bf16, any_spec()),
        "hidden": ((128, 1536), f32, vmem_spec()),
        "nrm": ((128, 1536), bf16, vmem_spec()),
        "ctx": ((128, 1536), bf16, vmem_spec()),
        "qry": ((128, 1536), bf16, vmem_spec()),
        "key": ((128, KV * HD), bf16, vmem_spec()),
        "val": ((128, KV * HD), bf16, vmem_spec()),
        "lse": ((128, HD), f32, vmem_spec()),
        "gains": ((8, 1536), f32, vmem_spec()),
    }
    scratch = {
        "q_buf": pltpu.VMEM((1536, 2048), bf16),
        "o_buf": pltpu.VMEM((1536, 1536), bf16),
        "g_buf": pltpu.VMEM((1536, WINDOW), bf16),
        "u_buf": pltpu.VMEM((1536, WINDOW), bf16),
        "d_buf": pltpu.VMEM((WINDOW, 1536), bf16),
        "n_all": pltpu.VMEM((1024, 1536), bf16),
        "cot_all": pltpu.VMEM((1024, 1536), bf16),
        "small_all": pltpu.VMEM((4, 16, 512), bf16),
        "prj": pltpu.VMEM((128, 2048), f32),
        "act_buf": pltpu.VMEM((1024, WINDOW), bf16),
        "gd_buf": pltpu.VMEM((1024, WINDOW), bf16),
        "ud_buf": pltpu.VMEM((1024, WINDOW), bf16),
        "n_t_buf": pltpu.VMEM((1536, 1024), bf16),
        "act_t": pltpu.VMEM((640, 1024), bf16),
        "gs": pltpu.VMEM((512, 640), f32),
        "us": pltpu.VMEM((512, 640), f32),
        "gr": pltpu.VMEM((512, 640), f32),
        "d_grad": pltpu.VMEM((WINDOW, 1536), bf16),
        "send": dma((27,)),
        "recv": dma((27,)),
        "zsend": dma((18,)),
        "zrecv": dma((18,)),
        "fsend": dma((20,)),
        "frecv": dma((20,)),
        "local": dma((24,)),
    }
    return dict(zip(outs, pl.pallas_call(
        functools.partial(forward_kernel, grad_scale, (*given, *outs, *scratch)),
        out_shape=[jax.ShapeDtypeStruct(s, dt) for s, dt, _ in outs.values()],
        in_specs=[vmem_spec() if name in in_vmem else any_spec() for name in given],
        out_specs=[spec for _, _, spec in outs.values()],
        scratch_shapes=list(scratch.values()),
        compiler_params=pltpu.CompilerParams(has_side_effects=True, vmem_limit_bytes=67043328),
    )(*given.values())))


def backward_kernel(levels, grad_scale, names, *refs):
    v = dict(zip(names, refs))
    replica, shard, core = place()
    other = 1 - core
    level = replica // 2
    mate = (replica + 1 - 2 * core, shard)
    above, below = (replica + 2, shard), (replica - 2, shard)
    f32 = jnp.float32
    bf16 = jnp.bfloat16
    order = (3, 1, 2)
    own_a, own_d, own_g = v["own_a"], v["own_d"], v["own_g"]
    mat, act, wbuf, back, out = v["mat"], v["act_buf"], v["wbuf"], v["back"], v["out"]
    odd_chip = lax.rem(shard, 2)

    def tokens(owner, c):
        return pl.ds(pl.multiple_of((c * 4 + owner) * 128, 128), 128)

    def chip_at(d):
        across = lax.rem(lax.rem(shard, 2) + lax.rem(d, 2), 2)
        return lax.rem(shard // 2 + d // 2, 2) * 2 + across

    def exchange(block, chip):
        return remote(
            v["blocks"].at[block - 2], own_g.at[pl.ds(pl.multiple_of(block * 384, 384), 384)],
            v["xsend"].at[block], v["xrecv"].at[block], (replica, chip),
        )

    load_down = pltpu.make_async_copy(v["pd"], own_d, v["in_sem"].at[0])
    load_normed = pltpu.make_async_copy(v["n_t"], wbuf.at[:, pl.ds(0, 1024)], v["in_sem"].at[1])
    load_gate = pltpu.make_async_copy(v["w_g"], wbuf.at[:, pl.ds(WINDOW, WINDOW)], v["in_sem"].at[2])
    load_up = pltpu.make_async_copy(v["w_u"], wbuf.at[:, pl.ds(0, WINDOW)], v["in_sem"].at[3])
    load_wd = pltpu.make_async_copy(v["w_d"], wbuf.at[pl.ds(0, WINDOW), pl.ds(0, 1536)], v["in_sem"].at[4])
    load_deltas = [
        pltpu.make_async_copy(v["gd"], mat.at[0], v["in_sem"].at[5]),
        pltpu.make_async_copy(v["ud"], mat.at[1], v["in_sem"].at[6]),
    ]
    load_act = pltpu.make_async_copy(v["act"], act, v["in_sem"].at[7])

    def staged(block):
        slot = lax.rem(block, 2)
        return pltpu.make_async_copy(
            back.at[pl.ds(pl.multiple_of(slot * 384, 384), 384), pl.ds(0, WINDOW)], v["blocks"].at[block - 2],
            v["stage_sem"].at[slot],
        )

    def stage_gradient(block):
        d, a = block // 2, lax.rem(block, 2)
        rows = pl.ds(pl.multiple_of(chip_at(d) * 384, 384), 384)

        @pl.when(block >= 4)
        def _():
            staged(block - 2).wait()

        for n in range(3):
            cols = pl.ds(n * 384, 384)
            part = (
                jnp.dot(wbuf[rows, 0:1024], mat[a, :, cols], preferred_element_type=f32) * grad_scale
            ).astype(bf16)

            @pl.when(d == 0)
            def _():
                own_g[pl.ds(pl.multiple_of(a * 384, 384), 384), cols] = part

            @pl.when(d > 0)
            def _():
                back[pl.ds(pl.multiple_of(a * 384, 384), 384), cols] = part

        @pl.when(block >= 2)
        def _():
            staged(block).start()

    def start_back():
        load_up.start()
        staged(6).wait()
        staged(7).wait()
        load_gate.wait()
        load_up.wait()

    def piece(i):
        return pl.ds(pl.multiple_of((i // 3) * 256, 256), 256), pl.ds(pl.multiple_of(lax.rem(i, 3) * 512, 512), 512)

    def stage_back(i):
        at, cols = piece(i)
        back[at, cols] = (
            dot_nt(mat[0, at, :], wbuf[cols, WINDOW : 2 * WINDOW]) + dot_nt(mat[1, at, :], wbuf[cols, 0:WINDOW])
        ).astype(bf16)

    def stage_out(i):
        at, cols = piece(i)
        out[at, cols] = jnp.dot(act[at, :], wbuf[0:WINDOW, cols], preferred_element_type=f32).astype(bf16)

    partial = (back, out)
    held, parts = v["held"], v["parts"]

    def kept(a, d):
        return partial[a].at[tokens(peer_of(shard, d), core)]

    def to_mate(a, d):
        n = a * 4 + d
        return remote(partial[a].at[tokens(peer_of(shard, d), other)], held.at[a, d], v["csend"].at[n], v["crecv"].at[n], mate)

    def to_owner(a, d):
        n = a * 3 + d - 1
        return remote(kept(a, d), parts.at[a, d - 1], v["psend"].at[n], v["precv"].at[n], (replica, peer_of(shard, d)))

    def pair_sums(a):
        for d in order:
            to_mate(a, d).wait_recv()
            mine = kept(a, d)

            def body(rows, carry):
                mine[rows, :] = (mine[rows, :].astype(f32) + held[a, d, rows, :].astype(f32)).astype(bf16)
                return carry

            row_loop(128, 32, body, 0)
            to_owner(a, d).start()

    def collect(a):
        to_mate(a, 0).wait_recv()
        for d in order:
            to_owner(a, d).wait_recv()

    def full_sum(a, rows):
        total = kept(a, 0)[rows, :].astype(f32) + held[a, 0, rows, :].astype(f32)
        for d in (1, 2, 3):
            total = total + parts[a, d - 1, rows, :].astype(f32)
        return total

    wide = ((v["hid"], mat.at[0, :, pl.ds(0, 768)], 768), (v["prj"], mat.at[1, :, pl.ds(0, 1024)], 1024))
    narrow = ((v["ctx"], v["ctx_all"], 384), (v["nrm"], v["nrm_all"], 384))

    def block(out, owner, c):
        return out.at[tokens(owner, c)]

    def columns(ref, index, width):
        return ref.at[:, pl.ds(pl.multiple_of(index * width, width), width)]

    def wide_copy(a, d, same, source_core, owner, t):
        ref, out, width = wide[a]
        c = core if same else other
        n = (a * 4 + d) * 2 + (0 if same else 1)
        return remote(
            columns(ref, c, width), block(out, owner, source_core), v["gsend"].at[n], v["grecv"].at[n],
            (replica - core + c, t),
        )

    def narrow_copy(a, d, owner, t):
        ref, out, width = narrow[a]
        n = 16 + a * 4 + d
        return remote(columns(ref, t, width), block(out, owner, core), v["gsend"].at[n], v["grecv"].at[n], (replica, t))

    def onward(a, d, source, owner, c):
        out = narrow[a][1]
        n = a * 4 + d
        return remote(source, block(out, owner, c), v["fsend"].at[n], v["frecv"].at[n], mate)

    def own_narrow(a):
        ref, out, width = narrow[a]
        return pltpu.make_async_copy(columns(ref, shard, width), block(out, shard, core), v["local"].at[a])

    def own_wide(a):
        ref, out, width = wide[a]
        return pltpu.make_async_copy(columns(ref, core, width), block(out, shard, core), v["local"].at[2 + a])

    load_out = pltpu.make_async_copy(v["wo"], wbuf.at[:, pl.ds(0, 1536)], v["local"].at[4])
    load_qkv = pltpu.make_async_copy(v["wq"], wbuf.at[:, pl.ds(0, 2048)], v["local"].at[5])

    def stage_sums():
        pair_sums(0)
        for d in order:
            for a in range(2):
                narrow_copy(a, d, shard, peer_of(shard, d)).start()
        send_blocks((1, 2))

    def send_blocks(offsets):
        for d in offsets:
            for a in range(2):
                exchange(d * 2 + a, peer_of(shard, d)).start()

    def stage_hidden():
        collect(0)
        gain = v["gain_two"][...]

        def body(rows, total):
            grad = full_sum(0, rows)
            hidden = v["hidden"][rows, :]
            inv = lax.rsqrt(jnp.mean(hidden * hidden, axis=-1, keepdims=True) + NORM_EPS)
            scaled = gain * grad
            out = v["cot"][rows, :].astype(f32) + inv * (
                scaled - hidden * inv * inv * jnp.mean(scaled * hidden, axis=-1, keepdims=True)
            )
            v["hgrad"][rows, :] = out
            v["hid"][rows, :] = out.astype(bf16)
            return total + jnp.sum(grad * hidden * inv, axis=0, keepdims=True)

        v["row_two"][...] = row_loop(128, 16, body, jnp.zeros((1, 1536), f32)) * grad_scale
        for d in (0,) + order:
            if d:
                wide_copy(0, d, True, core, shard, peer_of(shard, d)).start()
            wide_copy(0, d, False, core, shard, peer_of(shard, d)).start()
        own_wide(0).start()

    def stage_context(part):
        if part == 0:
            load_out.wait()
        for e in (2 * part, 2 * part + 1):
            cols = pl.ds(e * 384, 384)
            v["cgrad"][:, cols] = dot_nt(v["hid"][...], wbuf[cols, 0:1536]).astype(bf16)
        if part == 1:
            load_qkv.start()

    def unrotated(x):
        return x * v["cos"][...] + pltpu.roll(x, HD // 2, 1) * v["sin"][...]

    def stage_heads(g, part):
        keys = v["key"][:, g * HD : (g + 1) * HD]
        values = v["val"][:, g * HD : (g + 1) * HD]
        causal = lax.broadcasted_iota(jnp.int32, (128, 128), 0) >= lax.broadcasted_iota(jnp.int32, (128, 128), 1)
        key_grad = jnp.zeros((128, HD), f32) if part == 0 else v["kv_sum"][0]
        value_grad = jnp.zeros((128, HD), f32) if part == 0 else v["kv_sum"][1]
        first_head = g * (HEADS // KV) + part * 2
        for h in range(first_head, first_head + 2):
            at = slice(h * HD, (h + 1) * HD)
            query = v["qry"][:, at]
            grad = v["cgrad"][:, at]
            scores = jnp.where(causal, dot_nt(query, keys) * SCORE_SCALE, -1e30)
            probs = jnp.exp(scores - v["lse"][:, h : h + 1]).astype(bf16)
            wide_probs = probs.astype(f32)
            prob_grad = dot_nt(grad, values)
            delta = jnp.sum(wide_probs * prob_grad, axis=-1, keepdims=True)
            score_grad = (wide_probs * (prob_grad - delta) * SCORE_SCALE).astype(bf16)
            v["prj"][:, at] = unrotated(jnp.dot(score_grad, keys, preferred_element_type=f32)).astype(bf16)
            key_grad = key_grad + dot_tn(score_grad, query)
            value_grad = value_grad + dot_tn(probs, grad)
        if part < 2:
            v["kv_sum"][0] = key_grad
            v["kv_sum"][1] = value_grad
            return
        first = HEADS * HD + g * HD
        v["prj"][:, first : first + HD] = unrotated(key_grad).astype(bf16)
        first = first + KV * HD
        v["prj"][:, first : first + HD] = value_grad.astype(bf16)

    def stage_send_projected():
        for d in (0,) + order:
            if d:
                wide_copy(1, d, True, core, shard, peer_of(shard, d)).start()
            wide_copy(1, d, False, core, shard, peer_of(shard, d)).start()
        own_wide(1).start()

    def stage_normed(part):
        if part == 0:
            load_qkv.wait()
        for e in (2 * part, 2 * part + 1):
            cols = pl.ds(e * 384, 384)
            v["input_grad"][:, cols] = dot_nt(v["prj"][...], wbuf[cols, 0:2048])

    vec, vin, vall = v["vec"], v["vin"], v["vall"]
    replicas = 2 * levels

    def vec_hop(d):
        return remote(vec.at[peer_of(shard, d)], vin.at[d - 1], v["vsend"].at[d - 1], v["vrecv"].at[d - 1],
                      (replica, peer_of(shard, d)))

    def vec_spread(j, slot):
        target = lax.rem(replica + j, replicas)
        return remote(v["vsum"], vall.at[slot], v["vsend"].at[2 + j], v["vrecv"].at[2 + j], (target, shard))

    def stage_input():
        gain = v["gain_one"][...]

        def body(rows, totals):
            total, bias = totals
            x = v["x"][rows, :].astype(f32)
            grad = v["input_grad"][rows, :]
            inv = lax.rsqrt(jnp.mean(x * x, axis=-1, keepdims=True) + NORM_EPS)
            scaled = gain * grad
            v["input_grad"][rows, :] = v["hgrad"][rows, :] + inv * (
                scaled - x * inv * inv * jnp.mean(scaled * x, axis=-1, keepdims=True)
            )
            return (
                total + jnp.sum(grad * x * inv, axis=0, keepdims=True),
                bias + jnp.sum(v["prj"][rows, :].astype(f32), axis=0, keepdims=True),
            )

        row_one, row_bias = row_loop(128, 16, body, (jnp.zeros((1, 1536), f32), jnp.zeros((1, 2048), f32)))
        row_one = row_one * grad_scale
        row_bias = row_bias * grad_scale
        row_two = v["row_two"][...]
        for s in range(4):
            vec[s, :, 0:384] = jnp.broadcast_to(row_one[:, s * 384 : (s + 1) * 384], (8, 384))
            vec[s, :, 384:896] = jnp.broadcast_to(row_bias[:, s * 512 : (s + 1) * 512], (8, 512))
            vec[s, :, 896:1280] = jnp.broadcast_to(row_two[:, s * 384 : (s + 1) * 384], (8, 384))
        for d in order:
            vec_hop(d).start()

    def stage_vec():
        total = vec[shard]
        for d in (1, 2, 3):
            vec_hop(d).wait_recv()
            total = total + vin[d - 1]
        v["vsum"][...] = total
        for j in range(1, replicas):
            vec_spread(j, replica).start()

    def stage_vec_out():
        vall[replica] = v["vsum"][...]
        for j in range(1, replicas):
            vec_spread(j, lax.rem(replica + replicas - j, replicas)).wait_recv()
        total = vall[0]
        for j in range(1, replicas):
            total = total + vall[j]
        v["vec_out"][...] = total

    def stage_output():
        collect(1)

        def body(rows, carry):
            v["block_out"][rows, :] = (v["hidden"][rows, :] + full_sum(1, rows)).astype(bf16)
            return carry

        row_loop(128, 32, body, 0)

    def stage_relay():
        for d in order:
            p = peer_of(shard, d)
            for a in range(2):
                narrow_copy(a, d, p, p).wait_recv()
                onward(a, d, block(narrow[a][1], p, core), p, core).start()

    def stage_gathered():
        for a in range(2):
            own_narrow(a).wait()
            own_wide(a).wait()
            for d in (0, 1, 2, 3):
                p = peer_of(shard, d)
                if d:
                    wide_copy(a, d, True, core, p, p).wait_recv()
                wide_copy(a, d, False, other, p, p).wait_recv()
                onward(a, d, block(narrow[a][1], p, other), p, other).wait_recv()

    def stage_attention_parts(j):
        at = pl.ds(j * 128, 128)
        own_a[at, 0:1024] = (dot_tn(v["nrm_all"][:, at], mat[1, :, 0:1024]) * grad_scale).astype(bf16)
        own_a[at, 1024:1792] = (dot_tn(v["ctx_all"][:, at], mat[0, :, 0:768]) * grad_scale).astype(bf16)

    def down_at(c, j):
        first = odd_chip * (1088 * c - 64 * (1 - c)) + (1 - odd_chip) * 1152 * c
        return v["fd"].at[pl.ds(pl.multiple_of(first + j * 64, 64), 64)]

    def gate_at(c, j):
        group = j // 6
        rows = pl.ds(pl.multiple_of(lax.rem(j, 6) * 64, 64), 64)
        return v["fg"].at[lax.rem(group, 2), c, chip_at(group // 2), rows]

    def attention_at(c, j):
        return v["fa"].at[c, pl.ds(pl.multiple_of(j * 32, 32), 32)]

    segments = (
        (own_d, v["near_d"], v["far_d"], 64, 0, DOWN_STEPS, down_at),
        (own_g, v["near_g"], v["far_g"], 64, DOWN_STEPS, DOWN_STEPS + GATE_STEPS, gate_at),
        (own_a, v["near_a"], v["far_a"], 32, DOWN_STEPS + GATE_STEPS, CHUNKS, attention_at),
    )
    end = (level == 0) | (level == levels - 1)
    middle = levels // 2

    def on(k, stage, c=None):
        c = core if c is None else c
        for n, segment in enumerate(segments):
            j = k - segment[4]
            inside = (k >= segment[4]) & (k < segment[5])
            if n == 0:
                inside &= (j > 0) | (1 - odd_chip + c > 0)
                inside &= (j < DOWN_STEPS - 1) | (odd_chip + 1 - c > 0)
            pl.when(inside)(functools.partial(stage, n, segment, j, k))

    def rows_of(segment, j):
        size = segment[3]
        return pl.ds(pl.multiple_of(j * size, size), size)

    def message(segment, j, k, upward, near):
        own, near_ref, far_ref = segment[:3]
        target = near_ref.at[rows_of(segment, j)] if near else far_ref.at[rows_of(segment, j // 2)]
        sem = v["near_sem"] if near else v["far_sem"]
        return remote(own.at[rows_of(segment, j)], target, v["part_sem"].at[k], sem.at[k], above if upward else below)

    def result(segment, j, k, upward, from_own):
        place_ = segment[6](core, j)
        src = segment[0].at[rows_of(segment, j)] if from_own else place_
        sem = v["up_sem"] if upward else v["down_sem"]
        return remote(src, place_, sem.at[k], v["done_sem"].at[k], above if upward else below)

    def keep_result(segment, j, k):
        return pltpu.make_async_copy(segment[0].at[rows_of(segment, j)], segment[6](core, j), v["out_sem"].at[k])

    def to_other_core(segment, j, k, from_own, c):
        place_ = segment[6](c, j)
        src = segment[0].at[rows_of(segment, j)] if from_own else place_
        return remote(src, place_, v["mate_send"].at[k], v["mate_recv"].at[k], mate)

    def add(segment, j, with_far):
        own, near_ref, far_ref, size = segment[:4]

        def body(i, carry):
            rows = pl.ds(pl.multiple_of(j * size + i * 16, 16), 16)
            value = own[rows, :].astype(f32) + near_ref[rows, :].astype(f32)
            if with_far:
                value = value + far_ref[pl.ds(pl.multiple_of((j // 2) * size + i * 16, 16), 16), :].astype(f32)
            own[rows, :] = value.astype(own.dtype)
            return carry

        lax.fori_loop(0, size // 16, body, 0)

    def arrived(n, j):
        if n != 1:
            return
        group = j // 6

        @pl.when((lax.rem(j, 6) == 0) & (group >= 2))
        def _():
            exchange(group, shard).wait_recv()

    def root_of(k):
        return middle - 1 + lax.rem(k, 2)

    def end_gather(n, segment, j, k):
        @pl.when(end)
        def _():
            arrived(n, j)

        @pl.when(level == 0)
        def _():
            message(segment, j, k, True, True).start()

        @pl.when(level == levels - 1)
        def _():
            message(segment, j, k, False, True).start()

    def gather_step(n, segment, j, k):
        @pl.when(~end)
        def _():
            arrived(n, j)

            @pl.when(level != root_of(k))
            def _():
                message(segment, j, k, True, True).wait_recv()
                add(segment, j, False)

        for upward in (True, False):
            towards = (level > 0) & (level < root_of(k)) if upward else (level < levels - 1) & (level > root_of(k))
            crosses = level == (middle - 1 if upward else middle)

            @pl.when(towards & crosses)
            def _():
                message(segment, j, k, upward, False).start()

            if levels > 4:

                @pl.when(towards & ~crosses)
                def _():
                    message(segment, j, k, upward, True).start()

    def root_step(n, segment, j, k):
        @pl.when(level == root_of(k))
        def _():
            message(segment, j, k, True, True).wait_recv()
            message(segment, j, k, True, False).wait_recv()
            add(segment, j, True)
            result(segment, j, k, True, True).start()
            result(segment, j, k, False, True).start()
            keep_result(segment, j, k).start()
            to_other_core(segment, j, k, True, core).start()

    def spread_step(n, segment, j, k):
        @pl.when(~end & (level != root_of(k)))
        def _():
            result(segment, j, k, True, False).wait_recv()

            @pl.when(level < root_of(k))
            def _():
                result(segment, j, k, False, False).start()

            @pl.when(level > root_of(k))
            def _():
                result(segment, j, k, True, False).start()

            to_other_core(segment, j, k, False, core).start()

    def end_spread(n, segment, j, k):
        @pl.when(end)
        def _():
            result(segment, j, k, True, False).wait_recv()
            to_other_core(segment, j, k, False, core).start()

    def close(n, segment, j, k):
        root = root_of(k)

        @pl.when(level == root)
        def _():
            result(segment, j, k, True, True).wait_send()
            result(segment, j, k, False, True).wait_send()
            keep_result(segment, j, k).wait()

        @pl.when(level != root)
        def _():
            message(segment, j, k, True, True).wait_send()

        @pl.when(~end & (level < root))
        def _():
            result(segment, j, k, False, False).wait_send()

        @pl.when(~end & (level > root))
        def _():
            result(segment, j, k, True, False).wait_send()

        to_other_core(segment, j, k, True, core).wait_send()

    def close_mate(n, segment, j, k):
        to_other_core(segment, j, k, True, other).wait_recv()

    def start_mate(a):
        for d in order + (0,):
            to_mate(a, d).start()

    load_down.start()
    load_normed.start()
    for copy in load_deltas:
        copy.start()
    load_gate.start()
    load_act.start()
    for a in range(2):
        own_narrow(a).start()
        onward(a, 0, columns(narrow[a][0], shard, 384), shard, core).start()
    load_down.wait()
    lags = ((end_gather, 0), (gather_step, 8), (root_step, 14), (spread_step, 20), (end_spread, 28))
    steps = CHUNKS + lags[-1][1]

    def begin_products():
        load_normed.wait()
        for copy in load_deltas:
            copy.wait()

    def begin_out():
        start_mate(0)
        load_wd.start()
        load_act.wait()

    def end_out():
        start_mate(1)
        load_out.start()

    def stage_projected():
        stage_send_projected()
        send_blocks((3,))

    beside = [
        (0, 1, begin_products),
        (0, 8, stage_gradient),
        (8, 1, start_back),
        (8, 6, lambda i: (stage_back(2 * i), stage_back(2 * i + 1))),
        (14, 1, begin_out),
        (16, 1, stage_sums),
        (17, 1, load_wd.wait),
        (17, 4, lambda i: (stage_out(3 * i), stage_out(3 * i + 1), stage_out(3 * i + 2))),
        (21, 1, end_out),
        (22, 1, stage_hidden),
        (24, 1, functools.partial(stage_context, 0)),
        (25, 1, functools.partial(stage_context, 1)),
    ]
    for n in range(6):
        beside.append((26 + n, 1, functools.partial(stage_heads, n // 3, n % 3)))
    beside += [
        (31, 1, stage_projected),
        (32, 1, functools.partial(stage_normed, 0)),
        (34, 1, functools.partial(stage_normed, 1)),
        (36, 1, stage_input),
        (38, 1, stage_relay),
        (56, 1, stage_gathered),
        (56, 1, functools.partial(stage_attention_parts, 0)),
        (58, 1, functools.partial(stage_attention_parts, 1)),
        (60, 1, functools.partial(stage_attention_parts, 2)),
        (62, 1, functools.partial(pair_sums, 1)),
        (64, 1, stage_vec),
        (steps - 4, 1, stage_vec_out),
        (steps - 2, 1, stage_output),
    ]

    def step(t, carry):
        for stage, lag in lags:
            on(t - lag, stage)
        for first, count, stage in beside:
            if count == 1:
                pl.when(t == first)(stage)
            else:
                @pl.when((t >= first) & (t < first + count))
                def _():
                    stage(t - first)

        return carry

    lax.fori_loop(0, steps, step, 0)

    def finish_step(k, carry):
        on(k, close)
        on(k, close_mate, other)
        return carry

    lax.fori_loop(0, CHUNKS, finish_step, 0)
    for d in (1, 2, 3):
        for a in range(2):
            exchange(d * 2 + a, peer_of(shard, d)).wait_send()
    for a in range(2):
        for d in (0, 1, 2, 3):
            p = peer_of(shard, d)
            to_mate(a, d).wait_send()
            wide_copy(a, d, False, core, shard, p).wait_send()
            onward(a, d, block(narrow[a][1], p, core), p, core).wait_send()
            if d:
                to_owner(a, d).wait_send()
                wide_copy(a, d, True, core, shard, p).wait_send()
                narrow_copy(a, d, shard, p).wait_send()
    for d in order:
        vec_hop(d).wait_send()
    for j in range(1, replicas):
        vec_spread(j, replica).wait_send()


def backward(levels, grad_scale, **given):
    bf16 = jnp.bfloat16
    f32 = jnp.float32
    dma = pltpu.SemaphoreType.DMA
    in_hbm = ("pd", "act", "gd", "ud", "n_t", "w_g", "w_u", "w_d", "wo", "wq")
    outs = {
        "fa": ((2, 384, 1792), bf16, any_spec()),
        "fd": ((2240, 1536), bf16, any_spec()),
        "fg": ((2, 2, 4, 384, WINDOW), bf16, any_spec()),
        "blocks": ((6, 384, WINDOW), bf16, any_spec()),
        "block_out": ((128, 1536), bf16, vmem_spec()),
        "input_grad": ((128, 1536), f32, vmem_spec()),
        "vec_out": ((8, 1280), f32, vmem_spec()),
    }
    scratch = {
        "own_a": pltpu.VMEM((384, 1792), bf16),
        "own_d": pltpu.VMEM((WINDOW, 1536), bf16),
        "own_g": pltpu.VMEM((3072, WINDOW), bf16),
        "near_a": pltpu.VMEM((384, 1792), bf16),
        "near_d": pltpu.VMEM((WINDOW, 1536), bf16),
        "near_g": pltpu.VMEM((3072, WINDOW), bf16),
        "far_a": pltpu.VMEM((192, 1792), bf16),
        "far_d": pltpu.VMEM((WINDOW // 2, 1536), bf16),
        "far_g": pltpu.VMEM((1536, WINDOW), bf16),
        "mat": pltpu.VMEM((2, 1024, WINDOW), bf16),
        "act_buf": pltpu.VMEM((1024, WINDOW), bf16),
        "wbuf": pltpu.VMEM((1536, 2 * WINDOW), bf16),
        "back": pltpu.VMEM((1024, 1536), bf16),
        "out": pltpu.VMEM((1024, 1536), bf16),
        "held": pltpu.VMEM((2, 4, 128, 1536), bf16),
        "parts": pltpu.VMEM((2, 3, 128, 1536), bf16),
        "hgrad": pltpu.VMEM((128, 1536), f32),
        "hid": pltpu.VMEM((128, 1536), bf16),
        "cgrad": pltpu.VMEM((128, 1536), bf16),
        "prj": pltpu.VMEM((128, 2048), bf16),
        "ctx_all": pltpu.VMEM((1024, 384), bf16),
        "nrm_all": pltpu.VMEM((1024, 384), bf16),
        "row_two": pltpu.VMEM((1, 1536), f32),
        "kv_sum": pltpu.VMEM((2, 128, HD), f32),
        "vec": pltpu.VMEM((4, 8, 1280), f32),
        "vin": pltpu.VMEM((3, 8, 1280), f32),
        "vsum": pltpu.VMEM((8, 1280), f32),
        "vall": pltpu.VMEM((2 * levels, 8, 1280), f32),
    }
    counts = {
        "xsend": 8, "xrecv": 8, "stage_sem": 2, "csend": 8, "crecv": 8, "psend": 6, "precv": 6, "gsend": 24, "grecv": 24,
        "fsend": 8, "frecv": 8, "local": 6, "in_sem": 8, "vsend": 2 + 2 * levels, "vrecv": 2 + 2 * levels,
    }
    for name in (
        "part_sem", "near_sem", "far_sem", "up_sem", "down_sem", "done_sem", "mate_send", "mate_recv", "out_sem"
    ):
        counts[name] = CHUNKS
    scratch |= {name: dma((n,)) for name, n in counts.items()}
    return pl.pallas_call(
        functools.partial(backward_kernel, levels, grad_scale, (*given, *outs, *scratch)),
        out_shape=[jax.ShapeDtypeStruct(s, dt) for s, dt, _ in outs.values()],
        in_specs=[any_spec() if name in in_hbm else vmem_spec() for name in given],
        out_specs=[spec for _, _, spec in outs.values()],
        scratch_shapes=list(scratch.values()),
        compiler_params=pltpu.CompilerParams(has_side_effects=True, vmem_limit_bytes=67043328),
    )(*given.values())


def widen_kernel(gate, up, down, attn, out_gate, out_up, out_down, out_qkv, out_out):
    f32 = jnp.float32
    for x, out in ((gate, out_gate), (up, out_up)):
        for s in range(4):
            for c in range(2):
                first = (s * 35) // 2 + c * 9
                rest = 1 if s % 2 == 1 and c == 0 else 0
                out[:, (first + rest) * 128 : (first + 9) * 128] = x[c, s][:, rest * 128 :].astype(f32)
        for s in (1, 3):
            first = (s * 35) // 2
            out[:, first * 128 : (first + 1) * 128] = x[1, s - 1][:, 1024:].astype(f32) + x[0, s][:, :128].astype(f32)
    out_down[...] = down[...].astype(f32)
    for c in range(2):
        out_qkv[:, c * 1024 : (c + 1) * 1024] = attn[c][:, :1024].astype(f32)
        out_out[:, c * 768 : (c + 1) * 768] = attn[c][:, 1024:].astype(f32)


def widen(*sums):
    rows = 32
    f32 = jnp.float32
    def blocks(a):
        return pl.BlockSpec((None, 2, 4, rows, WINDOW), lambda i: (a, 0, 0, i, 0))

    down = pl.BlockSpec((224, 1536), lambda i: (jnp.minimum(i, 9), 0))

    def whole(width):
        return pl.BlockSpec((rows, width), lambda i: (i, 0))

    return pl.pallas_call(
        widen_kernel,
        grid=(384 // rows,),
        out_shape=[
            jax.ShapeDtypeStruct((384, 8960), f32),
            jax.ShapeDtypeStruct((384, 8960), f32),
            jax.ShapeDtypeStruct((2240, 1536), f32),
            jax.ShapeDtypeStruct((384, 2048), f32),
            jax.ShapeDtypeStruct((384, 1536), f32),
        ],
        in_specs=[blocks(0), blocks(1), down, pl.BlockSpec((2, rows, 1792), lambda i: (0, i, 0))],
        out_specs=[whole(8960), whole(8960), down, whole(2048), whole(1536)],
    )(*sums)


def fast_device(
    block_input,
    attn_gain,
    qkv_weight,
    qkv_bias,
    out_weight,
    mlp_gain,
    gate_weight,
    up_weight,
    down_weight,
    cotangent,
):
    f32 = jnp.float32
    tok_count = block_input.shape[0]
    levels = lax.axis_size("replica") // 2
    grad_scale = 1.0 / math.sqrt(tok_count * lax.axis_size("replica") * lax.axis_size("shard"))
    cosine, sine_table = rope_tables(tok_count)
    small = jnp.stack([jnp.pad(attn_gain, (0, 128)), qkv_bias, jnp.pad(mlp_gain, (0, 128))])
    small = jnp.pad(small, ((0, 13), (0, 0)))
    twice = jnp.concatenate([cosine[:, 0], cosine[:, 0]], axis=1)
    turn = jnp.concatenate([-sine_table[:, 0], sine_table[:, 0]], axis=1)
    got = forward(
        grad_scale,
        x=block_input,
        small=small,
        cos=twice,
        sin=turn,
        wq=qkv_weight,
        wo=out_weight,
        wg=gate_weight,
        wu=up_weight,
        wd=down_weight,
        cot=cotangent,
    )
    sum_attn, sum_down, sum_gate, _, block_output, input_grad, vectors = backward(
        levels,
        grad_scale,
        pd=got["pd"],
        act=got["act"],
        gd=got["gd"],
        ud=got["ud"],
        n_t=got["n_t"],
        w_g=got["w_g"],
        w_u=got["w_u"],
        w_d=got["w_d"],
        wo=got["o_full"],
        wq=got["q_full"],
        hidden=got["hidden"],
        x=block_input,
        cot=cotangent,
        gain_one=got["gains"][0:1],
        gain_two=got["gains"][1:2],
        ctx=got["ctx"],
        nrm=got["nrm"],
        qry=got["qry"],
        key=got["key"],
        val=got["val"],
        lse=got["lse"],
        cos=twice,
        sin=-turn,
    )
    gain_one_own, bias_own, gain_two_own = vectors[0, :384], vectors[0, 384:896], vectors[0, 896:]
    gate_grad, up_grad, down_grad, qkv_grad, out_grad = widen(sum_gate, sum_gate, sum_down, sum_attn)
    return (
        block_output,
        input_grad,
        gain_one_own,
        qkv_grad,
        bias_own,
        out_grad,
        gain_two_own,
        gate_grad,
        up_grad,
        down_grad,
    )


def solution(mesh):
    placed = (
        P(("replica", "shard"), None),
        P("shard"),
        P("shard", None),
        P("shard"),
        P("shard", None),
        P("shard"),
        P("shard", None),
        P("shard", None),
        P("shard", None),
        P(("replica", "shard"), None),
    )
    fits = mesh.shape["shard"] == 4 and mesh.shape["replica"] % 4 == 0
    per_device = fast_device if fits else general_device
    return jax.shard_map(
        per_device,
        mesh=mesh,
        in_specs=placed,
        out_specs=(
            P(("replica", "shard"), None),
            P(("replica", "shard"), None),
            P("shard"),
            P("shard", None),
            P("shard"),
            P("shard", None),
            P("shard"),
            P("shard", None),
            P("shard", None),
            P("shard", None),
        ),
        check_vma=False,
    )
```

```python
import functools
import math

import jax
import jax.numpy as jnp
from jax import lax
from jax.experimental import pallas as pl
from jax.experimental.pallas import tpu as pltpu
from jax.sharding import PartitionSpec as P

HEADS = 12
KV = 2
HD = 128


NORM_EPS = 1e-06
ROPE_BASE = 1000000.0


def rope_tables(tok_count):
    half_dim = HD // 2
    position = jnp.arange(tok_count, dtype=jnp.float32)
    inverse = ROPE_BASE ** (-(jnp.arange(half_dim, dtype=jnp.float32) * 2.0 / HD))
    angles = position[:, None] * inverse[None, :]
    return (jnp.cos(angles)[:, None, :], jnp.sin(angles)[:, None, :])


def rotate(vectors, cosine, sine_table):
    half_dim = HD // 2
    lower_half = vectors[..., :half_dim]
    upper_half = vectors[..., half_dim:]
    return jnp.concatenate(
        [
            lower_half * cosine - upper_half * sine_table,
            upper_half * cosine + lower_half * sine_table,
        ],
        axis=-1,
    )


def unrotate(grads, cosine, sine_table):
    half_dim = HD // 2
    lower_half = grads[..., :half_dim]
    upper_half = grads[..., half_dim:]
    return jnp.concatenate(
        [
            lower_half * cosine + upper_half * sine_table,
            upper_half * cosine - lower_half * sine_table,
        ],
        axis=-1,
    )


def block_scores(query_block, key_rot, first_row):
    row_count = query_block.shape[0]
    scores = jnp.einsum(
        "qkgd,skd->kgqs", query_block, key_rot, preferred_element_type=jnp.float32
    ) * (1.0 / math.sqrt(HD))
    causal = (first_row + jnp.arange(row_count))[:, None] >= jnp.arange(key_rot.shape[0])[None, :]
    return jnp.where(causal, scores, -1e30)


def block_layout(tok_count):
    block_rows = min(tok_count, 512)
    block_count = tok_count // block_rows
    firsts = jnp.arange(block_count, dtype=jnp.int32) * block_rows
    return (block_rows, block_count, firsts)


def attend_forward(queries, key_rot, values):
    tok_count = queries.shape[0]
    block_rows, block_count, firsts = block_layout(tok_count)
    query_blocks = queries.reshape(block_count, block_rows, KV, HEADS // KV, HD)

    def one_block(inputs):
        query_block, first_row = inputs
        scores = block_scores(query_block, key_rot, first_row)
        row_max = jnp.max(scores, axis=-1, keepdims=True)
        logsum = row_max + jnp.log(jnp.sum(jnp.exp(scores - row_max), axis=-1, keepdims=True))
        attn_probs = jnp.exp(scores - logsum).astype(jnp.bfloat16)
        context = jnp.einsum(
            "kgqs,skd->qkgd", attn_probs, values, preferred_element_type=jnp.float32
        ).astype(jnp.bfloat16)
        return (context, logsum)

    context, logsum = lax.map(one_block, (query_blocks, firsts))
    return (context.reshape(tok_count, HEADS * HD), logsum)


def attend_backward(queries, key_rot, values, logsum, context_grad):
    tok_count = queries.shape[0]
    block_rows, block_count, firsts = block_layout(tok_count)
    query_blocks = queries.reshape(block_count, block_rows, KV, HEADS // KV, HD)
    grad_blocks = context_grad.reshape(block_count, block_rows, KV, HEADS // KV, HD)
    score_scale = 1.0 / math.sqrt(HD)

    def one_block(running, inputs):
        key_total, value_total = running
        query_block, grad_block, log_block, first_row = inputs
        scores = block_scores(query_block, key_rot, first_row)
        attn_probs = jnp.exp(scores - log_block).astype(jnp.bfloat16)
        prob_grad = jnp.einsum(
            "qkgd,skd->kgqs", grad_block, values, preferred_element_type=jnp.float32
        )
        wide_probs = attn_probs.astype(jnp.float32)
        row_delta = jnp.sum(wide_probs * prob_grad, axis=-1, keepdims=True)
        score_grad = (wide_probs * (prob_grad - row_delta) * score_scale).astype(jnp.bfloat16)
        query_grad = jnp.einsum(
            "kgqs,skd->qkgd", score_grad, key_rot, preferred_element_type=jnp.float32
        )
        key_total = key_total + jnp.einsum(
            "kgqs,qkgd->skd", score_grad, query_block, preferred_element_type=jnp.float32
        )
        value_total = value_total + jnp.einsum(
            "kgqs,qkgd->skd", attn_probs, grad_block, preferred_element_type=jnp.float32
        )
        return ((key_total, value_total), query_grad)

    zero_keys = jnp.zeros((tok_count, KV, HD), jnp.float32)
    (key_grad, value_grad), query_grad = lax.scan(
        one_block, (zero_keys, zero_keys), (query_blocks, grad_blocks, logsum, firsts)
    )
    return (query_grad.reshape(tok_count, HEADS, HD), key_grad, value_grad)


def general_device(
    block_input,
    attn_gain,
    qkv_weight,
    qkv_bias,
    out_weight,
    mlp_gain,
    gate_weight,
    up_weight,
    down_weight,
    cotangent,
):
    f32 = jnp.float32
    bf16 = jnp.bfloat16
    tok_count = block_input.shape[0]
    grad_scale = 1.0 / math.sqrt(tok_count * lax.axis_size("replica") * lax.axis_size("shard"))
    q_width = HEADS * HD
    k_end = q_width + KV * HD
    cosine, sine_table = rope_tables(tok_count)
    attn_full = (
        lax.all_gather(attn_gain, "shard", axis=0, tiled=True),
        lax.all_gather(qkv_weight, "shard", axis=0, tiled=True),
        lax.all_gather(qkv_bias, "shard", axis=0, tiled=True),
        lax.all_gather(out_weight, "shard", axis=0, tiled=True),
    )
    gain_full, qkv_full, bias_full, out_full = attn_full
    gain_one = gain_full.astype(f32)
    xfloat = block_input.astype(f32)
    inv_one = lax.rsqrt(jnp.mean(xfloat * xfloat, axis=-1, keepdims=True) + NORM_EPS)
    normed_one = (xfloat * inv_one * gain_one).astype(bf16)
    projected = jnp.dot(normed_one, qkv_full, preferred_element_type=f32) + bias_full.astype(f32)
    queries = rotate(
        projected[:, :q_width].reshape(tok_count, HEADS, HD), cosine, sine_table
    ).astype(bf16)
    queries = queries.reshape(tok_count, KV, HEADS // KV, HD)
    key_rot = rotate(
        projected[:, q_width:k_end].reshape(tok_count, KV, HD), cosine, sine_table
    ).astype(bf16)
    values = projected[:, k_end:].reshape(tok_count, KV, HD).astype(bf16)
    context, logsum = attend_forward(queries, key_rot, values)
    hidden_res = xfloat + jnp.dot(context, out_full, preferred_element_type=f32)
    mlp_full = (
        lax.all_gather(mlp_gain, "shard", axis=0, tiled=True),
        lax.all_gather(gate_weight, "shard", axis=0, tiled=True),
        lax.all_gather(up_weight, "shard", axis=0, tiled=True),
        lax.all_gather(down_weight, "shard", axis=0, tiled=True),
    )
    gain_full_two, gate_full, up_full, down_full = mlp_full
    gain_two = gain_full_two.astype(f32)
    inv_two = lax.rsqrt(jnp.mean(hidden_res * hidden_res, axis=-1, keepdims=True) + NORM_EPS)
    normed_two = (hidden_res * inv_two * gain_two).astype(bf16)
    gate_pre = jnp.dot(normed_two, gate_full, preferred_element_type=f32)
    up_pre = jnp.dot(normed_two, up_full, preferred_element_type=f32)
    sigmoid_gate = jax.nn.sigmoid(gate_pre)
    silu_gate = gate_pre * sigmoid_gate
    activation = (silu_gate * up_pre).astype(bf16)
    block_output = (hidden_res + jnp.dot(activation, down_full, preferred_element_type=f32)).astype(
        bf16
    )
    act_grad = jnp.einsum("td,fd->tf", cotangent, down_full, preferred_element_type=f32)
    gate_delta = (
        act_grad * up_pre * sigmoid_gate * (1.0 + gate_pre * (1.0 - sigmoid_gate))
    ).astype(bf16)
    up_delta = (act_grad * silu_gate).astype(bf16)
    normed_two_grad = jnp.einsum(
        "tf,df->td", gate_delta, gate_full, preferred_element_type=f32
    ) + jnp.einsum("tf,df->td", up_delta, up_full, preferred_element_type=f32)
    gain_two_grad = jnp.sum(normed_two_grad * hidden_res * inv_two, axis=0) * grad_scale
    own_rows = (
        lax.all_to_all(activation, "shard", split_axis=1, concat_axis=0, tiled=True),
        lax.all_to_all(normed_two, "shard", split_axis=1, concat_axis=0, tiled=True),
    )
    group_act, group_normed = own_rows
    group_rows = (
        lax.all_gather(cotangent, "shard", axis=0, tiled=True),
        lax.all_gather(gate_delta, "shard", axis=0, tiled=True),
        lax.all_gather(up_delta, "shard", axis=0, tiled=True),
    )
    group_cot, group_gate, group_up = group_rows
    down_part = (
        jnp.einsum("tf,td->fd", group_act, group_cot, preferred_element_type=f32) * grad_scale
    )
    gate_own = (
        jnp.einsum("td,tf->df", group_normed, group_gate, preferred_element_type=f32) * grad_scale
    )
    up_own = (
        jnp.einsum("td,tf->df", group_normed, group_up, preferred_element_type=f32) * grad_scale
    )
    gain_two_own = lax.psum_scatter(gain_two_grad, "shard", scatter_dimension=0, tiled=True)
    mlp_parts = (gain_two_own, gate_own, up_own)
    hidden_grad = cotangent.astype(f32) + inv_two * (
        gain_two * normed_two_grad
        - hidden_res
        * inv_two
        * inv_two
        * jnp.mean(gain_two * normed_two_grad * hidden_res, axis=-1, keepdims=True)
    )
    hidden_low = hidden_grad.astype(bf16)
    context_grad = jnp.einsum("td,ed->te", hidden_low, out_full, preferred_element_type=f32).astype(
        bf16
    )
    query_grad, key_grad, value_grad = attend_backward(
        queries, key_rot, values, logsum, context_grad
    )
    query_grad = unrotate(query_grad, cosine, sine_table).reshape(tok_count, q_width)
    key_grad = unrotate(key_grad, cosine, sine_table).reshape(tok_count, KV * HD)
    projected_grad = jnp.concatenate(
        [query_grad, key_grad, value_grad.reshape(tok_count, KV * HD)], axis=-1
    ).astype(bf16)
    normed_one_grad = jnp.einsum("tc,dc->td", projected_grad, qkv_full, preferred_element_type=f32)
    gain_one_grad = jnp.sum(normed_one_grad * xfloat * inv_one, axis=0) * grad_scale
    bias_grad = jnp.sum(projected_grad.astype(f32), axis=0) * grad_scale
    own_attn = (
        lax.all_to_all(context, "shard", split_axis=1, concat_axis=0, tiled=True),
        lax.all_to_all(normed_one, "shard", split_axis=1, concat_axis=0, tiled=True),
    )
    group_context, group_normed_one = own_attn
    group_rows = (
        lax.all_gather(hidden_low, "shard", axis=0, tiled=True),
        lax.all_gather(projected_grad, "shard", axis=0, tiled=True),
    )
    group_hidden, group_projected = group_rows
    out_own = (
        jnp.einsum("te,td->ed", group_context, group_hidden, preferred_element_type=f32)
        * grad_scale
    )
    qkv_part = (
        jnp.einsum("td,tc->dc", group_normed_one, group_projected, preferred_element_type=f32)
        * grad_scale
    )
    small_parts = (
        lax.psum_scatter(gain_one_grad, "shard", scatter_dimension=0, tiled=True),
        lax.psum_scatter(bias_grad, "shard", scatter_dimension=0, tiled=True),
    )
    attn_parts = (small_parts[0], qkv_part, small_parts[1], out_own)
    input_grad = hidden_grad + inv_one * (
        gain_one * normed_one_grad
        - xfloat
        * inv_one
        * inv_one
        * jnp.mean(gain_one * normed_one_grad * xfloat, axis=-1, keepdims=True)
    )
    summed = lax.psum(
        (
            attn_parts[0],
            attn_parts[1],
            attn_parts[2],
            attn_parts[3],
            mlp_parts[0],
            mlp_parts[1],
            mlp_parts[2],
            down_part,
        ),
        "replica",
    )
    attn_parts = (summed[0], summed[1], summed[2], summed[3])
    mlp_parts = (summed[4], summed[5], summed[6])
    down_part = summed[7]
    return (
        block_output,
        input_grad,
        attn_parts[0],
        attn_parts[1],
        attn_parts[2],
        attn_parts[3],
        mlp_parts[0],
        mlp_parts[1],
        mlp_parts[2],
        down_part,
    )


MESH = pl.DeviceIdType.MESH
VMEM_BYTES = 62 * 2**20
WINDOW = 1152


def place():
    replica = lax.axis_index("replica")
    shard = lax.axis_index("shard")
    core = lax.rem(replica, 2)
    return replica, shard, core


def peer_of(shard, d):
    across = lax.rem(lax.rem(shard, 2) + d % 2, 2)
    up = lax.rem(shard // 2 + d // 2, 2)
    return up * 2 + across


def window_start(shard, core):
    return ((shard * 35) // 2 + core * 9) * 128


def remote(src, dst, send, recv, device):
    return pltpu.make_async_remote_copy(
        src_ref=src,
        dst_ref=dst,
        send_sem=send,
        recv_sem=recv,
        device_id=device,
        device_id_type=MESH,
    )


def any_spec():
    return pl.BlockSpec(memory_space=pl.ANY)


def vmem_spec():
    return pl.BlockSpec(memory_space=pltpu.VMEM)


def params(**more):
    return pltpu.CompilerParams(has_side_effects=True, vmem_limit_bytes=VMEM_BYTES, **more)


DOWN_STEPS, GATE_STEPS, ATTENTION_STEPS = 18, 48, 12
CHUNKS = DOWN_STEPS + GATE_STEPS + ATTENTION_STEPS
SCORE_SCALE = 1.0 / math.sqrt(HD)


def dot_nt(a, b):
    return lax.dot_general(a, b, (((1,), (1,)), ((), ())), preferred_element_type=jnp.float32)


def dot_tn(a, b):
    return lax.dot_general(a, b, (((0,), (0,)), ((), ())), preferred_element_type=jnp.float32)


def row_loop(rows, step, body, init):
    return lax.fori_loop(0, rows // step, lambda j, c: body(pl.ds(pl.multiple_of(j * step, step), step), c), init)


TILES = ((0, 640, 160), (640, 512, 160))


def forward_kernel(grad_scale, names, *refs):
    v = dict(zip(names, refs))
    f32 = jnp.float32
    bf16 = jnp.bfloat16
    replica, shard, core = place()
    other = 1 - core
    mate = (replica + 1 - 2 * core, shard)
    odd = lax.rem(replica // 2, 2)
    pair = (replica + 2 - 4 * odd, shard)
    order = (3, 1, 2)
    first_unit = window_start(shard, core)
    q_buf, o_buf, g_buf, u_buf, d_buf = v["q_buf"], v["o_buf"], v["g_buf"], v["u_buf"], v["d_buf"]
    n_all, cot_all, small_all = v["n_all"], v["cot_all"], v["small_all"]

    def span(start, size):
        return pl.ds(pl.multiple_of(start, 16), size)

    def units(target, offset, width):
        return pl.ds(pl.multiple_of(window_start(target, core) + offset, 128), width)

    def tokens(owner, c):
        return pl.ds(pl.multiple_of((c * 4 + owner) * 128, 128), 128)

    weights = [
        (lambda t: v["wq"], q_buf, 192, 80, True),
        (lambda t: v["wo"], o_buf, 192, 80, True),
    ]
    for offset, width, shared in TILES:
        for name, buf in (("wg", g_buf), ("wu", u_buf)):
            weights.append((
                lambda t, name=name, offset=offset, width=width: v[name].at[:, units(t, offset, width)],
                buf.at[:, pl.ds(offset, width)], 384, shared, False,
            ))

    def base(i, c):
        return c * 192 if weights[i][4] else 0

    def hop(i, d, t, o):
        source, out, size, shared, _ = weights[i]
        first = base(i, core) + odd * shared
        n = i * 3 + d - 1
        return remote(
            source(t).at[span(first, size - shared)], out.at[span(o * 384 + first, size - shared)],
            v["send"].at[n], v["recv"].at[n], (replica, t),
        )

    def relay(i, way, t, o):
        _, out, size, shared, _ = weights[i]
        first = o * 384 + base(i, core) + odd * shared
        ref = out.at[span(first, 64)] if way == 1 else out.at[span(first + 64, size - shared - 64)]
        n = i * 2 + way - 1
        return remote(ref, ref, v["rsend"].at[n], v["rrecv"].at[n], (replica, t))

    def across(i, d, o, whose):
        _, out, size, shared, _ = weights[i]
        ref = out.at[span(o * 384 + base(i, core) + whose * (size - shared), shared)]
        n = i * 3 + d - 1
        return remote(ref, ref, v["zsend"].at[n], v["zrecv"].at[n], pair)

    def onward(i, d, o, c, shared_part):
        _, out, size, shared, _ = weights[i]
        first = o * 384 + base(i, c) + ((1 - odd) * (size - shared) if shared_part else odd * shared)
        ref = out.at[span(first, shared if shared_part else size - shared)]
        n = i * 3 + d - 1 + (6 if shared_part else 0)
        return remote(ref, ref, v["fsend"].at[n], v["frecv"].at[n], mate)

    row_sets = (cot_all, n_all)

    def row_hop(a, d, t, o):
        n = 18 + a * 3 + d - 1
        return remote(row_sets[a].at[tokens(shard, core)], row_sets[a].at[tokens(o, core)], v["send"].at[n], v["recv"].at[n],
                      (replica, t))

    def row_relay(a, way, t, o):
        ref = row_sets[a].at[span((core * 4 + o) * 128 + 64 * (way - 1), 64)]
        n = 4 + a * 2 + way - 1
        return remote(ref, ref, v["rsend"].at[n], v["rrecv"].at[n], (replica, t))

    def row_onward(a, d, o, c):
        n = 12 + a * 4 + d
        ref = row_sets[a].at[tokens(o, c)]
        return remote(ref, ref, v["fsend"].at[n], v["frecv"].at[n], mate)

    def small_hop(d, t, o):
        n = 24 + d - 1
        return remote(v["small"], small_all.at[o], v["send"].at[n], v["recv"].at[n], (replica, t))

    def send_rows(a):
        for d in (1, 2):
            row_hop(a, d, peer_of(shard, d), shard).start()
        row_onward(a, 0, shard, core).start()

    def take_rows(a):
        for d in (1, 2):
            p = peer_of(shard, d)
            row_hop(a, d, p, p).wait_recv()
            row_relay(a, d, peer_of(shard, 3 - d), p).start()
            row_onward(a, d, p, core).start()

    def take_far_rows(a):
        p = peer_of(shard, 3)
        for way in (1, 2):
            row_relay(a, way, p, p).wait_recv()
        row_onward(a, 3, p, core).start()

    def have_rows(a):
        for d in (0,) + order:
            row_onward(a, d, peer_of(shard, d), other).wait_recv()

    def send_weight(i):
        for d in (1, 2) if weights[i][4] else order:
            hop(i, d, peer_of(shard, d), shard).start()

    def take(i, d):
        p = peer_of(shard, d)
        relayed = weights[i][4]
        if relayed and d == 3:
            for way in (1, 2):
                relay(i, way, p, p).wait_recv()
        else:
            hop(i, d, p, p).wait_recv()
            if relayed:
                relay(i, d, peer_of(shard, 3 - d), p).start()
        across(i, d, p, odd).start()
        if relayed:
            onward(i, d, p, core, False).start()

    def take_shared(i):
        for d in order:
            p = peer_of(shard, d)
            across(i, d, p, 1 - odd).wait_recv()
            if weights[i][4]:
                onward(i, d, p, core, True).start()

    def have_other_half(i):
        for d in order:
            for part in (False, True):
                onward(i, d, peer_of(shard, d), other, part).wait_recv()

    rows = span(shard * 384, 384)
    loads = [
        pltpu.make_async_copy(v["cot"], cot_all.at[tokens(shard, core)], v["local"].at[0]),
        pltpu.make_async_copy(v["wq"], q_buf.at[rows], v["local"].at[1]),
        pltpu.make_async_copy(v["wo"], o_buf.at[rows], v["local"].at[2]),
        pltpu.make_async_copy(v["wg"].at[:, units(shard, 0, WINDOW)], g_buf.at[rows], v["local"].at[3]),
        pltpu.make_async_copy(v["wu"].at[:, units(shard, 0, WINDOW)], u_buf.at[rows], v["local"].at[4]),
    ]
    odd_chip = lax.rem(shard, 2)
    inside = odd_chip == core
    loads.append(pltpu.make_async_copy(
        v["wd"].at[span((1152 - 64 * odd_chip) * core, 1088)],
        d_buf.at[span(odd_chip * (1 - core) * 64, 1088)], v["local"].at[5],
    ))

    for d in order:
        small_hop(d, peer_of(shard, d), shard).start()
    send_weight(0)
    send_weight(1)
    for copy in loads:
        copy.start()
    rest = pltpu.make_async_copy(
        v["wd"].at[span((2176 - 1088) * core + 1088, 64)], d_buf.at[pl.ds(1088, 64)], v["local"].at[6]
    )

    @pl.when(inside)
    def _():
        rest.start()

    @pl.when(~inside)
    def _():
        d_buf[span(1088 - 1088 * odd_chip, 64), :] = jnp.zeros((64, 1536), bf16)

    small_all[shard] = v["small"][...]
    for d in order:
        p = peer_of(shard, d)
        small_hop(d, p, p).wait_recv()

    def gathered(row, width):
        return jnp.concatenate([small_all[s, row : row + 1, 0:width].astype(f32) for s in range(4)], axis=1)

    gain_one = gathered(0, 384)

    def norm_body(at, carry):
        x = v["x"][at, :].astype(f32)
        inv = lax.rsqrt(jnp.mean(x * x, axis=-1, keepdims=True) + NORM_EPS)
        v["nrm"][at, :] = (x * inv * gain_one).astype(bf16)
        return carry

    row_loop(128, 16, norm_body, 0)
    for copy in loads:
        copy.wait()

    @pl.when(inside)
    def _():
        rest.wait()

    for i in (0, 1):
        for d in (1, 2):
            take(i, d)
    send_rows(0)
    send_weight(2)
    send_weight(3)
    take(0, 3)
    take(1, 3)
    take_shared(0)
    have_other_half(0)
    keep_q = pltpu.make_async_copy(q_buf, v["q_full"], v["local"].at[7])
    keep_q.start()
    bias = gathered(1, 512)

    def rotated(x):
        return x * v["cos"][...] + pltpu.roll(x, HD // 2, 1) * v["sin"][...]

    def project(head, out, at, turn):
        cols = slice(head * HD, (head + 1) * HD)
        x = v["prj"][:, cols] + bias[:, cols]
        out[:, at * HD : (at + 1) * HD] = (rotated(x) if turn else x).astype(bf16)

    for n in range(4):
        v["prj"][:, n * 512 : (n + 1) * 512] = jnp.dot(
            v["nrm"][...], q_buf[:, n * 512 : (n + 1) * 512], preferred_element_type=f32
        )
    take_shared(1)
    for h in range(HEADS):
        project(h, v["qry"], h, True)
    for g in range(KV):
        project(HEADS + g, v["key"], g, True)
        project(HEADS + KV + g, v["val"], g, False)
    causal = lax.broadcasted_iota(jnp.int32, (128, 128), 0) >= lax.broadcasted_iota(jnp.int32, (128, 128), 1)
    v["lse"][...] = jnp.zeros((128, HD), f32)
    for h in range(HEADS):
        g = h // (HEADS // KV)
        at = slice(h * HD, (h + 1) * HD)
        scores = dot_nt(v["qry"][:, at], v["key"][:, g * HD : (g + 1) * HD]) * SCORE_SCALE
        scores = jnp.where(causal, scores, -1e30)
        row_max = jnp.max(scores, axis=-1, keepdims=True)
        logsum = row_max + jnp.log(jnp.sum(jnp.exp(scores - row_max), axis=-1, keepdims=True))
        v["lse"][:, h : h + 1] = logsum
        probs = jnp.exp(scores - logsum).astype(bf16)
        v["ctx"][:, at] = jnp.dot(probs, v["val"][:, g * HD : (g + 1) * HD], preferred_element_type=f32).astype(bf16)
    have_other_half(1)
    keep_o = pltpu.make_async_copy(o_buf, v["o_full"], v["local"].at[8])
    keep_o.start()
    for n in range(3):
        cols = slice(n * 512, (n + 1) * 512)
        v["hidden"][:, cols] = v["x"][:, cols].astype(f32) + jnp.dot(
            v["ctx"][...], o_buf[:, cols], preferred_element_type=f32
        )
    gain_two = gathered(2, 384)
    v["gains"][0:1, :] = gain_one
    v["gains"][1:2, :] = gain_two

    def norm_two(j, carry):
        at = pl.ds(pl.multiple_of(j * 16, 16), 16)
        hidden = v["hidden"][at, :]
        inv = lax.rsqrt(jnp.mean(hidden * hidden, axis=-1, keepdims=True) + NORM_EPS)
        n_all[span((core * 4 + shard) * 128 + j * 16, 16), :] = (hidden * inv * gain_two).astype(bf16)
        return carry

    lax.fori_loop(0, 8, norm_two, 0)
    send_rows(1)
    take_rows(0)
    for i in (2, 3):
        for d in order:
            take(i, d)
    take_rows(1)
    send_weight(4)
    send_weight(5)
    take_far_rows(0)
    take_far_rows(1)
    take_shared(2)
    take_shared(3)
    have_rows(0)
    have_rows(1)

    act, gate_delta, up_delta = v["act_buf"], v["gd_buf"], v["ud_buf"]
    gs, us, gr = v["gs"], v["us"], v["gr"]
    pending = [(i, d) for i in (4, 5) for d in order]

    def service():
        if pending:
            take(*pending.pop(0))

    def products(offset, width, m):
        at = pl.ds(m * 512, 512)
        for n in range(0, width, 256):
            size = min(256, width - n)
            cols = pl.ds(offset + n, size)
            gs[:, n : n + size] = jnp.dot(n_all[at, :], g_buf[:, cols], preferred_element_type=f32)
            us[:, n : n + size] = jnp.dot(n_all[at, :], u_buf[:, cols], preferred_element_type=f32)
            gr[:, n : n + size] = dot_nt(cot_all[at, :], d_buf[cols, :])
        column = first_unit + offset + lax.broadcasted_iota(jnp.int32, (1, width), 1)
        owned = (column >= shard * 2240) & (column < (shard + 1) * 2240)

        def body(j, carry):
            part = pl.ds(pl.multiple_of(j * 16, 16), 16)
            to = pl.ds(pl.multiple_of(m * 512 + j * 16, 16), 16)
            cols = pl.ds(offset, width)
            gate, up, grad = gs[part, 0:width], us[part, 0:width], gr[part, 0:width]
            sig = jax.nn.sigmoid(gate)
            silu = gate * sig
            act[to, cols] = jnp.where(owned, silu * up, 0.0).astype(bf16)
            gate_delta[to, cols] = jnp.where(owned, grad * up * sig * (1.0 + gate * (1.0 - sig)), 0.0).astype(bf16)
            up_delta[to, cols] = jnp.where(owned, grad * silu, 0.0).astype(bf16)
            return carry

        lax.fori_loop(0, 32, body, 0)

    def transpose(src, cols, dst):
        def body(j, carry):
            at = pl.ds(pl.multiple_of(j * 128, 128), 128)
            dst[:, at] = src[at, cols].T
            return carry

        lax.fori_loop(0, 8, body, 0)

    outs = {}

    def write(name, buf, at, cols=None):
        n = 9 + len(outs)
        src = buf.at[at] if cols is None else buf.at[at, cols]
        dst = v[name].at[at] if cols is None else v[name].at[at, cols]
        copy = pltpu.make_async_copy(src, dst, v["local"].at[n])
        copy.start()
        outs[n] = copy

    for tile, (offset, width, _) in enumerate(TILES):
        cols = pl.ds(offset, width)
        for m in range(2):
            products(offset, width, m)
            service()
        transpose(act, cols, v["act_t"].at[pl.ds(0, width)])
        if tile == 0:
            transpose(n_all, pl.ds(0, 1536), v["n_t_buf"])
        service()
        for n in range(3):
            out = pl.ds(n * 512, 512)
            v["d_grad"][cols, out] = (
                jnp.dot(v["act_t"][0:width, :], cot_all[:, out], preferred_element_type=f32) * grad_scale
            ).astype(bf16)
        write("pd", v["d_grad"], cols)
        service()
        for name, buf in (("act", act), ("gd", gate_delta), ("ud", up_delta)):
            write(name, buf, pl.ds(0, 1024), cols)
        while pending:
            service()
        if tile == 0:
            write("n_t", v["n_t_buf"], pl.ds(0, 1536))
            take_shared(4)
            take_shared(5)
            write("w_g", g_buf, pl.ds(0, 1536))
            write("w_u", u_buf, pl.ds(0, 1536))
            write("w_d", d_buf, pl.ds(0, WINDOW))
    keep_q.wait()
    keep_o.wait()
    for i in (0, 1):
        for d in order:
            p = peer_of(shard, d)
            if d < 3:
                hop(i, d, p, shard).wait_send()
                relay(i, d, peer_of(shard, 3 - d), p).wait_send()
            across(i, d, p, odd).wait_send()
            for part in (False, True):
                onward(i, d, p, core, part).wait_send()
    for copy in outs.values():
        copy.wait()
    for d in order:
        p = peer_of(shard, d)
        small_hop(d, p, shard).wait_send()
        for i in (2, 3, 4, 5):
            hop(i, d, p, shard).wait_send()
            across(i, d, p, odd).wait_send()
        for a in range(2):
            if d < 3:
                row_hop(a, d, p, shard).wait_send()
                row_relay(a, d, peer_of(shard, 3 - d), p).wait_send()
    for a in range(2):
        for d in (0,) + order:
            row_onward(a, d, peer_of(shard, d), core).wait_send()


def forward(grad_scale, **given):
    bf16 = jnp.bfloat16
    f32 = jnp.float32
    dma = pltpu.SemaphoreType.DMA
    in_vmem = ("x", "small", "cos", "sin")
    outs = {
        "q_full": ((1536, 2048), bf16, any_spec()),
        "o_full": ((1536, 1536), bf16, any_spec()),
        "pd": ((WINDOW, 1536), bf16, any_spec()),
        "act": ((1024, WINDOW), bf16, any_spec()),
        "gd": ((1024, WINDOW), bf16, any_spec()),
        "ud": ((1024, WINDOW), bf16, any_spec()),
        "n_t": ((1536, 1024), bf16, any_spec()),
        "w_g": ((1536, WINDOW), bf16, any_spec()),
        "w_u": ((1536, WINDOW), bf16, any_spec()),
        "w_d": ((WINDOW, 1536), bf16, any_spec()),
        "hidden": ((128, 1536), f32, vmem_spec()),
        "nrm": ((128, 1536), bf16, vmem_spec()),
        "ctx": ((128, 1536), bf16, vmem_spec()),
        "qry": ((128, 1536), bf16, vmem_spec()),
        "key": ((128, KV * HD), bf16, vmem_spec()),
        "val": ((128, KV * HD), bf16, vmem_spec()),
        "lse": ((128, HD), f32, vmem_spec()),
        "gains": ((8, 1536), f32, vmem_spec()),
    }
    scratch = {
        "q_buf": pltpu.VMEM((1536, 2048), bf16),
        "o_buf": pltpu.VMEM((1536, 1536), bf16),
        "g_buf": pltpu.VMEM((1536, WINDOW), bf16),
        "u_buf": pltpu.VMEM((1536, WINDOW), bf16),
        "d_buf": pltpu.VMEM((WINDOW, 1536), bf16),
        "n_all": pltpu.VMEM((1024, 1536), bf16),
        "cot_all": pltpu.VMEM((1024, 1536), bf16),
        "small_all": pltpu.VMEM((4, 16, 512), bf16),
        "prj": pltpu.VMEM((128, 2048), f32),
        "act_buf": pltpu.VMEM((1024, WINDOW), bf16),
        "gd_buf": pltpu.VMEM((1024, WINDOW), bf16),
        "ud_buf": pltpu.VMEM((1024, WINDOW), bf16),
        "n_t_buf": pltpu.VMEM((1536, 1024), bf16),
        "act_t": pltpu.VMEM((640, 1024), bf16),
        "gs": pltpu.VMEM((512, 640), f32),
        "us": pltpu.VMEM((512, 640), f32),
        "gr": pltpu.VMEM((512, 640), f32),
        "d_grad": pltpu.VMEM((WINDOW, 1536), bf16),
        "send": dma((27,)),
        "recv": dma((27,)),
        "rsend": dma((8,)),
        "rrecv": dma((8,)),
        "zsend": dma((18,)),
        "zrecv": dma((18,)),
        "fsend": dma((20,)),
        "frecv": dma((20,)),
        "local": dma((24,)),
    }
    return dict(zip(outs, pl.pallas_call(
        functools.partial(forward_kernel, grad_scale, (*given, *outs, *scratch)),
        out_shape=[jax.ShapeDtypeStruct(s, dt) for s, dt, _ in outs.values()],
        in_specs=[vmem_spec() if name in in_vmem else any_spec() for name in given],
        out_specs=[spec for _, _, spec in outs.values()],
        scratch_shapes=list(scratch.values()),
        compiler_params=pltpu.CompilerParams(has_side_effects=True, vmem_limit_bytes=67043328),
    )(*given.values())))


def backward_kernel(levels, grad_scale, names, *refs):
    v = dict(zip(names, refs))
    replica, shard, core = place()
    other = 1 - core
    level = replica // 2
    mate = (replica + 1 - 2 * core, shard)
    above, below = (replica + 2, shard), (replica - 2, shard)
    f32 = jnp.float32
    bf16 = jnp.bfloat16
    order = (3, 1, 2)
    own_a, own_d, own_g = v["own_a"], v["own_d"], v["own_g"]
    mat, act, wbuf, back, out = v["mat"], v["act_buf"], v["wbuf"], v["back"], v["out"]
    odd_chip = lax.rem(shard, 2)

    def tokens(owner, c):
        return pl.ds(pl.multiple_of((c * 4 + owner) * 128, 128), 128)

    def chip_at(d):
        across = lax.rem(lax.rem(shard, 2) + lax.rem(d, 2), 2)
        return lax.rem(shard // 2 + d // 2, 2) * 2 + across

    def exchange(block, chip):
        return remote(
            v["blocks"].at[block - 2], own_g.at[pl.ds(pl.multiple_of(block * 384, 384), 384)],
            v["xsend"].at[block], v["xrecv"].at[block], (replica, chip),
        )

    load_down = pltpu.make_async_copy(v["pd"], own_d, v["in_sem"].at[0])
    load_normed = pltpu.make_async_copy(v["n_t"], wbuf.at[:, pl.ds(0, 1024)], v["in_sem"].at[1])
    load_gate = pltpu.make_async_copy(v["w_g"], wbuf.at[:, pl.ds(WINDOW, WINDOW)], v["in_sem"].at[2])
    load_up = pltpu.make_async_copy(v["w_u"], wbuf.at[:, pl.ds(0, WINDOW)], v["in_sem"].at[3])
    load_wd = pltpu.make_async_copy(v["w_d"], wbuf.at[pl.ds(0, WINDOW), pl.ds(0, 1536)], v["in_sem"].at[4])
    load_deltas = [
        pltpu.make_async_copy(v["gd"], mat.at[0], v["in_sem"].at[5]),
        pltpu.make_async_copy(v["ud"], mat.at[1], v["in_sem"].at[6]),
    ]
    load_act = pltpu.make_async_copy(v["act"], act, v["in_sem"].at[7])

    def staged(block):
        slot = lax.rem(block, 2)
        return pltpu.make_async_copy(
            back.at[pl.ds(pl.multiple_of(slot * 384, 384), 384), pl.ds(0, WINDOW)], v["blocks"].at[block - 2],
            v["stage_sem"].at[slot],
        )

    def stage_gradient(block):
        d, a = block // 2, lax.rem(block, 2)
        rows = pl.ds(pl.multiple_of(chip_at(d) * 384, 384), 384)

        @pl.when(block >= 4)
        def _():
            staged(block - 2).wait()

        for n in range(3):
            cols = pl.ds(n * 384, 384)
            part = (
                jnp.dot(wbuf[rows, 0:1024], mat[a, :, cols], preferred_element_type=f32) * grad_scale
            ).astype(bf16)

            @pl.when(d == 0)
            def _():
                own_g[pl.ds(pl.multiple_of(a * 384, 384), 384), cols] = part

            @pl.when(d > 0)
            def _():
                back[pl.ds(pl.multiple_of(a * 384, 384), 384), cols] = part

        @pl.when(block >= 2)
        def _():
            staged(block).start()

    def start_back():
        load_up.start()
        staged(6).wait()
        staged(7).wait()
        load_gate.wait()
        load_up.wait()

    def piece(i):
        return pl.ds(pl.multiple_of((i // 3) * 256, 256), 256), pl.ds(pl.multiple_of(lax.rem(i, 3) * 512, 512), 512)

    def stage_back(i):
        at, cols = piece(i)
        back[at, cols] = (
            dot_nt(mat[0, at, :], wbuf[cols, WINDOW : 2 * WINDOW]) + dot_nt(mat[1, at, :], wbuf[cols, 0:WINDOW])
        ).astype(bf16)

    def stage_out(i):
        at, cols = piece(i)
        out[at, cols] = jnp.dot(act[at, :], wbuf[0:WINDOW, cols], preferred_element_type=f32).astype(bf16)

    partial = (back, out)
    held, parts = v["held"], v["parts"]

    def kept(a, d):
        return partial[a].at[tokens(peer_of(shard, d), core)]

    def to_mate(a, d):
        n = a * 4 + d
        return remote(partial[a].at[tokens(peer_of(shard, d), other)], held.at[a, d], v["csend"].at[n], v["crecv"].at[n], mate)

    def to_owner(a, d):
        n = a * 3 + d - 1
        return remote(kept(a, d), parts.at[a, d - 1], v["psend"].at[n], v["precv"].at[n], (replica, peer_of(shard, d)))

    def pair_sums(a):
        for d in order:
            to_mate(a, d).wait_recv()
            mine = kept(a, d)

            def body(rows, carry):
                mine[rows, :] = (mine[rows, :].astype(f32) + held[a, d, rows, :].astype(f32)).astype(bf16)
                return carry

            row_loop(128, 32, body, 0)
            to_owner(a, d).start()

    def collect(a):
        to_mate(a, 0).wait_recv()
        for d in order:
            to_owner(a, d).wait_recv()

    def full_sum(a, rows):
        total = kept(a, 0)[rows, :].astype(f32) + held[a, 0, rows, :].astype(f32)
        for d in (1, 2, 3):
            total = total + parts[a, d - 1, rows, :].astype(f32)
        return total

    wide = ((v["hid"], mat.at[0, :, pl.ds(0, 768)], 768), (v["prj"], mat.at[1, :, pl.ds(0, 1024)], 1024))
    narrow = ((v["ctx"], v["ctx_all"], 384), (v["nrm"], v["nrm_all"], 384))

    def block(out, owner, c):
        return out.at[tokens(owner, c)]

    def columns(ref, index, width):
        return ref.at[:, pl.ds(pl.multiple_of(index * width, width), width)]

    def wide_copy(a, d, same, source_core, owner, t):
        ref, out, width = wide[a]
        c = core if same else other
        n = (a * 4 + d) * 2 + (0 if same else 1)
        return remote(
            columns(ref, c, width), block(out, owner, source_core), v["gsend"].at[n], v["grecv"].at[n],
            (replica - core + c, t),
        )

    def narrow_copy(a, d, owner, t):
        ref, out, width = narrow[a]
        n = 16 + a * 4 + d
        return remote(columns(ref, t, width), block(out, owner, core), v["gsend"].at[n], v["grecv"].at[n], (replica, t))

    def onward(a, d, source, owner, c):
        out = narrow[a][1]
        n = a * 4 + d
        return remote(source, block(out, owner, c), v["fsend"].at[n], v["frecv"].at[n], mate)

    def own_narrow(a):
        ref, out, width = narrow[a]
        return pltpu.make_async_copy(columns(ref, shard, width), block(out, shard, core), v["local"].at[a])

    def own_wide(a):
        ref, out, width = wide[a]
        return pltpu.make_async_copy(columns(ref, core, width), block(out, shard, core), v["local"].at[2 + a])

    load_out = pltpu.make_async_copy(v["wo"], wbuf.at[:, pl.ds(0, 1536)], v["local"].at[4])
    load_qkv = pltpu.make_async_copy(v["wq"], wbuf.at[:, pl.ds(0, 2048)], v["local"].at[5])

    def stage_sums():
        pair_sums(0)
        for d in order:
            for a in range(2):
                narrow_copy(a, d, shard, peer_of(shard, d)).start()
        send_blocks((1, 2))

    def send_blocks(offsets):
        for d in offsets:
            for a in range(2):
                exchange(d * 2 + a, peer_of(shard, d)).start()

    def stage_hidden():
        collect(0)
        gain = v["gains"][1:2, :]

        def body(rows, total):
            grad = full_sum(0, rows)
            hidden = v["hidden"][rows, :]
            inv = lax.rsqrt(jnp.mean(hidden * hidden, axis=-1, keepdims=True) + NORM_EPS)
            scaled = gain * grad
            out = v["cot"][rows, :].astype(f32) + inv * (
                scaled - hidden * inv * inv * jnp.mean(scaled * hidden, axis=-1, keepdims=True)
            )
            v["hgrad"][rows, :] = out
            v["hid"][rows, :] = out.astype(bf16)
            return total + jnp.sum(grad * hidden * inv, axis=0, keepdims=True)

        v["row_two"][...] = row_loop(128, 16, body, jnp.zeros((1, 1536), f32)) * grad_scale
        for d in (0,) + order:
            if d:
                wide_copy(0, d, True, core, shard, peer_of(shard, d)).start()
            wide_copy(0, d, False, core, shard, peer_of(shard, d)).start()
        own_wide(0).start()

    def stage_context(part):
        if part == 0:
            load_out.wait()
        for e in (2 * part, 2 * part + 1):
            cols = pl.ds(e * 384, 384)
            v["cgrad"][:, cols] = dot_nt(v["hid"][...], wbuf[cols, 0:1536]).astype(bf16)
        if part == 1:
            load_qkv.start()

    def unrotated(x):
        return x * v["cos"][...] - pltpu.roll(x, HD // 2, 1) * v["sin"][...]

    def stage_heads(g, part):
        keys = v["key"][:, g * HD : (g + 1) * HD]
        values = v["val"][:, g * HD : (g + 1) * HD]
        causal = lax.broadcasted_iota(jnp.int32, (128, 128), 0) >= lax.broadcasted_iota(jnp.int32, (128, 128), 1)
        key_grad = jnp.zeros((128, HD), f32) if part == 0 else v["kv_sum"][0]
        value_grad = jnp.zeros((128, HD), f32) if part == 0 else v["kv_sum"][1]
        first_head = g * (HEADS // KV) + part * 2
        for h in range(first_head, first_head + 2):
            at = slice(h * HD, (h + 1) * HD)
            query = v["qry"][:, at]
            grad = v["cgrad"][:, at]
            scores = jnp.where(causal, dot_nt(query, keys) * SCORE_SCALE, -1e30)
            probs = jnp.exp(scores - v["lse"][:, h : h + 1]).astype(bf16)
            wide_probs = probs.astype(f32)
            prob_grad = dot_nt(grad, values)
            delta = jnp.sum(wide_probs * prob_grad, axis=-1, keepdims=True)
            score_grad = (wide_probs * (prob_grad - delta) * SCORE_SCALE).astype(bf16)
            v["prj"][:, at] = unrotated(jnp.dot(score_grad, keys, preferred_element_type=f32)).astype(bf16)
            key_grad = key_grad + dot_tn(score_grad, query)
            value_grad = value_grad + dot_tn(probs, grad)
        if part < 2:
            v["kv_sum"][0] = key_grad
            v["kv_sum"][1] = value_grad
            return
        first = HEADS * HD + g * HD
        v["prj"][:, first : first + HD] = unrotated(key_grad).astype(bf16)
        first = first + KV * HD
        v["prj"][:, first : first + HD] = value_grad.astype(bf16)

    def stage_send_projected():
        for d in (0,) + order:
            if d:
                wide_copy(1, d, True, core, shard, peer_of(shard, d)).start()
            wide_copy(1, d, False, core, shard, peer_of(shard, d)).start()
        own_wide(1).start()

    def stage_normed(part):
        if part == 0:
            load_qkv.wait()
        for e in (2 * part, 2 * part + 1):
            cols = pl.ds(e * 384, 384)
            v["input_grad"][:, cols] = dot_nt(v["prj"][...], wbuf[cols, 0:2048])

    vec, vin, vall = v["vec"], v["vin"], v["vall"]
    replicas = 2 * levels

    def vec_hop(d):
        return remote(vec.at[peer_of(shard, d)], vin.at[d - 1], v["vsend"].at[d - 1], v["vrecv"].at[d - 1],
                      (replica, peer_of(shard, d)))

    def vec_spread(j, slot):
        target = lax.rem(replica + j, replicas)
        return remote(v["vsum"], vall.at[slot], v["vsend"].at[2 + j], v["vrecv"].at[2 + j], (target, shard))

    def stage_input():
        gain = v["gains"][0:1, :]

        def body(rows, totals):
            total, bias = totals
            x = v["x"][rows, :].astype(f32)
            grad = v["input_grad"][rows, :]
            inv = lax.rsqrt(jnp.mean(x * x, axis=-1, keepdims=True) + NORM_EPS)
            scaled = gain * grad
            v["input_grad"][rows, :] = v["hgrad"][rows, :] + inv * (
                scaled - x * inv * inv * jnp.mean(scaled * x, axis=-1, keepdims=True)
            )
            return (
                total + jnp.sum(grad * x * inv, axis=0, keepdims=True),
                bias + jnp.sum(v["prj"][rows, :].astype(f32), axis=0, keepdims=True),
            )

        row_one, row_bias = row_loop(128, 16, body, (jnp.zeros((1, 1536), f32), jnp.zeros((1, 2048), f32)))
        row_one = row_one * grad_scale
        row_bias = row_bias * grad_scale
        row_two = v["row_two"][...]
        for s in range(4):
            vec[s, :, 0:384] = jnp.broadcast_to(row_one[:, s * 384 : (s + 1) * 384], (8, 384))
            vec[s, :, 384:896] = jnp.broadcast_to(row_bias[:, s * 512 : (s + 1) * 512], (8, 512))
            vec[s, :, 896:1280] = jnp.broadcast_to(row_two[:, s * 384 : (s + 1) * 384], (8, 384))
        for d in order:
            vec_hop(d).start()

    def stage_vec():
        total = vec[shard]
        for d in (1, 2, 3):
            vec_hop(d).wait_recv()
            total = total + vin[d - 1]
        v["vsum"][...] = total
        for j in range(1, replicas):
            vec_spread(j, replica).start()

    def stage_vec_out():
        vall[replica] = v["vsum"][...]
        for j in range(1, replicas):
            vec_spread(j, lax.rem(replica + replicas - j, replicas)).wait_recv()
        total = vall[0]
        for j in range(1, replicas):
            total = total + vall[j]
        v["vec_out"][...] = total

    def stage_output():
        collect(1)

        def body(rows, carry):
            v["block_out"][rows, :] = (v["hidden"][rows, :] + full_sum(1, rows)).astype(bf16)
            return carry

        row_loop(128, 32, body, 0)

    def stage_relay():
        for d in order:
            p = peer_of(shard, d)
            for a in range(2):
                narrow_copy(a, d, p, p).wait_recv()
                onward(a, d, block(narrow[a][1], p, core), p, core).start()

    def stage_gathered():
        for a in range(2):
            own_narrow(a).wait()
            own_wide(a).wait()
            for d in (0, 1, 2, 3):
                p = peer_of(shard, d)
                if d:
                    wide_copy(a, d, True, core, p, p).wait_recv()
                wide_copy(a, d, False, other, p, p).wait_recv()
                onward(a, d, block(narrow[a][1], p, other), p, other).wait_recv()

    def stage_attention_parts(j):
        at = pl.ds(j * 128, 128)
        own_a[at, 0:1024] = (dot_tn(v["nrm_all"][:, at], mat[1, :, 0:1024]) * grad_scale).astype(bf16)
        own_a[at, 1024:1792] = (dot_tn(v["ctx_all"][:, at], mat[0, :, 0:768]) * grad_scale).astype(bf16)

    def down_at(c, j):
        first = odd_chip * (1088 * c - 64 * (1 - c)) + (1 - odd_chip) * 1152 * c
        return v["fd"].at[pl.ds(pl.multiple_of(first + j * 64, 64), 64)]

    def gate_at(c, j):
        group = j // 6
        rows = pl.ds(pl.multiple_of(lax.rem(j, 6) * 64, 64), 64)
        return v["fg"].at[lax.rem(group, 2), c, chip_at(group // 2), rows]

    def attention_at(c, j):
        return v["fa"].at[c, pl.ds(pl.multiple_of(j * 32, 32), 32)]

    segments = (
        (own_d, v["near_d"], v["far_d"], 64, 0, DOWN_STEPS, down_at),
        (own_g, v["near_g"], v["far_g"], 64, DOWN_STEPS, DOWN_STEPS + GATE_STEPS, gate_at),
        (own_a, v["near_a"], v["far_a"], 32, DOWN_STEPS + GATE_STEPS, CHUNKS, attention_at),
    )
    end = (level == 0) | (level == levels - 1)
    middle = levels // 2

    def on(k, stage, c=None):
        c = core if c is None else c
        for n, segment in enumerate(segments):
            j = k - segment[4]
            inside = (k >= segment[4]) & (k < segment[5])
            if n == 0:
                inside &= (j > 0) | (1 - odd_chip + c > 0)
                inside &= (j < DOWN_STEPS - 1) | (odd_chip + 1 - c > 0)
            pl.when(inside)(functools.partial(stage, n, segment, j, k))

    def rows_of(segment, j):
        size = segment[3]
        return pl.ds(pl.multiple_of(j * size, size), size)

    def message(segment, j, k, upward, near):
        own, near_ref, far_ref = segment[:3]
        target = near_ref.at[rows_of(segment, j)] if near else far_ref.at[rows_of(segment, j // 2)]
        sem = v["near_sem"] if near else v["far_sem"]
        return remote(own.at[rows_of(segment, j)], target, v["part_sem"].at[k], sem.at[k], above if upward else below)

    def result(segment, j, k, upward, from_own):
        place_ = segment[6](core, j)
        src = segment[0].at[rows_of(segment, j)] if from_own else place_
        sem = v["up_sem"] if upward else v["down_sem"]
        return remote(src, place_, sem.at[k], v["done_sem"].at[k], above if upward else below)

    def keep_result(segment, j, k):
        return pltpu.make_async_copy(segment[0].at[rows_of(segment, j)], segment[6](core, j), v["out_sem"].at[k])

    def to_other_core(segment, j, k, from_own, c):
        place_ = segment[6](c, j)
        src = segment[0].at[rows_of(segment, j)] if from_own else place_
        return remote(src, place_, v["mate_send"].at[k], v["mate_recv"].at[k], mate)

    def add(segment, j, with_far):
        own, near_ref, far_ref, size = segment[:4]

        def body(i, carry):
            rows = pl.ds(pl.multiple_of(j * size + i * 16, 16), 16)
            value = own[rows, :].astype(f32) + near_ref[rows, :].astype(f32)
            if with_far:
                value = value + far_ref[pl.ds(pl.multiple_of((j // 2) * size + i * 16, 16), 16), :].astype(f32)
            own[rows, :] = value.astype(own.dtype)
            return carry

        lax.fori_loop(0, size // 16, body, 0)

    def arrived(n, j):
        if n != 1:
            return
        group = j // 6

        @pl.when((lax.rem(j, 6) == 0) & (group >= 2))
        def _():
            exchange(group, shard).wait_recv()

    def root_of(k):
        return middle - 1 + lax.rem(k, 2)

    def end_gather(n, segment, j, k):
        @pl.when(end)
        def _():
            arrived(n, j)

        @pl.when(level == 0)
        def _():
            message(segment, j, k, True, True).start()

        @pl.when(level == levels - 1)
        def _():
            message(segment, j, k, False, True).start()

    def gather_step(n, segment, j, k):
        @pl.when(~end)
        def _():
            arrived(n, j)

            @pl.when(level != root_of(k))
            def _():
                message(segment, j, k, True, True).wait_recv()
                add(segment, j, False)

        for upward in (True, False):
            towards = (level > 0) & (level < root_of(k)) if upward else (level < levels - 1) & (level > root_of(k))
            crosses = level == (middle - 1 if upward else middle)

            @pl.when(towards & crosses)
            def _():
                message(segment, j, k, upward, False).start()

            if levels > 4:

                @pl.when(towards & ~crosses)
                def _():
                    message(segment, j, k, upward, True).start()

    def root_step(n, segment, j, k):
        @pl.when(level == root_of(k))
        def _():
            message(segment, j, k, True, True).wait_recv()
            message(segment, j, k, True, False).wait_recv()
            add(segment, j, True)
            result(segment, j, k, True, True).start()
            result(segment, j, k, False, True).start()
            keep_result(segment, j, k).start()
            to_other_core(segment, j, k, True, core).start()

    def spread_step(n, segment, j, k):
        @pl.when(~end & (level != root_of(k)))
        def _():
            result(segment, j, k, True, False).wait_recv()

            @pl.when(level < root_of(k))
            def _():
                result(segment, j, k, False, False).start()

            @pl.when(level > root_of(k))
            def _():
                result(segment, j, k, True, False).start()

            to_other_core(segment, j, k, False, core).start()

    def end_spread(n, segment, j, k):
        @pl.when(end)
        def _():
            result(segment, j, k, True, False).wait_recv()
            to_other_core(segment, j, k, False, core).start()

    def close(n, segment, j, k):
        root = root_of(k)

        @pl.when(level == root)
        def _():
            result(segment, j, k, True, True).wait_send()
            result(segment, j, k, False, True).wait_send()
            keep_result(segment, j, k).wait()

        @pl.when(level != root)
        def _():
            message(segment, j, k, True, True).wait_send()

        @pl.when(~end & (level < root))
        def _():
            result(segment, j, k, False, False).wait_send()

        @pl.when(~end & (level > root))
        def _():
            result(segment, j, k, True, False).wait_send()

        to_other_core(segment, j, k, True, core).wait_send()

    def close_mate(n, segment, j, k):
        to_other_core(segment, j, k, True, other).wait_recv()

    def start_mate(a):
        for d in order + (0,):
            to_mate(a, d).start()

    load_down.start()
    load_normed.start()
    for copy in load_deltas:
        copy.start()
    load_gate.start()
    load_act.start()
    for a in range(2):
        own_narrow(a).start()
        onward(a, 0, columns(narrow[a][0], shard, 384), shard, core).start()
    load_down.wait()
    lags = ((end_gather, 0), (gather_step, 8), (root_step, 14), (spread_step, 20), (end_spread, 28))
    steps = CHUNKS + lags[-1][1]

    def begin_products():
        load_normed.wait()
        for copy in load_deltas:
            copy.wait()

    def begin_out():
        start_mate(0)
        load_wd.start()
        load_act.wait()

    def end_out():
        start_mate(1)
        load_out.start()

    def stage_projected():
        stage_send_projected()
        send_blocks((3,))

    beside = [
        (9, 1, begin_products),
        (9, 4, lambda i: (stage_gradient(2 * i), stage_gradient(2 * i + 1))),
        (13, 1, start_back),
        (13, 4, lambda i: (stage_back(3 * i), stage_back(3 * i + 1), stage_back(3 * i + 2))),
        (17, 1, begin_out),
        (19, 1, stage_sums),
        (20, 1, load_wd.wait),
        (20, 4, lambda i: (stage_out(3 * i), stage_out(3 * i + 1), stage_out(3 * i + 2))),
        (24, 1, end_out),
        (25, 1, stage_hidden),
        (26, 1, functools.partial(stage_context, 0)),
        (27, 1, functools.partial(stage_context, 1)),
    ]
    for n in range(6):
        beside.append((28 + n, 1, functools.partial(stage_heads, n // 3, n % 3)))
    beside += [
        (33, 1, stage_projected),
        (34, 1, functools.partial(stage_normed, 0)),
        (36, 1, functools.partial(stage_normed, 1)),
        (38, 1, stage_input),
        (40, 1, stage_relay),
        (56, 1, stage_gathered),
        (56, 1, functools.partial(stage_attention_parts, 0)),
        (58, 1, functools.partial(stage_attention_parts, 1)),
        (60, 1, functools.partial(stage_attention_parts, 2)),
        (62, 1, functools.partial(pair_sums, 1)),
        (64, 1, stage_vec),
        (steps - 4, 1, stage_vec_out),
        (steps - 2, 1, stage_output),
    ]

    def step(t, carry):
        for stage, lag in lags:
            on(t - lag, stage)
        for first, count, stage in beside:
            if count == 1:
                pl.when(t == first)(stage)
            else:
                @pl.when((t >= first) & (t < first + count))
                def _():
                    stage(t - first)

        return carry

    lax.fori_loop(0, steps, step, 0)

    def finish_step(k, carry):
        on(k, close)
        on(k, close_mate, other)
        return carry

    lax.fori_loop(0, CHUNKS, finish_step, 0)
    for d in (1, 2, 3):
        for a in range(2):
            exchange(d * 2 + a, peer_of(shard, d)).wait_send()
    for a in range(2):
        for d in (0, 1, 2, 3):
            p = peer_of(shard, d)
            to_mate(a, d).wait_send()
            wide_copy(a, d, False, core, shard, p).wait_send()
            onward(a, d, block(narrow[a][1], p, core), p, core).wait_send()
            if d:
                to_owner(a, d).wait_send()
                wide_copy(a, d, True, core, shard, p).wait_send()
                narrow_copy(a, d, shard, p).wait_send()
    for d in order:
        vec_hop(d).wait_send()
    for j in range(1, replicas):
        vec_spread(j, replica).wait_send()


def backward(levels, grad_scale, **given):
    bf16 = jnp.bfloat16
    f32 = jnp.float32
    dma = pltpu.SemaphoreType.DMA
    in_hbm = ("pd", "act", "gd", "ud", "n_t", "w_g", "w_u", "w_d", "wo", "wq")
    outs = {
        "fa": ((2, 384, 1792), bf16, any_spec()),
        "fd": ((2240, 1536), bf16, any_spec()),
        "fg": ((2, 2, 4, 384, WINDOW), bf16, any_spec()),
        "blocks": ((6, 384, WINDOW), bf16, any_spec()),
        "block_out": ((128, 1536), bf16, vmem_spec()),
        "input_grad": ((128, 1536), f32, vmem_spec()),
        "vec_out": ((8, 1280), f32, vmem_spec()),
    }
    scratch = {
        "own_a": pltpu.VMEM((384, 1792), bf16),
        "own_d": pltpu.VMEM((WINDOW, 1536), bf16),
        "own_g": pltpu.VMEM((3072, WINDOW), bf16),
        "near_a": pltpu.VMEM((384, 1792), bf16),
        "near_d": pltpu.VMEM((WINDOW, 1536), bf16),
        "near_g": pltpu.VMEM((3072, WINDOW), bf16),
        "far_a": pltpu.VMEM((192, 1792), bf16),
        "far_d": pltpu.VMEM((WINDOW // 2, 1536), bf16),
        "far_g": pltpu.VMEM((1536, WINDOW), bf16),
        "mat": pltpu.VMEM((2, 1024, WINDOW), bf16),
        "act_buf": pltpu.VMEM((1024, WINDOW), bf16),
        "wbuf": pltpu.VMEM((1536, 2 * WINDOW), bf16),
        "back": pltpu.VMEM((1024, 1536), bf16),
        "out": pltpu.VMEM((1024, 1536), bf16),
        "held": pltpu.VMEM((2, 4, 128, 1536), bf16),
        "parts": pltpu.VMEM((2, 3, 128, 1536), bf16),
        "hgrad": pltpu.VMEM((128, 1536), f32),
        "hid": pltpu.VMEM((128, 1536), bf16),
        "cgrad": pltpu.VMEM((128, 1536), bf16),
        "prj": pltpu.VMEM((128, 2048), bf16),
        "ctx_all": pltpu.VMEM((1024, 384), bf16),
        "nrm_all": pltpu.VMEM((1024, 384), bf16),
        "row_two": pltpu.VMEM((1, 1536), f32),
        "kv_sum": pltpu.VMEM((2, 128, HD), f32),
        "vec": pltpu.VMEM((4, 8, 1280), f32),
        "vin": pltpu.VMEM((3, 8, 1280), f32),
        "vsum": pltpu.VMEM((8, 1280), f32),
        "vall": pltpu.VMEM((2 * levels, 8, 1280), f32),
    }
    counts = {
        "xsend": 8, "xrecv": 8, "stage_sem": 2, "csend": 8, "crecv": 8, "psend": 6, "precv": 6, "gsend": 24, "grecv": 24,
        "fsend": 8, "frecv": 8, "local": 6, "in_sem": 8, "vsend": 2 + 2 * levels, "vrecv": 2 + 2 * levels,
    }
    for name in (
        "part_sem", "near_sem", "far_sem", "up_sem", "down_sem", "done_sem", "mate_send", "mate_recv", "out_sem"
    ):
        counts[name] = CHUNKS
    scratch |= {name: dma((n,)) for name, n in counts.items()}
    return pl.pallas_call(
        functools.partial(backward_kernel, levels, grad_scale, (*given, *outs, *scratch)),
        out_shape=[jax.ShapeDtypeStruct(s, dt) for s, dt, _ in outs.values()],
        in_specs=[any_spec() if name in in_hbm else vmem_spec() for name in given],
        out_specs=[spec for _, _, spec in outs.values()],
        scratch_shapes=list(scratch.values()),
        compiler_params=pltpu.CompilerParams(has_side_effects=True, vmem_limit_bytes=67043328),
    )(*given.values())


def widen_kernel(gate, up, down, attn, block, grad, out_gate, out_up, out_down, out_qkv, out_out, out_block, out_grad):
    f32 = jnp.float32
    out_block[...] = block[...]
    out_grad[...] = grad[...]
    for x, out in ((gate, out_gate), (up, out_up)):
        for s in range(4):
            for c in range(2):
                first = (s * 35) // 2 + c * 9
                rest = 1 if s % 2 == 1 and c == 0 else 0
                out[:, (first + rest) * 128 : (first + 9) * 128] = x[c, s][:, rest * 128 :].astype(f32)
        for s in (1, 3):
            first = (s * 35) // 2
            out[:, first * 128 : (first + 1) * 128] = x[1, s - 1][:, 1024:].astype(f32) + x[0, s][:, :128].astype(f32)
    out_down[...] = down[...].astype(f32)
    for c in range(2):
        out_qkv[:, c * 1024 : (c + 1) * 1024] = attn[c][:, :1024].astype(f32)
        out_out[:, c * 768 : (c + 1) * 768] = attn[c][:, 1024:].astype(f32)


def widen(*sums):
    rows = 32
    f32 = jnp.float32
    def blocks(a):
        return pl.BlockSpec((None, 2, 4, rows, WINDOW), lambda i: (a, 0, 0, i, 0))

    down = pl.BlockSpec((224, 1536), lambda i: (jnp.minimum(i, 9), 0))

    own_rows = pl.BlockSpec((16, 1536), lambda i: (jnp.minimum(i, 7), 0))

    def whole(width):
        return pl.BlockSpec((rows, width), lambda i: (i, 0))

    return pl.pallas_call(
        widen_kernel,
        grid=(384 // rows,),
        out_shape=[
            jax.ShapeDtypeStruct((384, 8960), f32),
            jax.ShapeDtypeStruct((384, 8960), f32),
            jax.ShapeDtypeStruct((2240, 1536), f32),
            jax.ShapeDtypeStruct((384, 2048), f32),
            jax.ShapeDtypeStruct((384, 1536), f32),
            jax.ShapeDtypeStruct((128, 1536), jnp.bfloat16),
            jax.ShapeDtypeStruct((128, 1536), f32),
        ],
        in_specs=[blocks(0), blocks(1), down, pl.BlockSpec((2, rows, 1792), lambda i: (0, i, 0)), own_rows, own_rows],
        out_specs=[whole(8960), whole(8960), down, whole(2048), whole(1536), own_rows, own_rows],
    )(*sums)


def fast_device(
    block_input,
    attn_gain,
    qkv_weight,
    qkv_bias,
    out_weight,
    mlp_gain,
    gate_weight,
    up_weight,
    down_weight,
    cotangent,
):
    f32 = jnp.float32
    tok_count = block_input.shape[0]
    levels = lax.axis_size("replica") // 2
    grad_scale = 1.0 / math.sqrt(tok_count * lax.axis_size("replica") * lax.axis_size("shard"))
    cosine, sine_table = rope_tables(tok_count)
    gap = jnp.zeros((128,), jnp.bfloat16)
    rest = jnp.zeros((13 * 512,), jnp.bfloat16)
    small = jnp.concatenate([attn_gain, gap, qkv_bias, mlp_gain, gap, rest]).reshape(16, 512)
    twice = jnp.concatenate([cosine[:, 0], cosine[:, 0]], axis=1)
    turn = jnp.concatenate([-sine_table[:, 0], sine_table[:, 0]], axis=1)
    got = forward(
        grad_scale,
        x=block_input,
        small=small,
        cos=twice,
        sin=turn,
        wq=qkv_weight,
        wo=out_weight,
        wg=gate_weight,
        wu=up_weight,
        wd=down_weight,
        cot=cotangent,
    )
    sum_attn, sum_down, sum_gate, _, block_output, input_grad, vectors = backward(
        levels,
        grad_scale,
        pd=got["pd"],
        act=got["act"],
        gd=got["gd"],
        ud=got["ud"],
        n_t=got["n_t"],
        w_g=got["w_g"],
        w_u=got["w_u"],
        w_d=got["w_d"],
        wo=got["o_full"],
        wq=got["q_full"],
        hidden=got["hidden"],
        x=block_input,
        cot=cotangent,
        gains=got["gains"],
        ctx=got["ctx"],
        nrm=got["nrm"],
        qry=got["qry"],
        key=got["key"],
        val=got["val"],
        lse=got["lse"],
        cos=twice,
        sin=turn,
    )
    gain_one_own, bias_own, gain_two_own = vectors[0, :384], vectors[0, 384:896], vectors[0, 896:]
    gate_grad, up_grad, down_grad, qkv_grad, out_grad, block_output, input_grad = widen(
        sum_gate, sum_gate, sum_down, sum_attn, block_output, input_grad
    )
    return (
        block_output,
        input_grad,
        gain_one_own,
        qkv_grad,
        bias_own,
        out_grad,
        gain_two_own,
        gate_grad,
        up_grad,
        down_grad,
    )


def solution(mesh):
    placed = (
        P(("replica", "shard"), None),
        P("shard"),
        P("shard", None),
        P("shard"),
        P("shard", None),
        P("shard"),
        P("shard", None),
        P("shard", None),
        P("shard", None),
        P(("replica", "shard"), None),
    )
    fits = mesh.shape["shard"] == 4 and mesh.shape["replica"] % 4 == 0
    per_device = fast_device if fits else general_device
    return jax.shard_map(
        per_device,
        mesh=mesh,
        in_specs=placed,
        out_specs=(
            P(("replica", "shard"), None),
            P(("replica", "shard"), None),
            P("shard"),
            P("shard", None),
            P("shard"),
            P("shard", None),
            P("shard"),
            P("shard", None),
            P("shard", None),
            P("shard", None),
        ),
        check_vma=False,
    )
```

```python
import functools
import math

import jax
import jax.numpy as jnp
from jax import lax
from jax.experimental import pallas as pl
from jax.experimental.pallas import tpu as pltpu
from jax.sharding import PartitionSpec as P

HEADS = 12
KV = 2
HD = 128


NORM_EPS = 1e-06
ROPE_BASE = 1000000.0


def rope_tables(tok_count):
    half_dim = HD // 2
    position = jnp.arange(tok_count, dtype=jnp.float32)
    inverse = ROPE_BASE ** (-(jnp.arange(half_dim, dtype=jnp.float32) * 2.0 / HD))
    angles = position[:, None] * inverse[None, :]
    return (jnp.cos(angles)[:, None, :], jnp.sin(angles)[:, None, :])


def rotate(vectors, cosine, sine_table):
    half_dim = HD // 2
    lower_half = vectors[..., :half_dim]
    upper_half = vectors[..., half_dim:]
    return jnp.concatenate(
        [
            lower_half * cosine - upper_half * sine_table,
            upper_half * cosine + lower_half * sine_table,
        ],
        axis=-1,
    )


def unrotate(grads, cosine, sine_table):
    half_dim = HD // 2
    lower_half = grads[..., :half_dim]
    upper_half = grads[..., half_dim:]
    return jnp.concatenate(
        [
            lower_half * cosine + upper_half * sine_table,
            upper_half * cosine - lower_half * sine_table,
        ],
        axis=-1,
    )


def block_scores(query_block, key_rot, first_row):
    row_count = query_block.shape[0]
    scores = jnp.einsum(
        "qkgd,skd->kgqs", query_block, key_rot, preferred_element_type=jnp.float32
    ) * (1.0 / math.sqrt(HD))
    causal = (first_row + jnp.arange(row_count))[:, None] >= jnp.arange(key_rot.shape[0])[None, :]
    return jnp.where(causal, scores, -1e30)


def block_layout(tok_count):
    block_rows = min(tok_count, 512)
    block_count = tok_count // block_rows
    firsts = jnp.arange(block_count, dtype=jnp.int32) * block_rows
    return (block_rows, block_count, firsts)


def attend_forward(queries, key_rot, values):
    tok_count = queries.shape[0]
    block_rows, block_count, firsts = block_layout(tok_count)
    query_blocks = queries.reshape(block_count, block_rows, KV, HEADS // KV, HD)

    def one_block(inputs):
        query_block, first_row = inputs
        scores = block_scores(query_block, key_rot, first_row)
        row_max = jnp.max(scores, axis=-1, keepdims=True)
        logsum = row_max + jnp.log(jnp.sum(jnp.exp(scores - row_max), axis=-1, keepdims=True))
        attn_probs = jnp.exp(scores - logsum).astype(jnp.bfloat16)
        context = jnp.einsum(
            "kgqs,skd->qkgd", attn_probs, values, preferred_element_type=jnp.float32
        ).astype(jnp.bfloat16)
        return (context, logsum)

    context, logsum = lax.map(one_block, (query_blocks, firsts))
    return (context.reshape(tok_count, HEADS * HD), logsum)


def attend_backward(queries, key_rot, values, logsum, context_grad):
    tok_count = queries.shape[0]
    block_rows, block_count, firsts = block_layout(tok_count)
    query_blocks = queries.reshape(block_count, block_rows, KV, HEADS // KV, HD)
    grad_blocks = context_grad.reshape(block_count, block_rows, KV, HEADS // KV, HD)
    score_scale = 1.0 / math.sqrt(HD)

    def one_block(running, inputs):
        key_total, value_total = running
        query_block, grad_block, log_block, first_row = inputs
        scores = block_scores(query_block, key_rot, first_row)
        attn_probs = jnp.exp(scores - log_block).astype(jnp.bfloat16)
        prob_grad = jnp.einsum(
            "qkgd,skd->kgqs", grad_block, values, preferred_element_type=jnp.float32
        )
        wide_probs = attn_probs.astype(jnp.float32)
        row_delta = jnp.sum(wide_probs * prob_grad, axis=-1, keepdims=True)
        score_grad = (wide_probs * (prob_grad - row_delta) * score_scale).astype(jnp.bfloat16)
        query_grad = jnp.einsum(
            "kgqs,skd->qkgd", score_grad, key_rot, preferred_element_type=jnp.float32
        )
        key_total = key_total + jnp.einsum(
            "kgqs,qkgd->skd", score_grad, query_block, preferred_element_type=jnp.float32
        )
        value_total = value_total + jnp.einsum(
            "kgqs,qkgd->skd", attn_probs, grad_block, preferred_element_type=jnp.float32
        )
        return ((key_total, value_total), query_grad)

    zero_keys = jnp.zeros((tok_count, KV, HD), jnp.float32)
    (key_grad, value_grad), query_grad = lax.scan(
        one_block, (zero_keys, zero_keys), (query_blocks, grad_blocks, logsum, firsts)
    )
    return (query_grad.reshape(tok_count, HEADS, HD), key_grad, value_grad)


def general_device(
    block_input,
    attn_gain,
    qkv_weight,
    qkv_bias,
    out_weight,
    mlp_gain,
    gate_weight,
    up_weight,
    down_weight,
    cotangent,
):
    f32 = jnp.float32
    bf16 = jnp.bfloat16
    tok_count = block_input.shape[0]
    grad_scale = 1.0 / math.sqrt(tok_count * lax.axis_size("replica") * lax.axis_size("shard"))
    q_width = HEADS * HD
    k_end = q_width + KV * HD
    cosine, sine_table = rope_tables(tok_count)
    attn_full = (
        lax.all_gather(attn_gain, "shard", axis=0, tiled=True),
        lax.all_gather(qkv_weight, "shard", axis=0, tiled=True),
        lax.all_gather(qkv_bias, "shard", axis=0, tiled=True),
        lax.all_gather(out_weight, "shard", axis=0, tiled=True),
    )
    gain_full, qkv_full, bias_full, out_full = attn_full
    gain_one = gain_full.astype(f32)
    xfloat = block_input.astype(f32)
    inv_one = lax.rsqrt(jnp.mean(xfloat * xfloat, axis=-1, keepdims=True) + NORM_EPS)
    normed_one = (xfloat * inv_one * gain_one).astype(bf16)
    projected = jnp.dot(normed_one, qkv_full, preferred_element_type=f32) + bias_full.astype(f32)
    queries = rotate(
        projected[:, :q_width].reshape(tok_count, HEADS, HD), cosine, sine_table
    ).astype(bf16)
    queries = queries.reshape(tok_count, KV, HEADS // KV, HD)
    key_rot = rotate(
        projected[:, q_width:k_end].reshape(tok_count, KV, HD), cosine, sine_table
    ).astype(bf16)
    values = projected[:, k_end:].reshape(tok_count, KV, HD).astype(bf16)
    context, logsum = attend_forward(queries, key_rot, values)
    hidden_res = xfloat + jnp.dot(context, out_full, preferred_element_type=f32)
    mlp_full = (
        lax.all_gather(mlp_gain, "shard", axis=0, tiled=True),
        lax.all_gather(gate_weight, "shard", axis=0, tiled=True),
        lax.all_gather(up_weight, "shard", axis=0, tiled=True),
        lax.all_gather(down_weight, "shard", axis=0, tiled=True),
    )
    gain_full_two, gate_full, up_full, down_full = mlp_full
    gain_two = gain_full_two.astype(f32)
    inv_two = lax.rsqrt(jnp.mean(hidden_res * hidden_res, axis=-1, keepdims=True) + NORM_EPS)
    normed_two = (hidden_res * inv_two * gain_two).astype(bf16)
    gate_pre = jnp.dot(normed_two, gate_full, preferred_element_type=f32)
    up_pre = jnp.dot(normed_two, up_full, preferred_element_type=f32)
    sigmoid_gate = jax.nn.sigmoid(gate_pre)
    silu_gate = gate_pre * sigmoid_gate
    activation = (silu_gate * up_pre).astype(bf16)
    block_output = (hidden_res + jnp.dot(activation, down_full, preferred_element_type=f32)).astype(
        bf16
    )
    act_grad = jnp.einsum("td,fd->tf", cotangent, down_full, preferred_element_type=f32)
    gate_delta = (
        act_grad * up_pre * sigmoid_gate * (1.0 + gate_pre * (1.0 - sigmoid_gate))
    ).astype(bf16)
    up_delta = (act_grad * silu_gate).astype(bf16)
    normed_two_grad = jnp.einsum(
        "tf,df->td", gate_delta, gate_full, preferred_element_type=f32
    ) + jnp.einsum("tf,df->td", up_delta, up_full, preferred_element_type=f32)
    gain_two_grad = jnp.sum(normed_two_grad * hidden_res * inv_two, axis=0) * grad_scale
    own_rows = (
        lax.all_to_all(activation, "shard", split_axis=1, concat_axis=0, tiled=True),
        lax.all_to_all(normed_two, "shard", split_axis=1, concat_axis=0, tiled=True),
    )
    group_act, group_normed = own_rows
    group_rows = (
        lax.all_gather(cotangent, "shard", axis=0, tiled=True),
        lax.all_gather(gate_delta, "shard", axis=0, tiled=True),
        lax.all_gather(up_delta, "shard", axis=0, tiled=True),
    )
    group_cot, group_gate, group_up = group_rows
    down_part = (
        jnp.einsum("tf,td->fd", group_act, group_cot, preferred_element_type=f32) * grad_scale
    )
    gate_own = (
        jnp.einsum("td,tf->df", group_normed, group_gate, preferred_element_type=f32) * grad_scale
    )
    up_own = (
        jnp.einsum("td,tf->df", group_normed, group_up, preferred_element_type=f32) * grad_scale
    )
    gain_two_own = lax.psum_scatter(gain_two_grad, "shard", scatter_dimension=0, tiled=True)
    mlp_parts = (gain_two_own, gate_own, up_own)
    hidden_grad = cotangent.astype(f32) + inv_two * (
        gain_two * normed_two_grad
        - hidden_res
        * inv_two
        * inv_two
        * jnp.mean(gain_two * normed_two_grad * hidden_res, axis=-1, keepdims=True)
    )
    hidden_low = hidden_grad.astype(bf16)
    context_grad = jnp.einsum("td,ed->te", hidden_low, out_full, preferred_element_type=f32).astype(
        bf16
    )
    query_grad, key_grad, value_grad = attend_backward(
        queries, key_rot, values, logsum, context_grad
    )
    query_grad = unrotate(query_grad, cosine, sine_table).reshape(tok_count, q_width)
    key_grad = unrotate(key_grad, cosine, sine_table).reshape(tok_count, KV * HD)
    projected_grad = jnp.concatenate(
        [query_grad, key_grad, value_grad.reshape(tok_count, KV * HD)], axis=-1
    ).astype(bf16)
    normed_one_grad = jnp.einsum("tc,dc->td", projected_grad, qkv_full, preferred_element_type=f32)
    gain_one_grad = jnp.sum(normed_one_grad * xfloat * inv_one, axis=0) * grad_scale
    bias_grad = jnp.sum(projected_grad.astype(f32), axis=0) * grad_scale
    own_attn = (
        lax.all_to_all(context, "shard", split_axis=1, concat_axis=0, tiled=True),
        lax.all_to_all(normed_one, "shard", split_axis=1, concat_axis=0, tiled=True),
    )
    group_context, group_normed_one = own_attn
    group_rows = (
        lax.all_gather(hidden_low, "shard", axis=0, tiled=True),
        lax.all_gather(projected_grad, "shard", axis=0, tiled=True),
    )
    group_hidden, group_projected = group_rows
    out_own = (
        jnp.einsum("te,td->ed", group_context, group_hidden, preferred_element_type=f32)
        * grad_scale
    )
    qkv_part = (
        jnp.einsum("td,tc->dc", group_normed_one, group_projected, preferred_element_type=f32)
        * grad_scale
    )
    small_parts = (
        lax.psum_scatter(gain_one_grad, "shard", scatter_dimension=0, tiled=True),
        lax.psum_scatter(bias_grad, "shard", scatter_dimension=0, tiled=True),
    )
    attn_parts = (small_parts[0], qkv_part, small_parts[1], out_own)
    input_grad = hidden_grad + inv_one * (
        gain_one * normed_one_grad
        - xfloat
        * inv_one
        * inv_one
        * jnp.mean(gain_one * normed_one_grad * xfloat, axis=-1, keepdims=True)
    )
    summed = lax.psum(
        (
            attn_parts[0],
            attn_parts[1],
            attn_parts[2],
            attn_parts[3],
            mlp_parts[0],
            mlp_parts[1],
            mlp_parts[2],
            down_part,
        ),
        "replica",
    )
    attn_parts = (summed[0], summed[1], summed[2], summed[3])
    mlp_parts = (summed[4], summed[5], summed[6])
    down_part = summed[7]
    return (
        block_output,
        input_grad,
        attn_parts[0],
        attn_parts[1],
        attn_parts[2],
        attn_parts[3],
        mlp_parts[0],
        mlp_parts[1],
        mlp_parts[2],
        down_part,
    )


MESH = pl.DeviceIdType.MESH
VMEM_BYTES = 62 * 2**20
WINDOW = 1152


def place():
    replica = lax.axis_index("replica")
    shard = lax.axis_index("shard")
    core = lax.rem(replica, 2)
    return replica, shard, core


def peer_of(shard, d):
    across = lax.rem(lax.rem(shard, 2) + d % 2, 2)
    up = lax.rem(shard // 2 + d // 2, 2)
    return up * 2 + across


def window_start(shard, core):
    return ((shard * 35) // 2 + core * 9) * 128


def remote(src, dst, send, recv, device):
    return pltpu.make_async_remote_copy(
        src_ref=src,
        dst_ref=dst,
        send_sem=send,
        recv_sem=recv,
        device_id=device,
        device_id_type=MESH,
    )


def any_spec():
    return pl.BlockSpec(memory_space=pl.ANY)


def vmem_spec():
    return pl.BlockSpec(memory_space=pltpu.VMEM)


def params(**more):
    return pltpu.CompilerParams(has_side_effects=True, vmem_limit_bytes=VMEM_BYTES, **more)


DOWN_STEPS, GATE_STEPS, ATTENTION_STEPS = 18, 48, 12
CHUNKS = DOWN_STEPS + GATE_STEPS + ATTENTION_STEPS
SCORE_SCALE = 1.0 / math.sqrt(HD)


def dot_nt(a, b):
    return lax.dot_general(a, b, (((1,), (1,)), ((), ())), preferred_element_type=jnp.float32)


def dot_tn(a, b):
    return lax.dot_general(a, b, (((0,), (0,)), ((), ())), preferred_element_type=jnp.float32)


def row_loop(rows, step, body, init):
    return lax.fori_loop(0, rows // step, lambda j, c: body(pl.ds(pl.multiple_of(j * step, step), step), c), init)


TILES = ((0, 640, 160), (640, 512, 96))


def forward_kernel(grad_scale, names, *refs):
    v = dict(zip(names, refs))
    f32 = jnp.float32
    bf16 = jnp.bfloat16
    replica, shard, core = place()
    other = 1 - core
    mate = (replica + 1 - 2 * core, shard)
    odd = lax.rem(replica // 2, 2)
    pair = (replica + 2 - 4 * odd, shard)
    order = (3, 1, 2)
    first_unit = window_start(shard, core)
    q_buf, o_buf, g_buf, u_buf, d_buf = v["q_buf"], v["o_buf"], v["g_buf"], v["u_buf"], v["d_buf"]
    n_all, cot_all, small_all = v["n_all"], v["cot_all"], v["small_all"]

    def span(start, size):
        return pl.ds(pl.multiple_of(start, 16), size)

    def units(target, offset, width):
        return pl.ds(pl.multiple_of(window_start(target, core) + offset, 128), width)

    def tokens(owner, c):
        return pl.ds(pl.multiple_of((c * 4 + owner) * 128, 128), 128)

    weights = [
        (lambda t: v["wq"], q_buf, 192, 80, True),
        (lambda t: v["wo"], o_buf, 192, 80, True),
    ]
    for offset, width, shared in TILES:
        for name, buf in (("wg", g_buf), ("wu", u_buf)):
            weights.append((
                lambda t, name=name, offset=offset, width=width: v[name].at[:, units(t, offset, width)],
                buf.at[:, pl.ds(offset, width)], 384, shared, False,
            ))

    def base(i, c):
        return c * 192 if weights[i][4] else 0

    def hop(i, d, t, o):
        source, out, size, shared, _ = weights[i]
        first = base(i, core) + odd * shared
        n = i * 3 + d - 1
        return remote(
            source(t).at[span(first, size - shared)], out.at[span(o * 384 + first, size - shared)],
            v["send"].at[n], v["recv"].at[n], (replica, t),
        )

    def relay(i, way, t, o):
        _, out, size, shared, _ = weights[i]
        first = o * 384 + base(i, core) + odd * shared
        ref = out.at[span(first, 64)] if way == 1 else out.at[span(first + 64, size - shared - 64)]
        n = i * 2 + way - 1
        return remote(ref, ref, v["rsend"].at[n], v["rrecv"].at[n], (replica, t))

    def across(i, d, o, whose):
        _, out, size, shared, _ = weights[i]
        ref = out.at[span(o * 384 + base(i, core) + whose * (size - shared), shared)]
        n = i * 3 + d - 1
        return remote(ref, ref, v["zsend"].at[n], v["zrecv"].at[n], pair)

    def onward(i, d, o, c, shared_part):
        _, out, size, shared, _ = weights[i]
        first = o * 384 + base(i, c) + ((1 - odd) * (size - shared) if shared_part else odd * shared)
        ref = out.at[span(first, shared if shared_part else size - shared)]
        n = i * 3 + d - 1 + (6 if shared_part else 0)
        return remote(ref, ref, v["fsend"].at[n], v["frecv"].at[n], mate)

    row_sets = (cot_all, n_all)

    def row_hop(a, d, t, o):
        n = 18 + a * 3 + d - 1
        return remote(row_sets[a].at[tokens(shard, core)], row_sets[a].at[tokens(o, core)], v["send"].at[n], v["recv"].at[n],
                      (replica, t))

    def row_relay(a, way, t, o):
        ref = row_sets[a].at[span((core * 4 + o) * 128 + 64 * (way - 1), 64)]
        n = 4 + a * 2 + way - 1
        return remote(ref, ref, v["rsend"].at[n], v["rrecv"].at[n], (replica, t))

    def row_onward(a, d, o, c):
        n = 12 + a * 4 + d
        ref = row_sets[a].at[tokens(o, c)]
        return remote(ref, ref, v["fsend"].at[n], v["frecv"].at[n], mate)

    def small_hop(d, t, o):
        n = 24 + d - 1
        return remote(v["small"], small_all.at[o], v["send"].at[n], v["recv"].at[n], (replica, t))

    def send_rows(a):
        for d in (1, 2):
            row_hop(a, d, peer_of(shard, d), shard).start()
        row_onward(a, 0, shard, core).start()

    def take_rows(a):
        for d in (1, 2):
            p = peer_of(shard, d)
            row_hop(a, d, p, p).wait_recv()
            row_relay(a, d, peer_of(shard, 3 - d), p).start()
            row_onward(a, d, p, core).start()

    def take_far_rows(a):
        p = peer_of(shard, 3)
        for way in (1, 2):
            row_relay(a, way, p, p).wait_recv()
        row_onward(a, 3, p, core).start()

    def have_rows(a):
        for d in (0,) + order:
            row_onward(a, d, peer_of(shard, d), other).wait_recv()

    def send_weight(i):
        for d in (1, 2) if weights[i][4] else order:
            hop(i, d, peer_of(shard, d), shard).start()

    def take(i, d):
        p = peer_of(shard, d)
        relayed = weights[i][4]
        if relayed and d == 3:
            for way in (1, 2):
                relay(i, way, p, p).wait_recv()
        else:
            hop(i, d, p, p).wait_recv()
            if relayed:
                relay(i, d, peer_of(shard, 3 - d), p).start()
        across(i, d, p, odd).start()
        if relayed:
            onward(i, d, p, core, False).start()

    def take_shared(i):
        for d in order:
            p = peer_of(shard, d)
            across(i, d, p, 1 - odd).wait_recv()
            if weights[i][4]:
                onward(i, d, p, core, True).start()

    def have_other_half(i):
        for d in order:
            for part in (False, True):
                onward(i, d, peer_of(shard, d), other, part).wait_recv()

    rows = span(shard * 384, 384)
    loads = [
        pltpu.make_async_copy(v["cot"], cot_all.at[tokens(shard, core)], v["local"].at[0]),
        pltpu.make_async_copy(v["wq"], q_buf.at[rows], v["local"].at[1]),
        pltpu.make_async_copy(v["wo"], o_buf.at[rows], v["local"].at[2]),
        pltpu.make_async_copy(v["wg"].at[:, units(shard, 0, WINDOW)], g_buf.at[rows], v["local"].at[3]),
        pltpu.make_async_copy(v["wu"].at[:, units(shard, 0, WINDOW)], u_buf.at[rows], v["local"].at[4]),
    ]
    odd_chip = lax.rem(shard, 2)
    inside = odd_chip == core
    loads.append(pltpu.make_async_copy(
        v["wd"].at[span((1152 - 64 * odd_chip) * core, 1088)],
        d_buf.at[span(odd_chip * (1 - core) * 64, 1088)], v["local"].at[5],
    ))

    for d in order:
        small_hop(d, peer_of(shard, d), shard).start()
    send_weight(0)
    send_weight(1)
    for copy in loads:
        copy.start()
    rest = pltpu.make_async_copy(
        v["wd"].at[span((2176 - 1088) * core + 1088, 64)], d_buf.at[pl.ds(1088, 64)], v["local"].at[6]
    )

    @pl.when(inside)
    def _():
        rest.start()

    @pl.when(~inside)
    def _():
        d_buf[span(1088 - 1088 * odd_chip, 64), :] = jnp.zeros((64, 1536), bf16)

    small_all[shard] = v["small"][...]
    for d in order:
        p = peer_of(shard, d)
        small_hop(d, p, p).wait_recv()

    def gathered(row, width):
        return jnp.concatenate([small_all[s, row : row + 1, 0:width].astype(f32) for s in range(4)], axis=1)

    gain_one = gathered(0, 384)

    def norm_body(at, carry):
        x = v["x"][at, :].astype(f32)
        inv = lax.rsqrt(jnp.mean(x * x, axis=-1, keepdims=True) + NORM_EPS)
        v["nrm"][at, :] = (x * inv * gain_one).astype(bf16)
        return carry

    row_loop(128, 16, norm_body, 0)
    for copy in loads:
        copy.wait()

    @pl.when(inside)
    def _():
        rest.wait()

    for i in (0, 1):
        for d in (1, 2):
            take(i, d)
    send_rows(0)
    send_weight(2)
    send_weight(3)
    take(0, 3)
    take(1, 3)
    take_shared(0)
    have_other_half(0)
    keep_q = pltpu.make_async_copy(q_buf, v["q_full"], v["local"].at[7])
    keep_q.start()
    bias = gathered(1, 512)

    def rotated(x):
        return x * v["cos"][...] + pltpu.roll(x, HD // 2, 1) * v["sin"][...]

    def project(head, out, at, turn):
        cols = slice(head * HD, (head + 1) * HD)
        x = v["prj"][:, cols] + bias[:, cols]
        out[:, at * HD : (at + 1) * HD] = (rotated(x) if turn else x).astype(bf16)

    for n in range(4):
        v["prj"][:, n * 512 : (n + 1) * 512] = jnp.dot(
            v["nrm"][...], q_buf[:, n * 512 : (n + 1) * 512], preferred_element_type=f32
        )
    take_shared(1)
    for h in range(HEADS):
        project(h, v["qry"], h, True)
    for g in range(KV):
        project(HEADS + g, v["key"], g, True)
        project(HEADS + KV + g, v["val"], g, False)
    causal = lax.broadcasted_iota(jnp.int32, (128, 128), 0) >= lax.broadcasted_iota(jnp.int32, (128, 128), 1)
    v["lse"][...] = jnp.zeros((128, HD), f32)
    for h in range(HEADS):
        g = h // (HEADS // KV)
        at = slice(h * HD, (h + 1) * HD)
        scores = dot_nt(v["qry"][:, at], v["key"][:, g * HD : (g + 1) * HD]) * SCORE_SCALE
        scores = jnp.where(causal, scores, -1e30)
        row_max = jnp.max(scores, axis=-1, keepdims=True)
        logsum = row_max + jnp.log(jnp.sum(jnp.exp(scores - row_max), axis=-1, keepdims=True))
        v["lse"][:, h : h + 1] = logsum
        probs = jnp.exp(scores - logsum).astype(bf16)
        v["ctx"][:, at] = jnp.dot(probs, v["val"][:, g * HD : (g + 1) * HD], preferred_element_type=f32).astype(bf16)
    have_other_half(1)
    keep_o = pltpu.make_async_copy(o_buf, v["o_full"], v["local"].at[8])
    keep_o.start()
    for n in range(3):
        cols = slice(n * 512, (n + 1) * 512)
        v["hidden"][:, cols] = v["x"][:, cols].astype(f32) + jnp.dot(
            v["ctx"][...], o_buf[:, cols], preferred_element_type=f32
        )
    gain_two = gathered(2, 384)
    v["gains"][0:1, :] = gain_one
    v["gains"][1:2, :] = gain_two

    def norm_two(j, carry):
        at = pl.ds(pl.multiple_of(j * 16, 16), 16)
        hidden = v["hidden"][at, :]
        inv = lax.rsqrt(jnp.mean(hidden * hidden, axis=-1, keepdims=True) + NORM_EPS)
        n_all[span((core * 4 + shard) * 128 + j * 16, 16), :] = (hidden * inv * gain_two).astype(bf16)
        return carry

    lax.fori_loop(0, 8, norm_two, 0)
    send_rows(1)
    take_rows(0)
    for i in (2, 3):
        for d in order:
            take(i, d)
    take_rows(1)
    send_weight(4)
    send_weight(5)
    take_far_rows(0)
    take_far_rows(1)
    take_shared(2)
    take_shared(3)
    have_rows(0)
    have_rows(1)

    act, gate_delta, up_delta = v["act_buf"], v["gd_buf"], v["ud_buf"]
    gs, us, gr = v["gs"], v["us"], v["gr"]
    pending = [(i, d) for i in (4, 5) for d in order]

    def service():
        if pending:
            take(*pending.pop(0))

    def products(offset, width, m):
        at = pl.ds(m * 512, 512)
        for n in range(0, width, 256):
            size = min(256, width - n)
            cols = pl.ds(offset + n, size)
            gs[:, n : n + size] = jnp.dot(n_all[at, :], g_buf[:, cols], preferred_element_type=f32)
            us[:, n : n + size] = jnp.dot(n_all[at, :], u_buf[:, cols], preferred_element_type=f32)
            gr[:, n : n + size] = dot_nt(cot_all[at, :], d_buf[cols, :])
        column = first_unit + offset + lax.broadcasted_iota(jnp.int32, (1, width), 1)
        owned = (column >= shard * 2240) & (column < (shard + 1) * 2240)

        def body(j, carry):
            part = pl.ds(pl.multiple_of(j * 16, 16), 16)
            to = pl.ds(pl.multiple_of(m * 512 + j * 16, 16), 16)
            cols = pl.ds(offset, width)
            gate, up, grad = gs[part, 0:width], us[part, 0:width], gr[part, 0:width]
            sig = jax.nn.sigmoid(gate)
            silu = gate * sig
            act[to, cols] = jnp.where(owned, silu * up, 0.0).astype(bf16)
            gate_delta[to, cols] = jnp.where(owned, grad * up * sig * (1.0 + gate * (1.0 - sig)), 0.0).astype(bf16)
            up_delta[to, cols] = jnp.where(owned, grad * silu, 0.0).astype(bf16)
            return carry

        lax.fori_loop(0, 32, body, 0)

    def transpose(src, cols, dst):
        def body(j, carry):
            at = pl.ds(pl.multiple_of(j * 128, 128), 128)
            dst[:, at] = src[at, cols].T
            return carry

        lax.fori_loop(0, 8, body, 0)

    outs = {}

    def write(name, buf, at, cols=None):
        n = 9 + len(outs)
        src = buf.at[at] if cols is None else buf.at[at, cols]
        dst = v[name].at[at] if cols is None else v[name].at[at, cols]
        copy = pltpu.make_async_copy(src, dst, v["local"].at[n])
        copy.start()
        outs[n] = copy

    for tile, (offset, width, _) in enumerate(TILES):
        cols = pl.ds(offset, width)
        for m in range(2):
            products(offset, width, m)
            service()
        transpose(act, cols, v["act_t"].at[pl.ds(0, width)])
        if tile == 0:
            transpose(n_all, pl.ds(0, 1536), v["n_t_buf"])
        service()
        for n in range(3):
            out = pl.ds(n * 512, 512)
            v["d_grad"][cols, out] = (
                jnp.dot(v["act_t"][0:width, :], cot_all[:, out], preferred_element_type=f32) * grad_scale
            ).astype(bf16)
        write("pd", v["d_grad"], cols)
        service()
        for name, buf in (("act", act), ("gd", gate_delta), ("ud", up_delta)):
            write(name, buf, pl.ds(0, 1024), cols)
        while pending:
            service()
        if tile == 0:
            write("n_t", v["n_t_buf"], pl.ds(0, 1536))
            take_shared(4)
            take_shared(5)
            write("w_g", g_buf, pl.ds(0, 1536))
            write("w_u", u_buf, pl.ds(0, 1536))
            write("w_d", d_buf, pl.ds(0, WINDOW))
    keep_q.wait()
    keep_o.wait()
    for i in (0, 1):
        for d in order:
            p = peer_of(shard, d)
            if d < 3:
                hop(i, d, p, shard).wait_send()
                relay(i, d, peer_of(shard, 3 - d), p).wait_send()
            across(i, d, p, odd).wait_send()
            for part in (False, True):
                onward(i, d, p, core, part).wait_send()
    for copy in outs.values():
        copy.wait()
    for d in order:
        p = peer_of(shard, d)
        small_hop(d, p, shard).wait_send()
        for i in (2, 3, 4, 5):
            hop(i, d, p, shard).wait_send()
            across(i, d, p, odd).wait_send()
        for a in range(2):
            if d < 3:
                row_hop(a, d, p, shard).wait_send()
                row_relay(a, d, peer_of(shard, 3 - d), p).wait_send()
    for a in range(2):
        for d in (0,) + order:
            row_onward(a, d, peer_of(shard, d), core).wait_send()


def forward(grad_scale, **given):
    bf16 = jnp.bfloat16
    f32 = jnp.float32
    dma = pltpu.SemaphoreType.DMA
    in_vmem = ("x", "small", "cos", "sin")
    outs = {
        "q_full": ((1536, 2048), bf16, any_spec()),
        "o_full": ((1536, 1536), bf16, any_spec()),
        "pd": ((WINDOW, 1536), bf16, any_spec()),
        "act": ((1024, WINDOW), bf16, any_spec()),
        "gd": ((1024, WINDOW), bf16, any_spec()),
        "ud": ((1024, WINDOW), bf16, any_spec()),
        "n_t": ((1536, 1024), bf16, any_spec()),
        "w_g": ((1536, WINDOW), bf16, any_spec()),
        "w_u": ((1536, WINDOW), bf16, any_spec()),
        "w_d": ((WINDOW, 1536), bf16, any_spec()),
        "hidden": ((128, 1536), f32, vmem_spec()),
        "nrm": ((128, 1536), bf16, vmem_spec()),
        "ctx": ((128, 1536), bf16, vmem_spec()),
        "qry": ((128, 1536), bf16, vmem_spec()),
        "key": ((128, KV * HD), bf16, vmem_spec()),
        "val": ((128, KV * HD), bf16, vmem_spec()),
        "lse": ((128, HD), f32, vmem_spec()),
        "gains": ((8, 1536), f32, vmem_spec()),
    }
    scratch = {
        "q_buf": pltpu.VMEM((1536, 2048), bf16),
        "o_buf": pltpu.VMEM((1536, 1536), bf16),
        "g_buf": pltpu.VMEM((1536, WINDOW), bf16),
        "u_buf": pltpu.VMEM((1536, WINDOW), bf16),
        "d_buf": pltpu.VMEM((WINDOW, 1536), bf16),
        "n_all": pltpu.VMEM((1024, 1536), bf16),
        "cot_all": pltpu.VMEM((1024, 1536), bf16),
        "small_all": pltpu.VMEM((4, 16, 512), bf16),
        "prj": pltpu.VMEM((128, 2048), f32),
        "act_buf": pltpu.VMEM((1024, WINDOW), bf16),
        "gd_buf": pltpu.VMEM((1024, WINDOW), bf16),
        "ud_buf": pltpu.VMEM((1024, WINDOW), bf16),
        "n_t_buf": pltpu.VMEM((1536, 1024), bf16),
        "act_t": pltpu.VMEM((640, 1024), bf16),
        "gs": pltpu.VMEM((512, 640), f32),
        "us": pltpu.VMEM((512, 640), f32),
        "gr": pltpu.VMEM((512, 640), f32),
        "d_grad": pltpu.VMEM((WINDOW, 1536), bf16),
        "send": dma((27,)),
        "recv": dma((27,)),
        "rsend": dma((8,)),
        "rrecv": dma((8,)),
        "zsend": dma((18,)),
        "zrecv": dma((18,)),
        "fsend": dma((20,)),
        "frecv": dma((20,)),
        "local": dma((24,)),
    }
    return dict(zip(outs, pl.pallas_call(
        functools.partial(forward_kernel, grad_scale, (*given, *outs, *scratch)),
        out_shape=[jax.ShapeDtypeStruct(s, dt) for s, dt, _ in outs.values()],
        in_specs=[vmem_spec() if name in in_vmem else any_spec() for name in given],
        out_specs=[spec for _, _, spec in outs.values()],
        scratch_shapes=list(scratch.values()),
        compiler_params=pltpu.CompilerParams(has_side_effects=True, vmem_limit_bytes=67043328),
    )(*given.values())))


def backward_kernel(levels, grad_scale, names, *refs):
    v = dict(zip(names, refs))
    replica, shard, core = place()
    other = 1 - core
    level = replica // 2
    mate = (replica + 1 - 2 * core, shard)
    above, below = (replica + 2, shard), (replica - 2, shard)
    f32 = jnp.float32
    bf16 = jnp.bfloat16
    order = (3, 1, 2)
    own_a, own_d, own_g = v["own_a"], v["own_d"], v["own_g"]
    mat, act, wbuf, back, out = v["mat"], v["act_buf"], v["wbuf"], v["back"], v["out"]
    odd_chip = lax.rem(shard, 2)

    def tokens(owner, c):
        return pl.ds(pl.multiple_of((c * 4 + owner) * 128, 128), 128)

    def chip_at(d):
        across = lax.rem(lax.rem(shard, 2) + lax.rem(d, 2), 2)
        return lax.rem(shard // 2 + d // 2, 2) * 2 + across

    def exchange(block, chip):
        return remote(
            v["blocks"].at[block - 2], own_g.at[pl.ds(pl.multiple_of(block * 384, 384), 384)],
            v["xsend"].at[block], v["xrecv"].at[block], (replica, chip),
        )

    load_down = pltpu.make_async_copy(v["pd"], own_d, v["in_sem"].at[0])
    load_normed = pltpu.make_async_copy(v["n_t"], wbuf.at[:, pl.ds(0, 1024)], v["in_sem"].at[1])
    load_gate = pltpu.make_async_copy(v["w_g"], wbuf.at[:, pl.ds(WINDOW, WINDOW)], v["in_sem"].at[2])
    load_up = pltpu.make_async_copy(v["w_u"], wbuf.at[:, pl.ds(0, WINDOW)], v["in_sem"].at[3])
    load_wd = pltpu.make_async_copy(v["w_d"], wbuf.at[pl.ds(0, WINDOW), pl.ds(0, 1536)], v["in_sem"].at[4])
    load_deltas = [
        pltpu.make_async_copy(v["gd"], mat.at[0], v["in_sem"].at[5]),
        pltpu.make_async_copy(v["ud"], mat.at[1], v["in_sem"].at[6]),
    ]
    load_act = pltpu.make_async_copy(v["act"], act, v["in_sem"].at[7])

    def staged(block):
        slot = lax.rem(block, 2)
        return pltpu.make_async_copy(
            back.at[pl.ds(pl.multiple_of(slot * 384, 384), 384), pl.ds(0, WINDOW)], v["blocks"].at[block - 2],
            v["stage_sem"].at[slot],
        )

    def stage_gradient(block):
        d, a = block // 2, lax.rem(block, 2)
        rows = pl.ds(pl.multiple_of(chip_at(d) * 384, 384), 384)

        @pl.when(block >= 4)
        def _():
            staged(block - 2).wait()

        for n in range(3):
            cols = pl.ds(n * 384, 384)
            part = (
                jnp.dot(wbuf[rows, 0:1024], mat[a, :, cols], preferred_element_type=f32) * grad_scale
            ).astype(bf16)

            @pl.when(d == 0)
            def _():
                own_g[pl.ds(pl.multiple_of(a * 384, 384), 384), cols] = part

            @pl.when(d > 0)
            def _():
                back[pl.ds(pl.multiple_of(a * 384, 384), 384), cols] = part

        @pl.when(block >= 2)
        def _():
            staged(block).start()

    def start_back():
        load_up.start()
        staged(6).wait()
        staged(7).wait()
        load_gate.wait()
        load_up.wait()

    def piece(i):
        return pl.ds(pl.multiple_of((i // 3) * 256, 256), 256), pl.ds(pl.multiple_of(lax.rem(i, 3) * 512, 512), 512)

    def stage_back(i):
        at, cols = piece(i)
        back[at, cols] = (
            dot_nt(mat[0, at, :], wbuf[cols, WINDOW : 2 * WINDOW]) + dot_nt(mat[1, at, :], wbuf[cols, 0:WINDOW])
        ).astype(bf16)

    def stage_out(i):
        at, cols = piece(i)
        out[at, cols] = jnp.dot(act[at, :], wbuf[0:WINDOW, cols], preferred_element_type=f32).astype(bf16)

    partial = (back, out)
    held, parts = v["held"], v["parts"]

    def kept(a, d):
        return partial[a].at[tokens(peer_of(shard, d), core)]

    def to_mate(a, d):
        n = a * 4 + d
        return remote(partial[a].at[tokens(peer_of(shard, d), other)], held.at[a, d], v["csend"].at[n], v["crecv"].at[n], mate)

    def to_owner(a, d):
        n = a * 3 + d - 1
        return remote(kept(a, d), parts.at[a, d - 1], v["psend"].at[n], v["precv"].at[n], (replica, peer_of(shard, d)))

    def pair_sums(a):
        for d in order:
            to_mate(a, d).wait_recv()
            mine = kept(a, d)

            def body(rows, carry):
                mine[rows, :] = (mine[rows, :].astype(f32) + held[a, d, rows, :].astype(f32)).astype(bf16)
                return carry

            row_loop(128, 32, body, 0)
            to_owner(a, d).start()

    def collect(a):
        to_mate(a, 0).wait_recv()
        for d in order:
            to_owner(a, d).wait_recv()

    def full_sum(a, rows):
        total = kept(a, 0)[rows, :].astype(f32) + held[a, 0, rows, :].astype(f32)
        for d in (1, 2, 3):
            total = total + parts[a, d - 1, rows, :].astype(f32)
        return total

    wide = ((v["hid"], mat.at[0, :, pl.ds(0, 768)], 768), (v["prj"], mat.at[1, :, pl.ds(0, 1024)], 1024))
    narrow = ((v["ctx"], v["ctx_all"], 384), (v["nrm"], v["nrm_all"], 384))

    def block(out, owner, c):
        return out.at[tokens(owner, c)]

    def columns(ref, index, width):
        return ref.at[:, pl.ds(pl.multiple_of(index * width, width), width)]

    def wide_copy(a, d, same, source_core, owner, t):
        ref, out, width = wide[a]
        c = core if same else other
        n = (a * 4 + d) * 2 + (0 if same else 1)
        return remote(
            columns(ref, c, width), block(out, owner, source_core), v["gsend"].at[n], v["grecv"].at[n],
            (replica - core + c, t),
        )

    def narrow_copy(a, d, owner, t):
        ref, out, width = narrow[a]
        n = 16 + a * 4 + d
        return remote(columns(ref, t, width), block(out, owner, core), v["gsend"].at[n], v["grecv"].at[n], (replica, t))

    def onward(a, d, source, owner, c):
        out = narrow[a][1]
        n = a * 4 + d
        return remote(source, block(out, owner, c), v["fsend"].at[n], v["frecv"].at[n], mate)

    def own_narrow(a):
        ref, out, width = narrow[a]
        return pltpu.make_async_copy(columns(ref, shard, width), block(out, shard, core), v["local"].at[a])

    def own_wide(a):
        ref, out, width = wide[a]
        return pltpu.make_async_copy(columns(ref, core, width), block(out, shard, core), v["local"].at[2 + a])

    load_out = pltpu.make_async_copy(v["wo"], wbuf.at[:, pl.ds(0, 1536)], v["local"].at[4])
    load_qkv = pltpu.make_async_copy(v["wq"], wbuf.at[:, pl.ds(0, 2048)], v["local"].at[5])

    def stage_sums():
        pair_sums(0)
        for d in order:
            for a in range(2):
                narrow_copy(a, d, shard, peer_of(shard, d)).start()
        send_blocks((1, 2))

    def send_blocks(offsets):
        for d in offsets:
            for a in range(2):
                exchange(d * 2 + a, peer_of(shard, d)).start()

    def stage_hidden():
        collect(0)
        gain = v["gains"][1:2, :]

        def body(rows, total):
            grad = full_sum(0, rows)
            hidden = v["hidden"][rows, :]
            inv = lax.rsqrt(jnp.mean(hidden * hidden, axis=-1, keepdims=True) + NORM_EPS)
            scaled = gain * grad
            out = v["cot"][rows, :].astype(f32) + inv * (
                scaled - hidden * inv * inv * jnp.mean(scaled * hidden, axis=-1, keepdims=True)
            )
            v["hgrad"][rows, :] = out
            v["hid"][rows, :] = out.astype(bf16)
            return total + jnp.sum(grad * hidden * inv, axis=0, keepdims=True)

        v["row_two"][...] = row_loop(128, 16, body, jnp.zeros((1, 1536), f32)) * grad_scale
        for d in (0,) + order:
            if d:
                wide_copy(0, d, True, core, shard, peer_of(shard, d)).start()
            wide_copy(0, d, False, core, shard, peer_of(shard, d)).start()
        own_wide(0).start()

    def stage_context(part):
        if part == 0:
            load_out.wait()
        for e in (2 * part, 2 * part + 1):
            cols = pl.ds(e * 384, 384)
            v["cgrad"][:, cols] = dot_nt(v["hid"][...], wbuf[cols, 0:1536]).astype(bf16)
        if part == 1:
            load_qkv.start()

    def unrotated(x):
        return x * v["cos"][...] - pltpu.roll(x, HD // 2, 1) * v["sin"][...]

    def stage_heads(g, part):
        keys = v["key"][:, g * HD : (g + 1) * HD]
        values = v["val"][:, g * HD : (g + 1) * HD]
        causal = lax.broadcasted_iota(jnp.int32, (128, 128), 0) >= lax.broadcasted_iota(jnp.int32, (128, 128), 1)
        key_grad = jnp.zeros((128, HD), f32) if part == 0 else v["kv_sum"][0]
        value_grad = jnp.zeros((128, HD), f32) if part == 0 else v["kv_sum"][1]
        first_head = g * (HEADS // KV) + part * 2
        for h in range(first_head, first_head + 2):
            at = slice(h * HD, (h + 1) * HD)
            query = v["qry"][:, at]
            grad = v["cgrad"][:, at]
            scores = jnp.where(causal, dot_nt(query, keys) * SCORE_SCALE, -1e30)
            probs = jnp.exp(scores - v["lse"][:, h : h + 1]).astype(bf16)
            wide_probs = probs.astype(f32)
            prob_grad = dot_nt(grad, values)
            delta = jnp.sum(wide_probs * prob_grad, axis=-1, keepdims=True)
            score_grad = (wide_probs * (prob_grad - delta) * SCORE_SCALE).astype(bf16)
            v["prj"][:, at] = unrotated(jnp.dot(score_grad, keys, preferred_element_type=f32)).astype(bf16)
            key_grad = key_grad + dot_tn(score_grad, query)
            value_grad = value_grad + dot_tn(probs, grad)
        if part < 2:
            v["kv_sum"][0] = key_grad
            v["kv_sum"][1] = value_grad
            return
        first = HEADS * HD + g * HD
        v["prj"][:, first : first + HD] = unrotated(key_grad).astype(bf16)
        first = first + KV * HD
        v["prj"][:, first : first + HD] = value_grad.astype(bf16)

    def stage_send_projected():
        for d in (0,) + order:
            if d:
                wide_copy(1, d, True, core, shard, peer_of(shard, d)).start()
            wide_copy(1, d, False, core, shard, peer_of(shard, d)).start()
        own_wide(1).start()

    def stage_normed(part):
        if part == 0:
            load_qkv.wait()
        for e in (2 * part, 2 * part + 1):
            cols = pl.ds(e * 384, 384)
            v["input_grad"][:, cols] = dot_nt(v["prj"][...], wbuf[cols, 0:2048])

    vec, vin, vall = v["vec"], v["vin"], v["vall"]
    replicas = 2 * levels

    def vec_hop(d):
        return remote(vec.at[peer_of(shard, d)], vin.at[d - 1], v["vsend"].at[d - 1], v["vrecv"].at[d - 1],
                      (replica, peer_of(shard, d)))

    def vec_spread(j, slot):
        target = lax.rem(replica + j, replicas)
        return remote(v["vsum"], vall.at[slot], v["vsend"].at[2 + j], v["vrecv"].at[2 + j], (target, shard))

    def stage_input():
        gain = v["gains"][0:1, :]

        def body(rows, totals):
            total, bias = totals
            x = v["x"][rows, :].astype(f32)
            grad = v["input_grad"][rows, :]
            inv = lax.rsqrt(jnp.mean(x * x, axis=-1, keepdims=True) + NORM_EPS)
            scaled = gain * grad
            v["input_grad"][rows, :] = v["hgrad"][rows, :] + inv * (
                scaled - x * inv * inv * jnp.mean(scaled * x, axis=-1, keepdims=True)
            )
            return (
                total + jnp.sum(grad * x * inv, axis=0, keepdims=True),
                bias + jnp.sum(v["prj"][rows, :].astype(f32), axis=0, keepdims=True),
            )

        row_one, row_bias = row_loop(128, 16, body, (jnp.zeros((1, 1536), f32), jnp.zeros((1, 2048), f32)))
        row_one = row_one * grad_scale
        row_bias = row_bias * grad_scale
        row_two = v["row_two"][...]
        for s in range(4):
            vec[s, :, 0:384] = jnp.broadcast_to(row_one[:, s * 384 : (s + 1) * 384], (8, 384))
            vec[s, :, 384:896] = jnp.broadcast_to(row_bias[:, s * 512 : (s + 1) * 512], (8, 512))
            vec[s, :, 896:1280] = jnp.broadcast_to(row_two[:, s * 384 : (s + 1) * 384], (8, 384))
        for d in order:
            vec_hop(d).start()

    def stage_vec():
        total = vec[shard]
        for d in (1, 2, 3):
            vec_hop(d).wait_recv()
            total = total + vin[d - 1]
        v["vsum"][...] = total
        for j in range(1, replicas):
            vec_spread(j, replica).start()

    def stage_vec_out():
        vall[replica] = v["vsum"][...]
        for j in range(1, replicas):
            vec_spread(j, lax.rem(replica + replicas - j, replicas)).wait_recv()
        total = vall[0]
        for j in range(1, replicas):
            total = total + vall[j]
        v["vec_out"][...] = total

    def stage_output():
        collect(1)

        def body(rows, carry):
            v["block_out"][rows, :] = (v["hidden"][rows, :] + full_sum(1, rows)).astype(bf16)
            return carry

        row_loop(128, 32, body, 0)

    def stage_relay():
        for d in order:
            p = peer_of(shard, d)
            for a in range(2):
                narrow_copy(a, d, p, p).wait_recv()
                onward(a, d, block(narrow[a][1], p, core), p, core).start()

    def stage_gathered():
        for a in range(2):
            own_narrow(a).wait()
            own_wide(a).wait()
            for d in (0, 1, 2, 3):
                p = peer_of(shard, d)
                if d:
                    wide_copy(a, d, True, core, p, p).wait_recv()
                wide_copy(a, d, False, other, p, p).wait_recv()
                onward(a, d, block(narrow[a][1], p, other), p, other).wait_recv()

    def stage_attention_parts(j):
        at = pl.ds(j * 128, 128)
        own_a[at, 0:1024] = (dot_tn(v["nrm_all"][:, at], mat[1, :, 0:1024]) * grad_scale).astype(bf16)
        own_a[at, 1024:1792] = (dot_tn(v["ctx_all"][:, at], mat[0, :, 0:768]) * grad_scale).astype(bf16)

    def down_at(c, j):
        first = odd_chip * (1088 * c - 64 * (1 - c)) + (1 - odd_chip) * 1152 * c
        return v["fd"].at[pl.ds(pl.multiple_of(first + j * 64, 64), 64)]

    def gate_at(c, j):
        group = j // 6
        rows = pl.ds(pl.multiple_of(lax.rem(j, 6) * 64, 64), 64)
        return v["fg"].at[lax.rem(group, 2), c, chip_at(group // 2), rows]

    def attention_at(c, j):
        return v["fa"].at[c, pl.ds(pl.multiple_of(j * 32, 32), 32)]

    segments = (
        (own_d, v["near_d"], v["far_d"], 64, 0, DOWN_STEPS, down_at),
        (own_g, v["near_g"], v["far_g"], 64, DOWN_STEPS, DOWN_STEPS + GATE_STEPS, gate_at),
        (own_a, v["near_a"], v["far_a"], 32, DOWN_STEPS + GATE_STEPS, CHUNKS, attention_at),
    )
    end = (level == 0) | (level == levels - 1)
    middle = levels // 2

    def on(k, stage, c=None):
        c = core if c is None else c
        for n, segment in enumerate(segments):
            j = k - segment[4]
            inside = (k >= segment[4]) & (k < segment[5])
            if n == 0:
                inside &= (j > 0) | (1 - odd_chip + c > 0)
                inside &= (j < DOWN_STEPS - 1) | (odd_chip + 1 - c > 0)
            pl.when(inside)(functools.partial(stage, n, segment, j, k))

    def rows_of(segment, j):
        size = segment[3]
        return pl.ds(pl.multiple_of(j * size, size), size)

    def message(segment, j, k, upward, near):
        own, near_ref, far_ref = segment[:3]
        target = near_ref.at[rows_of(segment, j)] if near else far_ref.at[rows_of(segment, j // 2)]
        sem = v["near_sem"] if near else v["far_sem"]
        return remote(own.at[rows_of(segment, j)], target, v["part_sem"].at[k], sem.at[k], above if upward else below)

    def result(segment, j, k, upward, from_own):
        place_ = segment[6](core, j)
        src = segment[0].at[rows_of(segment, j)] if from_own else place_
        sem = v["up_sem"] if upward else v["down_sem"]
        return remote(src, place_, sem.at[k], v["done_sem"].at[k], above if upward else below)

    def keep_result(segment, j, k):
        return pltpu.make_async_copy(segment[0].at[rows_of(segment, j)], segment[6](core, j), v["out_sem"].at[k])

    def to_other_core(segment, j, k, from_own, c):
        place_ = segment[6](c, j)
        src = segment[0].at[rows_of(segment, j)] if from_own else place_
        return remote(src, place_, v["mate_send"].at[k], v["mate_recv"].at[k], mate)

    def add(segment, j, with_far):
        own, near_ref, far_ref, size = segment[:4]

        def body(i, carry):
            rows = pl.ds(pl.multiple_of(j * size + i * 16, 16), 16)
            value = own[rows, :].astype(f32) + near_ref[rows, :].astype(f32)
            if with_far:
                value = value + far_ref[pl.ds(pl.multiple_of((j // 2) * size + i * 16, 16), 16), :].astype(f32)
            own[rows, :] = value.astype(own.dtype)
            return carry

        lax.fori_loop(0, size // 16, body, 0)

    def arrived(n, j):
        if n != 1:
            return
        group = j // 6

        @pl.when((lax.rem(j, 6) == 0) & (group >= 2))
        def _():
            exchange(group, shard).wait_recv()

    def root_of(k):
        return middle - 1 + lax.rem(k, 2)

    def end_gather(n, segment, j, k):
        @pl.when(end)
        def _():
            arrived(n, j)

        @pl.when(level == 0)
        def _():
            message(segment, j, k, True, True).start()

        @pl.when(level == levels - 1)
        def _():
            message(segment, j, k, False, True).start()

    def gather_step(n, segment, j, k):
        @pl.when(~end)
        def _():
            arrived(n, j)

            @pl.when(level != root_of(k))
            def _():
                message(segment, j, k, True, True).wait_recv()
                add(segment, j, False)

        for upward in (True, False):
            towards = (level > 0) & (level < root_of(k)) if upward else (level < levels - 1) & (level > root_of(k))
            crosses = level == (middle - 1 if upward else middle)

            @pl.when(towards & crosses)
            def _():
                message(segment, j, k, upward, False).start()

            if levels > 4:

                @pl.when(towards & ~crosses)
                def _():
                    message(segment, j, k, upward, True).start()

    def root_step(n, segment, j, k):
        @pl.when(level == root_of(k))
        def _():
            message(segment, j, k, True, True).wait_recv()
            message(segment, j, k, True, False).wait_recv()
            add(segment, j, True)
            result(segment, j, k, True, True).start()
            result(segment, j, k, False, True).start()
            keep_result(segment, j, k).start()
            to_other_core(segment, j, k, True, core).start()

    def spread_step(n, segment, j, k):
        @pl.when(~end & (level != root_of(k)))
        def _():
            result(segment, j, k, True, False).wait_recv()

            @pl.when(level < root_of(k))
            def _():
                result(segment, j, k, False, False).start()

            @pl.when(level > root_of(k))
            def _():
                result(segment, j, k, True, False).start()

            to_other_core(segment, j, k, False, core).start()

    def end_spread(n, segment, j, k):
        @pl.when(end)
        def _():
            result(segment, j, k, True, False).wait_recv()
            to_other_core(segment, j, k, False, core).start()

    def close(n, segment, j, k):
        root = root_of(k)

        @pl.when(level == root)
        def _():
            result(segment, j, k, True, True).wait_send()
            result(segment, j, k, False, True).wait_send()
            keep_result(segment, j, k).wait()

        @pl.when(level != root)
        def _():
            message(segment, j, k, True, True).wait_send()

        @pl.when(~end & (level < root))
        def _():
            result(segment, j, k, False, False).wait_send()

        @pl.when(~end & (level > root))
        def _():
            result(segment, j, k, True, False).wait_send()

        to_other_core(segment, j, k, True, core).wait_send()

    def close_mate(n, segment, j, k):
        to_other_core(segment, j, k, True, other).wait_recv()

    def start_mate(a):
        for d in order + (0,):
            to_mate(a, d).start()

    load_down.start()
    load_normed.start()
    for copy in load_deltas:
        copy.start()
    load_gate.start()
    load_act.start()
    for a in range(2):
        own_narrow(a).start()
        onward(a, 0, columns(narrow[a][0], shard, 384), shard, core).start()
    load_down.wait()
    lags = ((end_gather, 0), (gather_step, 8), (root_step, 10), (spread_step, 12), (end_spread, 18))
    steps = CHUNKS + lags[-1][1]

    def begin_products():
        load_normed.wait()
        for copy in load_deltas:
            copy.wait()

    def begin_out():
        start_mate(0)
        load_wd.start()
        load_act.wait()

    def end_out():
        start_mate(1)
        load_out.start()

    def stage_projected():
        stage_send_projected()
        send_blocks((3,))

    beside = [
        (9, 1, begin_products),
        (9, 4, lambda i: (stage_gradient(2 * i), stage_gradient(2 * i + 1))),
        (13, 1, start_back),
        (13, 4, lambda i: (stage_back(3 * i), stage_back(3 * i + 1), stage_back(3 * i + 2))),
        (17, 1, begin_out),
        (19, 1, stage_sums),
        (20, 1, load_wd.wait),
        (20, 4, lambda i: (stage_out(3 * i), stage_out(3 * i + 1), stage_out(3 * i + 2))),
        (24, 1, end_out),
        (25, 1, stage_hidden),
        (26, 1, functools.partial(stage_context, 0)),
        (27, 1, functools.partial(stage_context, 1)),
    ]
    for n in range(6):
        beside.append((28 + n, 1, functools.partial(stage_heads, n // 3, n % 3)))
    beside += [
        (33, 1, stage_projected),
        (34, 1, functools.partial(stage_normed, 0)),
        (36, 1, functools.partial(stage_normed, 1)),
        (38, 1, stage_input),
        (40, 1, stage_relay),
        (56, 1, stage_gathered),
        (56, 1, functools.partial(stage_attention_parts, 0)),
        (58, 1, functools.partial(stage_attention_parts, 1)),
        (60, 1, functools.partial(stage_attention_parts, 2)),
        (62, 1, functools.partial(pair_sums, 1)),
        (64, 1, stage_vec),
        (steps - 4, 1, stage_vec_out),
        (steps - 2, 1, stage_output),
    ]

    def step(t, carry):
        for stage, lag in lags:
            on(t - lag, stage)
        for first, count, stage in beside:
            if count == 1:
                pl.when(t == first)(stage)
            else:
                @pl.when((t >= first) & (t < first + count))
                def _():
                    stage(t - first)

        return carry

    lax.fori_loop(0, steps, step, 0)

    def finish_step(k, carry):
        on(k, close)
        on(k, close_mate, other)
        return carry

    lax.fori_loop(0, CHUNKS, finish_step, 0)
    for d in (1, 2, 3):
        for a in range(2):
            exchange(d * 2 + a, peer_of(shard, d)).wait_send()
    for a in range(2):
        for d in (0, 1, 2, 3):
            p = peer_of(shard, d)
            to_mate(a, d).wait_send()
            wide_copy(a, d, False, core, shard, p).wait_send()
            onward(a, d, block(narrow[a][1], p, core), p, core).wait_send()
            if d:
                to_owner(a, d).wait_send()
                wide_copy(a, d, True, core, shard, p).wait_send()
                narrow_copy(a, d, shard, p).wait_send()
    for d in order:
        vec_hop(d).wait_send()
    for j in range(1, replicas):
        vec_spread(j, replica).wait_send()


def backward(levels, grad_scale, **given):
    bf16 = jnp.bfloat16
    f32 = jnp.float32
    dma = pltpu.SemaphoreType.DMA
    in_hbm = ("pd", "act", "gd", "ud", "n_t", "w_g", "w_u", "w_d", "wo", "wq")
    outs = {
        "fa": ((2, 384, 1792), bf16, any_spec()),
        "fd": ((2240, 1536), bf16, any_spec()),
        "fg": ((2, 2, 4, 384, WINDOW), bf16, any_spec()),
        "blocks": ((6, 384, WINDOW), bf16, any_spec()),
        "block_out": ((128, 1536), bf16, vmem_spec()),
        "input_grad": ((128, 1536), f32, vmem_spec()),
        "vec_out": ((8, 1280), f32, vmem_spec()),
    }
    scratch = {
        "own_a": pltpu.VMEM((384, 1792), bf16),
        "own_d": pltpu.VMEM((WINDOW, 1536), bf16),
        "own_g": pltpu.VMEM((3072, WINDOW), bf16),
        "near_a": pltpu.VMEM((384, 1792), bf16),
        "near_d": pltpu.VMEM((WINDOW, 1536), bf16),
        "near_g": pltpu.VMEM((3072, WINDOW), bf16),
        "far_a": pltpu.VMEM((192, 1792), bf16),
        "far_d": pltpu.VMEM((WINDOW // 2, 1536), bf16),
        "far_g": pltpu.VMEM((1536, WINDOW), bf16),
        "mat": pltpu.VMEM((2, 1024, WINDOW), bf16),
        "act_buf": pltpu.VMEM((1024, WINDOW), bf16),
        "wbuf": pltpu.VMEM((1536, 2 * WINDOW), bf16),
        "back": pltpu.VMEM((1024, 1536), bf16),
        "out": pltpu.VMEM((1024, 1536), bf16),
        "held": pltpu.VMEM((2, 4, 128, 1536), bf16),
        "parts": pltpu.VMEM((2, 3, 128, 1536), bf16),
        "hgrad": pltpu.VMEM((128, 1536), f32),
        "hid": pltpu.VMEM((128, 1536), bf16),
        "cgrad": pltpu.VMEM((128, 1536), bf16),
        "prj": pltpu.VMEM((128, 2048), bf16),
        "ctx_all": pltpu.VMEM((1024, 384), bf16),
        "nrm_all": pltpu.VMEM((1024, 384), bf16),
        "row_two": pltpu.VMEM((1, 1536), f32),
        "kv_sum": pltpu.VMEM((2, 128, HD), f32),
        "vec": pltpu.VMEM((4, 8, 1280), f32),
        "vin": pltpu.VMEM((3, 8, 1280), f32),
        "vsum": pltpu.VMEM((8, 1280), f32),
        "vall": pltpu.VMEM((2 * levels, 8, 1280), f32),
    }
    counts = {
        "xsend": 8, "xrecv": 8, "stage_sem": 2, "csend": 8, "crecv": 8, "psend": 6, "precv": 6, "gsend": 24, "grecv": 24,
        "fsend": 8, "frecv": 8, "local": 6, "in_sem": 8, "vsend": 2 + 2 * levels, "vrecv": 2 + 2 * levels,
    }
    for name in (
        "part_sem", "near_sem", "far_sem", "up_sem", "down_sem", "done_sem", "mate_send", "mate_recv", "out_sem"
    ):
        counts[name] = CHUNKS
    scratch |= {name: dma((n,)) for name, n in counts.items()}
    return pl.pallas_call(
        functools.partial(backward_kernel, levels, grad_scale, (*given, *outs, *scratch)),
        out_shape=[jax.ShapeDtypeStruct(s, dt) for s, dt, _ in outs.values()],
        in_specs=[any_spec() if name in in_hbm else vmem_spec() for name in given],
        out_specs=[spec for _, _, spec in outs.values()],
        scratch_shapes=list(scratch.values()),
        compiler_params=pltpu.CompilerParams(has_side_effects=True, vmem_limit_bytes=67043328),
    )(*given.values())


def widen_kernel(gate, up, down, attn, block, grad, out_gate, out_up, out_down, out_qkv, out_out, out_block, out_grad):
    f32 = jnp.float32
    out_block[...] = block[...]
    out_grad[...] = grad[...]
    for x, out in ((gate, out_gate), (up, out_up)):
        for s in range(4):
            for c in range(2):
                first = (s * 35) // 2 + c * 9
                rest = 1 if s % 2 == 1 and c == 0 else 0
                out[:, (first + rest) * 128 : (first + 9) * 128] = x[c, s][:, rest * 128 :].astype(f32)
        for s in (1, 3):
            first = (s * 35) // 2
            out[:, first * 128 : (first + 1) * 128] = x[1, s - 1][:, 1024:].astype(f32) + x[0, s][:, :128].astype(f32)
    out_down[...] = down[...].astype(f32)
    for c in range(2):
        out_qkv[:, c * 1024 : (c + 1) * 1024] = attn[c][:, :1024].astype(f32)
        out_out[:, c * 768 : (c + 1) * 768] = attn[c][:, 1024:].astype(f32)


def widen(*sums):
    rows = 32
    f32 = jnp.float32
    def blocks(a):
        return pl.BlockSpec((None, 2, 4, rows, WINDOW), lambda i: (a, 0, 0, i, 0))

    down = pl.BlockSpec((224, 1536), lambda i: (jnp.minimum(i, 9), 0))

    own_rows = pl.BlockSpec((16, 1536), lambda i: (jnp.minimum(i, 7), 0))

    def whole(width):
        return pl.BlockSpec((rows, width), lambda i: (i, 0))

    return pl.pallas_call(
        widen_kernel,
        grid=(384 // rows,),
        out_shape=[
            jax.ShapeDtypeStruct((384, 8960), f32),
            jax.ShapeDtypeStruct((384, 8960), f32),
            jax.ShapeDtypeStruct((2240, 1536), f32),
            jax.ShapeDtypeStruct((384, 2048), f32),
            jax.ShapeDtypeStruct((384, 1536), f32),
            jax.ShapeDtypeStruct((128, 1536), jnp.bfloat16),
            jax.ShapeDtypeStruct((128, 1536), f32),
        ],
        in_specs=[blocks(0), blocks(1), down, pl.BlockSpec((2, rows, 1792), lambda i: (0, i, 0)), own_rows, own_rows],
        out_specs=[whole(8960), whole(8960), down, whole(2048), whole(1536), own_rows, own_rows],
    )(*sums)


def fast_device(
    block_input,
    attn_gain,
    qkv_weight,
    qkv_bias,
    out_weight,
    mlp_gain,
    gate_weight,
    up_weight,
    down_weight,
    cotangent,
):
    f32 = jnp.float32
    tok_count = block_input.shape[0]
    levels = lax.axis_size("replica") // 2
    grad_scale = 1.0 / math.sqrt(tok_count * lax.axis_size("replica") * lax.axis_size("shard"))
    cosine, sine_table = rope_tables(tok_count)
    gap = jnp.zeros((128,), jnp.bfloat16)
    rest = jnp.zeros((13 * 512,), jnp.bfloat16)
    small = jnp.concatenate([attn_gain, gap, qkv_bias, mlp_gain, gap, rest]).reshape(16, 512)
    twice = jnp.concatenate([cosine[:, 0], cosine[:, 0]], axis=1)
    turn = jnp.concatenate([-sine_table[:, 0], sine_table[:, 0]], axis=1)
    got = forward(
        grad_scale,
        x=block_input,
        small=small,
        cos=twice,
        sin=turn,
        wq=qkv_weight,
        wo=out_weight,
        wg=gate_weight,
        wu=up_weight,
        wd=down_weight,
        cot=cotangent,
    )
    sum_attn, sum_down, sum_gate, _, block_output, input_grad, vectors = backward(
        levels,
        grad_scale,
        pd=got["pd"],
        act=got["act"],
        gd=got["gd"],
        ud=got["ud"],
        n_t=got["n_t"],
        w_g=got["w_g"],
        w_u=got["w_u"],
        w_d=got["w_d"],
        wo=got["o_full"],
        wq=got["q_full"],
        hidden=got["hidden"],
        x=block_input,
        cot=cotangent,
        gains=got["gains"],
        ctx=got["ctx"],
        nrm=got["nrm"],
        qry=got["qry"],
        key=got["key"],
        val=got["val"],
        lse=got["lse"],
        cos=twice,
        sin=turn,
    )
    gain_one_own, bias_own, gain_two_own = vectors[0, :384], vectors[0, 384:896], vectors[0, 896:]
    gate_grad, up_grad, down_grad, qkv_grad, out_grad, block_output, input_grad = widen(
        sum_gate, sum_gate, sum_down, sum_attn, block_output, input_grad
    )
    return (
        block_output,
        input_grad,
        gain_one_own,
        qkv_grad,
        bias_own,
        out_grad,
        gain_two_own,
        gate_grad,
        up_grad,
        down_grad,
    )


def solution(mesh):
    placed = (
        P(("replica", "shard"), None),
        P("shard"),
        P("shard", None),
        P("shard"),
        P("shard", None),
        P("shard"),
        P("shard", None),
        P("shard", None),
        P("shard", None),
        P(("replica", "shard"), None),
    )
    fits = mesh.shape["shard"] == 4 and mesh.shape["replica"] % 4 == 0
    per_device = fast_device if fits else general_device
    return jax.shard_map(
        per_device,
        mesh=mesh,
        in_specs=placed,
        out_specs=(
            P(("replica", "shard"), None),
            P(("replica", "shard"), None),
            P("shard"),
            P("shard", None),
            P("shard"),
            P("shard", None),
            P("shard"),
            P("shard", None),
            P("shard", None),
            P("shard", None),
        ),
        check_vma=False,
    )
```

```python
import functools
import math

import jax
import jax.numpy as jnp
from jax import lax
from jax.experimental import pallas as pl
from jax.experimental.pallas import tpu as pltpu
from jax.sharding import PartitionSpec as P

HEADS = 12
KV = 2
HD = 128


NORM_EPS = 1e-06
ROPE_BASE = 1000000.0


def rope_tables(tok_count):
    half_dim = HD // 2
    position = jnp.arange(tok_count, dtype=jnp.float32)
    inverse = ROPE_BASE ** (-(jnp.arange(half_dim, dtype=jnp.float32) * 2.0 / HD))
    angles = position[:, None] * inverse[None, :]
    return (jnp.cos(angles)[:, None, :], jnp.sin(angles)[:, None, :])


def rotate(vectors, cosine, sine_table):
    half_dim = HD // 2
    lower_half = vectors[..., :half_dim]
    upper_half = vectors[..., half_dim:]
    return jnp.concatenate(
        [
            lower_half * cosine - upper_half * sine_table,
            upper_half * cosine + lower_half * sine_table,
        ],
        axis=-1,
    )


def unrotate(grads, cosine, sine_table):
    half_dim = HD // 2
    lower_half = grads[..., :half_dim]
    upper_half = grads[..., half_dim:]
    return jnp.concatenate(
        [
            lower_half * cosine + upper_half * sine_table,
            upper_half * cosine - lower_half * sine_table,
        ],
        axis=-1,
    )


def block_scores(query_block, key_rot, first_row):
    row_count = query_block.shape[0]
    scores = jnp.einsum(
        "qkgd,skd->kgqs", query_block, key_rot, preferred_element_type=jnp.float32
    ) * (1.0 / math.sqrt(HD))
    causal = (first_row + jnp.arange(row_count))[:, None] >= jnp.arange(key_rot.shape[0])[None, :]
    return jnp.where(causal, scores, -1e30)


def block_layout(tok_count):
    block_rows = min(tok_count, 512)
    block_count = tok_count // block_rows
    firsts = jnp.arange(block_count, dtype=jnp.int32) * block_rows
    return (block_rows, block_count, firsts)


def attend_forward(queries, key_rot, values):
    tok_count = queries.shape[0]
    block_rows, block_count, firsts = block_layout(tok_count)
    query_blocks = queries.reshape(block_count, block_rows, KV, HEADS // KV, HD)

    def one_block(inputs):
        query_block, first_row = inputs
        scores = block_scores(query_block, key_rot, first_row)
        row_max = jnp.max(scores, axis=-1, keepdims=True)
        logsum = row_max + jnp.log(jnp.sum(jnp.exp(scores - row_max), axis=-1, keepdims=True))
        attn_probs = jnp.exp(scores - logsum).astype(jnp.bfloat16)
        context = jnp.einsum(
            "kgqs,skd->qkgd", attn_probs, values, preferred_element_type=jnp.float32
        ).astype(jnp.bfloat16)
        return (context, logsum)

    context, logsum = lax.map(one_block, (query_blocks, firsts))
    return (context.reshape(tok_count, HEADS * HD), logsum)


def attend_backward(queries, key_rot, values, logsum, context_grad):
    tok_count = queries.shape[0]
    block_rows, block_count, firsts = block_layout(tok_count)
    query_blocks = queries.reshape(block_count, block_rows, KV, HEADS // KV, HD)
    grad_blocks = context_grad.reshape(block_count, block_rows, KV, HEADS // KV, HD)
    score_scale = 1.0 / math.sqrt(HD)

    def one_block(running, inputs):
        key_total, value_total = running
        query_block, grad_block, log_block, first_row = inputs
        scores = block_scores(query_block, key_rot, first_row)
        attn_probs = jnp.exp(scores - log_block).astype(jnp.bfloat16)
        prob_grad = jnp.einsum(
            "qkgd,skd->kgqs", grad_block, values, preferred_element_type=jnp.float32
        )
        wide_probs = attn_probs.astype(jnp.float32)
        row_delta = jnp.sum(wide_probs * prob_grad, axis=-1, keepdims=True)
        score_grad = (wide_probs * (prob_grad - row_delta) * score_scale).astype(jnp.bfloat16)
        query_grad = jnp.einsum(
            "kgqs,skd->qkgd", score_grad, key_rot, preferred_element_type=jnp.float32
        )
        key_total = key_total + jnp.einsum(
            "kgqs,qkgd->skd", score_grad, query_block, preferred_element_type=jnp.float32
        )
        value_total = value_total + jnp.einsum(
            "kgqs,qkgd->skd", attn_probs, grad_block, preferred_element_type=jnp.float32
        )
        return ((key_total, value_total), query_grad)

    zero_keys = jnp.zeros((tok_count, KV, HD), jnp.float32)
    (key_grad, value_grad), query_grad = lax.scan(
        one_block, (zero_keys, zero_keys), (query_blocks, grad_blocks, logsum, firsts)
    )
    return (query_grad.reshape(tok_count, HEADS, HD), key_grad, value_grad)


def general_device(
    block_input,
    attn_gain,
    qkv_weight,
    qkv_bias,
    out_weight,
    mlp_gain,
    gate_weight,
    up_weight,
    down_weight,
    cotangent,
):
    f32 = jnp.float32
    bf16 = jnp.bfloat16
    tok_count = block_input.shape[0]
    grad_scale = 1.0 / math.sqrt(tok_count * lax.axis_size("replica") * lax.axis_size("shard"))
    q_width = HEADS * HD
    k_end = q_width + KV * HD
    cosine, sine_table = rope_tables(tok_count)
    attn_full = (
        lax.all_gather(attn_gain, "shard", axis=0, tiled=True),
        lax.all_gather(qkv_weight, "shard", axis=0, tiled=True),
        lax.all_gather(qkv_bias, "shard", axis=0, tiled=True),
        lax.all_gather(out_weight, "shard", axis=0, tiled=True),
    )
    gain_full, qkv_full, bias_full, out_full = attn_full
    gain_one = gain_full.astype(f32)
    xfloat = block_input.astype(f32)
    inv_one = lax.rsqrt(jnp.mean(xfloat * xfloat, axis=-1, keepdims=True) + NORM_EPS)
    normed_one = (xfloat * inv_one * gain_one).astype(bf16)
    projected = jnp.dot(normed_one, qkv_full, preferred_element_type=f32) + bias_full.astype(f32)
    queries = rotate(
        projected[:, :q_width].reshape(tok_count, HEADS, HD), cosine, sine_table
    ).astype(bf16)
    queries = queries.reshape(tok_count, KV, HEADS // KV, HD)
    key_rot = rotate(
        projected[:, q_width:k_end].reshape(tok_count, KV, HD), cosine, sine_table
    ).astype(bf16)
    values = projected[:, k_end:].reshape(tok_count, KV, HD).astype(bf16)
    context, logsum = attend_forward(queries, key_rot, values)
    hidden_res = xfloat + jnp.dot(context, out_full, preferred_element_type=f32)
    mlp_full = (
        lax.all_gather(mlp_gain, "shard", axis=0, tiled=True),
        lax.all_gather(gate_weight, "shard", axis=0, tiled=True),
        lax.all_gather(up_weight, "shard", axis=0, tiled=True),
        lax.all_gather(down_weight, "shard", axis=0, tiled=True),
    )
    gain_full_two, gate_full, up_full, down_full = mlp_full
    gain_two = gain_full_two.astype(f32)
    inv_two = lax.rsqrt(jnp.mean(hidden_res * hidden_res, axis=-1, keepdims=True) + NORM_EPS)
    normed_two = (hidden_res * inv_two * gain_two).astype(bf16)
    gate_pre = jnp.dot(normed_two, gate_full, preferred_element_type=f32)
    up_pre = jnp.dot(normed_two, up_full, preferred_element_type=f32)
    sigmoid_gate = jax.nn.sigmoid(gate_pre)
    silu_gate = gate_pre * sigmoid_gate
    activation = (silu_gate * up_pre).astype(bf16)
    block_output = (hidden_res + jnp.dot(activation, down_full, preferred_element_type=f32)).astype(
        bf16
    )
    act_grad = jnp.einsum("td,fd->tf", cotangent, down_full, preferred_element_type=f32)
    gate_delta = (
        act_grad * up_pre * sigmoid_gate * (1.0 + gate_pre * (1.0 - sigmoid_gate))
    ).astype(bf16)
    up_delta = (act_grad * silu_gate).astype(bf16)
    normed_two_grad = jnp.einsum(
        "tf,df->td", gate_delta, gate_full, preferred_element_type=f32
    ) + jnp.einsum("tf,df->td", up_delta, up_full, preferred_element_type=f32)
    gain_two_grad = jnp.sum(normed_two_grad * hidden_res * inv_two, axis=0) * grad_scale
    own_rows = (
        lax.all_to_all(activation, "shard", split_axis=1, concat_axis=0, tiled=True),
        lax.all_to_all(normed_two, "shard", split_axis=1, concat_axis=0, tiled=True),
    )
    group_act, group_normed = own_rows
    group_rows = (
        lax.all_gather(cotangent, "shard", axis=0, tiled=True),
        lax.all_gather(gate_delta, "shard", axis=0, tiled=True),
        lax.all_gather(up_delta, "shard", axis=0, tiled=True),
    )
    group_cot, group_gate, group_up = group_rows
    down_part = (
        jnp.einsum("tf,td->fd", group_act, group_cot, preferred_element_type=f32) * grad_scale
    )
    gate_own = (
        jnp.einsum("td,tf->df", group_normed, group_gate, preferred_element_type=f32) * grad_scale
    )
    up_own = (
        jnp.einsum("td,tf->df", group_normed, group_up, preferred_element_type=f32) * grad_scale
    )
    gain_two_own = lax.psum_scatter(gain_two_grad, "shard", scatter_dimension=0, tiled=True)
    mlp_parts = (gain_two_own, gate_own, up_own)
    hidden_grad = cotangent.astype(f32) + inv_two * (
        gain_two * normed_two_grad
        - hidden_res
        * inv_two
        * inv_two
        * jnp.mean(gain_two * normed_two_grad * hidden_res, axis=-1, keepdims=True)
    )
    hidden_low = hidden_grad.astype(bf16)
    context_grad = jnp.einsum("td,ed->te", hidden_low, out_full, preferred_element_type=f32).astype(
        bf16
    )
    query_grad, key_grad, value_grad = attend_backward(
        queries, key_rot, values, logsum, context_grad
    )
    query_grad = unrotate(query_grad, cosine, sine_table).reshape(tok_count, q_width)
    key_grad = unrotate(key_grad, cosine, sine_table).reshape(tok_count, KV * HD)
    projected_grad = jnp.concatenate(
        [query_grad, key_grad, value_grad.reshape(tok_count, KV * HD)], axis=-1
    ).astype(bf16)
    normed_one_grad = jnp.einsum("tc,dc->td", projected_grad, qkv_full, preferred_element_type=f32)
    gain_one_grad = jnp.sum(normed_one_grad * xfloat * inv_one, axis=0) * grad_scale
    bias_grad = jnp.sum(projected_grad.astype(f32), axis=0) * grad_scale
    own_attn = (
        lax.all_to_all(context, "shard", split_axis=1, concat_axis=0, tiled=True),
        lax.all_to_all(normed_one, "shard", split_axis=1, concat_axis=0, tiled=True),
    )
    group_context, group_normed_one = own_attn
    group_rows = (
        lax.all_gather(hidden_low, "shard", axis=0, tiled=True),
        lax.all_gather(projected_grad, "shard", axis=0, tiled=True),
    )
    group_hidden, group_projected = group_rows
    out_own = (
        jnp.einsum("te,td->ed", group_context, group_hidden, preferred_element_type=f32)
        * grad_scale
    )
    qkv_part = (
        jnp.einsum("td,tc->dc", group_normed_one, group_projected, preferred_element_type=f32)
        * grad_scale
    )
    small_parts = (
        lax.psum_scatter(gain_one_grad, "shard", scatter_dimension=0, tiled=True),
        lax.psum_scatter(bias_grad, "shard", scatter_dimension=0, tiled=True),
    )
    attn_parts = (small_parts[0], qkv_part, small_parts[1], out_own)
    input_grad = hidden_grad + inv_one * (
        gain_one * normed_one_grad
        - xfloat
        * inv_one
        * inv_one
        * jnp.mean(gain_one * normed_one_grad * xfloat, axis=-1, keepdims=True)
    )
    summed = lax.psum(
        (
            attn_parts[0],
            attn_parts[1],
            attn_parts[2],
            attn_parts[3],
            mlp_parts[0],
            mlp_parts[1],
            mlp_parts[2],
            down_part,
        ),
        "replica",
    )
    attn_parts = (summed[0], summed[1], summed[2], summed[3])
    mlp_parts = (summed[4], summed[5], summed[6])
    down_part = summed[7]
    return (
        block_output,
        input_grad,
        attn_parts[0],
        attn_parts[1],
        attn_parts[2],
        attn_parts[3],
        mlp_parts[0],
        mlp_parts[1],
        mlp_parts[2],
        down_part,
    )


MESH = pl.DeviceIdType.MESH
VMEM_BYTES = 62 * 2**20
WINDOW = 1152


def place():
    replica = lax.axis_index("replica")
    shard = lax.axis_index("shard")
    core = lax.rem(replica, 2)
    return replica, shard, core


def peer_of(shard, d):
    across = lax.rem(lax.rem(shard, 2) + d % 2, 2)
    up = lax.rem(shard // 2 + d // 2, 2)
    return up * 2 + across


def window_start(shard, core):
    return ((shard * 35) // 2 + core * 9) * 128


def remote(src, dst, send, recv, device):
    return pltpu.make_async_remote_copy(
        src_ref=src,
        dst_ref=dst,
        send_sem=send,
        recv_sem=recv,
        device_id=device,
        device_id_type=MESH,
    )


def any_spec():
    return pl.BlockSpec(memory_space=pl.ANY)


def vmem_spec():
    return pl.BlockSpec(memory_space=pltpu.VMEM)


def params(**more):
    return pltpu.CompilerParams(has_side_effects=True, vmem_limit_bytes=VMEM_BYTES, **more)


DOWN_STEPS, GATE_STEPS, ATTENTION_STEPS = 18, 48, 12
CHUNKS = DOWN_STEPS + GATE_STEPS + ATTENTION_STEPS
SCORE_SCALE = 1.0 / math.sqrt(HD)


def dot_nt(a, b):
    return lax.dot_general(a, b, (((1,), (1,)), ((), ())), preferred_element_type=jnp.float32)


def dot_tn(a, b):
    return lax.dot_general(a, b, (((0,), (0,)), ((), ())), preferred_element_type=jnp.float32)


def row_loop(rows, step, body, init):
    return lax.fori_loop(0, rows // step, lambda j, c: body(pl.ds(pl.multiple_of(j * step, step), step), c), init)


TILES = ((0, 640, 160), (640, 512, 96))


def forward_kernel(grad_scale, names, *refs):
    v = dict(zip(names, refs))
    f32 = jnp.float32
    bf16 = jnp.bfloat16
    replica, shard, core = place()
    other = 1 - core
    mate = (replica + 1 - 2 * core, shard)
    odd = lax.rem(replica // 2, 2)
    pair = (replica + 2 - 4 * odd, shard)
    order = (3, 1, 2)
    first_unit = window_start(shard, core)
    q_buf, o_buf, g_buf, u_buf, d_buf = v["q_buf"], v["o_buf"], v["g_buf"], v["u_buf"], v["d_buf"]
    n_all, cot_all, small_all = v["n_all"], v["cot_all"], v["small_all"]

    def span(start, size):
        return pl.ds(pl.multiple_of(start, 16), size)

    def units(target, offset, width):
        return pl.ds(pl.multiple_of(window_start(target, core) + offset, 128), width)

    def tokens(owner, c):
        return pl.ds(pl.multiple_of((c * 4 + owner) * 128, 128), 128)

    weights = [
        (lambda t: v["wq"], q_buf, 192, 80, True),
        (lambda t: v["wo"], o_buf, 192, 80, True),
    ]
    for offset, width, shared in TILES:
        for name, buf in (("wg", g_buf), ("wu", u_buf)):
            weights.append((
                lambda t, name=name, offset=offset, width=width: v[name].at[:, units(t, offset, width)],
                buf.at[:, pl.ds(offset, width)], 384, shared, False,
            ))

    def base(i, c):
        return c * 192 if weights[i][4] else 0

    def hop(i, d, t, o):
        source, out, size, shared, _ = weights[i]
        first = base(i, core) + odd * shared
        n = i * 3 + d - 1
        return remote(
            source(t).at[span(first, size - shared)], out.at[span(o * 384 + first, size - shared)],
            v["send"].at[n], v["recv"].at[n], (replica, t),
        )

    def relay(i, way, t, o):
        _, out, size, shared, _ = weights[i]
        first = o * 384 + base(i, core) + odd * shared
        ref = out.at[span(first, 64)] if way == 1 else out.at[span(first + 64, size - shared - 64)]
        n = i * 2 + way - 1
        return remote(ref, ref, v["rsend"].at[n], v["rrecv"].at[n], (replica, t))

    def across(i, d, o, whose):
        _, out, size, shared, _ = weights[i]
        ref = out.at[span(o * 384 + base(i, core) + whose * (size - shared), shared)]
        n = i * 3 + d - 1
        return remote(ref, ref, v["zsend"].at[n], v["zrecv"].at[n], pair)

    def onward(i, d, o, c, shared_part):
        _, out, size, shared, _ = weights[i]
        first = o * 384 + base(i, c) + ((1 - odd) * (size - shared) if shared_part else odd * shared)
        ref = out.at[span(first, shared if shared_part else size - shared)]
        n = i * 3 + d - 1 + (6 if shared_part else 0)
        return remote(ref, ref, v["fsend"].at[n], v["frecv"].at[n], mate)

    row_sets = (cot_all, n_all)

    def row_hop(a, d, t, o):
        n = 18 + a * 3 + d - 1
        return remote(row_sets[a].at[tokens(shard, core)], row_sets[a].at[tokens(o, core)], v["send"].at[n], v["recv"].at[n],
                      (replica, t))

    def row_relay(a, way, t, o):
        ref = row_sets[a].at[span((core * 4 + o) * 128 + 64 * (way - 1), 64)]
        n = 4 + a * 2 + way - 1
        return remote(ref, ref, v["rsend"].at[n], v["rrecv"].at[n], (replica, t))

    def row_onward(a, d, o, c):
        n = 12 + a * 4 + d
        ref = row_sets[a].at[tokens(o, c)]
        return remote(ref, ref, v["fsend"].at[n], v["frecv"].at[n], mate)

    def small_hop(d, t, o):
        n = 24 + d - 1
        return remote(v["small"], small_all.at[o], v["send"].at[n], v["recv"].at[n], (replica, t))

    def send_rows(a):
        for d in (1, 2):
            row_hop(a, d, peer_of(shard, d), shard).start()
        row_onward(a, 0, shard, core).start()

    def take_rows(a):
        for d in (1, 2):
            p = peer_of(shard, d)
            row_hop(a, d, p, p).wait_recv()
            row_relay(a, d, peer_of(shard, 3 - d), p).start()
            row_onward(a, d, p, core).start()

    def take_far_rows(a):
        p = peer_of(shard, 3)
        for way in (1, 2):
            row_relay(a, way, p, p).wait_recv()
        row_onward(a, 3, p, core).start()

    def have_rows(a):
        for d in (0,) + order:
            row_onward(a, d, peer_of(shard, d), other).wait_recv()

    def send_weight(i):
        for d in (1, 2) if weights[i][4] else order:
            hop(i, d, peer_of(shard, d), shard).start()

    def take(i, d):
        p = peer_of(shard, d)
        relayed = weights[i][4]
        if relayed and d == 3:
            for way in (1, 2):
                relay(i, way, p, p).wait_recv()
        else:
            hop(i, d, p, p).wait_recv()
            if relayed:
                relay(i, d, peer_of(shard, 3 - d), p).start()
        across(i, d, p, odd).start()
        if relayed:
            onward(i, d, p, core, False).start()

    def take_shared(i):
        for d in order:
            p = peer_of(shard, d)
            across(i, d, p, 1 - odd).wait_recv()
            if weights[i][4]:
                onward(i, d, p, core, True).start()

    def have_other_half(i):
        for d in order:
            for part in (False, True):
                onward(i, d, peer_of(shard, d), other, part).wait_recv()

    rows = span(shard * 384, 384)
    loads = [
        pltpu.make_async_copy(v["cot"], cot_all.at[tokens(shard, core)], v["local"].at[0]),
        pltpu.make_async_copy(v["wq"], q_buf.at[rows], v["local"].at[1]),
        pltpu.make_async_copy(v["wo"], o_buf.at[rows], v["local"].at[2]),
        pltpu.make_async_copy(v["wg"].at[:, units(shard, 0, WINDOW)], g_buf.at[rows], v["local"].at[3]),
        pltpu.make_async_copy(v["wu"].at[:, units(shard, 0, WINDOW)], u_buf.at[rows], v["local"].at[4]),
    ]
    odd_chip = lax.rem(shard, 2)
    inside = odd_chip == core
    loads.append(pltpu.make_async_copy(
        v["wd"].at[span((1152 - 64 * odd_chip) * core, 1088)],
        d_buf.at[span(odd_chip * (1 - core) * 64, 1088)], v["local"].at[5],
    ))

    send_weight(0)
    send_weight(1)
    v["small"][...] = jnp.zeros((16, 512), bf16)
    v["small"][0:1, 0:384] = v["gain_one"][...].reshape(1, 384)
    v["small"][1:2, :] = v["bias"][...].reshape(1, 512)
    v["small"][2:3, 0:384] = v["gain_two"][...].reshape(1, 384)
    for d in order:
        small_hop(d, peer_of(shard, d), shard).start()
    for copy in loads:
        copy.start()
    rest = pltpu.make_async_copy(
        v["wd"].at[span((2176 - 1088) * core + 1088, 64)], d_buf.at[pl.ds(1088, 64)], v["local"].at[6]
    )

    @pl.when(inside)
    def _():
        rest.start()

    @pl.when(~inside)
    def _():
        d_buf[span(1088 - 1088 * odd_chip, 64), :] = jnp.zeros((64, 1536), bf16)

    small_all[shard] = v["small"][...]
    for d in order:
        p = peer_of(shard, d)
        small_hop(d, p, p).wait_recv()

    def gathered(row, width):
        return jnp.concatenate([small_all[s, row : row + 1, 0:width].astype(f32) for s in range(4)], axis=1)

    gain_one = gathered(0, 384)

    def norm_body(at, carry):
        x = v["x"][at, :].astype(f32)
        inv = lax.rsqrt(jnp.mean(x * x, axis=-1, keepdims=True) + NORM_EPS)
        v["nrm"][at, :] = (x * inv * gain_one).astype(bf16)
        return carry

    row_loop(128, 16, norm_body, 0)
    for copy in loads:
        copy.wait()

    @pl.when(inside)
    def _():
        rest.wait()

    for i in (0, 1):
        for d in (1, 2):
            take(i, d)
    send_rows(0)
    send_weight(2)
    send_weight(3)
    take(0, 3)
    take(1, 3)
    take_shared(0)
    have_other_half(0)
    keep_q = pltpu.make_async_copy(q_buf, v["q_full"], v["local"].at[7])
    keep_q.start()
    bias = gathered(1, 512)

    def rotated(x):
        return x * v["cos"][...] + pltpu.roll(x, HD // 2, 1) * v["sin"][...]

    def project(head, out, at, turn):
        cols = slice(head * HD, (head + 1) * HD)
        x = v["prj"][:, cols] + bias[:, cols]
        out[:, at * HD : (at + 1) * HD] = (rotated(x) if turn else x).astype(bf16)

    for n in range(4):
        v["prj"][:, n * 512 : (n + 1) * 512] = jnp.dot(
            v["nrm"][...], q_buf[:, n * 512 : (n + 1) * 512], preferred_element_type=f32
        )
    take_shared(1)
    for h in range(HEADS):
        project(h, v["qry"], h, True)
    for g in range(KV):
        project(HEADS + g, v["key"], g, True)
        project(HEADS + KV + g, v["val"], g, False)
    causal = lax.broadcasted_iota(jnp.int32, (128, 128), 0) >= lax.broadcasted_iota(jnp.int32, (128, 128), 1)
    v["lse"][...] = jnp.zeros((128, HD), f32)
    for h in range(HEADS):
        g = h // (HEADS // KV)
        at = slice(h * HD, (h + 1) * HD)
        scores = dot_nt(v["qry"][:, at], v["key"][:, g * HD : (g + 1) * HD]) * SCORE_SCALE
        scores = jnp.where(causal, scores, -1e30)
        row_max = jnp.max(scores, axis=-1, keepdims=True)
        logsum = row_max + jnp.log(jnp.sum(jnp.exp(scores - row_max), axis=-1, keepdims=True))
        v["lse"][:, h : h + 1] = logsum
        probs = jnp.exp(scores - logsum).astype(bf16)
        v["ctx"][:, at] = jnp.dot(probs, v["val"][:, g * HD : (g + 1) * HD], preferred_element_type=f32).astype(bf16)
    have_other_half(1)
    keep_o = pltpu.make_async_copy(o_buf, v["o_full"], v["local"].at[8])
    keep_o.start()
    for n in range(3):
        cols = slice(n * 512, (n + 1) * 512)
        v["hidden"][:, cols] = v["x"][:, cols].astype(f32) + jnp.dot(
            v["ctx"][...], o_buf[:, cols], preferred_element_type=f32
        )
    gain_two = gathered(2, 384)
    v["gains"][0:1, :] = gain_one
    v["gains"][1:2, :] = gain_two

    def norm_two(j, carry):
        at = pl.ds(pl.multiple_of(j * 16, 16), 16)
        hidden = v["hidden"][at, :]
        inv = lax.rsqrt(jnp.mean(hidden * hidden, axis=-1, keepdims=True) + NORM_EPS)
        n_all[span((core * 4 + shard) * 128 + j * 16, 16), :] = (hidden * inv * gain_two).astype(bf16)
        return carry

    lax.fori_loop(0, 8, norm_two, 0)
    send_rows(1)
    take_rows(0)
    for i in (2, 3):
        for d in order:
            take(i, d)
    take_rows(1)
    send_weight(4)
    send_weight(5)
    take_far_rows(0)
    take_far_rows(1)
    take_shared(2)
    take_shared(3)
    have_rows(0)
    have_rows(1)

    act, gate_delta, up_delta = v["act_buf"], v["gd_buf"], v["ud_buf"]
    gs, us, gr = v["gs"], v["us"], v["gr"]
    pending = [(i, d) for i in (4, 5) for d in order]

    def service():
        if pending:
            take(*pending.pop(0))

    def product(out, offset, width, m, one):
        at = pl.ds(m * 512, 512)
        for n in range(0, width, 256):
            size = min(256, width - n)
            out[at, n : n + size] = one(at, pl.ds(offset + n, size))

    def gate_product(offset, width, m):
        product(gs, offset, width, m, lambda at, cols: jnp.dot(n_all[at, :], g_buf[:, cols], preferred_element_type=f32))

    def up_product(offset, width, m):
        product(us, offset, width, m, lambda at, cols: jnp.dot(n_all[at, :], u_buf[:, cols], preferred_element_type=f32))

    def grad_product(offset, width, m):
        product(gr, offset, width, m, lambda at, cols: dot_nt(cot_all[at, :], d_buf[cols, :]))

    def activate(offset, width, m):
        column = first_unit + offset + lax.broadcasted_iota(jnp.int32, (1, width), 1)
        owned = (column >= shard * 2240) & (column < (shard + 1) * 2240)

        def body(j, carry):
            to = pl.ds(pl.multiple_of(m * 512 + j * 16, 16), 16)
            cols = pl.ds(offset, width)
            gate, up, grad = gs[to, 0:width], us[to, 0:width], gr[to, 0:width]
            sig = jax.nn.sigmoid(gate)
            silu = gate * sig
            act[to, cols] = jnp.where(owned, silu * up, 0.0).astype(bf16)
            gate_delta[to, cols] = jnp.where(owned, grad * up * sig * (1.0 + gate * (1.0 - sig)), 0.0).astype(bf16)
            up_delta[to, cols] = jnp.where(owned, grad * silu, 0.0).astype(bf16)
            return carry

        lax.fori_loop(0, 32, body, 0)

    def transpose(src, cols, dst):
        def body(j, carry):
            at = pl.ds(pl.multiple_of(j * 128, 128), 128)
            dst[:, at] = src[at, cols].T
            return carry

        lax.fori_loop(0, 8, body, 0)

    outs = {}

    def write(name, buf, at, cols=None):
        n = 9 + len(outs)
        src = buf.at[at] if cols is None else buf.at[at, cols]
        dst = v[name].at[at] if cols is None else v[name].at[at, cols]
        copy = pltpu.make_async_copy(src, dst, v["local"].at[n])
        copy.start()
        outs[n] = copy

    write("w_d", d_buf, pl.ds(0, WINDOW))
    for tile, (offset, width, _) in enumerate(TILES):
        cols = pl.ds(offset, width)
        if tile == 0:
            for m in range(2):
                gate_product(offset, width, m)
                up_product(offset, width, m)
                grad_product(offset, width, m)
                activate(offset, width, m)
                service()
        else:
            for m in range(2):
                grad_product(offset, width, m)
                if len(pending) > 2:
                    service()
            while len(pending) > 3:
                service()
            take_shared(4)
            for m in range(2):
                gate_product(offset, width, m)
            while pending:
                service()
            take_shared(5)
            for m in range(2):
                up_product(offset, width, m)
                activate(offset, width, m)
        write("w_g", g_buf, pl.ds(0, 1536), cols)
        write("w_u", u_buf, pl.ds(0, 1536), cols)
        transpose(act, cols, v["act_t"].at[pl.ds(0, width)])
        if tile == 0:
            transpose(n_all, pl.ds(0, 1536), v["n_t_buf"])
            write("n_t", v["n_t_buf"], pl.ds(0, 1536))
            service()
        for name, buf in (("act", act), ("gd", gate_delta), ("ud", up_delta)):
            write(name, buf, pl.ds(0, 1024), cols)
        for n in range(3):
            out = pl.ds(n * 512, 512)
            v["d_grad"][cols, out] = (
                jnp.dot(v["act_t"][0:width, :], cot_all[:, out], preferred_element_type=f32) * grad_scale
            ).astype(bf16)
        write("pd", v["d_grad"], cols)
        if tile == 0:
            service()
    keep_q.wait()
    keep_o.wait()
    for i in (0, 1):
        for d in order:
            p = peer_of(shard, d)
            if d < 3:
                hop(i, d, p, shard).wait_send()
                relay(i, d, peer_of(shard, 3 - d), p).wait_send()
            across(i, d, p, odd).wait_send()
            for part in (False, True):
                onward(i, d, p, core, part).wait_send()
    for copy in outs.values():
        copy.wait()
    for d in order:
        p = peer_of(shard, d)
        small_hop(d, p, shard).wait_send()
        for i in (2, 3, 4, 5):
            hop(i, d, p, shard).wait_send()
            across(i, d, p, odd).wait_send()
        for a in range(2):
            if d < 3:
                row_hop(a, d, p, shard).wait_send()
                row_relay(a, d, peer_of(shard, 3 - d), p).wait_send()
    for a in range(2):
        for d in (0,) + order:
            row_onward(a, d, peer_of(shard, d), core).wait_send()


def forward(grad_scale, **given):
    bf16 = jnp.bfloat16
    f32 = jnp.float32
    dma = pltpu.SemaphoreType.DMA
    in_vmem = ("x", "gain_one", "bias", "gain_two", "cos", "sin")
    outs = {
        "q_full": ((1536, 2048), bf16, any_spec()),
        "o_full": ((1536, 1536), bf16, any_spec()),
        "pd": ((WINDOW, 1536), bf16, any_spec()),
        "act": ((1024, WINDOW), bf16, any_spec()),
        "gd": ((1024, WINDOW), bf16, any_spec()),
        "ud": ((1024, WINDOW), bf16, any_spec()),
        "n_t": ((1536, 1024), bf16, any_spec()),
        "w_g": ((1536, WINDOW), bf16, any_spec()),
        "w_u": ((1536, WINDOW), bf16, any_spec()),
        "w_d": ((WINDOW, 1536), bf16, any_spec()),
        "hidden": ((128, 1536), f32, vmem_spec()),
        "nrm": ((128, 1536), bf16, vmem_spec()),
        "ctx": ((128, 1536), bf16, vmem_spec()),
        "qry": ((128, 1536), bf16, vmem_spec()),
        "key": ((128, KV * HD), bf16, vmem_spec()),
        "val": ((128, KV * HD), bf16, vmem_spec()),
        "lse": ((128, HD), f32, vmem_spec()),
        "gains": ((8, 1536), f32, vmem_spec()),
    }
    scratch = {
        "q_buf": pltpu.VMEM((1536, 2048), bf16),
        "o_buf": pltpu.VMEM((1536, 1536), bf16),
        "g_buf": pltpu.VMEM((1536, WINDOW), bf16),
        "u_buf": pltpu.VMEM((1536, WINDOW), bf16),
        "d_buf": pltpu.VMEM((WINDOW, 1536), bf16),
        "n_all": pltpu.VMEM((1024, 1536), bf16),
        "cot_all": pltpu.VMEM((1024, 1536), bf16),
        "small": pltpu.VMEM((16, 512), bf16),
        "small_all": pltpu.VMEM((4, 16, 512), bf16),
        "prj": pltpu.VMEM((128, 2048), f32),
        "act_buf": pltpu.VMEM((1024, WINDOW), bf16),
        "gd_buf": pltpu.VMEM((1024, WINDOW), bf16),
        "ud_buf": pltpu.VMEM((1024, WINDOW), bf16),
        "n_t_buf": pltpu.VMEM((1536, 1024), bf16),
        "act_t": pltpu.VMEM((640, 1024), bf16),
        "gs": pltpu.VMEM((1024, 640), f32),
        "us": pltpu.VMEM((1024, 640), f32),
        "gr": pltpu.VMEM((1024, 640), f32),
        "d_grad": pltpu.VMEM((WINDOW, 1536), bf16),
        "send": dma((27,)),
        "recv": dma((27,)),
        "rsend": dma((8,)),
        "rrecv": dma((8,)),
        "zsend": dma((18,)),
        "zrecv": dma((18,)),
        "fsend": dma((20,)),
        "frecv": dma((20,)),
        "local": dma((24,)),
    }
    return dict(zip(outs, pl.pallas_call(
        functools.partial(forward_kernel, grad_scale, (*given, *outs, *scratch)),
        out_shape=[jax.ShapeDtypeStruct(s, dt) for s, dt, _ in outs.values()],
        in_specs=[vmem_spec() if name in in_vmem else any_spec() for name in given],
        out_specs=[spec for _, _, spec in outs.values()],
        scratch_shapes=list(scratch.values()),
        compiler_params=pltpu.CompilerParams(has_side_effects=True, vmem_limit_bytes=67043328),
    )(*given.values())))


def backward_kernel(levels, grad_scale, names, *refs):
    v = dict(zip(names, refs))
    replica, shard, core = place()
    other = 1 - core
    level = replica // 2
    mate = (replica + 1 - 2 * core, shard)
    above, below = (replica + 2, shard), (replica - 2, shard)
    f32 = jnp.float32
    bf16 = jnp.bfloat16
    order = (3, 1, 2)
    own_a, own_d, own_g = v["own_a"], v["own_d"], v["own_g"]
    mat, act, wbuf, back, out = v["mat"], v["act_buf"], v["wbuf"], v["back"], v["out"]
    odd_chip = lax.rem(shard, 2)

    def tokens(owner, c):
        return pl.ds(pl.multiple_of((c * 4 + owner) * 128, 128), 128)

    def chip_at(d):
        across = lax.rem(lax.rem(shard, 2) + lax.rem(d, 2), 2)
        return lax.rem(shard // 2 + d // 2, 2) * 2 + across

    def exchange(block, chip):
        return remote(
            v["blocks"].at[block - 2], own_g.at[pl.ds(pl.multiple_of(block * 384, 384), 384)],
            v["xsend"].at[block], v["xrecv"].at[block], (replica, chip),
        )

    load_down = pltpu.make_async_copy(v["pd"], own_d, v["in_sem"].at[0])
    load_normed = pltpu.make_async_copy(v["n_t"], wbuf.at[:, pl.ds(0, 1024)], v["in_sem"].at[1])
    load_gate = pltpu.make_async_copy(v["w_g"], wbuf.at[:, pl.ds(WINDOW, WINDOW)], v["in_sem"].at[2])
    load_up = pltpu.make_async_copy(v["w_u"], wbuf.at[:, pl.ds(0, WINDOW)], v["in_sem"].at[3])
    load_wd = pltpu.make_async_copy(v["w_d"], wbuf.at[pl.ds(0, WINDOW), pl.ds(0, 1536)], v["in_sem"].at[4])
    load_deltas = [
        pltpu.make_async_copy(v["gd"], mat.at[0], v["in_sem"].at[5]),
        pltpu.make_async_copy(v["ud"], mat.at[1], v["in_sem"].at[6]),
    ]
    load_act = pltpu.make_async_copy(v["act"], act, v["in_sem"].at[7])

    def staged(block):
        slot = lax.rem(block, 2)
        return pltpu.make_async_copy(
            back.at[pl.ds(pl.multiple_of(slot * 384, 384), 384), pl.ds(0, WINDOW)], v["blocks"].at[block - 2],
            v["stage_sem"].at[slot],
        )

    def stage_gradient(block):
        d, a = block // 2, lax.rem(block, 2)
        rows = pl.ds(pl.multiple_of(chip_at(d) * 384, 384), 384)

        @pl.when(block >= 4)
        def _():
            staged(block - 2).wait()

        for n in range(3):
            cols = pl.ds(n * 384, 384)
            part = (
                jnp.dot(wbuf[rows, 0:1024], mat[a, :, cols], preferred_element_type=f32) * grad_scale
            ).astype(bf16)

            @pl.when(d == 0)
            def _():
                own_g[pl.ds(pl.multiple_of(a * 384, 384), 384), cols] = part

            @pl.when(d > 0)
            def _():
                back[pl.ds(pl.multiple_of(a * 384, 384), 384), cols] = part

        @pl.when(block >= 2)
        def _():
            staged(block).start()

    def start_back():
        load_up.start()
        staged(6).wait()
        staged(7).wait()
        load_gate.wait()
        load_up.wait()

    def piece(i):
        return pl.ds(pl.multiple_of((i // 3) * 256, 256), 256), pl.ds(pl.multiple_of(lax.rem(i, 3) * 512, 512), 512)

    def stage_back(i):
        at, cols = piece(i)
        back[at, cols] = (
            dot_nt(mat[0, at, :], wbuf[cols, WINDOW : 2 * WINDOW]) + dot_nt(mat[1, at, :], wbuf[cols, 0:WINDOW])
        ).astype(bf16)

    def stage_out(i):
        at, cols = piece(i)
        out[at, cols] = jnp.dot(act[at, :], wbuf[0:WINDOW, cols], preferred_element_type=f32).astype(bf16)

    partial = (back, out)
    held, parts = v["held"], v["parts"]

    def kept(a, d):
        return partial[a].at[tokens(peer_of(shard, d), core)]

    def to_mate(a, d):
        n = a * 4 + d
        return remote(partial[a].at[tokens(peer_of(shard, d), other)], held.at[a, d], v["csend"].at[n], v["crecv"].at[n], mate)

    def to_owner(a, d):
        n = a * 3 + d - 1
        return remote(kept(a, d), parts.at[a, d - 1], v["psend"].at[n], v["precv"].at[n], (replica, peer_of(shard, d)))

    def pair_sums(a):
        for d in order:
            to_mate(a, d).wait_recv()
            mine = kept(a, d)

            def body(rows, carry):
                mine[rows, :] = (mine[rows, :].astype(f32) + held[a, d, rows, :].astype(f32)).astype(bf16)
                return carry

            row_loop(128, 32, body, 0)
            to_owner(a, d).start()

    def collect(a):
        to_mate(a, 0).wait_recv()
        for d in order:
            to_owner(a, d).wait_recv()

    def full_sum(a, rows):
        total = kept(a, 0)[rows, :].astype(f32) + held[a, 0, rows, :].astype(f32)
        for d in (1, 2, 3):
            total = total + parts[a, d - 1, rows, :].astype(f32)
        return total

    wide = ((v["hid"], mat.at[0, :, pl.ds(0, 768)], 768), (v["prj"], mat.at[1, :, pl.ds(0, 1024)], 1024))
    narrow = ((v["ctx"], v["ctx_all"], 384), (v["nrm"], v["nrm_all"], 384))

    def block(out, owner, c):
        return out.at[tokens(owner, c)]

    def columns(ref, index, width):
        return ref.at[:, pl.ds(pl.multiple_of(index * width, width), width)]

    def wide_copy(a, d, same, source_core, owner, t):
        ref, out, width = wide[a]
        c = core if same else other
        n = (a * 4 + d) * 2 + (0 if same else 1)
        return remote(
            columns(ref, c, width), block(out, owner, source_core), v["gsend"].at[n], v["grecv"].at[n],
            (replica - core + c, t),
        )

    def narrow_copy(a, d, owner, t):
        ref, out, width = narrow[a]
        n = 16 + a * 4 + d
        return remote(columns(ref, t, width), block(out, owner, core), v["gsend"].at[n], v["grecv"].at[n], (replica, t))

    def onward(a, d, source, owner, c):
        out = narrow[a][1]
        n = a * 4 + d
        return remote(source, block(out, owner, c), v["fsend"].at[n], v["frecv"].at[n], mate)

    def own_narrow(a):
        ref, out, width = narrow[a]
        return pltpu.make_async_copy(columns(ref, shard, width), block(out, shard, core), v["local"].at[a])

    def own_wide(a):
        ref, out, width = wide[a]
        return pltpu.make_async_copy(columns(ref, core, width), block(out, shard, core), v["local"].at[2 + a])

    load_out = pltpu.make_async_copy(v["wo"], wbuf.at[:, pl.ds(0, 1536)], v["local"].at[4])
    load_qkv = pltpu.make_async_copy(v["wq"], wbuf.at[:, pl.ds(0, 2048)], v["local"].at[5])

    def stage_sums():
        pair_sums(0)
        for d in order:
            for a in range(2):
                narrow_copy(a, d, shard, peer_of(shard, d)).start()
        send_blocks((1, 2))

    def send_blocks(offsets):
        for d in offsets:
            for a in range(2):
                exchange(d * 2 + a, peer_of(shard, d)).start()

    def stage_hidden():
        collect(0)
        gain = v["gains"][1:2, :]

        def body(rows, total):
            grad = full_sum(0, rows)
            hidden = v["hidden"][rows, :]
            inv = lax.rsqrt(jnp.mean(hidden * hidden, axis=-1, keepdims=True) + NORM_EPS)
            scaled = gain * grad
            out = v["cot"][rows, :].astype(f32) + inv * (
                scaled - hidden * inv * inv * jnp.mean(scaled * hidden, axis=-1, keepdims=True)
            )
            v["hgrad"][rows, :] = out
            v["hid"][rows, :] = out.astype(bf16)
            return total + jnp.sum(grad * hidden * inv, axis=0, keepdims=True)

        v["row_two"][...] = row_loop(128, 16, body, jnp.zeros((1, 1536), f32)) * grad_scale
        for d in (0,) + order:
            if d:
                wide_copy(0, d, True, core, shard, peer_of(shard, d)).start()
            wide_copy(0, d, False, core, shard, peer_of(shard, d)).start()
        own_wide(0).start()

    def stage_context(part):
        if part == 0:
            load_out.wait()
        for e in (2 * part, 2 * part + 1):
            cols = pl.ds(e * 384, 384)
            v["cgrad"][:, cols] = dot_nt(v["hid"][...], wbuf[cols, 0:1536]).astype(bf16)
        if part == 1:
            load_qkv.start()

    def unrotated(x):
        return x * v["cos"][...] - pltpu.roll(x, HD // 2, 1) * v["sin"][...]

    def stage_heads(g, part):
        keys = v["key"][:, g * HD : (g + 1) * HD]
        values = v["val"][:, g * HD : (g + 1) * HD]
        causal = lax.broadcasted_iota(jnp.int32, (128, 128), 0) >= lax.broadcasted_iota(jnp.int32, (128, 128), 1)
        key_grad = jnp.zeros((128, HD), f32) if part == 0 else v["kv_sum"][0]
        value_grad = jnp.zeros((128, HD), f32) if part == 0 else v["kv_sum"][1]
        first_head = g * (HEADS // KV) + part * 2
        for h in range(first_head, first_head + 2):
            at = slice(h * HD, (h + 1) * HD)
            query = v["qry"][:, at]
            grad = v["cgrad"][:, at]
            scores = jnp.where(causal, dot_nt(query, keys) * SCORE_SCALE, -1e30)
            probs = jnp.exp(scores - v["lse"][:, h : h + 1]).astype(bf16)
            wide_probs = probs.astype(f32)
            prob_grad = dot_nt(grad, values)
            delta = jnp.sum(wide_probs * prob_grad, axis=-1, keepdims=True)
            score_grad = (wide_probs * (prob_grad - delta) * SCORE_SCALE).astype(bf16)
            v["prj"][:, at] = unrotated(jnp.dot(score_grad, keys, preferred_element_type=f32)).astype(bf16)
            key_grad = key_grad + dot_tn(score_grad, query)
            value_grad = value_grad + dot_tn(probs, grad)
        if part < 2:
            v["kv_sum"][0] = key_grad
            v["kv_sum"][1] = value_grad
            return
        first = HEADS * HD + g * HD
        v["prj"][:, first : first + HD] = unrotated(key_grad).astype(bf16)
        first = first + KV * HD
        v["prj"][:, first : first + HD] = value_grad.astype(bf16)

    def stage_send_projected():
        for d in (0,) + order:
            if d:
                wide_copy(1, d, True, core, shard, peer_of(shard, d)).start()
            wide_copy(1, d, False, core, shard, peer_of(shard, d)).start()
        own_wide(1).start()

    def stage_normed(part):
        if part == 0:
            load_qkv.wait()
        for e in (2 * part, 2 * part + 1):
            cols = pl.ds(e * 384, 384)
            v["input_grad"][:, cols] = dot_nt(v["prj"][...], wbuf[cols, 0:2048])

    vec, vin, vall = v["vec"], v["vin"], v["vall"]
    replicas = 2 * levels

    def vec_hop(d):
        return remote(vec.at[peer_of(shard, d)], vin.at[d - 1], v["vsend"].at[d - 1], v["vrecv"].at[d - 1],
                      (replica, peer_of(shard, d)))

    def vec_spread(j, slot):
        target = lax.rem(replica + j, replicas)
        return remote(v["vsum"], vall.at[slot], v["vsend"].at[2 + j], v["vrecv"].at[2 + j], (target, shard))

    def stage_input():
        gain = v["gains"][0:1, :]

        def body(rows, totals):
            total, bias = totals
            x = v["x"][rows, :].astype(f32)
            grad = v["input_grad"][rows, :]
            inv = lax.rsqrt(jnp.mean(x * x, axis=-1, keepdims=True) + NORM_EPS)
            scaled = gain * grad
            v["input_grad"][rows, :] = v["hgrad"][rows, :] + inv * (
                scaled - x * inv * inv * jnp.mean(scaled * x, axis=-1, keepdims=True)
            )
            return (
                total + jnp.sum(grad * x * inv, axis=0, keepdims=True),
                bias + jnp.sum(v["prj"][rows, :].astype(f32), axis=0, keepdims=True),
            )

        row_one, row_bias = row_loop(128, 16, body, (jnp.zeros((1, 1536), f32), jnp.zeros((1, 2048), f32)))
        row_one = row_one * grad_scale
        row_bias = row_bias * grad_scale
        row_two = v["row_two"][...]
        for s in range(4):
            vec[s, :, 0:384] = jnp.broadcast_to(row_one[:, s * 384 : (s + 1) * 384], (8, 384))
            vec[s, :, 384:896] = jnp.broadcast_to(row_bias[:, s * 512 : (s + 1) * 512], (8, 512))
            vec[s, :, 896:1280] = jnp.broadcast_to(row_two[:, s * 384 : (s + 1) * 384], (8, 384))
        for d in order:
            vec_hop(d).start()

    def stage_vec():
        total = vec[shard]
        for d in (1, 2, 3):
            vec_hop(d).wait_recv()
            total = total + vin[d - 1]
        v["vsum"][...] = total
        for j in range(1, replicas):
            vec_spread(j, replica).start()

    def stage_vec_out():
        vall[replica] = v["vsum"][...]
        for j in range(1, replicas):
            vec_spread(j, lax.rem(replica + replicas - j, replicas)).wait_recv()
        total = vall[0]
        for j in range(1, replicas):
            total = total + vall[j]
        v["vec_out"][...] = total

    def stage_output():
        collect(1)

        def body(rows, carry):
            v["block_out"][rows, :] = (v["hidden"][rows, :] + full_sum(1, rows)).astype(bf16)
            return carry

        row_loop(128, 32, body, 0)

    def stage_relay():
        for d in order:
            p = peer_of(shard, d)
            for a in range(2):
                narrow_copy(a, d, p, p).wait_recv()
                onward(a, d, block(narrow[a][1], p, core), p, core).start()

    def stage_gathered():
        for a in range(2):
            own_narrow(a).wait()
            own_wide(a).wait()
            for d in (0, 1, 2, 3):
                p = peer_of(shard, d)
                if d:
                    wide_copy(a, d, True, core, p, p).wait_recv()
                wide_copy(a, d, False, other, p, p).wait_recv()
                onward(a, d, block(narrow[a][1], p, other), p, other).wait_recv()

    def stage_attention_parts(j):
        at = pl.ds(j * 128, 128)
        own_a[at, 0:1024] = (dot_tn(v["nrm_all"][:, at], mat[1, :, 0:1024]) * grad_scale).astype(bf16)
        own_a[at, 1024:1792] = (dot_tn(v["ctx_all"][:, at], mat[0, :, 0:768]) * grad_scale).astype(bf16)

    def down_at(c, j):
        first = odd_chip * (1088 * c - 64 * (1 - c)) + (1 - odd_chip) * 1152 * c
        return v["fd"].at[pl.ds(pl.multiple_of(first + j * 64, 64), 64)]

    def gate_at(c, j):
        group = j // 6
        rows = pl.ds(pl.multiple_of(lax.rem(j, 6) * 64, 64), 64)
        return v["fg"].at[lax.rem(group, 2), c, chip_at(group // 2), rows]

    def attention_at(c, j):
        return v["fa"].at[c, pl.ds(pl.multiple_of(j * 32, 32), 32)]

    segments = (
        (own_d, v["near_d"], v["far_d"], 64, 0, DOWN_STEPS, down_at),
        (own_g, v["near_g"], v["far_g"], 64, DOWN_STEPS, DOWN_STEPS + GATE_STEPS, gate_at),
        (own_a, v["near_a"], v["far_a"], 32, DOWN_STEPS + GATE_STEPS, CHUNKS, attention_at),
    )
    end = (level == 0) | (level == levels - 1)
    middle = levels // 2

    def on(k, stage, c=None):
        c = core if c is None else c
        for n, segment in enumerate(segments):
            j = k - segment[4]
            inside = (k >= segment[4]) & (k < segment[5])
            if n == 0:
                inside &= (j > 0) | (1 - odd_chip + c > 0)
                inside &= (j < DOWN_STEPS - 1) | (odd_chip + 1 - c > 0)
            pl.when(inside)(functools.partial(stage, n, segment, j, k))

    def rows_of(segment, j):
        size = segment[3]
        return pl.ds(pl.multiple_of(j * size, size), size)

    def message(segment, j, k, upward, near):
        own, near_ref, far_ref = segment[:3]
        target = near_ref.at[rows_of(segment, j)] if near else far_ref.at[rows_of(segment, j // 2)]
        sem = v["near_sem"] if near else v["far_sem"]
        return remote(own.at[rows_of(segment, j)], target, v["part_sem"].at[k], sem.at[k], above if upward else below)

    def result(segment, j, k, upward, from_own):
        place_ = segment[6](core, j)
        src = segment[0].at[rows_of(segment, j)] if from_own else place_
        sem = v["up_sem"] if upward else v["down_sem"]
        return remote(src, place_, sem.at[k], v["done_sem"].at[k], above if upward else below)

    def keep_result(segment, j, k):
        return pltpu.make_async_copy(segment[0].at[rows_of(segment, j)], segment[6](core, j), v["out_sem"].at[k])

    def to_other_core(segment, j, k, from_own, c):
        place_ = segment[6](c, j)
        src = segment[0].at[rows_of(segment, j)] if from_own else place_
        return remote(src, place_, v["mate_send"].at[k], v["mate_recv"].at[k], mate)

    def add(segment, j, with_far):
        own, near_ref, far_ref, size = segment[:4]

        def body(i, carry):
            rows = pl.ds(pl.multiple_of(j * size + i * 16, 16), 16)
            value = own[rows, :].astype(f32) + near_ref[rows, :].astype(f32)
            if with_far:
                value = value + far_ref[pl.ds(pl.multiple_of((j // 2) * size + i * 16, 16), 16), :].astype(f32)
            own[rows, :] = value.astype(own.dtype)
            return carry

        lax.fori_loop(0, size // 16, body, 0)

    def arrived(n, j):
        if n != 1:
            return
        group = j // 6

        @pl.when((lax.rem(j, 6) == 0) & (group >= 2))
        def _():
            exchange(group, shard).wait_recv()

    def root_of(k):
        return middle - 1 + lax.rem(k, 2)

    def end_gather(n, segment, j, k):
        @pl.when(end)
        def _():
            arrived(n, j)

        @pl.when(level == 0)
        def _():
            message(segment, j, k, True, True).start()

        @pl.when(level == levels - 1)
        def _():
            message(segment, j, k, False, True).start()

    def gather_step(n, segment, j, k):
        @pl.when(~end)
        def _():
            arrived(n, j)

            @pl.when(level != root_of(k))
            def _():
                message(segment, j, k, True, True).wait_recv()
                add(segment, j, False)

        for upward in (True, False):
            towards = (level > 0) & (level < root_of(k)) if upward else (level < levels - 1) & (level > root_of(k))
            crosses = level == (middle - 1 if upward else middle)

            @pl.when(towards & crosses)
            def _():
                message(segment, j, k, upward, False).start()

            if levels > 4:

                @pl.when(towards & ~crosses)
                def _():
                    message(segment, j, k, upward, True).start()

    def root_step(n, segment, j, k):
        @pl.when(level == root_of(k))
        def _():
            message(segment, j, k, True, True).wait_recv()
            message(segment, j, k, True, False).wait_recv()
            add(segment, j, True)
            result(segment, j, k, True, True).start()
            result(segment, j, k, False, True).start()
            keep_result(segment, j, k).start()
            to_other_core(segment, j, k, True, core).start()

    def spread_step(n, segment, j, k):
        @pl.when(~end & (level != root_of(k)))
        def _():
            result(segment, j, k, True, False).wait_recv()

            @pl.when(level < root_of(k))
            def _():
                result(segment, j, k, False, False).start()

            @pl.when(level > root_of(k))
            def _():
                result(segment, j, k, True, False).start()

            to_other_core(segment, j, k, False, core).start()

    def end_spread(n, segment, j, k):
        @pl.when(end)
        def _():
            result(segment, j, k, True, False).wait_recv()
            to_other_core(segment, j, k, False, core).start()

    def close(n, segment, j, k):
        root = root_of(k)

        @pl.when(level == root)
        def _():
            result(segment, j, k, True, True).wait_send()
            result(segment, j, k, False, True).wait_send()
            keep_result(segment, j, k).wait()

        @pl.when(level != root)
        def _():
            message(segment, j, k, True, True).wait_send()

        @pl.when(~end & (level < root))
        def _():
            result(segment, j, k, False, False).wait_send()

        @pl.when(~end & (level > root))
        def _():
            result(segment, j, k, True, False).wait_send()

        to_other_core(segment, j, k, True, core).wait_send()

    def close_mate(n, segment, j, k):
        to_other_core(segment, j, k, True, other).wait_recv()

    def start_mate(a):
        for d in order + (0,):
            to_mate(a, d).start()

    load_down.start()
    load_normed.start()
    for copy in load_deltas:
        copy.start()
    load_gate.start()
    load_act.start()
    for a in range(2):
        own_narrow(a).start()
        onward(a, 0, columns(narrow[a][0], shard, 384), shard, core).start()
    load_down.wait()
    lags = ((end_gather, 0), (gather_step, 8), (root_step, 10), (spread_step, 12), (end_spread, 18))
    steps = CHUNKS + lags[-1][1]

    def begin_products():
        load_normed.wait()
        for copy in load_deltas:
            copy.wait()

    def begin_out():
        start_mate(0)
        load_wd.start()
        load_act.wait()

    def end_out():
        start_mate(1)
        load_out.start()

    def stage_projected():
        stage_send_projected()
        send_blocks((3,))

    beside = [
        (9, 1, begin_products),
        (9, 4, lambda i: (stage_gradient(2 * i), stage_gradient(2 * i + 1))),
        (13, 1, start_back),
        (13, 4, lambda i: (stage_back(3 * i), stage_back(3 * i + 1), stage_back(3 * i + 2))),
        (17, 1, begin_out),
        (19, 1, stage_sums),
        (20, 1, load_wd.wait),
        (20, 4, lambda i: (stage_out(3 * i), stage_out(3 * i + 1), stage_out(3 * i + 2))),
        (24, 1, end_out),
        (25, 1, stage_hidden),
        (26, 1, functools.partial(stage_context, 0)),
        (27, 1, functools.partial(stage_context, 1)),
    ]
    for n in range(6):
        beside.append((28 + n, 1, functools.partial(stage_heads, n // 3, n % 3)))
    beside += [
        (33, 1, stage_projected),
        (34, 1, functools.partial(stage_normed, 0)),
        (36, 1, functools.partial(stage_normed, 1)),
        (38, 1, stage_input),
        (40, 1, stage_relay),
        (56, 1, stage_gathered),
        (56, 1, functools.partial(stage_attention_parts, 0)),
        (58, 1, functools.partial(stage_attention_parts, 1)),
        (60, 1, functools.partial(stage_attention_parts, 2)),
        (62, 1, functools.partial(pair_sums, 1)),
        (64, 1, stage_vec),
        (steps - 4, 1, stage_vec_out),
        (steps - 2, 1, stage_output),
    ]

    def step(t, carry):
        for stage, lag in lags:
            on(t - lag, stage)
        for first, count, stage in beside:
            if count == 1:
                pl.when(t == first)(stage)
            else:
                @pl.when((t >= first) & (t < first + count))
                def _():
                    stage(t - first)

        return carry

    lax.fori_loop(0, steps, step, 0)

    def finish_step(k, carry):
        on(k, close)
        on(k, close_mate, other)
        return carry

    lax.fori_loop(0, CHUNKS, finish_step, 0)
    for d in (1, 2, 3):
        for a in range(2):
            exchange(d * 2 + a, peer_of(shard, d)).wait_send()
    for a in range(2):
        for d in (0, 1, 2, 3):
            p = peer_of(shard, d)
            to_mate(a, d).wait_send()
            wide_copy(a, d, False, core, shard, p).wait_send()
            onward(a, d, block(narrow[a][1], p, core), p, core).wait_send()
            if d:
                to_owner(a, d).wait_send()
                wide_copy(a, d, True, core, shard, p).wait_send()
                narrow_copy(a, d, shard, p).wait_send()
    for d in order:
        vec_hop(d).wait_send()
    for j in range(1, replicas):
        vec_spread(j, replica).wait_send()


def backward(levels, grad_scale, **given):
    bf16 = jnp.bfloat16
    f32 = jnp.float32
    dma = pltpu.SemaphoreType.DMA
    in_hbm = ("pd", "act", "gd", "ud", "n_t", "w_g", "w_u", "w_d", "wo", "wq")
    outs = {
        "fa": ((2, 384, 1792), bf16, any_spec()),
        "fd": ((2240, 1536), bf16, any_spec()),
        "fg": ((2, 2, 4, 384, WINDOW), bf16, any_spec()),
        "blocks": ((6, 384, WINDOW), bf16, any_spec()),
        "block_out": ((128, 1536), bf16, vmem_spec()),
        "input_grad": ((128, 1536), f32, vmem_spec()),
        "vec_out": ((8, 1280), f32, vmem_spec()),
    }
    scratch = {
        "own_a": pltpu.VMEM((384, 1792), bf16),
        "own_d": pltpu.VMEM((WINDOW, 1536), bf16),
        "own_g": pltpu.VMEM((3072, WINDOW), bf16),
        "near_a": pltpu.VMEM((384, 1792), bf16),
        "near_d": pltpu.VMEM((WINDOW, 1536), bf16),
        "near_g": pltpu.VMEM((3072, WINDOW), bf16),
        "far_a": pltpu.VMEM((192, 1792), bf16),
        "far_d": pltpu.VMEM((WINDOW // 2, 1536), bf16),
        "far_g": pltpu.VMEM((1536, WINDOW), bf16),
        "mat": pltpu.VMEM((2, 1024, WINDOW), bf16),
        "act_buf": pltpu.VMEM((1024, WINDOW), bf16),
        "wbuf": pltpu.VMEM((1536, 2 * WINDOW), bf16),
        "back": pltpu.VMEM((1024, 1536), bf16),
        "out": pltpu.VMEM((1024, 1536), bf16),
        "held": pltpu.VMEM((2, 4, 128, 1536), bf16),
        "parts": pltpu.VMEM((2, 3, 128, 1536), bf16),
        "hgrad": pltpu.VMEM((128, 1536), f32),
        "hid": pltpu.VMEM((128, 1536), bf16),
        "cgrad": pltpu.VMEM((128, 1536), bf16),
        "prj": pltpu.VMEM((128, 2048), bf16),
        "ctx_all": pltpu.VMEM((1024, 384), bf16),
        "nrm_all": pltpu.VMEM((1024, 384), bf16),
        "row_two": pltpu.VMEM((1, 1536), f32),
        "kv_sum": pltpu.VMEM((2, 128, HD), f32),
        "vec": pltpu.VMEM((4, 8, 1280), f32),
        "vin": pltpu.VMEM((3, 8, 1280), f32),
        "vsum": pltpu.VMEM((8, 1280), f32),
        "vall": pltpu.VMEM((2 * levels, 8, 1280), f32),
    }
    counts = {
        "xsend": 8, "xrecv": 8, "stage_sem": 2, "csend": 8, "crecv": 8, "psend": 6, "precv": 6, "gsend": 24, "grecv": 24,
        "fsend": 8, "frecv": 8, "local": 6, "in_sem": 8, "vsend": 2 + 2 * levels, "vrecv": 2 + 2 * levels,
    }
    for name in (
        "part_sem", "near_sem", "far_sem", "up_sem", "down_sem", "done_sem", "mate_send", "mate_recv", "out_sem"
    ):
        counts[name] = CHUNKS
    scratch |= {name: dma((n,)) for name, n in counts.items()}
    return pl.pallas_call(
        functools.partial(backward_kernel, levels, grad_scale, (*given, *outs, *scratch)),
        out_shape=[jax.ShapeDtypeStruct(s, dt) for s, dt, _ in outs.values()],
        in_specs=[any_spec() if name in in_hbm else vmem_spec() for name in given],
        out_specs=[spec for _, _, spec in outs.values()],
        scratch_shapes=list(scratch.values()),
        compiler_params=pltpu.CompilerParams(has_side_effects=True, vmem_limit_bytes=67043328),
    )(*given.values())


def widen_kernel(
    gate, up, down, attn, block, grad, vec, out_gate, out_up, out_down, out_qkv, out_out, out_block, out_grad, gain_one, bias, gain_two
):
    f32 = jnp.float32
    gain_one[...] = vec[0, 0:384]
    bias[...] = vec[0, 384:896]
    gain_two[...] = vec[0, 896:1280]
    out_block[...] = block[...]
    out_grad[...] = grad[...]
    for x, out in ((gate, out_gate), (up, out_up)):
        for s in range(4):
            for c in range(2):
                first = (s * 35) // 2 + c * 9
                rest = 1 if s % 2 == 1 and c == 0 else 0
                out[:, (first + rest) * 128 : (first + 9) * 128] = x[c, s][:, rest * 128 :].astype(f32)
        for s in (1, 3):
            first = (s * 35) // 2
            out[:, first * 128 : (first + 1) * 128] = x[1, s - 1][:, 1024:].astype(f32) + x[0, s][:, :128].astype(f32)
    out_down[...] = down[...].astype(f32)
    for c in range(2):
        out_qkv[:, c * 1024 : (c + 1) * 1024] = attn[c][:, :1024].astype(f32)
        out_out[:, c * 768 : (c + 1) * 768] = attn[c][:, 1024:].astype(f32)


def widen(*sums):
    rows = 96
    f32 = jnp.float32
    def blocks(a):
        return pl.BlockSpec((None, 2, 4, rows, WINDOW), lambda i: (a, 0, 0, i, 0))

    down = pl.BlockSpec((560, 1536), lambda i: (i, 0))

    own_rows = pl.BlockSpec((32, 1536), lambda i: (i, 0))

    def line(width):
        return pl.BlockSpec((width,), lambda i: (0,))

    def whole(width):
        return pl.BlockSpec((rows, width), lambda i: (i, 0))

    return pl.pallas_call(
        widen_kernel,
        grid=(384 // rows,),
        out_shape=[
            jax.ShapeDtypeStruct((384, 8960), f32),
            jax.ShapeDtypeStruct((384, 8960), f32),
            jax.ShapeDtypeStruct((2240, 1536), f32),
            jax.ShapeDtypeStruct((384, 2048), f32),
            jax.ShapeDtypeStruct((384, 1536), f32),
            jax.ShapeDtypeStruct((128, 1536), jnp.bfloat16),
            jax.ShapeDtypeStruct((128, 1536), f32),
            jax.ShapeDtypeStruct((384,), f32),
            jax.ShapeDtypeStruct((512,), f32),
            jax.ShapeDtypeStruct((384,), f32),
        ],
        in_specs=[blocks(0), blocks(1), down, pl.BlockSpec((2, rows, 1792), lambda i: (0, i, 0)), own_rows, own_rows,
                  pl.BlockSpec((8, 1280), lambda i: (0, 0))],
        out_specs=[whole(8960), whole(8960), down, whole(2048), whole(1536), own_rows, own_rows, line(384), line(512), line(384)],
    )(*sums)


def fast_device(
    block_input,
    attn_gain,
    qkv_weight,
    qkv_bias,
    out_weight,
    mlp_gain,
    gate_weight,
    up_weight,
    down_weight,
    cotangent,
):
    f32 = jnp.float32
    tok_count = block_input.shape[0]
    levels = lax.axis_size("replica") // 2
    grad_scale = 1.0 / math.sqrt(tok_count * lax.axis_size("replica") * lax.axis_size("shard"))
    cosine, sine_table = rope_tables(tok_count)
    twice = jnp.concatenate([cosine[:, 0], cosine[:, 0]], axis=1)
    turn = jnp.concatenate([-sine_table[:, 0], sine_table[:, 0]], axis=1)
    got = forward(
        grad_scale,
        x=block_input,
        gain_one=attn_gain,
        bias=qkv_bias,
        gain_two=mlp_gain,
        cos=twice,
        sin=turn,
        wq=qkv_weight,
        wo=out_weight,
        wg=gate_weight,
        wu=up_weight,
        wd=down_weight,
        cot=cotangent,
    )
    sum_attn, sum_down, sum_gate, _, block_output, input_grad, vectors = backward(
        levels,
        grad_scale,
        pd=got["pd"],
        act=got["act"],
        gd=got["gd"],
        ud=got["ud"],
        n_t=got["n_t"],
        w_g=got["w_g"],
        w_u=got["w_u"],
        w_d=got["w_d"],
        wo=got["o_full"],
        wq=got["q_full"],
        hidden=got["hidden"],
        x=block_input,
        cot=cotangent,
        gains=got["gains"],
        ctx=got["ctx"],
        nrm=got["nrm"],
        qry=got["qry"],
        key=got["key"],
        val=got["val"],
        lse=got["lse"],
        cos=twice,
        sin=turn,
    )
    gate_grad, up_grad, down_grad, qkv_grad, out_grad, block_output, input_grad, gain_one_own, bias_own, gain_two_own = widen(
        sum_gate, sum_gate, sum_down, sum_attn, block_output, input_grad, vectors
    )
    return (
        block_output,
        input_grad,
        gain_one_own,
        qkv_grad,
        bias_own,
        out_grad,
        gain_two_own,
        gate_grad,
        up_grad,
        down_grad,
    )


def solution(mesh):
    placed = (
        P(("replica", "shard"), None),
        P("shard"),
        P("shard", None),
        P("shard"),
        P("shard", None),
        P("shard"),
        P("shard", None),
        P("shard", None),
        P("shard", None),
        P(("replica", "shard"), None),
    )
    fits = mesh.shape["shard"] == 4 and mesh.shape["replica"] % 4 == 0
    per_device = fast_device if fits else general_device
    return jax.shard_map(
        per_device,
        mesh=mesh,
        in_specs=placed,
        out_specs=(
            P(("replica", "shard"), None),
            P(("replica", "shard"), None),
            P("shard"),
            P("shard", None),
            P("shard"),
            P("shard", None),
            P("shard"),
            P("shard", None),
            P("shard", None),
            P("shard", None),
        ),
        check_vma=False,
    )
```

```python
import functools
import math

import jax
import jax.numpy as jnp
from jax import lax
from jax.experimental import pallas as pl
from jax.experimental.pallas import tpu as pltpu
from jax.sharding import PartitionSpec as P

HEADS = 12
KV = 2
HD = 128


NORM_EPS = 1e-06
ROPE_BASE = 1000000.0


def rope_tables(tok_count):
    half_dim = HD // 2
    position = jnp.arange(tok_count, dtype=jnp.float32)
    inverse = ROPE_BASE ** (-(jnp.arange(half_dim, dtype=jnp.float32) * 2.0 / HD))
    angles = position[:, None] * inverse[None, :]
    return (jnp.cos(angles)[:, None, :], jnp.sin(angles)[:, None, :])


def rotate(vectors, cosine, sine_table):
    half_dim = HD // 2
    lower_half = vectors[..., :half_dim]
    upper_half = vectors[..., half_dim:]
    return jnp.concatenate(
        [
            lower_half * cosine - upper_half * sine_table,
            upper_half * cosine + lower_half * sine_table,
        ],
        axis=-1,
    )


def unrotate(grads, cosine, sine_table):
    half_dim = HD // 2
    lower_half = grads[..., :half_dim]
    upper_half = grads[..., half_dim:]
    return jnp.concatenate(
        [
            lower_half * cosine + upper_half * sine_table,
            upper_half * cosine - lower_half * sine_table,
        ],
        axis=-1,
    )


def block_scores(query_block, key_rot, first_row):
    row_count = query_block.shape[0]
    scores = jnp.einsum(
        "qkgd,skd->kgqs", query_block, key_rot, preferred_element_type=jnp.float32
    ) * (1.0 / math.sqrt(HD))
    causal = (first_row + jnp.arange(row_count))[:, None] >= jnp.arange(key_rot.shape[0])[None, :]
    return jnp.where(causal, scores, -1e30)


def block_layout(tok_count):
    block_rows = min(tok_count, 512)
    block_count = tok_count // block_rows
    firsts = jnp.arange(block_count, dtype=jnp.int32) * block_rows
    return (block_rows, block_count, firsts)


def attend_forward(queries, key_rot, values):
    tok_count = queries.shape[0]
    block_rows, block_count, firsts = block_layout(tok_count)
    query_blocks = queries.reshape(block_count, block_rows, KV, HEADS // KV, HD)

    def one_block(inputs):
        query_block, first_row = inputs
        scores = block_scores(query_block, key_rot, first_row)
        row_max = jnp.max(scores, axis=-1, keepdims=True)
        logsum = row_max + jnp.log(jnp.sum(jnp.exp(scores - row_max), axis=-1, keepdims=True))
        attn_probs = jnp.exp(scores - logsum).astype(jnp.bfloat16)
        context = jnp.einsum(
            "kgqs,skd->qkgd", attn_probs, values, preferred_element_type=jnp.float32
        ).astype(jnp.bfloat16)
        return (context, logsum)

    context, logsum = lax.map(one_block, (query_blocks, firsts))
    return (context.reshape(tok_count, HEADS * HD), logsum)


def attend_backward(queries, key_rot, values, logsum, context_grad):
    tok_count = queries.shape[0]
    block_rows, block_count, firsts = block_layout(tok_count)
    query_blocks = queries.reshape(block_count, block_rows, KV, HEADS // KV, HD)
    grad_blocks = context_grad.reshape(block_count, block_rows, KV, HEADS // KV, HD)
    score_scale = 1.0 / math.sqrt(HD)

    def one_block(running, inputs):
        key_total, value_total = running
        query_block, grad_block, log_block, first_row = inputs
        scores = block_scores(query_block, key_rot, first_row)
        attn_probs = jnp.exp(scores - log_block).astype(jnp.bfloat16)
        prob_grad = jnp.einsum(
            "qkgd,skd->kgqs", grad_block, values, preferred_element_type=jnp.float32
        )
        wide_probs = attn_probs.astype(jnp.float32)
        row_delta = jnp.sum(wide_probs * prob_grad, axis=-1, keepdims=True)
        score_grad = (wide_probs * (prob_grad - row_delta) * score_scale).astype(jnp.bfloat16)
        query_grad = jnp.einsum(
            "kgqs,skd->qkgd", score_grad, key_rot, preferred_element_type=jnp.float32
        )
        key_total = key_total + jnp.einsum(
            "kgqs,qkgd->skd", score_grad, query_block, preferred_element_type=jnp.float32
        )
        value_total = value_total + jnp.einsum(
            "kgqs,qkgd->skd", attn_probs, grad_block, preferred_element_type=jnp.float32
        )
        return ((key_total, value_total), query_grad)

    zero_keys = jnp.zeros((tok_count, KV, HD), jnp.float32)
    (key_grad, value_grad), query_grad = lax.scan(
        one_block, (zero_keys, zero_keys), (query_blocks, grad_blocks, logsum, firsts)
    )
    return (query_grad.reshape(tok_count, HEADS, HD), key_grad, value_grad)


def general_device(
    block_input,
    attn_gain,
    qkv_weight,
    qkv_bias,
    out_weight,
    mlp_gain,
    gate_weight,
    up_weight,
    down_weight,
    cotangent,
):
    f32 = jnp.float32
    bf16 = jnp.bfloat16
    tok_count = block_input.shape[0]
    grad_scale = 1.0 / math.sqrt(tok_count * lax.axis_size("replica") * lax.axis_size("shard"))
    q_width = HEADS * HD
    k_end = q_width + KV * HD
    cosine, sine_table = rope_tables(tok_count)
    attn_full = (
        lax.all_gather(attn_gain, "shard", axis=0, tiled=True),
        lax.all_gather(qkv_weight, "shard", axis=0, tiled=True),
        lax.all_gather(qkv_bias, "shard", axis=0, tiled=True),
        lax.all_gather(out_weight, "shard", axis=0, tiled=True),
    )
    gain_full, qkv_full, bias_full, out_full = attn_full
    gain_one = gain_full.astype(f32)
    xfloat = block_input.astype(f32)
    inv_one = lax.rsqrt(jnp.mean(xfloat * xfloat, axis=-1, keepdims=True) + NORM_EPS)
    normed_one = (xfloat * inv_one * gain_one).astype(bf16)
    projected = jnp.dot(normed_one, qkv_full, preferred_element_type=f32) + bias_full.astype(f32)
    queries = rotate(
        projected[:, :q_width].reshape(tok_count, HEADS, HD), cosine, sine_table
    ).astype(bf16)
    queries = queries.reshape(tok_count, KV, HEADS // KV, HD)
    key_rot = rotate(
        projected[:, q_width:k_end].reshape(tok_count, KV, HD), cosine, sine_table
    ).astype(bf16)
    values = projected[:, k_end:].reshape(tok_count, KV, HD).astype(bf16)
    context, logsum = attend_forward(queries, key_rot, values)
    hidden_res = xfloat + jnp.dot(context, out_full, preferred_element_type=f32)
    mlp_full = (
        lax.all_gather(mlp_gain, "shard", axis=0, tiled=True),
        lax.all_gather(gate_weight, "shard", axis=0, tiled=True),
        lax.all_gather(up_weight, "shard", axis=0, tiled=True),
        lax.all_gather(down_weight, "shard", axis=0, tiled=True),
    )
    gain_full_two, gate_full, up_full, down_full = mlp_full
    gain_two = gain_full_two.astype(f32)
    inv_two = lax.rsqrt(jnp.mean(hidden_res * hidden_res, axis=-1, keepdims=True) + NORM_EPS)
    normed_two = (hidden_res * inv_two * gain_two).astype(bf16)
    gate_pre = jnp.dot(normed_two, gate_full, preferred_element_type=f32)
    up_pre = jnp.dot(normed_two, up_full, preferred_element_type=f32)
    sigmoid_gate = jax.nn.sigmoid(gate_pre)
    silu_gate = gate_pre * sigmoid_gate
    activation = (silu_gate * up_pre).astype(bf16)
    block_output = (hidden_res + jnp.dot(activation, down_full, preferred_element_type=f32)).astype(
        bf16
    )
    act_grad = jnp.einsum("td,fd->tf", cotangent, down_full, preferred_element_type=f32)
    gate_delta = (
        act_grad * up_pre * sigmoid_gate * (1.0 + gate_pre * (1.0 - sigmoid_gate))
    ).astype(bf16)
    up_delta = (act_grad * silu_gate).astype(bf16)
    normed_two_grad = jnp.einsum(
        "tf,df->td", gate_delta, gate_full, preferred_element_type=f32
    ) + jnp.einsum("tf,df->td", up_delta, up_full, preferred_element_type=f32)
    gain_two_grad = jnp.sum(normed_two_grad * hidden_res * inv_two, axis=0) * grad_scale
    own_rows = (
        lax.all_to_all(activation, "shard", split_axis=1, concat_axis=0, tiled=True),
        lax.all_to_all(normed_two, "shard", split_axis=1, concat_axis=0, tiled=True),
    )
    group_act, group_normed = own_rows
    group_rows = (
        lax.all_gather(cotangent, "shard", axis=0, tiled=True),
        lax.all_gather(gate_delta, "shard", axis=0, tiled=True),
        lax.all_gather(up_delta, "shard", axis=0, tiled=True),
    )
    group_cot, group_gate, group_up = group_rows
    down_part = (
        jnp.einsum("tf,td->fd", group_act, group_cot, preferred_element_type=f32) * grad_scale
    )
    gate_own = (
        jnp.einsum("td,tf->df", group_normed, group_gate, preferred_element_type=f32) * grad_scale
    )
    up_own = (
        jnp.einsum("td,tf->df", group_normed, group_up, preferred_element_type=f32) * grad_scale
    )
    gain_two_own = lax.psum_scatter(gain_two_grad, "shard", scatter_dimension=0, tiled=True)
    mlp_parts = (gain_two_own, gate_own, up_own)
    hidden_grad = cotangent.astype(f32) + inv_two * (
        gain_two * normed_two_grad
        - hidden_res
        * inv_two
        * inv_two
        * jnp.mean(gain_two * normed_two_grad * hidden_res, axis=-1, keepdims=True)
    )
    hidden_low = hidden_grad.astype(bf16)
    context_grad = jnp.einsum("td,ed->te", hidden_low, out_full, preferred_element_type=f32).astype(
        bf16
    )
    query_grad, key_grad, value_grad = attend_backward(
        queries, key_rot, values, logsum, context_grad
    )
    query_grad = unrotate(query_grad, cosine, sine_table).reshape(tok_count, q_width)
    key_grad = unrotate(key_grad, cosine, sine_table).reshape(tok_count, KV * HD)
    projected_grad = jnp.concatenate(
        [query_grad, key_grad, value_grad.reshape(tok_count, KV * HD)], axis=-1
    ).astype(bf16)
    normed_one_grad = jnp.einsum("tc,dc->td", projected_grad, qkv_full, preferred_element_type=f32)
    gain_one_grad = jnp.sum(normed_one_grad * xfloat * inv_one, axis=0) * grad_scale
    bias_grad = jnp.sum(projected_grad.astype(f32), axis=0) * grad_scale
    own_attn = (
        lax.all_to_all(context, "shard", split_axis=1, concat_axis=0, tiled=True),
        lax.all_to_all(normed_one, "shard", split_axis=1, concat_axis=0, tiled=True),
    )
    group_context, group_normed_one = own_attn
    group_rows = (
        lax.all_gather(hidden_low, "shard", axis=0, tiled=True),
        lax.all_gather(projected_grad, "shard", axis=0, tiled=True),
    )
    group_hidden, group_projected = group_rows
    out_own = (
        jnp.einsum("te,td->ed", group_context, group_hidden, preferred_element_type=f32)
        * grad_scale
    )
    qkv_part = (
        jnp.einsum("td,tc->dc", group_normed_one, group_projected, preferred_element_type=f32)
        * grad_scale
    )
    small_parts = (
        lax.psum_scatter(gain_one_grad, "shard", scatter_dimension=0, tiled=True),
        lax.psum_scatter(bias_grad, "shard", scatter_dimension=0, tiled=True),
    )
    attn_parts = (small_parts[0], qkv_part, small_parts[1], out_own)
    input_grad = hidden_grad + inv_one * (
        gain_one * normed_one_grad
        - xfloat
        * inv_one
        * inv_one
        * jnp.mean(gain_one * normed_one_grad * xfloat, axis=-1, keepdims=True)
    )
    summed = lax.psum(
        (
            attn_parts[0],
            attn_parts[1],
            attn_parts[2],
            attn_parts[3],
            mlp_parts[0],
            mlp_parts[1],
            mlp_parts[2],
            down_part,
        ),
        "replica",
    )
    attn_parts = (summed[0], summed[1], summed[2], summed[3])
    mlp_parts = (summed[4], summed[5], summed[6])
    down_part = summed[7]
    return (
        block_output,
        input_grad,
        attn_parts[0],
        attn_parts[1],
        attn_parts[2],
        attn_parts[3],
        mlp_parts[0],
        mlp_parts[1],
        mlp_parts[2],
        down_part,
    )


MESH = pl.DeviceIdType.MESH
VMEM_BYTES = 62 * 2**20
WINDOW = 1152


def place():
    replica = lax.axis_index("replica")
    shard = lax.axis_index("shard")
    core = lax.rem(replica, 2)
    return replica, shard, core


def peer_of(shard, d):
    across = lax.rem(lax.rem(shard, 2) + d % 2, 2)
    up = lax.rem(shard // 2 + d // 2, 2)
    return up * 2 + across


def window_start(shard, core):
    return ((shard * 35) // 2 + core * 9) * 128


def remote(src, dst, send, recv, device):
    return pltpu.make_async_remote_copy(
        src_ref=src,
        dst_ref=dst,
        send_sem=send,
        recv_sem=recv,
        device_id=device,
        device_id_type=MESH,
    )


def any_spec():
    return pl.BlockSpec(memory_space=pl.ANY)


def vmem_spec():
    return pl.BlockSpec(memory_space=pltpu.VMEM)


def params(**more):
    return pltpu.CompilerParams(has_side_effects=True, vmem_limit_bytes=VMEM_BYTES, **more)


DOWN_STEPS, GATE_STEPS, ATTENTION_STEPS = 18, 48, 12
CHUNKS = DOWN_STEPS + GATE_STEPS + ATTENTION_STEPS
SCORE_SCALE = 1.0 / math.sqrt(HD)


def dot_nt(a, b):
    return lax.dot_general(a, b, (((1,), (1,)), ((), ())), preferred_element_type=jnp.float32)


def dot_tn(a, b):
    return lax.dot_general(a, b, (((0,), (0,)), ((), ())), preferred_element_type=jnp.float32)


def row_loop(rows, step, body, init):
    return lax.fori_loop(0, rows // step, lambda j, c: body(pl.ds(pl.multiple_of(j * step, step), step), c), init)


TILES = ((0, 640, 192), (640, 512, 128))


def forward_kernel(grad_scale, names, *refs):
    v = dict(zip(names, refs))
    f32 = jnp.float32
    bf16 = jnp.bfloat16
    replica, shard, core = place()
    other = 1 - core
    mate = (replica + 1 - 2 * core, shard)
    odd = lax.rem(replica // 2, 2)
    pair = (replica + 2 - 4 * odd, shard)
    order = (3, 1, 2)
    first_unit = window_start(shard, core)
    q_buf, o_buf, g_buf, u_buf, d_buf = v["q_buf"], v["o_buf"], v["g_buf"], v["u_buf"], v["d_buf"]
    n_all, cot_all, small_all = v["n_all"], v["cot_all"], v["small_all"]

    def span(start, size):
        return pl.ds(pl.multiple_of(start, 16), size)

    def units(target, offset, width):
        return pl.ds(pl.multiple_of(window_start(target, core) + offset, 128), width)

    def tokens(owner, c):
        return pl.ds(pl.multiple_of((c * 4 + owner) * 128, 128), 128)

    weights = [
        (lambda t: v["wq"], q_buf, 192, 48, True),
        (lambda t: v["wo"], o_buf, 192, 48, True),
    ]
    for offset, width, shared in TILES:
        for name, buf in (("wg", g_buf), ("wu", u_buf)):
            weights.append((
                lambda t, name=name, offset=offset, width=width: v[name].at[:, units(t, offset, width)],
                buf.at[:, pl.ds(offset, width)], 384, shared, False,
            ))

    def base(i, c):
        return c * 192 if weights[i][4] else 0

    def hop(i, d, t, o):
        source, out, size, shared, _ = weights[i]
        first = base(i, core) + odd * shared
        n = i * 3 + d - 1
        return remote(
            source(t).at[span(first, size - shared)], out.at[span(o * 384 + first, size - shared)],
            v["send"].at[n], v["recv"].at[n], (replica, t),
        )

    def relay(i, way, t, o):
        _, out, size, shared, _ = weights[i]
        first = o * 384 + base(i, core) + odd * shared
        ref = out.at[span(first, 64)] if way == 1 else out.at[span(first + 64, size - shared - 64)]
        n = i * 2 + way - 1
        return remote(ref, ref, v["rsend"].at[n], v["rrecv"].at[n], (replica, t))

    def across(i, d, o, whose):
        _, out, size, shared, _ = weights[i]
        ref = out.at[span(o * 384 + base(i, core) + whose * (size - shared), shared)]
        n = i * 3 + d - 1
        return remote(ref, ref, v["zsend"].at[n], v["zrecv"].at[n], pair)

    def onward(i, d, o, c, shared_part):
        _, out, size, shared, _ = weights[i]
        first = o * 384 + base(i, c) + ((1 - odd) * (size - shared) if shared_part else odd * shared)
        ref = out.at[span(first, shared if shared_part else size - shared)]
        n = i * 3 + d - 1 + (6 if shared_part else 0)
        return remote(ref, ref, v["fsend"].at[n], v["frecv"].at[n], mate)

    row_sets = (cot_all, n_all)

    def row_hop(a, d, t, o):
        n = 18 + a * 3 + d - 1
        return remote(row_sets[a].at[tokens(shard, core)], row_sets[a].at[tokens(o, core)], v["send"].at[n], v["recv"].at[n],
                      (replica, t))

    def row_relay(a, way, t, o):
        ref = row_sets[a].at[span((core * 4 + o) * 128 + 64 * (way - 1), 64)]
        n = 4 + a * 2 + way - 1
        return remote(ref, ref, v["rsend"].at[n], v["rrecv"].at[n], (replica, t))

    def row_onward(a, d, o, c):
        n = 12 + a * 4 + d
        ref = row_sets[a].at[tokens(o, c)]
        return remote(ref, ref, v["fsend"].at[n], v["frecv"].at[n], mate)

    def small_hop(d, t, o):
        n = 24 + d - 1
        return remote(v["small"], small_all.at[o], v["send"].at[n], v["recv"].at[n], (replica, t))

    def send_rows(a):
        for d in (1, 2):
            row_hop(a, d, peer_of(shard, d), shard).start()
        row_onward(a, 0, shard, core).start()

    def take_rows(a):
        for d in (1, 2):
            p = peer_of(shard, d)
            row_hop(a, d, p, p).wait_recv()
            row_relay(a, d, peer_of(shard, 3 - d), p).start()
            row_onward(a, d, p, core).start()

    def take_far_rows(a):
        p = peer_of(shard, 3)
        for way in (1, 2):
            row_relay(a, way, p, p).wait_recv()
        row_onward(a, 3, p, core).start()

    def have_rows(a):
        for d in (0,) + order:
            row_onward(a, d, peer_of(shard, d), other).wait_recv()

    def send_weight(i):
        for d in (1, 2) if weights[i][4] else order:
            hop(i, d, peer_of(shard, d), shard).start()

    def take(i, d):
        p = peer_of(shard, d)
        relayed = weights[i][4]
        if relayed and d == 3:
            for way in (1, 2):
                relay(i, way, p, p).wait_recv()
        else:
            hop(i, d, p, p).wait_recv()
            if relayed:
                relay(i, d, peer_of(shard, 3 - d), p).start()
        across(i, d, p, odd).start()
        if relayed:
            onward(i, d, p, core, False).start()

    def take_shared(i):
        for d in order:
            p = peer_of(shard, d)
            across(i, d, p, 1 - odd).wait_recv()
            if weights[i][4]:
                onward(i, d, p, core, True).start()

    def have_other_half(i):
        for d in order:
            for part in (False, True):
                onward(i, d, peer_of(shard, d), other, part).wait_recv()

    rows = span(shard * 384, 384)
    loads = [
        pltpu.make_async_copy(v["cot"], cot_all.at[tokens(shard, core)], v["local"].at[0]),
        pltpu.make_async_copy(v["wq"], q_buf.at[rows], v["local"].at[1]),
        pltpu.make_async_copy(v["wo"], o_buf.at[rows], v["local"].at[2]),
        pltpu.make_async_copy(v["wg"].at[:, units(shard, 0, WINDOW)], g_buf.at[rows], v["local"].at[3]),
        pltpu.make_async_copy(v["wu"].at[:, units(shard, 0, WINDOW)], u_buf.at[rows], v["local"].at[4]),
    ]
    odd_chip = lax.rem(shard, 2)
    inside = odd_chip == core
    loads.append(pltpu.make_async_copy(
        v["wd"].at[span((1152 - 64 * odd_chip) * core, 1088)],
        d_buf.at[span(odd_chip * (1 - core) * 64, 1088)], v["local"].at[5],
    ))

    send_weight(0)
    send_weight(1)
    v["small"][...] = jnp.zeros((16, 512), bf16)
    v["small"][0:1, 0:384] = v["gain_one"][...].reshape(1, 384)
    v["small"][1:2, :] = v["bias"][...].reshape(1, 512)
    v["small"][2:3, 0:384] = v["gain_two"][...].reshape(1, 384)
    for d in order:
        small_hop(d, peer_of(shard, d), shard).start()
    for copy in loads:
        copy.start()
    rest = pltpu.make_async_copy(
        v["wd"].at[span((2176 - 1088) * core + 1088, 64)], d_buf.at[pl.ds(1088, 64)], v["local"].at[6]
    )

    @pl.when(inside)
    def _():
        rest.start()

    @pl.when(~inside)
    def _():
        d_buf[span(1088 - 1088 * odd_chip, 64), :] = jnp.zeros((64, 1536), bf16)

    small_all[shard] = v["small"][...]
    for d in order:
        p = peer_of(shard, d)
        small_hop(d, p, p).wait_recv()

    def gathered(row, width):
        return jnp.concatenate([small_all[s, row : row + 1, 0:width].astype(f32) for s in range(4)], axis=1)

    gain_one = gathered(0, 384)

    def norm_body(at, carry):
        x = v["x"][at, :].astype(f32)
        inv = lax.rsqrt(jnp.mean(x * x, axis=-1, keepdims=True) + NORM_EPS)
        v["nrm"][at, :] = (x * inv * gain_one).astype(bf16)
        return carry

    row_loop(128, 16, norm_body, 0)
    for copy in loads:
        copy.wait()

    @pl.when(inside)
    def _():
        rest.wait()

    for i in (0, 1):
        for d in (1, 2):
            take(i, d)
    send_rows(0)
    send_weight(2)
    send_weight(3)
    take(0, 3)
    take(1, 3)
    take_shared(0)
    have_other_half(0)
    keep_q = pltpu.make_async_copy(q_buf, v["q_full"], v["local"].at[7])
    keep_q.start()
    bias = gathered(1, 512)

    def rotated(x):
        return x * v["cos"][...] + pltpu.roll(x, HD // 2, 1) * v["sin"][...]

    def project(head, out, at, turn):
        cols = slice(head * HD, (head + 1) * HD)
        x = v["prj"][:, cols] + bias[:, cols]
        out[:, at * HD : (at + 1) * HD] = (rotated(x) if turn else x).astype(bf16)

    for n in range(4):
        v["prj"][:, n * 512 : (n + 1) * 512] = jnp.dot(
            v["nrm"][...], q_buf[:, n * 512 : (n + 1) * 512], preferred_element_type=f32
        )
    take_shared(1)
    for h in range(HEADS):
        project(h, v["qry"], h, True)
    for g in range(KV):
        project(HEADS + g, v["key"], g, True)
        project(HEADS + KV + g, v["val"], g, False)
    causal = lax.broadcasted_iota(jnp.int32, (128, 128), 0) >= lax.broadcasted_iota(jnp.int32, (128, 128), 1)
    v["lse"][...] = jnp.zeros((128, HD), f32)
    for h in range(HEADS):
        g = h // (HEADS // KV)
        at = slice(h * HD, (h + 1) * HD)
        scores = dot_nt(v["qry"][:, at], v["key"][:, g * HD : (g + 1) * HD]) * SCORE_SCALE
        scores = jnp.where(causal, scores, -1e30)
        row_max = jnp.max(scores, axis=-1, keepdims=True)
        logsum = row_max + jnp.log(jnp.sum(jnp.exp(scores - row_max), axis=-1, keepdims=True))
        v["lse"][:, h : h + 1] = logsum
        probs = jnp.exp(scores - logsum).astype(bf16)
        v["ctx"][:, at] = jnp.dot(probs, v["val"][:, g * HD : (g + 1) * HD], preferred_element_type=f32).astype(bf16)
    have_other_half(1)
    keep_o = pltpu.make_async_copy(o_buf, v["o_full"], v["local"].at[8])
    keep_o.start()
    for n in range(3):
        cols = slice(n * 512, (n + 1) * 512)
        v["hidden"][:, cols] = v["x"][:, cols].astype(f32) + jnp.dot(
            v["ctx"][...], o_buf[:, cols], preferred_element_type=f32
        )
    gain_two = gathered(2, 384)
    v["gains"][0:1, :] = gain_one
    v["gains"][1:2, :] = gain_two

    def norm_two(j, carry):
        at = pl.ds(pl.multiple_of(j * 16, 16), 16)
        hidden = v["hidden"][at, :]
        inv = lax.rsqrt(jnp.mean(hidden * hidden, axis=-1, keepdims=True) + NORM_EPS)
        n_all[span((core * 4 + shard) * 128 + j * 16, 16), :] = (hidden * inv * gain_two).astype(bf16)
        return carry

    lax.fori_loop(0, 8, norm_two, 0)
    send_rows(1)
    take_rows(0)
    for i in (2, 3):
        for d in order:
            take(i, d)
    take_rows(1)
    send_weight(4)
    send_weight(5)
    take_far_rows(0)
    take_far_rows(1)
    take_shared(2)
    take_shared(3)
    have_rows(0)
    have_rows(1)

    act, gate_delta, up_delta = v["act_buf"], v["gd_buf"], v["ud_buf"]
    gs, us, gr = v["gs"], v["us"], v["gr"]
    pending = [(i, d) for i in (4, 5) for d in order]

    def service():
        if pending:
            take(*pending.pop(0))

    def product(out, offset, width, m, one):
        at = pl.ds(m * 512, 512)
        for n in range(0, width, 256):
            size = min(256, width - n)
            out[at, n : n + size] = one(at, pl.ds(offset + n, size))

    def gate_product(offset, width, m):
        product(gs, offset, width, m, lambda at, cols: jnp.dot(n_all[at, :], g_buf[:, cols], preferred_element_type=f32))

    def up_product(offset, width, m):
        product(us, offset, width, m, lambda at, cols: jnp.dot(n_all[at, :], u_buf[:, cols], preferred_element_type=f32))

    def grad_product(offset, width, m):
        product(gr, offset, width, m, lambda at, cols: dot_nt(cot_all[at, :], d_buf[cols, :]))

    def activate(offset, width, m):
        column = first_unit + offset + lax.broadcasted_iota(jnp.int32, (1, width), 1)
        owned = (column >= shard * 2240) & (column < (shard + 1) * 2240)

        def body(j, carry):
            to = pl.ds(pl.multiple_of(m * 512 + j * 16, 16), 16)
            cols = pl.ds(offset, width)
            gate, up, grad = gs[to, 0:width], us[to, 0:width], gr[to, 0:width]
            sig = jax.nn.sigmoid(gate)
            silu = gate * sig
            act[to, cols] = jnp.where(owned, silu * up, 0.0).astype(bf16)
            gate_delta[to, cols] = jnp.where(owned, grad * up * sig * (1.0 + gate * (1.0 - sig)), 0.0).astype(bf16)
            up_delta[to, cols] = jnp.where(owned, grad * silu, 0.0).astype(bf16)
            return carry

        lax.fori_loop(0, 32, body, 0)

    def transpose(src, cols, dst):
        def body(j, carry):
            at = pl.ds(pl.multiple_of(j * 128, 128), 128)
            dst[:, at] = src[at, cols].T
            return carry

        lax.fori_loop(0, 8, body, 0)

    outs = {}

    def write(name, buf, at, cols=None):
        n = 9 + len(outs)
        src = buf.at[at] if cols is None else buf.at[at, cols]
        dst = v[name].at[at] if cols is None else v[name].at[at, cols]
        copy = pltpu.make_async_copy(src, dst, v["local"].at[n])
        copy.start()
        outs[n] = copy

    write("w_d", d_buf, pl.ds(0, WINDOW))
    write("cot_rows", cot_all, pl.ds(0, 1024))
    for tile, (offset, width, _) in enumerate(TILES):
        cols = pl.ds(offset, width)
        if tile == 0:
            for m in range(2):
                gate_product(offset, width, m)
                up_product(offset, width, m)
                grad_product(offset, width, m)
                activate(offset, width, m)
                service()
        else:
            for m in range(2):
                grad_product(offset, width, m)
                if len(pending) > 2:
                    service()
            while len(pending) > 3:
                service()
            take_shared(4)
            for m in range(2):
                gate_product(offset, width, m)
            while pending:
                service()
            take_shared(5)
            for m in range(2):
                up_product(offset, width, m)
                activate(offset, width, m)
        write("w_g", g_buf, pl.ds(0, 1536), cols)
        write("w_u", u_buf, pl.ds(0, 1536), cols)
        for name, buf in (("act", act), ("gd", gate_delta), ("ud", up_delta)):
            write(name, buf, pl.ds(0, 1024), cols)
        if tile == 0:
            transpose(act, cols, v["act_t"])
            transpose(n_all, pl.ds(0, 1536), v["n_t_buf"])
            write("n_t", v["n_t_buf"], pl.ds(0, 1536))
            service()
            for n in range(3):
                out = pl.ds(n * 512, 512)
                v["d_grad"][:, out] = (
                    jnp.dot(v["act_t"][...], cot_all[:, out], preferred_element_type=f32) * grad_scale
                ).astype(bf16)
            write("pd", v["d_grad"], cols)
            service()
    keep_q.wait()
    keep_o.wait()
    for i in (0, 1):
        for d in order:
            p = peer_of(shard, d)
            if d < 3:
                hop(i, d, p, shard).wait_send()
                relay(i, d, peer_of(shard, 3 - d), p).wait_send()
            across(i, d, p, odd).wait_send()
            for part in (False, True):
                onward(i, d, p, core, part).wait_send()
    for copy in outs.values():
        copy.wait()
    for d in order:
        p = peer_of(shard, d)
        small_hop(d, p, shard).wait_send()
        for i in (2, 3, 4, 5):
            hop(i, d, p, shard).wait_send()
            across(i, d, p, odd).wait_send()
        for a in range(2):
            if d < 3:
                row_hop(a, d, p, shard).wait_send()
                row_relay(a, d, peer_of(shard, 3 - d), p).wait_send()
    for a in range(2):
        for d in (0,) + order:
            row_onward(a, d, peer_of(shard, d), core).wait_send()


def forward(grad_scale, **given):
    bf16 = jnp.bfloat16
    f32 = jnp.float32
    dma = pltpu.SemaphoreType.DMA
    in_vmem = ("x", "gain_one", "bias", "gain_two", "cos", "sin")
    outs = {
        "q_full": ((1536, 2048), bf16, any_spec()),
        "o_full": ((1536, 1536), bf16, any_spec()),
        "pd": ((640, 1536), bf16, any_spec()),
        "cot_rows": ((1024, 1536), bf16, any_spec()),
        "act": ((1024, WINDOW), bf16, any_spec()),
        "gd": ((1024, WINDOW), bf16, any_spec()),
        "ud": ((1024, WINDOW), bf16, any_spec()),
        "n_t": ((1536, 1024), bf16, any_spec()),
        "w_g": ((1536, WINDOW), bf16, any_spec()),
        "w_u": ((1536, WINDOW), bf16, any_spec()),
        "w_d": ((WINDOW, 1536), bf16, any_spec()),
        "hidden": ((128, 1536), f32, vmem_spec()),
        "nrm": ((128, 1536), bf16, vmem_spec()),
        "ctx": ((128, 1536), bf16, vmem_spec()),
        "qry": ((128, 1536), bf16, vmem_spec()),
        "key": ((128, KV * HD), bf16, vmem_spec()),
        "val": ((128, KV * HD), bf16, vmem_spec()),
        "lse": ((128, HD), f32, vmem_spec()),
        "gains": ((8, 1536), f32, vmem_spec()),
    }
    scratch = {
        "q_buf": pltpu.VMEM((1536, 2048), bf16),
        "o_buf": pltpu.VMEM((1536, 1536), bf16),
        "g_buf": pltpu.VMEM((1536, WINDOW), bf16),
        "u_buf": pltpu.VMEM((1536, WINDOW), bf16),
        "d_buf": pltpu.VMEM((WINDOW, 1536), bf16),
        "n_all": pltpu.VMEM((1024, 1536), bf16),
        "cot_all": pltpu.VMEM((1024, 1536), bf16),
        "small": pltpu.VMEM((16, 512), bf16),
        "small_all": pltpu.VMEM((4, 16, 512), bf16),
        "prj": pltpu.VMEM((128, 2048), f32),
        "act_buf": pltpu.VMEM((1024, WINDOW), bf16),
        "gd_buf": pltpu.VMEM((1024, WINDOW), bf16),
        "ud_buf": pltpu.VMEM((1024, WINDOW), bf16),
        "n_t_buf": pltpu.VMEM((1536, 1024), bf16),
        "act_t": pltpu.VMEM((640, 1024), bf16),
        "gs": pltpu.VMEM((1024, 640), f32),
        "us": pltpu.VMEM((1024, 640), f32),
        "gr": pltpu.VMEM((1024, 640), f32),
        "d_grad": pltpu.VMEM((640, 1536), bf16),
        "send": dma((27,)),
        "recv": dma((27,)),
        "rsend": dma((8,)),
        "rrecv": dma((8,)),
        "zsend": dma((18,)),
        "zrecv": dma((18,)),
        "fsend": dma((20,)),
        "frecv": dma((20,)),
        "local": dma((24,)),
    }
    return dict(zip(outs, pl.pallas_call(
        functools.partial(forward_kernel, grad_scale, (*given, *outs, *scratch)),
        out_shape=[jax.ShapeDtypeStruct(s, dt) for s, dt, _ in outs.values()],
        in_specs=[vmem_spec() if name in in_vmem else any_spec() for name in given],
        out_specs=[spec for _, _, spec in outs.values()],
        scratch_shapes=list(scratch.values()),
        compiler_params=pltpu.CompilerParams(has_side_effects=True, vmem_limit_bytes=67043328),
    )(*given.values())))


def backward_kernel(levels, grad_scale, names, *refs):
    v = dict(zip(names, refs))
    replica, shard, core = place()
    other = 1 - core
    level = replica // 2
    mate = (replica + 1 - 2 * core, shard)
    above, below = (replica + 2, shard), (replica - 2, shard)
    f32 = jnp.float32
    bf16 = jnp.bfloat16
    order = (3, 1, 2)
    own_a, own_d, own_g = v["own_a"], v["own_d"], v["own_g"]
    mat, act, wbuf, back, out = v["mat"], v["act_buf"], v["wbuf"], v["back"], v["out"]
    odd_chip = lax.rem(shard, 2)

    def tokens(owner, c):
        return pl.ds(pl.multiple_of((c * 4 + owner) * 128, 128), 128)

    def chip_at(d):
        across = lax.rem(lax.rem(shard, 2) + lax.rem(d, 2), 2)
        return lax.rem(shard // 2 + d // 2, 2) * 2 + across

    def exchange(block, chip):
        return remote(
            v["blocks"].at[block - 2], own_g.at[pl.ds(pl.multiple_of(block * 384, 384), 384)],
            v["xsend"].at[block], v["xrecv"].at[block], (replica, chip),
        )

    load_down = pltpu.make_async_copy(v["pd"], own_d.at[pl.ds(0, 640)], v["in_sem"].at[0])
    load_normed = pltpu.make_async_copy(v["n_t"], wbuf.at[:, pl.ds(0, 1024)], v["in_sem"].at[1])
    load_gate = pltpu.make_async_copy(v["w_g"], wbuf.at[:, pl.ds(WINDOW, WINDOW)], v["in_sem"].at[2])
    load_up = pltpu.make_async_copy(v["w_u"], wbuf.at[:, pl.ds(0, WINDOW)], v["in_sem"].at[3])
    load_wd = pltpu.make_async_copy(v["w_d"], wbuf.at[pl.ds(0, WINDOW), pl.ds(0, 1536)], v["in_sem"].at[4])
    load_deltas = [
        pltpu.make_async_copy(v["gd"], mat.at[0], v["in_sem"].at[5]),
        pltpu.make_async_copy(v["ud"], mat.at[1], v["in_sem"].at[6]),
    ]
    load_act = pltpu.make_async_copy(v["act"], act, v["in_sem"].at[7])
    load_cot = pltpu.make_async_copy(v["cot_rows"], out, v["in_sem"].at[8])

    def stage_down(n):
        if n == 0:
            load_act.wait()
            load_cot.wait()
        cols = pl.ds(n * 512, 512)
        own_d[640:WINDOW, cols] = (dot_tn(act[:, 640:WINDOW], out[:, cols]) * grad_scale).astype(bf16)

    def staged(block):
        slot = lax.rem(block, 2)
        return pltpu.make_async_copy(
            back.at[pl.ds(pl.multiple_of(slot * 384, 384), 384), pl.ds(0, WINDOW)], v["blocks"].at[block - 2],
            v["stage_sem"].at[slot],
        )

    def stage_gradient(block):
        d, a = block // 2, lax.rem(block, 2)
        rows = pl.ds(pl.multiple_of(chip_at(d) * 384, 384), 384)

        @pl.when(block >= 4)
        def _():
            staged(block - 2).wait()

        for n in range(3):
            cols = pl.ds(n * 384, 384)
            part = (
                jnp.dot(wbuf[rows, 0:1024], mat[a, :, cols], preferred_element_type=f32) * grad_scale
            ).astype(bf16)

            @pl.when(d == 0)
            def _():
                own_g[pl.ds(pl.multiple_of(a * 384, 384), 384), cols] = part

            @pl.when(d > 0)
            def _():
                back[pl.ds(pl.multiple_of(a * 384, 384), 384), cols] = part

        @pl.when(block >= 2)
        def _():
            staged(block).start()

    def start_back():
        load_up.start()
        staged(6).wait()
        staged(7).wait()
        load_gate.wait()
        load_up.wait()

    def piece(i):
        return pl.ds(pl.multiple_of((i // 3) * 256, 256), 256), pl.ds(pl.multiple_of(lax.rem(i, 3) * 512, 512), 512)

    def stage_back(i):
        at, cols = piece(i)
        back[at, cols] = (
            dot_nt(mat[0, at, :], wbuf[cols, WINDOW : 2 * WINDOW]) + dot_nt(mat[1, at, :], wbuf[cols, 0:WINDOW])
        ).astype(bf16)

    def stage_out(i):
        at, cols = piece(i)
        out[at, cols] = jnp.dot(act[at, :], wbuf[0:WINDOW, cols], preferred_element_type=f32).astype(bf16)

    partial = (back, out)
    held, parts = v["held"], v["parts"]

    def kept(a, d):
        return partial[a].at[tokens(peer_of(shard, d), core)]

    def to_mate(a, d):
        n = a * 4 + d
        return remote(partial[a].at[tokens(peer_of(shard, d), other)], held.at[a, d], v["csend"].at[n], v["crecv"].at[n], mate)

    def to_owner(a, d):
        n = a * 3 + d - 1
        return remote(kept(a, d), parts.at[a, d - 1], v["psend"].at[n], v["precv"].at[n], (replica, peer_of(shard, d)))

    def pair_sums(a):
        for d in order:
            to_mate(a, d).wait_recv()
            mine = kept(a, d)

            def body(rows, carry):
                mine[rows, :] = (mine[rows, :].astype(f32) + held[a, d, rows, :].astype(f32)).astype(bf16)
                return carry

            row_loop(128, 32, body, 0)
            to_owner(a, d).start()

    def collect(a):
        to_mate(a, 0).wait_recv()
        for d in order:
            to_owner(a, d).wait_recv()

    def full_sum(a, rows):
        total = kept(a, 0)[rows, :].astype(f32) + held[a, 0, rows, :].astype(f32)
        for d in (1, 2, 3):
            total = total + parts[a, d - 1, rows, :].astype(f32)
        return total

    wide = ((v["hid"], mat.at[0, :, pl.ds(0, 768)], 768), (v["prj"], mat.at[1, :, pl.ds(0, 1024)], 1024))
    narrow = ((v["ctx"], v["ctx_all"], 384), (v["nrm"], v["nrm_all"], 384))

    def block(out, owner, c):
        return out.at[tokens(owner, c)]

    def columns(ref, index, width):
        return ref.at[:, pl.ds(pl.multiple_of(index * width, width), width)]

    def wide_copy(a, d, same, source_core, owner, t):
        ref, out, width = wide[a]
        c = core if same else other
        n = (a * 4 + d) * 2 + (0 if same else 1)
        return remote(
            columns(ref, c, width), block(out, owner, source_core), v["gsend"].at[n], v["grecv"].at[n],
            (replica - core + c, t),
        )

    def narrow_copy(a, d, owner, t):
        ref, out, width = narrow[a]
        n = 16 + a * 4 + d
        return remote(columns(ref, t, width), block(out, owner, core), v["gsend"].at[n], v["grecv"].at[n], (replica, t))

    def onward(a, d, source, owner, c):
        out = narrow[a][1]
        n = a * 4 + d
        return remote(source, block(out, owner, c), v["fsend"].at[n], v["frecv"].at[n], mate)

    def own_narrow(a):
        ref, out, width = narrow[a]
        return pltpu.make_async_copy(columns(ref, shard, width), block(out, shard, core), v["local"].at[a])

    def own_wide(a):
        ref, out, width = wide[a]
        return pltpu.make_async_copy(columns(ref, core, width), block(out, shard, core), v["local"].at[2 + a])

    load_out = pltpu.make_async_copy(v["wo"], wbuf.at[:, pl.ds(0, 1536)], v["local"].at[4])
    load_qkv = pltpu.make_async_copy(v["wq"], wbuf.at[:, pl.ds(0, 2048)], v["local"].at[5])

    def stage_sums():
        pair_sums(0)
        for d in order:
            for a in range(2):
                narrow_copy(a, d, shard, peer_of(shard, d)).start()
        send_blocks((1, 2))

    def send_blocks(offsets):
        for d in offsets:
            for a in range(2):
                exchange(d * 2 + a, peer_of(shard, d)).start()

    def stage_hidden():
        collect(0)
        gain = v["gains"][1:2, :]

        def body(rows, total):
            grad = full_sum(0, rows)
            hidden = v["hidden"][rows, :]
            inv = lax.rsqrt(jnp.mean(hidden * hidden, axis=-1, keepdims=True) + NORM_EPS)
            scaled = gain * grad
            out = v["cot"][rows, :].astype(f32) + inv * (
                scaled - hidden * inv * inv * jnp.mean(scaled * hidden, axis=-1, keepdims=True)
            )
            v["hgrad"][rows, :] = out
            v["hid"][rows, :] = out.astype(bf16)
            return total + jnp.sum(grad * hidden * inv, axis=0, keepdims=True)

        v["row_two"][...] = row_loop(128, 16, body, jnp.zeros((1, 1536), f32)) * grad_scale
        for d in (0,) + order:
            if d:
                wide_copy(0, d, True, core, shard, peer_of(shard, d)).start()
            wide_copy(0, d, False, core, shard, peer_of(shard, d)).start()
        own_wide(0).start()

    def stage_context(part):
        if part == 0:
            load_out.wait()
        for e in (2 * part, 2 * part + 1):
            cols = pl.ds(e * 384, 384)
            v["cgrad"][:, cols] = dot_nt(v["hid"][...], wbuf[cols, 0:1536]).astype(bf16)
        if part == 1:
            load_qkv.start()

    def unrotated(x):
        return x * v["cos"][...] - pltpu.roll(x, HD // 2, 1) * v["sin"][...]

    def stage_heads(g, part):
        keys = v["key"][:, g * HD : (g + 1) * HD]
        values = v["val"][:, g * HD : (g + 1) * HD]
        causal = lax.broadcasted_iota(jnp.int32, (128, 128), 0) >= lax.broadcasted_iota(jnp.int32, (128, 128), 1)
        key_grad = jnp.zeros((128, HD), f32) if part == 0 else v["kv_sum"][0]
        value_grad = jnp.zeros((128, HD), f32) if part == 0 else v["kv_sum"][1]
        first_head = g * (HEADS // KV) + part * 2
        for h in range(first_head, first_head + 2):
            at = slice(h * HD, (h + 1) * HD)
            query = v["qry"][:, at]
            grad = v["cgrad"][:, at]
            scores = jnp.where(causal, dot_nt(query, keys) * SCORE_SCALE, -1e30)
            probs = jnp.exp(scores - v["lse"][:, h : h + 1]).astype(bf16)
            wide_probs = probs.astype(f32)
            prob_grad = dot_nt(grad, values)
            delta = jnp.sum(wide_probs * prob_grad, axis=-1, keepdims=True)
            score_grad = (wide_probs * (prob_grad - delta) * SCORE_SCALE).astype(bf16)
            v["prj"][:, at] = unrotated(jnp.dot(score_grad, keys, preferred_element_type=f32)).astype(bf16)
            key_grad = key_grad + dot_tn(score_grad, query)
            value_grad = value_grad + dot_tn(probs, grad)
        if part < 2:
            v["kv_sum"][0] = key_grad
            v["kv_sum"][1] = value_grad
            return
        first = HEADS * HD + g * HD
        v["prj"][:, first : first + HD] = unrotated(key_grad).astype(bf16)
        first = first + KV * HD
        v["prj"][:, first : first + HD] = value_grad.astype(bf16)

    def stage_send_projected():
        for d in (0,) + order:
            if d:
                wide_copy(1, d, True, core, shard, peer_of(shard, d)).start()
            wide_copy(1, d, False, core, shard, peer_of(shard, d)).start()
        own_wide(1).start()

    def stage_normed(part):
        if part == 0:
            load_qkv.wait()
        for e in (2 * part, 2 * part + 1):
            cols = pl.ds(e * 384, 384)
            v["input_grad"][:, cols] = dot_nt(v["prj"][...], wbuf[cols, 0:2048])

    vec, vin, vall = v["vec"], v["vin"], v["vall"]
    replicas = 2 * levels

    def vec_hop(d):
        return remote(vec.at[peer_of(shard, d)], vin.at[d - 1], v["vsend"].at[d - 1], v["vrecv"].at[d - 1],
                      (replica, peer_of(shard, d)))

    def vec_spread(j, slot):
        target = lax.rem(replica + j, replicas)
        return remote(v["vsum"], vall.at[slot], v["vsend"].at[2 + j], v["vrecv"].at[2 + j], (target, shard))

    def stage_input():
        gain = v["gains"][0:1, :]

        def body(rows, totals):
            total, bias = totals
            x = v["x"][rows, :].astype(f32)
            grad = v["input_grad"][rows, :]
            inv = lax.rsqrt(jnp.mean(x * x, axis=-1, keepdims=True) + NORM_EPS)
            scaled = gain * grad
            v["input_grad"][rows, :] = v["hgrad"][rows, :] + inv * (
                scaled - x * inv * inv * jnp.mean(scaled * x, axis=-1, keepdims=True)
            )
            return (
                total + jnp.sum(grad * x * inv, axis=0, keepdims=True),
                bias + jnp.sum(v["prj"][rows, :].astype(f32), axis=0, keepdims=True),
            )

        row_one, row_bias = row_loop(128, 16, body, (jnp.zeros((1, 1536), f32), jnp.zeros((1, 2048), f32)))
        row_one = row_one * grad_scale
        row_bias = row_bias * grad_scale
        row_two = v["row_two"][...]
        for s in range(4):
            vec[s, :, 0:384] = jnp.broadcast_to(row_one[:, s * 384 : (s + 1) * 384], (8, 384))
            vec[s, :, 384:896] = jnp.broadcast_to(row_bias[:, s * 512 : (s + 1) * 512], (8, 512))
            vec[s, :, 896:1280] = jnp.broadcast_to(row_two[:, s * 384 : (s + 1) * 384], (8, 384))
        for d in order:
            vec_hop(d).start()

    def stage_vec():
        total = vec[shard]
        for d in (1, 2, 3):
            vec_hop(d).wait_recv()
            total = total + vin[d - 1]
        v["vsum"][...] = total
        for j in range(1, replicas):
            vec_spread(j, replica).start()

    def stage_vec_out():
        vall[replica] = v["vsum"][...]
        for j in range(1, replicas):
            vec_spread(j, lax.rem(replica + replicas - j, replicas)).wait_recv()
        total = vall[0]
        for j in range(1, replicas):
            total = total + vall[j]
        v["vec_out"][...] = total

    def stage_output():
        collect(1)

        def body(rows, carry):
            v["block_out"][rows, :] = (v["hidden"][rows, :] + full_sum(1, rows)).astype(bf16)
            return carry

        row_loop(128, 32, body, 0)

    def stage_relay():
        for d in order:
            p = peer_of(shard, d)
            for a in range(2):
                narrow_copy(a, d, p, p).wait_recv()
                onward(a, d, block(narrow[a][1], p, core), p, core).start()

    def stage_gathered():
        for a in range(2):
            own_narrow(a).wait()
            own_wide(a).wait()
            for d in (0, 1, 2, 3):
                p = peer_of(shard, d)
                if d:
                    wide_copy(a, d, True, core, p, p).wait_recv()
                wide_copy(a, d, False, other, p, p).wait_recv()
                onward(a, d, block(narrow[a][1], p, other), p, other).wait_recv()

    def stage_attention_parts(j):
        at = pl.ds(j * 128, 128)
        own_a[at, 0:1024] = (dot_tn(v["nrm_all"][:, at], mat[1, :, 0:1024]) * grad_scale).astype(bf16)
        own_a[at, 1024:1792] = (dot_tn(v["ctx_all"][:, at], mat[0, :, 0:768]) * grad_scale).astype(bf16)

    def down_at(c, j):
        first = odd_chip * (1088 * c - 64 * (1 - c)) + (1 - odd_chip) * 1152 * c
        return v["fd"].at[pl.ds(pl.multiple_of(first + j * 64, 64), 64)]

    def gate_at(c, j):
        group = j // 6
        rows = pl.ds(pl.multiple_of(lax.rem(j, 6) * 64, 64), 64)
        return v["fg"].at[lax.rem(group, 2), c, chip_at(group // 2), rows]

    def attention_at(c, j):
        return v["fa"].at[c, pl.ds(pl.multiple_of(j * 32, 32), 32)]

    segments = (
        (own_d, v["near_d"], v["far_d"], 64, 0, DOWN_STEPS, down_at),
        (own_g, v["near_g"], v["far_g"], 64, DOWN_STEPS, DOWN_STEPS + GATE_STEPS, gate_at),
        (own_a, v["near_a"], v["far_a"], 32, DOWN_STEPS + GATE_STEPS, CHUNKS, attention_at),
    )
    end = (level == 0) | (level == levels - 1)
    middle = levels // 2

    def on(k, stage, c=None):
        c = core if c is None else c
        for n, segment in enumerate(segments):
            j = k - segment[4]
            inside = (k >= segment[4]) & (k < segment[5])
            if n == 0:
                inside &= (j > 0) | (1 - odd_chip + c > 0)
                inside &= (j < DOWN_STEPS - 1) | (odd_chip + 1 - c > 0)
            pl.when(inside)(functools.partial(stage, n, segment, j, k))

    def rows_of(segment, j):
        size = segment[3]
        return pl.ds(pl.multiple_of(j * size, size), size)

    def message(segment, j, k, upward, near):
        own, near_ref, far_ref = segment[:3]
        target = near_ref.at[rows_of(segment, j)] if near else far_ref.at[rows_of(segment, j // 2)]
        sem = v["near_sem"] if near else v["far_sem"]
        return remote(own.at[rows_of(segment, j)], target, v["part_sem"].at[k], sem.at[k], above if upward else below)

    def result(segment, j, k, upward, from_own):
        place_ = segment[6](core, j)
        src = segment[0].at[rows_of(segment, j)] if from_own else place_
        sem = v["up_sem"] if upward else v["down_sem"]
        return remote(src, place_, sem.at[k], v["done_sem"].at[k], above if upward else below)

    def keep_result(segment, j, k):
        return pltpu.make_async_copy(segment[0].at[rows_of(segment, j)], segment[6](core, j), v["out_sem"].at[k])

    def to_other_core(segment, j, k, from_own, c):
        place_ = segment[6](c, j)
        src = segment[0].at[rows_of(segment, j)] if from_own else place_
        return remote(src, place_, v["mate_send"].at[k], v["mate_recv"].at[k], mate)

    def add(segment, j, with_far):
        own, near_ref, far_ref, size = segment[:4]

        def body(i, carry):
            rows = pl.ds(pl.multiple_of(j * size + i * 16, 16), 16)
            value = own[rows, :].astype(f32) + near_ref[rows, :].astype(f32)
            if with_far:
                value = value + far_ref[pl.ds(pl.multiple_of((j // 2) * size + i * 16, 16), 16), :].astype(f32)
            own[rows, :] = value.astype(own.dtype)
            return carry

        lax.fori_loop(0, size // 16, body, 0)

    def arrived(n, j):
        if n != 1:
            return
        group = j // 6

        @pl.when((lax.rem(j, 6) == 0) & (group >= 2))
        def _():
            exchange(group, shard).wait_recv()

    def root_of(k):
        return middle - 1 + lax.rem(k, 2)

    def end_gather(n, segment, j, k):
        @pl.when(end)
        def _():
            arrived(n, j)

        @pl.when(level == 0)
        def _():
            message(segment, j, k, True, True).start()

        @pl.when(level == levels - 1)
        def _():
            message(segment, j, k, False, True).start()

    def gather_step(n, segment, j, k):
        @pl.when(~end)
        def _():
            arrived(n, j)

            @pl.when(level != root_of(k))
            def _():
                message(segment, j, k, True, True).wait_recv()
                add(segment, j, False)

        for upward in (True, False):
            towards = (level > 0) & (level < root_of(k)) if upward else (level < levels - 1) & (level > root_of(k))
            crosses = level == (middle - 1 if upward else middle)

            @pl.when(towards & crosses)
            def _():
                message(segment, j, k, upward, False).start()

            if levels > 4:

                @pl.when(towards & ~crosses)
                def _():
                    message(segment, j, k, upward, True).start()

    def root_step(n, segment, j, k):
        @pl.when(level == root_of(k))
        def _():
            message(segment, j, k, True, True).wait_recv()
            message(segment, j, k, True, False).wait_recv()
            add(segment, j, True)
            result(segment, j, k, True, True).start()
            result(segment, j, k, False, True).start()
            keep_result(segment, j, k).start()
            to_other_core(segment, j, k, True, core).start()

    def spread_step(n, segment, j, k):
        @pl.when(~end & (level != root_of(k)))
        def _():
            result(segment, j, k, True, False).wait_recv()

            @pl.when(level < root_of(k))
            def _():
                result(segment, j, k, False, False).start()

            @pl.when(level > root_of(k))
            def _():
                result(segment, j, k, True, False).start()

            to_other_core(segment, j, k, False, core).start()

    def end_spread(n, segment, j, k):
        @pl.when(end)
        def _():
            result(segment, j, k, True, False).wait_recv()
            to_other_core(segment, j, k, False, core).start()

    def close(n, segment, j, k):
        root = root_of(k)

        @pl.when(level == root)
        def _():
            result(segment, j, k, True, True).wait_send()
            result(segment, j, k, False, True).wait_send()
            keep_result(segment, j, k).wait()

        @pl.when(level != root)
        def _():
            message(segment, j, k, True, True).wait_send()

        @pl.when(~end & (level < root))
        def _():
            result(segment, j, k, False, False).wait_send()

        @pl.when(~end & (level > root))
        def _():
            result(segment, j, k, True, False).wait_send()

        to_other_core(segment, j, k, True, core).wait_send()

    def close_mate(n, segment, j, k):
        to_other_core(segment, j, k, True, other).wait_recv()

    def start_mate(a):
        for d in order + (0,):
            to_mate(a, d).start()

    load_down.start()
    load_act.start()
    load_cot.start()
    load_normed.start()
    for copy in load_deltas:
        copy.start()
    load_gate.start()
    for a in range(2):
        own_narrow(a).start()
        onward(a, 0, columns(narrow[a][0], shard, 384), shard, core).start()
    load_down.wait()
    lags = ((end_gather, 0), (gather_step, 8), (root_step, 10), (spread_step, 12), (end_spread, 18))
    steps = CHUNKS + lags[-1][1]

    def begin_products():
        load_normed.wait()
        for copy in load_deltas:
            copy.wait()

    def begin_out():
        start_mate(0)
        load_wd.start()

    def end_out():
        start_mate(1)
        load_out.start()

    def stage_projected():
        stage_send_projected()
        send_blocks((3,))

    beside = [
        (2, 1, functools.partial(stage_down, 0)),
        (4, 1, functools.partial(stage_down, 1)),
        (6, 1, functools.partial(stage_down, 2)),
        (9, 1, begin_products),
        (9, 4, lambda i: (stage_gradient(2 * i), stage_gradient(2 * i + 1))),
        (13, 1, start_back),
        (13, 4, lambda i: (stage_back(3 * i), stage_back(3 * i + 1), stage_back(3 * i + 2))),
        (17, 1, begin_out),
        (19, 1, stage_sums),
        (20, 1, load_wd.wait),
        (20, 4, lambda i: (stage_out(3 * i), stage_out(3 * i + 1), stage_out(3 * i + 2))),
        (24, 1, end_out),
        (25, 1, stage_hidden),
        (26, 1, functools.partial(stage_context, 0)),
        (27, 1, functools.partial(stage_context, 1)),
    ]
    for n in range(6):
        beside.append((28 + n, 1, functools.partial(stage_heads, n // 3, n % 3)))
    beside += [
        (33, 1, stage_projected),
        (34, 1, functools.partial(stage_normed, 0)),
        (36, 1, functools.partial(stage_normed, 1)),
        (38, 1, stage_input),
        (40, 1, stage_relay),
        (56, 1, stage_gathered),
        (56, 1, functools.partial(stage_attention_parts, 0)),
        (58, 1, functools.partial(stage_attention_parts, 1)),
        (60, 1, functools.partial(stage_attention_parts, 2)),
        (62, 1, functools.partial(pair_sums, 1)),
        (64, 1, stage_vec),
        (steps - 4, 1, stage_vec_out),
        (steps - 2, 1, stage_output),
    ]

    def step(t, carry):
        for stage, lag in lags:
            on(t - lag, stage)
        for first, count, stage in beside:
            if count == 1:
                pl.when(t == first)(stage)
            else:
                @pl.when((t >= first) & (t < first + count))
                def _():
                    stage(t - first)

        return carry

    lax.fori_loop(0, steps, step, 0)

    def finish_step(k, carry):
        on(k, close)
        on(k, close_mate, other)
        return carry

    lax.fori_loop(0, CHUNKS, finish_step, 0)
    for d in (1, 2, 3):
        for a in range(2):
            exchange(d * 2 + a, peer_of(shard, d)).wait_send()
    for a in range(2):
        for d in (0, 1, 2, 3):
            p = peer_of(shard, d)
            to_mate(a, d).wait_send()
            wide_copy(a, d, False, core, shard, p).wait_send()
            onward(a, d, block(narrow[a][1], p, core), p, core).wait_send()
            if d:
                to_owner(a, d).wait_send()
                wide_copy(a, d, True, core, shard, p).wait_send()
                narrow_copy(a, d, shard, p).wait_send()
    for d in order:
        vec_hop(d).wait_send()
    for j in range(1, replicas):
        vec_spread(j, replica).wait_send()


def backward(levels, grad_scale, **given):
    bf16 = jnp.bfloat16
    f32 = jnp.float32
    dma = pltpu.SemaphoreType.DMA
    in_hbm = ("pd", "cot_rows", "act", "gd", "ud", "n_t", "w_g", "w_u", "w_d", "wo", "wq")
    outs = {
        "fa": ((2, 384, 1792), bf16, any_spec()),
        "fd": ((2240, 1536), bf16, any_spec()),
        "fg": ((2, 2, 4, 384, WINDOW), bf16, any_spec()),
        "blocks": ((6, 384, WINDOW), bf16, any_spec()),
        "block_out": ((128, 1536), bf16, vmem_spec()),
        "input_grad": ((128, 1536), f32, vmem_spec()),
        "vec_out": ((8, 1280), f32, vmem_spec()),
    }
    scratch = {
        "own_a": pltpu.VMEM((384, 1792), bf16),
        "own_d": pltpu.VMEM((WINDOW, 1536), bf16),
        "own_g": pltpu.VMEM((3072, WINDOW), bf16),
        "near_a": pltpu.VMEM((384, 1792), bf16),
        "near_d": pltpu.VMEM((WINDOW, 1536), bf16),
        "near_g": pltpu.VMEM((3072, WINDOW), bf16),
        "far_a": pltpu.VMEM((192, 1792), bf16),
        "far_d": pltpu.VMEM((WINDOW // 2, 1536), bf16),
        "far_g": pltpu.VMEM((1536, WINDOW), bf16),
        "mat": pltpu.VMEM((2, 1024, WINDOW), bf16),
        "act_buf": pltpu.VMEM((1024, WINDOW), bf16),
        "wbuf": pltpu.VMEM((1536, 2 * WINDOW), bf16),
        "back": pltpu.VMEM((1024, 1536), bf16),
        "out": pltpu.VMEM((1024, 1536), bf16),
        "held": pltpu.VMEM((2, 4, 128, 1536), bf16),
        "parts": pltpu.VMEM((2, 3, 128, 1536), bf16),
        "hgrad": pltpu.VMEM((128, 1536), f32),
        "hid": pltpu.VMEM((128, 1536), bf16),
        "cgrad": pltpu.VMEM((128, 1536), bf16),
        "prj": pltpu.VMEM((128, 2048), bf16),
        "ctx_all": pltpu.VMEM((1024, 384), bf16),
        "nrm_all": pltpu.VMEM((1024, 384), bf16),
        "row_two": pltpu.VMEM((1, 1536), f32),
        "kv_sum": pltpu.VMEM((2, 128, HD), f32),
        "vec": pltpu.VMEM((4, 8, 1280), f32),
        "vin": pltpu.VMEM((3, 8, 1280), f32),
        "vsum": pltpu.VMEM((8, 1280), f32),
        "vall": pltpu.VMEM((2 * levels, 8, 1280), f32),
    }
    counts = {
        "xsend": 8, "xrecv": 8, "stage_sem": 2, "csend": 8, "crecv": 8, "psend": 6, "precv": 6, "gsend": 24, "grecv": 24,
        "fsend": 8, "frecv": 8, "local": 6, "in_sem": 9, "vsend": 2 + 2 * levels, "vrecv": 2 + 2 * levels,
    }
    for name in (
        "part_sem", "near_sem", "far_sem", "up_sem", "down_sem", "done_sem", "mate_send", "mate_recv", "out_sem"
    ):
        counts[name] = CHUNKS
    scratch |= {name: dma((n,)) for name, n in counts.items()}
    return pl.pallas_call(
        functools.partial(backward_kernel, levels, grad_scale, (*given, *outs, *scratch)),
        out_shape=[jax.ShapeDtypeStruct(s, dt) for s, dt, _ in outs.values()],
        in_specs=[any_spec() if name in in_hbm else vmem_spec() for name in given],
        out_specs=[spec for _, _, spec in outs.values()],
        scratch_shapes=list(scratch.values()),
        compiler_params=pltpu.CompilerParams(has_side_effects=True, vmem_limit_bytes=67043328),
    )(*given.values())


def widen_kernel(
    gate, up, down, attn, block, grad, vec, out_gate, out_up, out_down, out_qkv, out_out, out_block, out_grad, gain_one, bias, gain_two
):
    f32 = jnp.float32
    gain_one[...] = vec[0, 0:384]
    bias[...] = vec[0, 384:896]
    gain_two[...] = vec[0, 896:1280]
    out_block[...] = block[...]
    out_grad[...] = grad[...]
    for x, out in ((gate, out_gate), (up, out_up)):
        for s in range(4):
            for c in range(2):
                first = (s * 35) // 2 + c * 9
                rest = 1 if s % 2 == 1 and c == 0 else 0
                out[:, (first + rest) * 128 : (first + 9) * 128] = x[c, s][:, rest * 128 :].astype(f32)
        for s in (1, 3):
            first = (s * 35) // 2
            out[:, first * 128 : (first + 1) * 128] = x[1, s - 1][:, 1024:].astype(f32) + x[0, s][:, :128].astype(f32)
    out_down[...] = down[...].astype(f32)
    for c in range(2):
        out_qkv[:, c * 1024 : (c + 1) * 1024] = attn[c][:, :1024].astype(f32)
        out_out[:, c * 768 : (c + 1) * 768] = attn[c][:, 1024:].astype(f32)


def widen(*sums):
    rows = 96
    f32 = jnp.float32
    def blocks(a):
        return pl.BlockSpec((None, 2, 4, rows, WINDOW), lambda i: (a, 0, 0, i, 0))

    down = pl.BlockSpec((560, 1536), lambda i: (i, 0))

    own_rows = pl.BlockSpec((32, 1536), lambda i: (i, 0))

    def line(width):
        return pl.BlockSpec((width,), lambda i: (0,))

    def whole(width):
        return pl.BlockSpec((rows, width), lambda i: (i, 0))

    return pl.pallas_call(
        widen_kernel,
        grid=(384 // rows,),
        out_shape=[
            jax.ShapeDtypeStruct((384, 8960), f32),
            jax.ShapeDtypeStruct((384, 8960), f32),
            jax.ShapeDtypeStruct((2240, 1536), f32),
            jax.ShapeDtypeStruct((384, 2048), f32),
            jax.ShapeDtypeStruct((384, 1536), f32),
            jax.ShapeDtypeStruct((128, 1536), jnp.bfloat16),
            jax.ShapeDtypeStruct((128, 1536), f32),
            jax.ShapeDtypeStruct((384,), f32),
            jax.ShapeDtypeStruct((512,), f32),
            jax.ShapeDtypeStruct((384,), f32),
        ],
        in_specs=[blocks(0), blocks(1), down, pl.BlockSpec((2, rows, 1792), lambda i: (0, i, 0)), own_rows, own_rows,
                  pl.BlockSpec((8, 1280), lambda i: (0, 0))],
        out_specs=[whole(8960), whole(8960), down, whole(2048), whole(1536), own_rows, own_rows, line(384), line(512), line(384)],
    )(*sums)


def fast_device(
    block_input,
    attn_gain,
    qkv_weight,
    qkv_bias,
    out_weight,
    mlp_gain,
    gate_weight,
    up_weight,
    down_weight,
    cotangent,
):
    f32 = jnp.float32
    tok_count = block_input.shape[0]
    levels = lax.axis_size("replica") // 2
    grad_scale = 1.0 / math.sqrt(tok_count * lax.axis_size("replica") * lax.axis_size("shard"))
    cosine, sine_table = rope_tables(tok_count)
    twice = jnp.concatenate([cosine[:, 0], cosine[:, 0]], axis=1)
    turn = jnp.concatenate([-sine_table[:, 0], sine_table[:, 0]], axis=1)
    got = forward(
        grad_scale,
        x=block_input,
        gain_one=attn_gain,
        bias=qkv_bias,
        gain_two=mlp_gain,
        cos=twice,
        sin=turn,
        wq=qkv_weight,
        wo=out_weight,
        wg=gate_weight,
        wu=up_weight,
        wd=down_weight,
        cot=cotangent,
    )
    sum_attn, sum_down, sum_gate, _, block_output, input_grad, vectors = backward(
        levels,
        grad_scale,
        pd=got["pd"],
        cot_rows=got["cot_rows"],
        act=got["act"],
        gd=got["gd"],
        ud=got["ud"],
        n_t=got["n_t"],
        w_g=got["w_g"],
        w_u=got["w_u"],
        w_d=got["w_d"],
        wo=got["o_full"],
        wq=got["q_full"],
        hidden=got["hidden"],
        x=block_input,
        cot=cotangent,
        gains=got["gains"],
        ctx=got["ctx"],
        nrm=got["nrm"],
        qry=got["qry"],
        key=got["key"],
        val=got["val"],
        lse=got["lse"],
        cos=twice,
        sin=turn,
    )
    gate_grad, up_grad, down_grad, qkv_grad, out_grad, block_output, input_grad, gain_one_own, bias_own, gain_two_own = widen(
        sum_gate, sum_gate, sum_down, sum_attn, block_output, input_grad, vectors
    )
    return (
        block_output,
        input_grad,
        gain_one_own,
        qkv_grad,
        bias_own,
        out_grad,
        gain_two_own,
        gate_grad,
        up_grad,
        down_grad,
    )


def solution(mesh):
    placed = (
        P(("replica", "shard"), None),
        P("shard"),
        P("shard", None),
        P("shard"),
        P("shard", None),
        P("shard"),
        P("shard", None),
        P("shard", None),
        P("shard", None),
        P(("replica", "shard"), None),
    )
    fits = mesh.shape["shard"] == 4 and mesh.shape["replica"] % 4 == 0
    per_device = fast_device if fits else general_device
    return jax.shard_map(
        per_device,
        mesh=mesh,
        in_specs=placed,
        out_specs=(
            P(("replica", "shard"), None),
            P(("replica", "shard"), None),
            P("shard"),
            P("shard", None),
            P("shard"),
            P("shard", None),
            P("shard"),
            P("shard", None),
            P("shard", None),
            P("shard", None),
        ),
        check_vma=False,
    )
```
